128 devices in a mesh: vp: 128 (over z, y, x, core).
Axes of the slice: x: 4, y: 4, z: 4, core: 2. Of those that a mesh axis runs over, the one named last changes fastest.
Arguments:
- residual: bfloat16 [16384, 2048], replicated
- labels: int32 [16384], replicated
- loss_mask: float32 [16384], replicated
- norm_gain: float32 [2048], replicated
- embed_table: bfloat16 [49408, 2048], P('vp')
Outputs:
- output 1: float32 [], replicated
- output 2: float32 [16384, 2048], P('vp')
- output 3: float32 [49408, 2048], P('vp')
- output 4: float32 [2048], replicated
All inputs are finite; a program needn't handle non-finite values.
Results may differ from the reference program's by a relative error of at most 0.001.
Values sent between devices are 32-bit elements.
A program may use at most 1 GiB of HBM per device.

```python
import jax
import jax.numpy as jnp
from jax import lax

TOKENS = 16384
DIM = 2048
VOCAB_REAL = 49155
VOCAB_PAD = 49408

LOGIT_SCALE = 6.0
NORM_EPS = 1e-6


def draw_labels(label_key):
    k_pick, k_wide, k_low = jax.random.split(label_key, 3)
    pick_wide = jax.random.randint(k_pick, (TOKENS,), 0, 2)
    wide_ids = jax.random.randint(k_wide, (TOKENS,), 0, VOCAB_REAL)
    low_ids = jax.random.randint(k_low, (TOKENS,), 0, VOCAB_REAL // 16)
    label_ids = jnp.where(pick_wide == 0, wide_ids, low_ids).astype(jnp.int32)
    return label_ids.at[0].set(0).at[1].set(VOCAB_REAL - 1)


def draw_mask(mask_key):
    keep_draw = jax.random.randint(mask_key, (TOKENS,), 0, 5)
    mask_vals = (keep_draw > 0).astype(jnp.float32)
    return mask_vals.at[0].set(1.0)


def setup_inputs(seed: int = 0) -> dict:
    base_key = jax.random.key(seed)
    k_table, k_noise, k_peak, k_gain, k_label, k_mask = jax.random.split(base_key, 6)
    emb_std = LOGIT_SCALE * DIM ** -0.5
    table_f32 = jax.random.normal(k_table, (VOCAB_PAD, DIM), jnp.float32) * emb_std
    peak_ids = jax.random.randint(k_peak, (TOKENS, 4), 0, VOCAB_REAL)
    peak_sum = jnp.zeros((TOKENS, DIM), jnp.float32)
    for peak in range(4):
        peak_sum = peak_sum + table_f32[peak_ids[:, peak]] / emb_std
    peak_weight = 14.0 * DIM ** -0.5
    noise = jax.random.normal(k_noise, (TOKENS, DIM), jnp.float32)
    residual = (noise + peak_weight * peak_sum).astype(jnp.bfloat16)
    norm_gain = 1.0 + 0.3 * jax.random.normal(k_gain, (DIM,), jnp.float32)
    return {
        'residual': residual,
        'labels': draw_labels(k_label),
        'loss_mask': draw_mask(k_mask),
        'norm_gain': norm_gain,
        'embed_table': table_f32.astype(jnp.bfloat16),
    }


def reference(residual, labels, loss_mask, norm_gain, embed_table):
    x_f32 = residual.astype(jnp.float32)
    inv_rms = lax.rsqrt(jnp.mean(x_f32 * x_f32, axis=-1, keepdims=True) + NORM_EPS)
    x_hat = x_f32 * inv_rms
    hidden = (x_hat * norm_gain).astype(jnp.bfloat16)
    mask_total = jnp.sum(loss_mask)
    tok_weight = loss_mask / mask_total
    col_ids = jnp.arange(VOCAB_PAD)[None, :]
    row_block = min(TOKENS, 256)
    n_blocks = TOKENS // row_block

    def block_step(grad_table, block_in):
        h_blk, lab_blk, w_blk = block_in
        logits = jnp.dot(h_blk, embed_table.T, preferred_element_type=jnp.float32) / LOGIT_SCALE
        logits = jnp.where(col_ids < VOCAB_REAL, logits, -jnp.inf)
        row_max = jnp.max(logits, axis=-1, keepdims=True)
        shifted = jnp.exp(logits - row_max)
        sum_exp = jnp.sum(shifted, axis=-1, keepdims=True)
        is_label = col_ids == lab_blk[:, None]
        target = jnp.sum(jnp.where(is_label, logits, 0.0), axis=-1)
        tok_loss = row_max[:, 0] + jnp.log(sum_exp[:, 0]) - target
        row_prob = shifted / sum_exp
        d_logits = (jnp.where(is_label, row_prob - 1.0, row_prob) * w_blk[:, None]).astype(jnp.bfloat16)
        d_hidden = jnp.dot(d_logits, embed_table, preferred_element_type=jnp.float32) / LOGIT_SCALE
        grad_table = grad_table + jnp.dot(d_logits.T, h_blk, preferred_element_type=jnp.float32) / LOGIT_SCALE
        return grad_table, (tok_loss, d_hidden)

    blocks = (hidden.reshape(n_blocks, row_block, DIM), labels.reshape(n_blocks, row_block), tok_weight.reshape(n_blocks, row_block))
    d_embed, (tok_loss, d_hidden) = lax.scan(block_step, jnp.zeros((VOCAB_PAD, DIM), jnp.float32), blocks)
    tok_loss = tok_loss.reshape(TOKENS)
    d_hidden = d_hidden.reshape(TOKENS, DIM)
    mean_loss = jnp.sum(loss_mask * tok_loss) / mask_total
    d_gain = jnp.sum(d_hidden * x_hat, axis=0)
    d_xhat = d_hidden * norm_gain
    d_residual = inv_rms * (d_xhat - x_hat * jnp.mean(d_xhat * x_hat, axis=-1, keepdims=True))
    return (mean_loss, d_residual, d_embed, d_gain)
```

```python
import functools

import jax
import jax.numpy as jnp
from jax import lax
from jax.experimental import pallas as pl
from jax.experimental.pallas import tpu as pltpu
from jax.sharding import PartitionSpec as P

VOCAB_REAL = 49155
LOGIT_SCALE = 6.0
NORM_EPS = 1e-6

AXIS = "vp"
MESH = pl.DeviceIdType.MESH
F32 = jnp.float32
BF16 = jnp.bfloat16
HBM = pltpu.HBM
VMEM = pltpu.VMEM
DMA = pltpu.SemaphoreType.DMA


def _coords():
    me = lax.axis_index(AXIS)
    return me // 32, (me // 8) % 4, (me // 2) % 4, me % 2


def _dev(z, y, x, c):
    return ((z * 4 + y) * 4 + x) * 2 + c


def _mod4(v):
    return lax.rem(v + 8, 4)


def _barrier(peers):
    sem = pltpu.get_barrier_semaphore()
    for p in peers:
        pl.semaphore_signal(sem, inc=1, device_id=(p,), device_id_type=MESH)
    pl.semaphore_wait(sem, len(peers))


def _remote(src, dst, send, recv, k, dev):
    return pltpu.make_async_remote_copy(
        src_ref=src,
        dst_ref=dst,
        send_sem=send.at[k],
        recv_sem=recv.at[k],
        device_id=(dev,),
        device_id_type=MESH,
    )


def _gather_kernel(ra, e_ref, out_ref, tmp, send, recv, lsem):
    z, y, x, c = _coords()
    rows = e_ref.shape[0]
    right, left = _dev(z, y, _mod4(x + 1), c), _dev(z, y, _mod4(x - 1), c)
    sib = _dev(z, y, x, 1 - c)
    _barrier((right, left, sib))
    a, b = pl.ds(0, ra), pl.ds(ra, rows - ra)

    def slot(xx):
        return _mod4(xx) * 2 + c

    own = slot(x)
    cp_in = pltpu.make_async_copy(e_ref, tmp, lsem.at[0])
    cp_in.start()
    r_a = _remote(e_ref.at[a], out_ref.at[own, a], send, recv, 0, right)
    r_b = _remote(e_ref.at[b], out_ref.at[own, b], send, recv, 1, right)
    l_b = _remote(e_ref.at[b], out_ref.at[own, b], send, recv, 2, left)
    l_a = _remote(e_ref.at[a], out_ref.at[own, a], send, recv, 3, left)
    s_o = _remote(e_ref, out_ref.at[own], send, recv, 6, sib)
    for cp in (r_a, l_b, r_b, l_a, s_o):
        cp.start()
    cp_in.wait()
    cp_out = pltpu.make_async_copy(tmp, out_ref.at[own], lsem.at[1])
    cp_out.start()

    def fwd(s, half, k, dev):
        ref = out_ref.at[s, half]
        return _remote(ref, ref, send, recv, k, dev)

    sl, sr, sf = slot(x - 1), slot(x + 1), slot(x + 2)
    later = []
    r_a.wait_recv()
    r_f = fwd(sl, a, 4, right)
    r_f.start()
    later.append(fwd(sl, a, 7, sib))
    later[-1].start()
    l_b.wait_recv()
    l_f = fwd(sr, b, 5, left)
    l_f.start()
    later.append(fwd(sr, b, 8, sib))
    later[-1].start()
    r_b.wait_recv()
    later.append(fwd(sl, b, 9, sib))
    later[-1].start()
    l_a.wait_recv()
    later.append(fwd(sr, a, 10, sib))
    later[-1].start()
    r_f.wait_recv()
    later.append(fwd(sf, a, 11, sib))
    later[-1].start()
    l_f.wait_recv()
    later.append(fwd(sf, b, 12, sib))
    later[-1].start()
    cp_out.wait()
    s_o.wait_recv()
    for cp in later:
        cp.wait_recv()
    for cp in (r_a, r_b, l_b, l_a, s_o, r_f, l_f, *later):
        cp.wait_send()


def _gather(e32, ra):
    rows, d = e32.shape
    return pl.pallas_call(
        functools.partial(_gather_kernel, ra),
        name="table_gather",
        out_shape=jax.ShapeDtypeStruct((8, rows, d), F32),
        in_specs=[pl.BlockSpec(memory_space=HBM)],
        out_specs=pl.BlockSpec(memory_space=HBM),
        scratch_shapes=[VMEM((rows, d), F32), DMA((13,)), DMA((13,)), DMA((2,))],
        compiler_params=pltpu.CompilerParams(
            collective_id=0, has_side_effects=True, vmem_limit_bytes=60 << 20
        ),
    )(e32)


def _stats_kernel(st_ref, lse_ref, tgt_ref, got, send, recv):
    z, y, x, c = _coords()
    peers = [
        (_mod4(z + dz), _mod4(y + dy)) for dz in range(4) for dy in range(4) if dz or dy
    ]
    ids = [_dev(pz, py, x, c) for pz, py in peers]
    _barrier(ids)
    cps = []
    for k, dev in enumerate(ids):
        cp = _remote(st_ref, got.at[k], send, recv, k, dev)
        cp.start()
        cps.append(cp)
    n = lse_ref.shape[0]
    m, s, t = st_ref[0:n], st_ref[n : 2 * n], st_ref[2 * n : 3 * n]
    for cp in cps:
        cp.wait_recv()
    top = m
    for k in range(15):
        top = jnp.maximum(top, got[k, 0:n])
    s = s * jnp.exp(m - top)
    for k in range(15):
        s = s + got[k, n : 2 * n] * jnp.exp(got[k, 0:n] - top)
        t = t + got[k, 2 * n : 3 * n]
    lse_ref[...] = top + jnp.log(s)
    tgt_ref[...] = t
    for cp in cps:
        cp.wait_send()


def _stats(st):
    n = st.shape[0] // 3
    vm = pl.BlockSpec(memory_space=VMEM)
    one = jax.ShapeDtypeStruct((n, 128), F32)
    return pl.pallas_call(
        _stats_kernel,
        name="row_stats",
        out_shape=(one, one),
        in_specs=[vm],
        out_specs=(vm, vm),
        scratch_shapes=[VMEM((15, 3 * n, 128), F32), DMA((15,)), DMA((15,))],
        compiler_params=pltpu.CompilerParams(collective_id=1, has_side_effects=True),
    )(st)


def _add_rows(dst, srcs, step):
    rows = dst.shape[0]

    @pl.loop(0, rows // step)
    def _(i):
        r = pl.ds(pl.multiple_of(i * step, step), step)
        acc = dst[r, :]
        for s in srcs:
            acc = acc + s[r, :]
        dst[r, :] = acc


def _reduce_kernel(
    dh_ref, de_ref, dh_out, de_out,
    q, s, xa, xb, xl, xr,
    acc_r, acc_l, own, ya, yb, yl, yr, za, zb, zl, zr,
    send_e, recv_e, send_h, recv_h, lsem,
):
    z, y, x, c = _coords()
    half = dh_ref.shape[-1] // 2
    chunk = dh_ref.shape[2]
    hc = chunk // 2
    xp, xm = _dev(z, y, _mod4(x + 1), c), _dev(z, y, _mod4(x - 1), c)
    yp, ym = _dev(z, _mod4(y + 1), x, c), _dev(z, _mod4(y - 1), x, c)
    zp, zm = _dev(_mod4(z + 1), y, x, c), _dev(_mod4(z - 1), y, x, c)
    sib = _dev(z, y, x, 1 - c)
    _barrier((xp, xm, yp, ym, zp, zm, sib))

    order = (_mod4(x + 2), _mod4(x + 1), _mod4(x - 1), x)
    cols = (pl.ds(0, half), pl.ds(half, half))
    ring1, ring2 = ((yp, ym), (zp, zm)), ((zp, zm), (yp, ym))
    pos1, pos2 = (y, z), (z, y)

    def part(k, p, lo, n):
        if k == 0:
            return dh_ref.at[pl.ds(lo, n), p, :, cols[0]]
        return dh_ref.at[p, pl.ds(lo, n), :, cols[1]]

    loads = []
    d2d = []
    for i in range(4):
        cp = _remote(de_ref.at[order[i] * 2 + 1 - c], s.at[i], send_e, recv_e, i, sib)
        cp.start()
        d2d.append(cp)
        ld = pltpu.make_async_copy(de_ref.at[order[i] * 2 + c], q.at[i], lsem.at[i])
        ld.start()
        loads.append(ld)
    first = []
    for k in range(2):
        p = pos1[k]
        rt, lt = ring1[k]
        cps = [
            _remote(part(k, _mod4(p + 2), 0, 2), ya.at[k], send_h, recv_h, (k, 0), rt),
            _remote(part(k, _mod4(p + 2), 2, 2), yb.at[k], send_h, recv_h, (k, 1), lt),
            _remote(part(k, _mod4(p + 1), 2, 2), yl.at[k, pl.ds(2, 2)], send_h, recv_h, (k, 2), rt),
            _remote(part(k, _mod4(p - 1), 0, 2), yr.at[k, pl.ds(0, 2)], send_h, recv_h, (k, 3), lt),
        ]
        for cp in cps:
            cp.start()
        first.append(cps)
        lds = [
            pltpu.make_async_copy(part(k, _mod4(p + 1), 0, 2), acc_r.at[k], lsem.at[4 + 3 * k]),
            pltpu.make_async_copy(part(k, _mod4(p - 1), 2, 2), acc_l.at[k], lsem.at[5 + 3 * k]),
            pltpu.make_async_copy(part(k, p, 0, 4), own.at[k], lsem.at[6 + 3 * k]),
        ]
        for ld in lds:
            ld.start()
        loads += lds

    sent = list(d2d) + first[0] + first[1]

    def go(cp):
        cp.start()
        sent.append(cp)
        return cp

    for i in range(4):
        loads[i].wait()
        d2d[i].wait_recv()
        _add_rows(q.at[i], [s.at[i]], 8)
        if i == 0:
            e0 = go(_remote(q.at[0, :, cols[0]], xa, send_e, recv_e, 4, xp))
            e1 = go(_remote(q.at[0, :, cols[1]], xb, send_e, recv_e, 5, xm))
        if i == 1:
            e2 = go(_remote(q.at[1, :, cols[1]], xl.at[:, cols[1]], send_e, recv_e, 6, xp))
        if i == 2:
            e3 = go(_remote(q.at[2, :, cols[0]], xr.at[:, cols[0]], send_e, recv_e, 7, xm))

    for k in range(2):
        rt, lt = ring1[k]
        loads[4 + 3 * k].wait()
        first[k][0].wait_recv()
        for i in range(2):
            _add_rows(acc_r.at[k, i], [ya.at[k, i]], 8)
        first[k].append(go(_remote(acc_r.at[k], yl.at[k, pl.ds(0, 2)], send_h, recv_h, (k, 4), rt)))
        loads[5 + 3 * k].wait()
        first[k][1].wait_recv()
        for i in range(2):
            _add_rows(acc_l.at[k, i], [yb.at[k, i]], 8)
        first[k].append(go(_remote(acc_l.at[k], yr.at[k, pl.ds(2, 2)], send_h, recv_h, (k, 5), lt)))

    e0.wait_recv()
    _add_rows(q.at[1, :, cols[0]], [xa], 8)
    e4 = go(_remote(q.at[1, :, cols[0]], xl.at[:, cols[0]], send_e, recv_e, 8, xp))
    e1.wait_recv()
    _add_rows(q.at[2, :, cols[1]], [xb], 8)
    e5 = go(_remote(q.at[2, :, cols[1]], xr.at[:, cols[1]], send_e, recv_e, 9, xm))

    lo, hi = pl.ds(0, hc), pl.ds(hc, hc)
    second = []
    for k in range(2):
        loads[6 + 3 * k].wait()
        for cp in first[k][2:]:
            cp.wait_recv()
        for i in range(4):
            _add_rows(own.at[k, i], [yl.at[k, i], yr.at[k, i]], 8)
        r = pos2[k]
        rt, lt = ring2[k]
        second.append([
            go(_remote(own.at[k, _mod4(r + 2), lo], za.at[k], send_h, recv_h, (k, 6), rt)),
            go(_remote(own.at[k, _mod4(r + 2), hi], zb.at[k], send_h, recv_h, (k, 7), lt)),
            go(_remote(own.at[k, _mod4(r + 1), hi], zl.at[k, hi], send_h, recv_h, (k, 8), rt)),
            go(_remote(own.at[k, _mod4(r - 1), lo], zr.at[k, lo], send_h, recv_h, (k, 9), lt)),
        ])
    for k in range(2):
        r = pos2[k]
        rt, lt = ring2[k]
        second[k][0].wait_recv()
        _add_rows(own.at[k, _mod4(r + 1), lo], [za.at[k]], 8)
        second[k].append(go(_remote(own.at[k, _mod4(r + 1), lo], zl.at[k, lo], send_h, recv_h, (k, 10), rt)))
        second[k][1].wait_recv()
        _add_rows(own.at[k, _mod4(r - 1), hi], [zb.at[k]], 8)
        second[k].append(go(_remote(own.at[k, _mod4(r - 1), hi], zr.at[k, hi], send_h, recv_h, (k, 11), lt)))
    outs = []
    for k in range(2):
        r = pos2[k]
        for cp in second[k][2:]:
            cp.wait_recv()
        _add_rows(own.at[k, r], [zl.at[k], zr.at[k]], 8)
        cp = pltpu.make_async_copy(own.at[k, r], dh_out.at[:, cols[k]], lsem.at[10 + k])
        cp.start()
        outs.append(cp)

    for cp in (e2, e3, e4, e5):
        cp.wait_recv()
    _add_rows(q.at[3], [xl, xr], 8)
    cp = pltpu.make_async_copy(q.at[3], de_out, lsem.at[12])
    cp.start()
    outs.append(cp)
    for cp in outs:
        cp.wait()
    for cp in sent:
        cp.wait_send()


def _reduce(dh, de):
    _, _, chunk, d = dh.shape
    _, rows, _ = de.shape
    h, hc = d // 2, chunk // 2
    hbm = pl.BlockSpec(memory_space=HBM)
    return pl.pallas_call(
        _reduce_kernel,
        name="grad_reduce",
        out_shape=(jax.ShapeDtypeStruct((chunk, d), F32), jax.ShapeDtypeStruct((rows, d), F32)),
        in_specs=[hbm, hbm],
        out_specs=(hbm, hbm),
        scratch_shapes=[
            VMEM((4, rows, d), F32), VMEM((4, rows, d), F32),
            VMEM((rows, h), F32), VMEM((rows, h), F32), VMEM((rows, d), F32), VMEM((rows, d), F32),
            VMEM((2, 2, chunk, h), F32), VMEM((2, 2, chunk, h), F32), VMEM((2, 4, chunk, h), F32),
            VMEM((2, 2, chunk, h), F32), VMEM((2, 2, chunk, h), F32),
            VMEM((2, 4, chunk, h), F32), VMEM((2, 4, chunk, h), F32),
            VMEM((2, hc, h), F32), VMEM((2, hc, h), F32), VMEM((2, chunk, h), F32), VMEM((2, chunk, h), F32),
            DMA((10,)), DMA((10,)), DMA((2, 12)), DMA((2, 12)), DMA((13,)),
        ],
        compiler_params=pltpu.CompilerParams(
            collective_id=2, has_side_effects=True, vmem_limit_bytes=67043328
        ),
    )(dh, de)


def _allsum_kernel(v_ref, o_ref, mid, got1, got2, send1, recv1, send2, recv2):
    z, y, x, c = _coords()
    near = [_dev(_mod4(z + a), _mod4(y + b), x, c) for a in range(4) for b in range(4) if a or b]
    far = [_dev(z, y, _mod4(x + a), lax.rem(c + b, 2)) for a in range(4) for b in range(2) if a or b]
    _barrier(near + far)
    cps = [_remote(v_ref, got1.at[k], send1, recv1, k, dev) for k, dev in enumerate(near)]
    for cp in cps:
        cp.start()
    for cp in cps:
        cp.wait_recv()
    tot = v_ref[...]
    for k in range(15):
        tot = tot + got1[k]
    mid[...] = tot
    cps2 = [_remote(mid, got2.at[k], send2, recv2, k, dev) for k, dev in enumerate(far)]
    for cp in cps2:
        cp.start()
    for cp in cps2:
        cp.wait_recv()
    tot = mid[...]
    for k in range(7):
        tot = tot + got2[k]
    o_ref[...] = tot
    for cp in cps + cps2:
        cp.wait_send()


def _allsum(v):
    vm = pl.BlockSpec(memory_space=VMEM)
    return pl.pallas_call(
        _allsum_kernel,
        name="small_sum",
        out_shape=jax.ShapeDtypeStruct(v.shape, F32),
        in_specs=[vm],
        out_specs=vm,
        scratch_shapes=[
            VMEM(v.shape, F32), VMEM((15, *v.shape), F32), VMEM((7, *v.shape), F32),
            DMA((15,)), DMA((15,)), DMA((7,)), DMA((7,)),
        ],
        compiler_params=pltpu.CompilerParams(collective_id=3, has_side_effects=True),
    )(v)


def solution(mesh):
    group = mesh.shape[AXIS]

    def local_step(residual, labels, loss_mask, norm_gain, table_shard):
        tokens, dim = residual.shape
        rows = table_shard.shape[0]
        chunk = tokens // group
        pad = -rows % 8 + rows
        me = lax.axis_index(AXIS)
        xc, zy = lax.rem(me, 8), me // 8
        tok = tokens // 8

        e32 = jnp.pad(table_shard.astype(F32), ((0, pad - rows), (0, 0)))
        ra = (pad // 2) // 8 * 8
        table = _gather(e32, ra).astype(BF16).reshape(8 * pad, dim)

        def mine(v):
            v = v.reshape(16, 8, chunk, *v.shape[1:])
            return lax.dynamic_index_in_dim(v, xc, 1, keepdims=False).reshape(tok, *v.shape[3:])

        x_f32 = mine(residual).astype(F32)
        lab = mine(labels)
        msk = mine(loss_mask)
        inv_rms = lax.rsqrt(jnp.mean(x_f32 * x_f32, axis=-1, keepdims=True) + NORM_EPS)
        hidden = (x_f32 * inv_rms * norm_gain).astype(BF16)
        mask_total = jnp.sum(loss_mask)

        row = lax.broadcasted_iota(jnp.int32, (8, pad), 1)
        col_ids = (zy * 8 + lax.broadcasted_iota(jnp.int32, (8, pad), 0)) * rows + row
        col_ids = jnp.where((row < rows) & (col_ids < VOCAB_REAL), col_ids, -1).reshape(1, 8 * pad)
        z = jnp.einsum('td,vd->tv', hidden, table, preferred_element_type=F32) / LOGIT_SCALE
        z = jnp.where(col_ids >= 0, z, -jnp.inf)
        is_label = col_ids == lab[:, None]
        top = jnp.max(z, axis=-1)
        part_sum = jnp.sum(jnp.exp(z - top[:, None]), axis=-1)
        part_tgt = jnp.sum(jnp.where(is_label, z, 0.0), axis=-1)
        st = jnp.concatenate([v.reshape(tok // 128, 128) for v in (top, part_sum, part_tgt)])
        lse, tgt = _stats(st)
        lse, tgt = lse.reshape(tok), tgt.reshape(tok)
        prob = jnp.exp(z - lse[:, None])
        dz = (jnp.where(is_label, prob - 1.0, prob) * (msk / mask_total)[:, None]).astype(BF16)
        dh_part = jnp.dot(dz, table, preferred_element_type=F32)
        de_part = jnp.einsum('tv,td->vd', dz, hidden, preferred_element_type=F32)
        dh, de = _reduce(dh_part.reshape(4, 4, chunk, dim), de_part.reshape(8, pad, dim))

        dh = dh / LOGIT_SCALE
        d_embed = de[:rows] / LOGIT_SCALE
        x_loc = lax.dynamic_slice_in_dim(residual, me * chunk, chunk, axis=0).astype(F32)
        inv_loc = lax.rsqrt(jnp.mean(x_loc * x_loc, axis=-1, keepdims=True) + NORM_EPS)
        x_hat = x_loc * inv_loc
        dg_part = jnp.sum(dh * x_hat, axis=0)
        loss_part = jnp.where(zy == 0, jnp.sum(msk * (lse - tgt)), 0.0)
        small = jnp.concatenate([dg_part, jnp.full((1024,), loss_part)]).reshape(-1, 128)
        small = _allsum(small).reshape(-1)
        u = dh * norm_gain
        d_res = inv_loc * (u - x_hat * jnp.mean(u * x_hat, axis=-1, keepdims=True))
        return small[dim] / mask_total, d_res, d_embed, small[:dim]

    return jax.shard_map(
        local_step,
        mesh=mesh,
        in_specs=(P(), P(), P(), P(), P(AXIS, None)),
        out_specs=(P(), P(AXIS, None), P(AXIS, None), P()),
        check_vma=False,
    )
```

```python
import functools

import jax
import jax.numpy as jnp
from jax import lax
from jax.experimental import pallas as pl
from jax.experimental.pallas import tpu as pltpu
from jax.sharding import PartitionSpec as P

VOCAB_REAL = 49155
LOGIT_SCALE = 6.0
NORM_EPS = 1e-6

AXIS = "vp"
MESH = pl.DeviceIdType.MESH
F32 = jnp.float32
BF16 = jnp.bfloat16
HBM = pltpu.HBM
VMEM = pltpu.VMEM
DMA = pltpu.SemaphoreType.DMA


def _coords():
    me = lax.axis_index(AXIS)
    return me // 32, (me // 8) % 4, (me // 2) % 4, me % 2


def _dev(z, y, x, c):
    return ((z * 4 + y) * 4 + x) * 2 + c


def _mod4(v):
    return lax.rem(v + 8, 4)


def _barrier(peers):
    sem = pltpu.get_barrier_semaphore()
    for p in peers:
        pl.semaphore_signal(sem, inc=1, device_id=(p,), device_id_type=MESH)
    pl.semaphore_wait(sem, len(peers))


def _remote(src, dst, send, recv, k, dev):
    return pltpu.make_async_remote_copy(
        src_ref=src,
        dst_ref=dst,
        send_sem=send.at[k],
        recv_sem=recv.at[k],
        device_id=(dev,),
        device_id_type=MESH,
    )


class Dims:
    def __init__(self, tokens, dim, rows, group):
        self.dim, self.rows = dim, rows
        unit = 128 if rows >= 128 else 64
        self.rm = rows // unit * unit
        self.ha = self.rm // 2
        self.pad = self.rm + 8
        self.chunk = tokens // group
        self.tok = 16 * self.chunk
        self.nt = 2 * self.chunk
        self.main = 8 * self.rm
        self.wide = self.main + 128
        self.h = dim // 2


def _loop_rows(rows, step, fn):
    @pl.loop(0, rows // step)
    def _(i):
        fn(pl.ds(pl.multiple_of(i * step, step), step))


def _fwd_kernel(
    dm, x4, e_ref, g_ref, lab, msk,
    eg, zh, zeh, hh, et, lse_o, pos_o, w_o,
    hv, xst, est, ebf, oext, ext, extb, etst, zst, st, got,
    send, recv, ssend, srecv, esem, xsem, zsem, tsem, hsem,
):
    z, y, x, c = _coords()
    xc, zy = x * 2 + c, z * 4 + y
    rows, rm, ha, dim, chunk, tok, nt = dm.rows, dm.rm, dm.ha, dm.dim, dm.chunk, dm.tok, dm.nt
    right, left = _dev(z, y, _mod4(x + 1), c), _dev(z, y, _mod4(x - 1), c)
    sib = _dev(z, y, x, 1 - c)
    peers = [_dev(_mod4(z + a), _mod4(y + b), x, c) for a in range(4) for b in range(4) if a or b]
    bar = pltpu.get_barrier_semaphore()
    for p in (right, left, sib, *peers):
        pl.semaphore_signal(bar, inc=1, device_id=(p,), device_id_type=MESH)

    def xload(k):
        return pltpu.make_async_copy(x4.at[k, xc], xst.at[lax.rem(k, 2)], xsem.at[lax.rem(k, 2)])

    xload(0).start()

    own = xc
    for j in range(2):
        def widen(r, j=j):
            est[0, j, r, :] = e_ref[pl.ds(j * ha + r.start, r.size), :].astype(F32)

        _loop_rows(ha, 16, widen)
    oext[...] = jnp.zeros_like(oext)
    oext[0 : rows - rm, :] = e_ref[rm:rows, :].astype(F32)
    cps = [pltpu.make_async_copy(est.at[0, j], eg.at[own, pl.ds(j * ha, ha)], esem.at[j]) for j in range(2)]
    cps.append(pltpu.make_async_copy(oext, eg.at[own, pl.ds(rm, 8)], esem.at[2]))
    for cp in cps:
        cp.start()
    for cp in cps:
        cp.wait()
    pl.semaphore_wait(bar, 18)

    a, b = pl.ds(0, ha), pl.ds(ha, ha + 8)

    def piece(s, half, k, dev):
        ref = eg.at[s, half]
        return _remote(ref, ref, send, recv, k, dev)

    def slot(xx):
        return _mod4(xx) * 2 + c

    r_a, r_b = piece(own, a, 0, right), piece(own, b, 1, right)
    l_b, l_a = piece(own, b, 2, left), piece(own, a, 3, left)
    s_o = _remote(eg.at[own], eg.at[own], send, recv, 6, sib)
    for cp in (r_a, l_b, s_o, r_b, l_a):
        cp.start()

    gain = g_ref[...]

    @pl.loop(0, 16)
    def _(k):
        @pl.when(k < 15)
        def _():
            xload(k + 1).start()

        xload(k).wait()

        def norm(r):
            v = xst[lax.rem(k, 2), r, :].astype(F32)
            inv = lax.rsqrt(jnp.mean(v * v, axis=-1, keepdims=True) + NORM_EPS)
            at = pl.multiple_of(k * chunk + r.start, r.size)
            hv[pl.ds(at, r.size), :] = (v * inv * gain).astype(BF16)

        _loop_rows(chunk, 16, norm)

    hout = pltpu.make_async_copy(hv, hh, hsem.at[0])
    hout.start()

    total = jnp.sum(msk[...])
    for k in range(16):
        at = pl.ds(k * chunk, chunk)
        w_o[:, at] = msk[k, xc] / total
        q = lab[k, xc] - zy * (8 * rows)
        s = jnp.zeros_like(q)
        for i in range(1, 8):
            s = s + jnp.where(q >= i * rows, 1, 0)
        r = q - s * rows
        hi = jnp.where(r >= ha, 1, 0)
        at_main = ((s // 2 * 2 + hi) * 2 + s % 2) * ha + r - hi * ha
        at_ext = 8 * rm + s * 8 + r - rm
        place = jnp.where(r < rm, at_main, at_ext)
        pos_o[:, at] = jnp.where((q >= 0) & (q < 8 * rows), place, -1)
    st[0:1, :] = jnp.full((1, tok), -1e30, F32)
    st[1:2, :] = jnp.zeros((1, tok), F32)

    def load(i, xx, half):
        return [
            pltpu.make_async_copy(eg.at[xx * 2 + j, pl.ds(half * ha, ha)], est.at[i, j], esem.at[i * 2 + j])
            for j in range(2)
        ]

    def add_stats(v, lanes):
        m_old, s_old = st[0:1, lanes], st[1:2, lanes]
        m = jnp.maximum(m_old, jnp.max(v, axis=0, keepdims=True))
        s = jnp.sum(jnp.exp(v - m), axis=0, keepdims=True)
        st[0:1, lanes] = m
        st[1:2, lanes] = s_old * jnp.exp(m_old - m) + s

    def product(lhs, lanes):
        v = lax.dot_general(lhs, hv[lanes, :], (((1,), (1,)), ((), ())), preferred_element_type=F32)
        return v * (1.0 / LOGIT_SCALE)

    def logits(i, xx, half):
        first = VOCAB_REAL - ((zy * 8 + xx * 2) * rows + half * ha)
        base = pl.multiple_of((xx * 2 + half) * rm, rm)

        def out(t, s):
            lanes = pl.ds(pl.multiple_of(t * nt, nt), nt)
            return pltpu.make_async_copy(zst.at[s], zh.at[pl.ds(base, rm), lanes], zsem.at[s])

        @pl.loop(0, tok // nt)
        def _(t):
            s = lax.rem(t, 2)

            @pl.when(t >= 2)
            def _():
                out(t, s).wait()

            lanes = pl.ds(pl.multiple_of(t * nt, nt), nt)
            v = product(ebf[i], lanes)
            row = lax.broadcasted_iota(jnp.int32, v.shape, 0)
            lim = jnp.where(row < ha, first, first - rows + ha)
            v = jnp.where(row < lim, v, -jnp.inf)
            zst[s] = v
            out(t, s).start()
            add_stats(v, lanes)

        for s in range(2):
            out(s, s).wait()

    def pair(blocks):
        for i, (xx, half) in enumerate(blocks):
            for cp in load(i, xx, half):
                cp.start()

        @pl.loop(0, 2)
        def _(i):
            xx = jnp.where(i == 0, blocks[0][0], blocks[1][0])
            half = jnp.where(i == 0, blocks[0][1], blocks[1][1])
            for cp in load(i, xx, half):
                cp.wait()
            for j in range(2):
                def narrow(r, j=j):
                    at = pl.multiple_of(j * ha + r.start, r.size)
                    ebf[i, pl.ds(at, r.size), :] = est[i, j, r, :].astype(BF16)

                _loop_rows(ha, 16, narrow)
            logits(i, xx, half)

    def turn(blocks):
        @pl.loop(0, 2)
        def _(i):
            xx = jnp.where(i == 0, blocks[0][0], blocks[1][0])
            half = jnp.where(i == 0, blocks[0][1], blocks[1][1])

            @pl.loop(0, dim // 128)
            def _(d):
                at = pl.ds(pl.multiple_of(d * 128, 128), 128)
                etst[at, 0:rm] = ebf[i, :, at].T

            lanes = pl.ds(pl.multiple_of((xx * 2 + half) * rm, rm), rm)
            cp = pltpu.make_async_copy(etst.at[:, pl.ds(0, rm)], et.at[:, lanes], tsem.at[0])
            cp.start()
            cp.wait()

    xl, xr, xf = _mod4(x - 1), _mod4(x + 1), _mod4(x + 2)
    sl, sr, sf = slot(x - 1), slot(x + 1), slot(x + 2)
    s_o.wait_recv()
    mine = ((x, 0), (x, 1))
    pair(mine)
    turn(mine)

    def ahead(s, half, k, dev):
        cp = piece(s, half, k, dev)
        cp.start()
        return cp

    r_a.wait_recv()
    r_f = ahead(sl, a, 4, right)
    d0 = ahead(sl, a, 7, sib)
    l_b.wait_recv()
    l_f = ahead(sr, b, 5, left)
    d1 = ahead(sr, b, 8, sib)
    d0.wait_recv()
    d1.wait_recv()
    near = ((xl, 0), (xr, 1))
    pair(near)
    turn(near)
    r_b.wait_recv()
    d2 = ahead(sl, b, 9, sib)
    l_a.wait_recv()
    d3 = ahead(sr, a, 10, sib)
    d2.wait_recv()
    d3.wait_recv()
    near = ((xl, 1), (xr, 0))
    pair(near)
    turn(near)
    r_f.wait_recv()
    d4 = ahead(sf, a, 11, sib)
    l_f.wait_recv()
    d5 = ahead(sf, b, 12, sib)
    d4.wait_recv()
    d5.wait_recv()
    ext_loads = [
        pltpu.make_async_copy(eg.at[s, pl.ds(rm, 8)], ext.at[pl.ds(s * 8, 8)], hsem.at[1 + s]) for s in range(8)
    ]
    for cp in ext_loads:
        cp.start()
    far = ((xf, 0), (xf, 1))
    pair(far)
    for cp in ext_loads:
        cp.wait()
    extb[0:64, :] = ext[...].astype(BF16)
    extb[64:128, :] = jnp.zeros((64, dim), BF16)

    @pl.loop(0, tok // nt)
    def _(t):
        lanes = pl.ds(pl.multiple_of(t * nt, nt), nt)
        v = product(extb[0:64, :], lanes)
        row = lax.broadcasted_iota(jnp.int32, v.shape, 0)
        ok = ((row & 7) < rows - rm) & ((zy * 8 + (row >> 3)) * rows + rm + (row & 7) < VOCAB_REAL)
        v = jnp.where(ok, v, -jnp.inf)
        zst[0, 0:64, :] = v
        cp = pltpu.make_async_copy(zst.at[0, pl.ds(0, 64)], zeh.at[:, lanes], zsem.at[0])
        cp.start()
        add_stats(v, lanes)
        cp.wait()

    scps = [_remote(st, got.at[k], ssend, srecv, k, p) for k, p in enumerate(peers)]
    for cp in scps:
        cp.start()
    turn(far)

    @pl.loop(0, dim // 128)
    def _(d):
        at = pl.ds(pl.multiple_of(d * 128, 128), 128)
        etst[at, 0:128] = extb[:, at].T

    ext_out = pltpu.make_async_copy(etst.at[:, pl.ds(0, 128)], et.at[:, pl.ds(dm.main, 128)], tsem.at[0])
    ext_out.start()
    for cp in scps:
        cp.wait_recv()
    m = st[0:1, :]
    top = m
    for k in range(15):
        top = jnp.maximum(top, got[k, 0:1, :])
    s = st[1:2, :] * jnp.exp(m - top)
    for k in range(15):
        s = s + got[k, 1:2, :] * jnp.exp(got[k, 0:1, :] - top)
    lse_o[...] = top + jnp.log(s)
    ext_out.wait()
    hout.wait()
    for cp in (r_a, r_b, l_b, l_a, s_o, r_f, l_f, d0, d1, d2, d3, d4, d5, *scps):
        cp.wait_send()


def _forward(dm, x4, table, gain, labels, mask):
    hbm, vm = pl.BlockSpec(memory_space=HBM), pl.BlockSpec(memory_space=VMEM)
    sd = jax.ShapeDtypeStruct
    d, tok = dm.dim, dm.tok
    return pl.pallas_call(
        functools.partial(_fwd_kernel, dm),
        name="forward",
        out_shape=(
            sd((8, dm.pad, d), F32), sd((dm.main, tok), F32), sd((64, tok), F32), sd((tok, d), BF16),
            sd((d, dm.wide), BF16), sd((1, tok), F32), sd((1, tok), jnp.int32), sd((1, tok), F32),
        ),
        in_specs=[hbm, vm, vm, vm, vm],
        out_specs=(hbm, hbm, hbm, hbm, hbm, vm, vm, vm),
        scratch_shapes=[
            VMEM((tok, d), BF16), VMEM((2, dm.chunk, d), BF16), VMEM((2, 2, dm.ha, d), F32), VMEM((2, dm.rm, d), BF16),
            VMEM((8, d), F32), VMEM((64, d), F32), VMEM((128, d), BF16), VMEM((d, max(dm.rm, 128)), BF16),
            VMEM((2, dm.rm, dm.nt), F32), VMEM((2, tok), F32), VMEM((15, 2, tok), F32),
            DMA((13,)), DMA((13,)), DMA((15,)), DMA((15,)), DMA((4,)), DMA((2,)), DMA((2,)), DMA((1,)), DMA((9,)),
        ],
        compiler_params=pltpu.CompilerParams(
            collective_id=0, has_side_effects=True, vmem_limit_bytes=67043328
        ),
    )(x4, table, gain, labels, mask)


def _bwd_kernel(
    dm, zh, zeh, hh, et, lse, pos, w,
    dh_out, tgt_out, s_h, q_h, xa, xb, xl, xr, dhp, yr,
    hv, etv, dz, zst, od, sst, dee, dht, ya, yb, yl, za, zb, zl, zr, tst,
    send_e, recv_e, send_h, recv_h, bsem, zsem, dsem, osem, hsem, tsem,
):
    z, y, x, c = _coords()
    rm, ha, dim, chunk, tok, h = dm.rm, dm.ha, dm.dim, dm.chunk, dm.tok, dm.h
    hc = h // 2
    xp, xm = _dev(z, y, _mod4(x + 1), c), _dev(z, y, _mod4(x - 1), c)
    yp, ym = _dev(z, _mod4(y + 1), x, c), _dev(z, _mod4(y - 1), x, c)
    zp, zm = _dev(_mod4(z + 1), y, x, c), _dev(_mod4(z - 1), y, x, c)
    sib = _dev(z, y, x, 1 - c)
    peers = (xp, xm, yp, ym, zp, zm, sib)
    bar = pltpu.get_barrier_semaphore()
    for p in peers:
        pl.semaphore_signal(bar, inc=1, device_id=(p,), device_id_type=MESH)
    x_far, x_p, x_m = _mod4(x + 2), _mod4(x + 1), _mod4(x - 1)
    sent = []

    def go(cp):
        cp.start()
        sent.append(cp)
        return cp

    rc = min(64, rm)
    ln = min(512, tok)

    def zload(first, i):
        at = pl.multiple_of(lax.rem(first + i * rc, dm.main), rc)
        s = lax.rem(i, 2)
        return pltpu.make_async_copy(zh.at[pl.ds(at, rc)], zst.at[s], zsem.at[s])

    def dz_tile(s, n, place, store):
        for l in range(tok // ln):
            lanes = pl.ds(l * ln, ln)
            v = zst[s, 0:n, lanes]
            row = lax.broadcasted_iota(jnp.int32, v.shape, 0) + place
            hit = row == pos[:, lanes]
            tgt_out[:, lanes] += jnp.sum(jnp.where(hit, v, 0.0), axis=0, keepdims=True)
            p = jnp.exp(v - lse[:, lanes])
            dz[store, lanes] = (jnp.where(hit, p - 1.0, p) * w[:, lanes]).astype(BF16)

    def dz_rows(first, n):
        @pl.loop(0, n)
        def _(i):
            @pl.when(i + 1 < n)
            def _():
                zload(first, i + 1).start()

            zload(first, i).wait()
            at = pl.multiple_of(lax.rem(first + i * rc, dm.main), rc)
            dz_tile(lax.rem(i, 2), rc, at, pl.ds(at, rc))

    zload(x_far * 2 * rm, 0).start()
    big = [pltpu.make_async_copy(hh, hv, bsem.at[0]), pltpu.make_async_copy(et, etv, bsem.at[1])]
    for cp in big:
        cp.start()
    tgt_out[...] = jnp.zeros_like(tgt_out)
    dz_rows(x_far * 2 * rm, 2 * rm // rc)
    cp = pltpu.make_async_copy(zeh, zst.at[0, pl.ds(0, 64)] if rc >= 64 else zst.at[0], zsem.at[0])
    cp.start()
    cp.wait()
    dz_tile(0, 64, dm.main, pl.ds(dm.main, 64))
    dz[dm.main + 64 : dm.wide, :] = jnp.zeros((64, tok), BF16)
    big[0].wait()

    nd = min(256, dim)

    @pl.loop(0, dim // nd)
    def _(i):
        lanes = pl.ds(pl.multiple_of(i * nd, nd), nd)
        dee[:, lanes] = jnp.dot(dz[dm.main : dm.main + 64, :], hv[:, lanes], preferred_element_type=F32)

    pl.semaphore_wait(bar, len(peers))
    counts = {"d": 0}

    def de_block(xx, half, s):
        at = pl.ds(pl.multiple_of((xx * 2 + half) * rm, rm), rm)

        @pl.loop(0, dim // nd)
        def _(i):
            lanes = pl.ds(pl.multiple_of(i * nd, nd), nd)
            v = jnp.dot(dz[at, :], hv[:, lanes], preferred_element_type=F32)
            od[s, 0, 0:ha, lanes] = v[0:ha]
            od[s, 1, 0:ha, lanes] = v[ha:rm]

        n = ha + 8 * half
        if half:
            for j in range(2):
                od[s, j, ha : ha + 8, :] = dee[pl.ds(pl.multiple_of((xx * 2 + j) * 8, 8), 8), :]
        k = counts["d"]
        counts["d"] += 1
        there = pl.ds(half * ha, n)
        cp = _remote(od.at[s, 1 - c, pl.ds(0, n)], s_h.at[xx, there], send_e, recv_e, k, sib)
        cp.start()
        return xx, half, s, n, cp

    def de_sum(blk):
        xx, half, s, n, cp = blk
        there = pl.ds(half * ha, n)
        cp.wait_recv()
        ld = pltpu.make_async_copy(s_h.at[xx, there], sst.at[pl.ds(0, n)], dsem.at[0])
        ld.start()
        ld.wait()

        def add(r):
            od[s, c, r, :] = od[s, c, r, :] + sst[r, :]

        _loop_rows(n, 8, add)
        out = pltpu.make_async_copy(od.at[s, c, pl.ds(0, n)], q_h.at[xx, there], dsem.at[1])
        out.start()
        out.wait()
        cp.wait_send()

    rows_a, rows_b = pl.ds(0, ha), pl.ds(ha, ha + 8)
    b0 = de_block(x_far, 0, 0)
    b1 = de_block(x_far, 1, 1)
    zload((x_far + 1) * 2 * rm, 0).start()
    dz_rows((x_far + 1) * 2 * rm, 6 * rm // rc)
    de_sum(b0)
    e0 = go(_remote(q_h.at[x_far, rows_a], xa, send_e, recv_e, 8, xp))
    de_sum(b1)
    e1 = go(_remote(q_h.at[x_far, rows_b], xb, send_e, recv_e, 9, xm))

    big[1].wait()
    mt = min(256, h)

    def dh_group(q, n, where):
        def outs(i, s):
            zz, pr = where(i)
            return [
                pltpu.make_async_copy(dht.at[s, j], dhp.at[zz, pr * 2 + j, pl.ds(q * h, h)], hsem.at[s * 2 + j])
                for j in range(2)
            ]

        @pl.loop(0, n)
        def _(i):
            s = lax.rem(i, 2)

            @pl.when(i >= 2)
            def _():
                for cp in outs(i, s):
                    cp.wait()

            zz, pr = where(i)
            lanes = pl.ds(pl.multiple_of((zz * 4 + pr * 2) * chunk, 2 * chunk), 2 * chunk)

            @pl.loop(0, h // mt)
            def _(m):
                v = jnp.dot(
                    etv[pl.ds(pl.multiple_of(q * h + m * mt, mt), mt), :], dz[:, lanes], preferred_element_type=F32
                )
                at = pl.ds(pl.multiple_of(m * mt, mt), mt)
                dht[s, 0, at, :] = v[:, 0:chunk]
                dht[s, 1, at, :] = v[:, chunk : 2 * chunk]

            for cp in outs(i, s):
                cp.start()

        for s in range(2):
            for cp in outs(s, s):
                cp.wait()

    def part(q, p, lo, n):
        rows = pl.ds(q * h, h)
        if q == 0:
            return dhp.at[pl.ds(lo, n), p, rows]
        return dhp.at[p, pl.ds(lo, n), rows]

    ring1, ring2 = ((yp, ym), (zp, zm)), ((zp, zm), (yp, ym))
    pos1, pos2 = (y, z), (z, y)
    first = [[None] * 6, [None] * 6]

    def send_far(q):
        p, (rt, lt) = pos1[q], ring1[q]
        first[q][0] = go(_remote(part(q, _mod4(p + 2), 0, 2), ya.at[q], send_h, recv_h, (q, 0), rt))
        first[q][1] = go(_remote(part(q, _mod4(p + 2), 2, 2), yb.at[q], send_h, recv_h, (q, 1), lt))

    def send_near(q):
        p, (rt, lt) = pos1[q], ring1[q]
        first[q][2] = go(_remote(part(q, _mod4(p + 1), 2, 2), yl.at[q, pl.ds(2, 2)], send_h, recv_h, (q, 2), rt))
        first[q][3] = go(_remote(part(q, _mod4(p - 1), 0, 2), yr.at[q, pl.ds(0, 2)], send_h, recv_h, (q, 3), lt))

    def add_stream(items):
        def loads(i):
            return [
                pltpu.make_async_copy(src, tst.at[i % 2, j], tsem.at[i % 2, j]) for j, src in enumerate(items[i][1])
            ]

        for cp in loads(0):
            cp.start()
        for i, (dst, srcs) in enumerate(items):
            if i + 1 < len(items):
                for cp in loads(i + 1):
                    cp.start()
            for cp in loads(i):
                cp.wait()

            def add(r, i=i, dst=dst, srcs=srcs):
                v = dst[r, :]
                for j in range(len(srcs)):
                    v = v + tst[i % 2, j, r, :]
                dst[r, :] = v

            _loop_rows(h, min(64, h), add)

    def pass_on(q):
        p, (rt, lt) = pos1[q], ring1[q]
        first[q][0].wait_recv()
        add_stream([(ya.at[q, i], [part(q, _mod4(p + 1), i, 1).at[0]]) for i in range(2)] if q == 1 else
                   [(ya.at[q, i], [part(q, _mod4(p + 1), i, 1).at[0]]) for i in range(2)])
        first[q][4] = go(_remote(ya.at[q], yl.at[q, pl.ds(0, 2)], send_h, recv_h, (q, 4), rt))
        first[q][1].wait_recv()
        add_stream([(yb.at[q, i], [part(q, _mod4(p - 1), 2 + i, 1).at[0]]) for i in range(2)])
        first[q][5] = go(_remote(yb.at[q], yr.at[q, pl.ds(2, 2)], send_h, recv_h, (q, 5), lt))

    lo, hi = pl.ds(0, hc), pl.ds(hc, hc)
    second = [[None] * 6, [None] * 6]

    def second_phase(q):
        for cp in first[q][2:]:
            cp.wait_recv()
        add_stream([(yl.at[q, i], [yr.at[q, i], part(q, pos1[q], i, 1).at[0]]) for i in range(4)])
        r, (rt, lt) = pos2[q], ring2[q]
        second[q][0] = go(_remote(yl.at[q, _mod4(r + 2), lo], za.at[q], send_h, recv_h, (q, 6), rt))
        second[q][1] = go(_remote(yl.at[q, _mod4(r + 2), hi], zb.at[q], send_h, recv_h, (q, 7), lt))
        second[q][2] = go(_remote(yl.at[q, _mod4(r + 1), hi], zl.at[q, hi], send_h, recv_h, (q, 8), rt))
        second[q][3] = go(_remote(yl.at[q, _mod4(r - 1), lo], zr.at[q, lo], send_h, recv_h, (q, 9), lt))

    def second_pass(q):
        r, (rt, lt) = pos2[q], ring2[q]
        second[q][0].wait_recv()
        _add_rows(yl.at[q, _mod4(r + 1), lo], [za.at[q]], min(64, hc))
        second[q][4] = go(_remote(yl.at[q, _mod4(r + 1), lo], zl.at[q, lo], send_h, recv_h, (q, 10), rt))
        second[q][1].wait_recv()
        _add_rows(yl.at[q, _mod4(r - 1), hi], [zb.at[q]], min(64, hc))
        second[q][5] = go(_remote(yl.at[q, _mod4(r - 1), hi], zr.at[q, hi], send_h, recv_h, (q, 11), lt))

    def last(q):
        r = pos2[q]
        for cp in second[q][2:]:
            cp.wait_recv()
        _add_rows(yl.at[q, r], [zl.at[q], zr.at[q]], min(64, h))
        cp = pltpu.make_async_copy(yl.at[q, r], dh_out.at[pl.ds(q * h, h)], osem.at[q])
        cp.start()
        return cp

    def ring_sum(xx, rows, n, src, s, k, dst, dev):
        lds = [
            pltpu.make_async_copy(q_h.at[xx, rows], od.at[s, 0, pl.ds(0, n)], dsem.at[0]),
            pltpu.make_async_copy(src, sst.at[pl.ds(0, n)], dsem.at[1]),
        ]
        for cp in lds:
            cp.start()
        for cp in lds:
            cp.wait()

        def add(r):
            od[s, 0, r, :] = od[s, 0, r, :] + sst[r, :]

        _loop_rows(n, 8, add)
        out = pltpu.make_async_copy(od.at[s, 0, pl.ds(0, n)], q_h.at[xx, rows], dsem.at[0])
        out.start()
        out.wait()
        return go(_remote(q_h.at[xx, rows], dst, send_e, recv_e, k, dev))

    pf = _mod4(y + 2) // 2
    dh_group(1, 2, lambda i: (_mod4(z + 2), i))
    send_far(1)
    dh_group(0, 4, lambda i: (i, pf))
    send_far(0)
    dh_group(1, 4, lambda i: (_mod4(z + 1 + 2 * lax.rem(i, 2)), (i < 1) * 1 + (i > 2) * 1))
    send_near(1)
    dh_group(0, 4, lambda i: (i, 1 - pf))
    send_near(0)
    b2 = de_block(x_p, 1, 0)
    b3 = de_block(x_m, 0, 1)
    pass_on(1)
    de_sum(b2)
    e2 = go(_remote(q_h.at[x_p, rows_b], xl.at[rows_b], send_e, recv_e, 10, xp))
    de_sum(b3)
    e3 = go(_remote(q_h.at[x_m, rows_a], xr.at[rows_a], send_e, recv_e, 11, xm))
    pass_on(0)
    dh_group(1, 2, lambda i: (z, i))
    b4 = de_block(x_p, 0, 0)
    b5 = de_block(x_m, 1, 1)
    de_sum(b4)
    e0.wait_recv()
    e4 = ring_sum(x_p, rows_a, ha, xa, 0, 12, xl.at[rows_a], xp)
    de_sum(b5)
    e1.wait_recv()
    e5 = ring_sum(x_m, rows_b, ha + 8, xb, 1, 13, xr.at[rows_b], xm)
    b6 = de_block(x, 0, 0)
    b7 = de_block(x, 1, 1)
    de_sum(b6)
    de_sum(b7)
    second_phase(1)
    second_phase(0)
    second_pass(1)
    second_pass(0)
    outs = [last(1), last(0)]
    for cp in (e2, e3, e4, e5):
        cp.wait_recv()
    for cp in outs:
        cp.wait()
    for cp in sent:
        cp.wait_send()


def _add_rows(dst, srcs, step):
    def add(r):
        acc = dst[r, :]
        for s in srcs:
            acc = acc + s[r, :]
        dst[r, :] = acc

    _loop_rows(dst.shape[0], step, add)


def _backward(dm, zh, zeh, hh, et, lse, pos, w):
    hbm, vm = pl.BlockSpec(memory_space=HBM), pl.BlockSpec(memory_space=VMEM)
    sd = jax.ShapeDtypeStruct
    d, tok, h, ck = dm.dim, dm.tok, dm.h, dm.chunk
    out = pl.pallas_call(
        functools.partial(_bwd_kernel, dm),
        name="backward",
        out_shape=(
            sd((d, ck), F32), sd((1, tok), F32), sd((4, dm.pad, d), F32), sd((4, dm.pad, d), F32),
            sd((dm.ha, d), F32), sd((dm.ha + 8, d), F32), sd((dm.pad, d), F32), sd((dm.pad, d), F32),
            sd((4, 4, d, ck), F32), sd((2, 4, h, ck), F32),
        ),
        in_specs=[hbm, hbm, hbm, hbm, vm, vm, vm],
        out_specs=(hbm, vm, hbm, hbm, hbm, hbm, hbm, hbm, hbm, hbm),
        scratch_shapes=[
            VMEM((tok, d), BF16), VMEM((d, dm.wide), BF16), VMEM((dm.wide, tok), BF16), VMEM((2, 64, tok), F32),
            VMEM((2, 2, dm.ha + 8, d), F32), VMEM((dm.ha + 8, d), F32), VMEM((64, d), F32), VMEM((2, 2, h, ck), F32),
            VMEM((2, 2, h, ck), F32), VMEM((2, 2, h, ck), F32), VMEM((2, 4, h, ck), F32),
            VMEM((2, h // 2, ck), F32), VMEM((2, h // 2, ck), F32), VMEM((2, h, ck), F32), VMEM((2, h, ck), F32),
            VMEM((2, 2, h, ck), F32),
            DMA((14,)), DMA((14,)), DMA((2, 12)), DMA((2, 12)), DMA((2,)), DMA((2,)), DMA((2,)), DMA((2,)),
            DMA((4,)), DMA((2, 2)),
        ],
        compiler_params=pltpu.CompilerParams(
            collective_id=1, has_side_effects=True, vmem_limit_bytes=67043328
        ),
    )(zh, zeh, hh, et, lse, pos, w)
    dh_t, tgt, _, q_h, _, _, xl, xr, _, _ = out
    return dh_t, tgt, q_h, xl, xr


def _allsum_kernel(v_ref, o_ref, mid, got1, got2, send1, recv1, send2, recv2):
    z, y, x, c = _coords()
    near = [_dev(_mod4(z + a), _mod4(y + b), x, c) for a in range(4) for b in range(4) if a or b]
    far = [_dev(z, y, _mod4(x + a), lax.rem(c + b, 2)) for a in range(4) for b in range(2) if a or b]
    _barrier(near + far)
    cps = [_remote(v_ref, got1.at[k], send1, recv1, k, dev) for k, dev in enumerate(near)]
    for cp in cps:
        cp.start()
    for cp in cps:
        cp.wait_recv()
    tot = v_ref[...]
    for k in range(15):
        tot = tot + got1[k]
    mid[...] = tot
    cps2 = [_remote(mid, got2.at[k], send2, recv2, k, dev) for k, dev in enumerate(far)]
    for cp in cps2:
        cp.start()
    for cp in cps2:
        cp.wait_recv()
    tot = mid[...]
    for k in range(7):
        tot = tot + got2[k]
    o_ref[...] = tot
    for cp in cps + cps2:
        cp.wait_send()


def _allsum(v):
    vm = pl.BlockSpec(memory_space=VMEM)
    return pl.pallas_call(
        _allsum_kernel,
        name="small_sum",
        out_shape=jax.ShapeDtypeStruct(v.shape, F32),
        in_specs=[vm],
        out_specs=vm,
        scratch_shapes=[
            VMEM(v.shape, F32), VMEM((15, *v.shape), F32), VMEM((7, *v.shape), F32),
            DMA((15,)), DMA((15,)), DMA((7,)), DMA((7,)),
        ],
        compiler_params=pltpu.CompilerParams(collective_id=3, has_side_effects=True),
    )(v)


def solution(mesh):
    group = mesh.shape[AXIS]

    def local_step(residual, labels, loss_mask, norm_gain, table_shard):
        tokens, dim = residual.shape
        rows = table_shard.shape[0]
        dm = Dims(tokens, dim, rows, group)
        chunk = dm.chunk
        me = lax.axis_index(AXIS)
        x4 = residual.reshape(16, 8, chunk, dim)
        lab = labels.reshape(16, 8, 1, chunk)
        msk = loss_mask.reshape(16, 8, 1, chunk)
        _, zh, zeh, hh, et, lse, pos, w = _forward(dm, x4, table_shard, norm_gain[None, :], lab, msk)
        dh_t, tgt, q_h, xl, xr = _backward(dm, zh, zeh, hh, et, lse, pos, w)

        own = lax.dynamic_index_in_dim(q_h, (me // 2) % 4, 0, keepdims=False)
        d_embed = (own + xl + xr)[:rows] / LOGIT_SCALE
        dh = dh_t.T / LOGIT_SCALE
        x_loc = lax.dynamic_slice_in_dim(residual, me * chunk, chunk, axis=0).astype(F32)
        inv_loc = lax.rsqrt(jnp.mean(x_loc * x_loc, axis=-1, keepdims=True) + NORM_EPS)
        x_hat = x_loc * inv_loc
        dg_part = jnp.sum(dh * x_hat, axis=0)
        loss_part = jnp.sum(w * (jnp.where(me // 8 == 0, lse, 0.0) - tgt))
        small = jnp.concatenate([dg_part, jnp.full((1024,), loss_part)]).reshape(-1, 128)
        small = _allsum(small).reshape(-1)
        u = dh * norm_gain
        d_res = inv_loc * (u - x_hat * jnp.mean(u * x_hat, axis=-1, keepdims=True))
        return small[dim], d_res, d_embed, small[:dim]

    return jax.shard_map(
        local_step,
        mesh=mesh,
        in_specs=(P(), P(), P(), P(), P(AXIS, None)),
        out_specs=(P(), P(AXIS, None), P(AXIS, None), P()),
        check_vma=False,
    )
```

```python
import functools
import itertools

import jax
import jax.numpy as jnp
from jax import lax
from jax.experimental import pallas as pl
from jax.experimental.pallas import tpu as pltpu
from jax.sharding import PartitionSpec as P

VOCAB_REAL = 49155
LOGIT_SCALE = 6.0
NORM_EPS = 1e-6

AXIS = "vp"
MESH = pl.DeviceIdType.MESH
F32 = jnp.float32
BF16 = jnp.bfloat16
HBM = pltpu.HBM
VMEM = pltpu.VMEM
DMA = pltpu.SemaphoreType.DMA


def _coords():
    me = lax.axis_index(AXIS)
    return me // 32, (me // 8) % 4, (me // 2) % 4, me % 2


def _dev(z, y, x, c):
    return ((z * 4 + y) * 4 + x) * 2 + c


def _mod4(v):
    return lax.rem(v + 8, 4)


def _barrier(peers):
    sem = pltpu.get_barrier_semaphore()
    for p in peers:
        pl.semaphore_signal(sem, inc=1, device_id=(p,), device_id_type=MESH)
    pl.semaphore_wait(sem, len(peers))


def _remote(src, dst, send, recv, k, dev):
    return pltpu.make_async_remote_copy(
        src_ref=src,
        dst_ref=dst,
        send_sem=send.at[k],
        recv_sem=recv.at[k],
        device_id=(dev,),
        device_id_type=MESH,
    )


class Dims:
    def __init__(self, tokens, dim, rows, group):
        self.dim, self.rows = dim, rows
        unit = 128 if rows >= 128 else 64
        self.rm = rows // unit * unit
        self.ha = self.rm // 2
        self.hs = self.ha // 2
        self.pad = self.rm + 8
        self.chunk = tokens // group
        self.tok = 16 * self.chunk
        self.nt = 4 * self.chunk
        self.main = 8 * self.rm
        self.wide = self.main + 128
        self.h = dim // 2


def _loop_rows(rows, step, fn):
    @pl.loop(0, rows // step)
    def _(i):
        fn(pl.ds(pl.multiple_of(i * step, step), step))


def _add_rows(dst, srcs, step):
    def add(r):
        acc = dst[r, :]
        for s in srcs:
            acc = acc + s[r, :]
        dst[r, :] = acc

    _loop_rows(dst.shape[0], step, add)


SLOTS = 8
NEAR_KEYS = ("near_r", "near_l", "sum_r", "sum_l")
scope = jax.named_scope


def _kernel(
    dm, x4, e_ref, g_ref, lab, msk,
    dx_out, de_out, dg_out, loss_out, q_o, xl, xr, eg, zh, zeh, s_h, q_h, xa, xb, dhp, yr,
    hv, etv, dz, od, sst, dee, oext, ext, dht, ya, yb, yl, za, zb, zl, zr, tst, xo,
    st, w_row, pos_row, lse_row, tgt_row, got, sm, got1, got2,
    send, recv,
    esem, xsem, zsem, tsem, hsem, dsem, osem, lsem,
):
    z, y, x, c = _coords()
    xc, zy = x * 2 + c, z * 4 + y
    rows, rm, ha, hs, dim, h = dm.rows, dm.rm, dm.ha, dm.hs, dm.dim, dm.h
    chunk, tok, nt, hc = dm.chunk, dm.tok, dm.nt, dm.h // 2
    x_far, x_p, x_m = _mod4(x + 2), _mod4(x + 1), _mod4(x - 1)
    xp, xm = _dev(z, y, x_p, c), _dev(z, y, x_m, c)
    yp, ym = _dev(z, _mod4(y + 1), x, c), _dev(z, _mod4(y - 1), x, c)
    zp, zm = _dev(_mod4(z + 1), y, x, c), _dev(_mod4(z - 1), y, x, c)
    sib = _dev(z, y, x, 1 - c)
    near = [_dev(_mod4(z + a), _mod4(y + b), x, c) for a in range(4) for b in range(4) if a or b]
    line = [_dev(z, y, _mod4(x + a), lax.rem(c + b, 2)) for a in range(4) for b in range(2) if a or b]
    bar = pltpu.get_barrier_semaphore()
    for p in (*near, *line):
        pl.semaphore_signal(bar, inc=1, device_id=(p,), device_id_type=MESH)
    sent = []
    ids = itertools.count()

    def remote(src, dst, dev):
        cp = _remote(src, dst, send, recv, next(ids), dev)
        cp.start()
        sent.append(cp)
        return cp

    def local(src, dst, sem):
        cp = pltpu.make_async_copy(src, dst, sem)
        cp.start()
        return cp

    x_at, ext_at = 2 * rm, 4 * rm

    def xload(k):
        s = lax.rem(k, 4)
        to = dz.at[pl.ds(pl.multiple_of(x_at + s * chunk, chunk), chunk)]
        return pltpu.make_async_copy(x4.at[k, xc], to, xsem.at[s])

    with scope("prep"):
        for k in range(3):
            xload(k).start()
        own = xc
        for j in range(2):
            def widen(r, j=j):
                od[0, j, r, :] = e_ref[pl.ds(j * ha + r.start, r.size), :].astype(F32)

            _loop_rows(ha, 16, widen)
        oext[...] = jnp.zeros_like(oext)
        oext[0 : rows - rm, :] = e_ref[rm:rows, :].astype(F32)
        cps = [local(od.at[0, j, pl.ds(0, ha)], eg.at[own, pl.ds(j * ha, ha)], esem.at[0, j]) for j in range(2)]
        cps.append(local(oext, eg.at[own, pl.ds(rm, 8)], esem.at[1, 0]))
        for cp in cps:
            cp.wait()
        pl.semaphore_wait(bar, 22)

    half_a, half_b = pl.ds(0, ha), pl.ds(ha, ha + 8)

    def piece(s, r, dev):
        return remote(eg.at[s, r], eg.at[s, r], dev)

    def slot(xx):
        return xx * 2 + c

    r_a, l_b = piece(own, half_a, xp), piece(own, half_b, xm)
    s_o = piece(own, pl.ds(0, dm.pad), sib)
    r_b, l_a = piece(own, half_b, xp), piece(own, half_a, xm)

    gain = g_ref[...]

    with scope("norm"):
        @pl.loop(0, 16)
        def _(k):
            @pl.when(k < 13)
            def _():
                xload(k + 3).start()

            xload(k).wait()

            def norm(r):
                v = dz[pl.ds(pl.multiple_of(x_at + lax.rem(k, 4) * chunk + r.start, r.size), r.size), :].astype(F32)
                inv = lax.rsqrt(jnp.mean(v * v, axis=-1, keepdims=True) + NORM_EPS)
                hv[pl.ds(pl.multiple_of(k * chunk + r.start, r.size), r.size), :] = (v * inv * gain).astype(BF16)

            _loop_rows(chunk, 16, norm)

    def product(lhs, lanes):
        v = lax.dot_general(lhs, hv[lanes, :], (((1,), (1,)), ((), ())), preferred_element_type=F32)
        return v * (1.0 / LOGIT_SCALE)

    def add_stats(v, lanes):
        m_old, s_old = st[0:1, lanes], st[1:2, lanes]
        m = jnp.maximum(m_old, jnp.max(v, axis=0, keepdims=True))
        s = jnp.sum(jnp.exp(v - m), axis=0, keepdims=True)
        st[0:1, lanes] = m
        st[1:2, lanes] = s_old * jnp.exp(m_old - m) + s

    st[0:1, :] = jnp.full((1, tok), -1e30, F32)
    st[1:2, :] = jnp.zeros((1, tok), F32)
    segs = [(half, j) for half in range(2) for j in range(2)]

    def load(s, xx):
        return [
            pltpu.make_async_copy(
                eg.at[xx[half] * 2 + j, pl.ds(pl.multiple_of(half * ha + s * hs, hs), hs)],
                od.at[s, half, pl.ds(j * hs, hs)],
                esem.at[s, half * 2 + j],
            )
            for half, j in segs
        ]

    def block(s, xx):
        for cp in load(s, xx):
            cp.wait()
        for half, j in segs:
            def narrow(r, half=half, j=j):
                at = pl.multiple_of((half * 2 + j) * ha + s * hs + r.start, r.size)
                dz[pl.ds(at, r.size), :] = od[s, half, pl.ds(j * hs + r.start, r.size), :].astype(BF16)

            _loop_rows(hs, 16, narrow)
        left = [VOCAB_REAL - ((zy * 8 + xx[half] * 2 + j) * rows + half * ha + s * hs) for half, j in segs]

        w = nt // chunk
        deep = SLOTS // w

        def out(t):
            u = lax.rem(t, deep) * w
            return [
                pltpu.make_async_copy(
                    tst.at[u + i, pl.ds(n * hs, hs)],
                    zh.at[
                        t * w + i, pl.ds(pl.multiple_of((xx[half] * 2 + half) * rm + j * ha + s * hs, hs), hs)
                    ],
                    zsem.at[u + i, n],
                )
                for i in range(w)
                for n, (half, j) in enumerate(segs)
            ]

        @pl.loop(0, tok // nt)
        def _(t):
            @pl.when(t >= deep)
            def _():
                for cp in out(t - deep):
                    cp.wait()

            lanes = pl.ds(pl.multiple_of(t * nt, nt), nt)
            lhs = jnp.concatenate(
                [dz[pl.ds(pl.multiple_of((half * 2 + j) * ha + s * hs, hs), hs), :] for half, j in segs], axis=0
            )
            v = product(lhs, lanes)
            r = lax.broadcasted_iota(jnp.int32, (hs, nt), 0)
            v = jnp.concatenate(
                [jnp.where(r < left[n], v[n * hs : (n + 1) * hs], -jnp.inf) for n in range(4)], axis=0
            )
            u = lax.rem(t, deep) * w
            for i in range(w):
                tst[u + i, 0 : 4 * hs, :] = v[:, i * chunk : (i + 1) * chunk]
            for cp in out(t):
                cp.start()
            add_stats(v, lanes)

        for t in range(deep):
            for cp in out(t + tok // nt - deep):
                cp.wait()

    def both(xx):
        for s in (1, 0):
            for cp in load(s, xx):
                cp.start()

        @pl.loop(0, 2)
        def _(i):
            block(1 - i, xx)

    def turn(xx):
        for half in range(2):
            base = pl.multiple_of((xx[half] * 2 + half) * rm, rm)

            @pl.loop(0, dim // 128)
            def _(d, half=half, base=base):
                at = pl.ds(pl.multiple_of(d * 128, 128), 128)
                etv[at, pl.ds(base, rm)] = dz[half * rm : (half + 1) * rm, at].T

    with scope("own"):
        s_o.wait_recv()
        both((x, x))
        turn((x, x))

    with scope("labels"):
        total = jnp.sum(msk[...])
        for k in range(16):
            at = pl.ds(k * chunk, chunk)
            w_row[:, at] = msk[k, xc] / total
            q = lab[k, xc] - zy * (8 * rows)
            s = jnp.zeros_like(q)
            for i in range(1, 8):
                s = s + jnp.where(q >= i * rows, 1, 0)
            r = q - s * rows
            up = jnp.where(r >= ha, 1, 0)
            at_main = ((s // 2 * 2 + up) * 2 + s % 2) * ha + r - up * ha
            at_ext = dm.main + s * 8 + r - rm
            place = jnp.where(r < rm, at_main, at_ext)
            pos_row[:, at] = jnp.where((q >= 0) & (q < 8 * rows), place, -1).astype(F32)

    with scope("wait_1"):
        r_a.wait_recv()
        f1 = pl.ds(hs, hs)
        f0 = pl.ds(0, hs)
        r_f1 = piece(slot(x_m), f1, xp)
        r_f0 = piece(slot(x_m), f0, xp)
        d = [piece(slot(x_m), half_a, sib)]
        l_b.wait_recv()
        g1, g0 = pl.ds(ha + hs, hs + 8), pl.ds(ha, hs)
        l_f1 = piece(slot(x_p), g1, xm)
        l_f0 = piece(slot(x_p), g0, xm)
        d.append(piece(slot(x_p), half_b, sib))
        for cp in d:
            cp.wait_recv()

    with scope("near_1"):
        both((x_m, x_p))
        turn((x_m, x_p))

    with scope("wait_2"):
        r_b.wait_recv()
        d = [piece(slot(x_m), half_b, sib)]
        l_a.wait_recv()
        d.append(piece(slot(x_p), half_a, sib))
        for cp in d:
            cp.wait_recv()

    with scope("near_2"):
        both((x_p, x_m))
        turn((x_p, x_m))

    with scope("wait_3"):
        r_f1.wait_recv()
        d = [piece(slot(x_far), f1, sib)]
        l_f1.wait_recv()
        d.append(piece(slot(x_far), g1, sib))
        for cp in d:
            cp.wait_recv()

    far = (x_far, x_far)
    with scope("far_1"):
        for cp in load(1, far):
            cp.start()
        ext_loads = [local(eg.at[s, pl.ds(rm, 8)], ext.at[pl.ds(s * 8, 8)], lsem.at[s]) for s in range(8)]
        block(1, far)
        for cp in ext_loads:
            cp.wait()
        dz[ext_at : ext_at + 64, :] = ext[...].astype(BF16)
        dz[ext_at + 64 : ext_at + 128, :] = jnp.zeros((64, dim), BF16)

        @pl.loop(0, tok // nt)
        def _(t):
            lanes = pl.ds(pl.multiple_of(t * nt, nt), nt)
            v = product(dz[ext_at : ext_at + 64, :], lanes)
            r = lax.broadcasted_iota(jnp.int32, v.shape, 0)
            ok = ((r & 7) < rows - rm) & ((zy * 8 + (r >> 3)) * rows + rm + (r & 7) < VOCAB_REAL)
            v = jnp.where(ok, v, -jnp.inf)
            zeh[:, lanes] = v
            add_stats(v, lanes)

    with scope("wait_4"):
        r_f0.wait_recv()
        d = [piece(slot(x_far), f0, sib)]
        l_f0.wait_recv()
        d.append(piece(slot(x_far), g0, sib))
        for cp in d:
            cp.wait_recv()

    with scope("far_0"):
        for cp in load(0, far):
            cp.start()
        block(0, far)

    with scope("turn_far"):
        scps = [remote(st, got.at[k], p) for k, p in enumerate(near)]
        turn(far)

        @pl.loop(0, dim // 128)
        def _(i):
            at = pl.ds(pl.multiple_of(i * 128, 128), 128)
            etv[at, dm.main : dm.wide] = dz[ext_at : ext_at + 128, at].T

    wide = 2 * rm

    def zload(first, i):
        at = pl.multiple_of(lax.rem(first + i // 16, 4) * wide, wide)
        s = lax.rem(i, SLOTS)
        return pltpu.make_async_copy(zh.at[lax.rem(i, 16), pl.ds(at, wide)], tst.at[s, pl.ds(0, wide)], tsem.at[s])

    def zahead(first):
        for i in range(SLOTS - 1):
            zload(first, i).start()

    with scope("stats"):
        zahead(x_far)
        xo_load = local(x4.at[zy, xc], xo, xsem.at[0])
        for cp in scps:
            cp.wait_recv()
        m = st[0:1, :]
        top = m
        for k in range(len(near)):
            top = jnp.maximum(top, got[k, 0:1, :])
        s = st[1:2, :] * jnp.exp(m - top)
        for k in range(len(near)):
            s = s + got[k, 1:2, :] * jnp.exp(got[k, 0:1, :] - top)
        lse_row[:, :] = top + jnp.log(s)
        tgt_row[:, :] = jnp.zeros((1, tok), F32)

    def dz_part(v, place, at, lanes):
        r = lax.broadcasted_iota(jnp.int32, v.shape, 0).astype(F32)
        hit = r == pos_row[:, lanes] - place.astype(F32)
        p = jnp.exp(v - lse_row[:, lanes])
        dz[at, lanes] = (jnp.where(hit, p - 1.0, p) * w_row[:, lanes]).astype(BF16)
        tgt_row[:, lanes] += jnp.sum(jnp.where(hit, v, 0.0), axis=0, keepdims=True)

    step = min(128, wide)

    def dz_rows(first, start, stop, n):
        @pl.loop(start, stop)
        def _(i):
            @pl.when(i + SLOTS - 1 < n)
            def _():
                zload(first, i + SLOTS - 1).start()

            zload(first, i).wait()
            base = lax.rem(first + i // 16, 4) * wide
            lanes = pl.ds(pl.multiple_of(lax.rem(i, 16) * chunk, chunk), chunk)

            @pl.loop(0, wide // step)
            def _(j):
                at = pl.multiple_of(base + j * step, step)
                r = pl.ds(pl.multiple_of(j * step, step), step)
                dz_part(tst[lax.rem(i, SLOTS), r, :], at, pl.ds(at, step), lanes)

    with scope("dz_far"):
        dz_rows(x_far, 0, 16, 16)
        for l in range(0, tok, nt):
            lanes = pl.ds(l, nt)
            dz_part(zeh[:, lanes], jnp.int32(dm.main), pl.ds(dm.main, 64), lanes)
        dz[dm.main + 64 : dm.wide, :] = jnp.zeros((64, tok), BF16)

    nd = min(1024, dim)

    @pl.loop(0, dim // nd)
    def _(i):
        lanes = pl.ds(pl.multiple_of(i * nd, nd), nd)
        dee[:, lanes] = jnp.dot(dz[dm.main : dm.main + 64, :], hv[:, lanes], preferred_element_type=F32)

    def de_block(xx, half, s):
        at = pl.ds(pl.multiple_of((xx * 2 + half) * rm, rm), rm)

        @pl.loop(0, dim // nd)
        def _(i):
            lanes = pl.ds(pl.multiple_of(i * nd, nd), nd)
            v = jnp.dot(dz[at, :], hv[:, lanes], preferred_element_type=F32)
            od[s, 0, 0:ha, lanes] = v[0:ha]
            od[s, 1, 0:ha, lanes] = v[ha:rm]

        n = ha + 8 * half
        if half:
            for j in range(2):
                od[s, j, ha : ha + 8, :] = dee[pl.ds(pl.multiple_of((xx * 2 + j) * 8, 8), 8), :]
        cp = _remote(od.at[s, 1 - c, pl.ds(0, n)], s_h.at[xx, pl.ds(half * ha, n)], send, recv, next(ids), sib)
        cp.start()
        return xx, half, s, n, cp

    def sum_load(blk):
        xx, half, s, n, cp = blk
        cp.wait_recv()
        return local(s_h.at[xx, pl.ds(half * ha, n)], sst.at[pl.ds(0, n)], dsem.at[s])

    def sum_add(blk, load_cp, to=None):
        xx, half, s, n, cp = blk
        there = pl.ds(half * ha, n)
        load_cp.wait()

        def add(r):
            od[s, c, r, :] = od[s, c, r, :] + sst[r, :]

        _loop_rows(n, 8, add)
        cp.wait_send()
        return local(od.at[s, c, pl.ds(0, n)], q_h.at[xx, there] if to is None else to.at[there], dsem.at[s])

    def ring_sum(xx, rows_, n, src, s, dst, dev):
        lds = [
            local(q_h.at[xx, rows_], od.at[s, 0, pl.ds(0, n)], lsem.at[0]),
            local(src, sst.at[pl.ds(0, n)], lsem.at[1]),
        ]
        for cp in lds:
            cp.wait()

        def add(r):
            od[s, 0, r, :] = od[s, 0, r, :] + sst[r, :]

        _loop_rows(n, 8, add)
        local(od.at[s, 0, pl.ds(0, n)], q_h.at[xx, rows_], lsem.at[0]).wait()
        return remote(q_h.at[xx, rows_], dst, dev)

    mt = min(1024, h)

    def dh_group(q, n, where):
        def outs(i, s):
            zz, pr = where(i)
            return [
                pltpu.make_async_copy(dht.at[s, j], dhp.at[zz, pr * 2 + j, pl.ds(q * h, h)], hsem.at[s * 2 + j])
                for j in range(2)
            ]

        @pl.loop(0, n)
        def _(i):
            s = lax.rem(i, 2)

            @pl.when(i >= 2)
            def _():
                for cp in outs(i, s):
                    cp.wait()

            zz, pr = where(i)
            lanes = pl.ds(pl.multiple_of((zz * 4 + pr * 2) * chunk, 2 * chunk), 2 * chunk)

            @pl.loop(0, h // mt)
            def _(m):
                v = jnp.dot(
                    etv[pl.ds(pl.multiple_of(q * h + m * mt, mt), mt), :], dz[:, lanes], preferred_element_type=F32
                )
                at = pl.ds(pl.multiple_of(m * mt, mt), mt)
                dht[s, 0, at, :] = v[:, 0:chunk]
                dht[s, 1, at, :] = v[:, chunk : 2 * chunk]

            for cp in outs(i, s):
                cp.start()

        for s in range(2):
            for cp in outs(s, s):
                cp.wait()

    def part(q, p, lo, n):
        r = pl.ds(q * h, h)
        if q == 0:
            return dhp.at[pl.ds(lo, n), p, r]
        return dhp.at[p, pl.ds(lo, n), r]

    def one(q, p, i):
        r = pl.ds(q * h, h)
        return dhp.at[i, p, r] if q == 0 else dhp.at[p, i, r]

    ring1, ring2 = ((yp, ym), (zp, zm)), ((zp, zm), (yp, ym))
    pos1, pos2 = (y, z), (z, y)
    first, second = ({}, {}), ({}, {})

    def send_far(q):
        p, (rt, lt) = pos1[q], ring1[q]
        first[q]["far_r"] = remote(part(q, _mod4(p + 2), 0, 2), ya.at[q], rt)
        first[q]["far_l"] = remote(part(q, _mod4(p + 2), 2, 2), yb.at[q], lt)

    def send_near(q):
        p, (rt, lt) = pos1[q], ring1[q]
        first[q]["near_r"] = remote(part(q, _mod4(p + 1), 2, 2), yl.at[q, pl.ds(2, 2)], rt)
        first[q]["near_l"] = remote(part(q, _mod4(p - 1), 0, 2), yr.at[q, pl.ds(0, 2)], lt)

    def fetch(i, src):
        return local(src, tst.at[i, pl.ds(0, h)], tsem.at[i])

    def pass_on(q):
        p, (rt, lt) = pos1[q], ring1[q]
        lds = [fetch(i, one(q, _mod4(p + 1), i)) for i in range(2)]
        lds += [fetch(2 + i, one(q, _mod4(p - 1), 2 + i)) for i in range(2)]
        first[q]["far_r"].wait_recv()
        for i in range(2):
            lds[i].wait()
            _add_rows(ya.at[q, i], [tst.at[i, pl.ds(0, h)]], min(64, h))
        first[q]["sum_r"] = remote(ya.at[q], yl.at[q, pl.ds(0, 2)], rt)
        first[q]["far_l"].wait_recv()
        for i in range(2):
            lds[2 + i].wait()
            _add_rows(yb.at[q, i], [tst.at[2 + i, pl.ds(0, h)]], min(64, h))
        first[q]["sum_l"] = remote(yb.at[q], yr.at[q, pl.ds(2, 2)], lt)

    lo, hi = pl.ds(0, hc), pl.ds(hc, hc)

    def second_phase(q):
        r, (rt, lt) = pos2[q], ring2[q]
        r2, r1, rm1 = _mod4(r + 2), _mod4(r + 1), _mod4(r - 1)
        order = (r2, r1, rm1, r)
        lds = [fetch(i, one(q, pos1[q], k)) for i, k in enumerate(order)]
        for k in NEAR_KEYS:
            first[q][k].wait_recv()
        lds2 = [fetch(4 + i, yr.at[q, k]) for i, k in enumerate(order)]
        for i, k in enumerate(order):
            lds[i].wait()
            lds2[i].wait()
            _add_rows(yl.at[q, k], [tst.at[i, pl.ds(0, h)], tst.at[4 + i, pl.ds(0, h)]], min(64, h))
            if i == 0:
                second[q]["far_r"] = remote(yl.at[q, r2, lo], za.at[q], rt)
                second[q]["far_l"] = remote(yl.at[q, r2, hi], zb.at[q], lt)
            if i == 1:
                second[q]["near_r"] = remote(yl.at[q, r1, hi], zl.at[q, hi], rt)
            if i == 2:
                second[q]["near_l"] = remote(yl.at[q, rm1, lo], zr.at[q, lo], lt)

    def second_pass(q):
        r, (rt, lt) = pos2[q], ring2[q]
        r1, rm1 = _mod4(r + 1), _mod4(r - 1)
        second[q]["far_r"].wait_recv()
        _add_rows(yl.at[q, r1, lo], [za.at[q]], min(64, hc))
        second[q]["sum_r"] = remote(yl.at[q, r1, lo], zl.at[q, lo], rt)
        second[q]["far_l"].wait_recv()
        _add_rows(yl.at[q, rm1, hi], [zb.at[q]], min(64, hc))
        second[q]["sum_l"] = remote(yl.at[q, rm1, hi], zr.at[q, hi], lt)

    def last(q):
        r = pos2[q]
        for k in NEAR_KEYS:
            second[q][k].wait_recv()
        n = min(128, h)

        @pl.loop(0, h // n)
        def _(i):
            at = pl.ds(pl.multiple_of(i * n, n), n)
            v = yl[q, r, at, :] + zl[q, at, :] + zr[q, at, :]
            od[0, 0, 0:chunk, pl.ds(pl.multiple_of(q * h + i * n, n), n)] = (v * (1.0 / LOGIT_SCALE)).T

    with scope("de_far"):
        b0 = de_block(x_far, 0, 0)
        b1 = de_block(x_far, 1, 1)
        rest = x_far + 1
        zahead(rest)
        c0 = sum_load(b0)
    with scope("dz_1"):
        dz_rows(rest, 0, 16, 48)
    with scope("sum_1"):
        c0 = sum_add(b0, c0)
        c1 = sum_load(b1)
    with scope("dz_2"):
        dz_rows(rest, 16, 32, 48)
    with scope("sum_2"):
        c0.wait()
        e0 = remote(q_h.at[x_far, half_a], xa, xp)
        c1 = sum_add(b1, c1)
    with scope("dz_3"):
        dz_rows(rest, 32, 48, 48)
        c1.wait()
        e1 = remote(q_h.at[x_far, half_b], xb, xm)
    pf = _mod4(y + 2) // 2
    with scope("dh_1"):
        dh_group(1, 2, lambda i: (_mod4(z + 2), i))
        send_far(1)
    with scope("dh_2"):
        dh_group(0, 4, lambda i: (i, pf))
        send_far(0)
    with scope("dh_3"):
        dh_group(1, 4, lambda i: (_mod4(z + 1 + 2 * lax.rem(i, 2)), (i < 1) * 1 + (i > 2) * 1))
        send_near(1)
    with scope("de_2"):
        b2 = de_block(x_p, 1, 0)
        b3 = de_block(x_m, 0, 1)
        c2 = sum_load(b2)
    with scope("dh_4"):
        dh_group(0, 2, lambda i: (i, 1 - pf))
        c2 = sum_add(b2, c2)
        c3 = sum_load(b3)
        dh_group(0, 2, lambda i: (i + 2, 1 - pf))
        send_near(0)
    with scope("sum_3"):
        c2.wait()
        e2 = remote(q_h.at[x_p, half_b], xl.at[half_b], xp)
        c3 = sum_add(b3, c3)
    with scope("pass_1"):
        pass_on(1)
        c3.wait()
        e3 = remote(q_h.at[x_m, half_a], xr.at[half_a], xm)
    with scope("dh_5"):
        dh_group(1, 2, lambda i: (z, i))
    with scope("pass_0"):
        pass_on(0)
    with scope("de_4"):
        b4 = de_block(x_p, 0, 0)
        b5 = de_block(x_m, 1, 1)
        c4 = sum_load(b4)
        c4 = sum_add(b4, c4)
        c5 = sum_load(b5)
        c4.wait()
        c5 = sum_add(b5, c5)
        e0.wait_recv()
        e4 = ring_sum(x_p, half_a, ha, xa, 0, xl.at[half_a], xp)
        c5.wait()
        e1.wait_recv()
        e5 = ring_sum(x_m, half_b, ha + 8, xb, 1, xr.at[half_b], xm)
    with scope("de_6"):
        b6 = de_block(x, 0, 0)
        b7 = de_block(x, 1, 1)
        c6 = sum_load(b6)
    with scope("second_1"):
        second_phase(1)
    with scope("sum_6"):
        c6 = sum_add(b6, c6, q_o)
        c7 = sum_load(b7)
    with scope("second_0"):
        second_phase(0)
        c7 = sum_add(b7, c7, q_o)
        c6.wait()
        c7.wait()
    with scope("spass_1"):
        second_pass(1)
    with scope("spass_0"):
        second_pass(0)
    with scope("last_1"):
        last(1)
    with scope("last_0"):
        last(0)

    with scope("finish"):
        xo_load.wait()
        sm[...] = jnp.zeros_like(sm)

        def finish(r):
            v = xo[r, :].astype(F32)
            inv = lax.rsqrt(jnp.mean(v * v, axis=-1, keepdims=True) + NORM_EPS)
            x_hat = v * inv
            dh = od[0, 0, r, :]
            sm[:, 0:dim] += jnp.sum(dh * x_hat, axis=0, keepdims=True)
            u = dh * gain
            od[0, 1, r, :] = inv * (u - x_hat * jnp.mean(u * x_hat, axis=-1, keepdims=True))

        _loop_rows(chunk, 16, finish)
        lse = jnp.where(zy == 0, lse_row[:, :], 0.0)
        loss = jnp.sum(w_row[:, :] * (lse - tgt_row[:, :]))
        sm[:, dim : dim + 128] = jnp.full((1, 128), loss)

    with scope("small_1"):
        cps = [remote(sm, got1.at[k], p) for k, p in enumerate(near)]
        dx_copy = local(od.at[0, 1, pl.ds(0, chunk)], dx_out, osem.at[0])
        for cp in cps:
            cp.wait_recv()
    with scope("small_2"):
        tot = sm[...]
        for k in range(len(near)):
            tot = tot + got1[k]
        got2[len(line)] = tot
        cps = [remote(got2.at[len(line)], got2.at[k], p) for k, p in enumerate(line)]
    with scope("ring_end"):
        for cp in (e2, e3, e4, e5):
            cp.wait_recv()
    with scope("de_out"):
        dx_copy.wait()
        spans = [(pl.ds(i * ha, ha + 8 * i), pl.ds(0, ha + 8 * i)) for i in range(2)]
        own_rows = local(q_o.at[spans[0][0]], sst.at[spans[0][1]], dsem.at[0])
        lds = [
            [local(src.at[r], od.at[k, i, n], lsem.at[i * 2 + k]) for k, src in enumerate((xl, xr))]
            for i, (r, n) in enumerate(spans)
        ]
        outs = []
        for i, (r, n) in enumerate(spans):
            own_rows.wait()
            for cp in lds[i]:
                cp.wait()

            def total_up(r_, i=i):
                v = sst[r_, :] + od[0, i, r_, :] + od[1, i, r_, :]
                od[0, i, r_, :] = v * (1.0 / LOGIT_SCALE)

            _loop_rows(n.size, 8, total_up)
            outs.append(local(od.at[0, i, n], de_out.at[r], osem.at[i]))
            if i == 0:
                own_rows = local(q_o.at[spans[1][0]], sst.at[spans[1][1]], dsem.at[0])
    with scope("small_3"):
        for cp in cps:
            cp.wait_recv()
        for k in range(len(line)):
            tot = tot + got2[k]
        dg_out[...] = tot[:, 0:dim]
        loss_out[...] = tot[:, dim : dim + 128]
    for cp in outs:
        cp.wait()
    for cp in sent:
        cp.wait_send()


def _run(dm, x4, table, gain, labels, mask):
    hbm, vm = pl.BlockSpec(memory_space=HBM), pl.BlockSpec(memory_space=VMEM)
    sd = jax.ShapeDtypeStruct
    d, tok, h, ck, pad, ha = dm.dim, dm.tok, dm.h, dm.chunk, dm.pad, dm.ha
    line, quad, pair = VMEM((1, tok), F32), VMEM((2, 2, h, ck), F32), VMEM((2, h, ck), F32)
    part, shard = VMEM((2, h // 2, ck), F32), sd((pad, d), F32)
    out = pl.pallas_call(
        functools.partial(_kernel, dm),
        name="head",
        out_shape=(
            sd((ck, d), F32), shard, sd((1, d), F32), sd((1, 128), F32),
            shard, shard, shard,
            sd((8, pad, d), F32), sd((16, dm.main, ck), F32), sd((64, tok), F32),
            sd((4, pad, d), F32), sd((4, pad, d), F32), sd((ha, d), F32), sd((ha + 8, d), F32),
            sd((4, 4, d, ck), F32), sd((2, 4, h, ck), F32),
        ),
        in_specs=[hbm, vm, vm, vm, vm],
        out_specs=(hbm, hbm, vm, vm, hbm, hbm, hbm, hbm, hbm, vm, hbm, hbm, hbm, hbm, hbm, hbm),
        scratch_shapes=[
            VMEM((tok, d), BF16), VMEM((d, dm.wide), BF16), VMEM((dm.wide, tok), BF16),
            VMEM((2, 2, ha + 8, d), F32), VMEM((ha + 8, d), F32), VMEM((64, d), F32), VMEM((8, d), F32), VMEM((64, d), F32),
            quad, quad, quad, VMEM((2, 4, h, ck), F32),
            part, part, pair, pair,
            VMEM((SLOTS, max(h, 2 * dm.rm), ck), F32), VMEM((ck, d), BF16),
            VMEM((2, tok), F32), line, line, line, line, VMEM((15, 2, tok), F32),
            VMEM((1, d + 128), F32), VMEM((15, 1, d + 128), F32), VMEM((8, 1, d + 128), F32),
            DMA((96,)), DMA((96,)),
            DMA((2, 4)), DMA((4,)), DMA((SLOTS, 4)), DMA((SLOTS,)), DMA((4,)), DMA((2,)), DMA((2,)), DMA((8,)),
        ],
        compiler_params=pltpu.CompilerParams(
            collective_id=0, has_side_effects=True, vmem_limit_bytes=67043328
        ),
    )(x4, table, gain, labels, mask)
    return out[:4]


def solution(mesh):
    group = mesh.shape[AXIS]

    def local_step(residual, labels, loss_mask, norm_gain, table_shard):
        tokens, dim = residual.shape
        rows = table_shard.shape[0]
        dm = Dims(tokens, dim, rows, group)
        x4 = residual.reshape(16, 8, dm.chunk, dim)
        lab = labels.reshape(16, 8, 1, dm.chunk)
        msk = loss_mask.reshape(16, 8, 1, dm.chunk)
        d_res, d_embed, d_gain, loss = _run(dm, x4, table_shard, norm_gain[None, :], lab, msk)
        return loss[0, 0], d_res, d_embed[:rows], d_gain[0]

    return jax.shard_map(
        local_step,
        mesh=mesh,
        in_specs=(P(), P(), P(), P(), P(AXIS, None)),
        out_specs=(P(), P(AXIS, None), P(AXIS, None), P()),
        check_vma=False,
    )
```

```python
import functools
import itertools
import math

import jax
import jax.numpy as jnp
from jax import lax
from jax.experimental import pallas as pl
from jax.experimental.pallas import tpu as pltpu
from jax.sharding import PartitionSpec as P

VOCAB_REAL = 49155
LOGIT_SCALE = 6.0
NORM_EPS = 1e-6

AXIS = "vp"
MESH = pl.DeviceIdType.MESH
F32 = jnp.float32
BF16 = jnp.bfloat16
HBM = pltpu.HBM
VMEM = pltpu.VMEM
DMA = pltpu.SemaphoreType.DMA


def _coords():
    me = lax.axis_index(AXIS)
    return me // 32, (me // 8) % 4, (me // 2) % 4, me % 2


def _dev(z, y, x, c):
    return ((z * 4 + y) * 4 + x) * 2 + c


def _mod4(v):
    return lax.rem(v + 8, 4)


def _barrier(peers):
    sem = pltpu.get_barrier_semaphore()
    for p in peers:
        pl.semaphore_signal(sem, inc=1, device_id=(p,), device_id_type=MESH)
    pl.semaphore_wait(sem, len(peers))


def _remote(src, dst, send, recv, k, dev):
    return pltpu.make_async_remote_copy(
        src_ref=src,
        dst_ref=dst,
        send_sem=send.at[k],
        recv_sem=recv.at[k],
        device_id=(dev,),
        device_id_type=MESH,
    )


class Dims:
    def __init__(self, tokens, dim, rows, group):
        self.dim, self.rows = dim, rows
        unit = 128 if rows >= 128 else 64
        self.rm = rows // unit * unit
        self.ha = self.rm // 2
        self.last = self.ha // 4
        self.pad = self.rm + 8
        self.chunk = tokens // group
        self.tok = 16 * self.chunk
        self.nt = 4 * self.chunk
        self.main = 8 * self.rm
        self.wide = self.main + 128
        self.h = dim // 2


def _loop_rows(rows, step, fn):
    @pl.loop(0, rows // step)
    def _(i):
        fn(pl.ds(pl.multiple_of(i * step, step), step))


def _add_rows(dst, srcs, step):
    def add(r):
        acc = dst[r, :]
        for s in srcs:
            acc = acc + s[r, :]
        dst[r, :] = acc

    _loop_rows(dst.shape[0], step, add)


SLOTS = 12
LOG2E = math.log2(math.e)
NEAR_KEYS = ("near_r", "near_l", "sum_r", "sum_l")
scope = jax.named_scope


def _kernel(
    dm, x4, e_ref, g_ref, lab, msk,
    dx_out, de_out, dg_out, loss_out, q_o, xl, xr, eg, zh, zeh, s_h, q_h, xa, xb, dhp, yr,
    hv, etv, dz, od, sst, dee, oext, ext, ya, yb, yl, za, zb, zl, zr, tst, xo,
    st, w_row, pos_row, lse_row, tgt_row, got, sm, got1, got2,
    send, recv,
    esem, xsem, zsem, tsem, hsem, dsem, osem, lsem,
):
    z, y, x, c = _coords()
    xc, zy = x * 2 + c, z * 4 + y
    rows, rm, ha, last_n, dim, h = dm.rows, dm.rm, dm.ha, dm.last, dm.dim, dm.h
    chunk, tok, nt, hc = dm.chunk, dm.tok, dm.nt, dm.h // 2
    x_far, x_p, x_m = _mod4(x + 2), _mod4(x + 1), _mod4(x - 1)
    xp, xm = _dev(z, y, x_p, c), _dev(z, y, x_m, c)
    yp, ym = _dev(z, _mod4(y + 1), x, c), _dev(z, _mod4(y - 1), x, c)
    zp, zm = _dev(_mod4(z + 1), y, x, c), _dev(_mod4(z - 1), y, x, c)
    sib = _dev(z, y, x, 1 - c)
    near = [_dev(_mod4(z + a), _mod4(y + b), x, c) for a in range(4) for b in range(4) if a or b]
    line = [_dev(z, y, _mod4(x + a), lax.rem(c + b, 2)) for a in range(4) for b in range(2) if a or b]
    bar = pltpu.get_barrier_semaphore()
    for p in (*near, *line):
        pl.semaphore_signal(bar, inc=1, device_id=(p,), device_id_type=MESH)
    sent = []
    ids = itertools.count()

    def remote(src, dst, dev):
        cp = _remote(src, dst, send, recv, next(ids), dev)
        cp.start()
        sent.append(cp)
        return cp

    def local(src, dst, sem):
        cp = pltpu.make_async_copy(src, dst, sem)
        cp.start()
        return cp

    x_at, ext_at = 2 * rm, 4 * rm

    def xload(k):
        s = lax.rem(k, 4)
        to = dz.at[pl.ds(pl.multiple_of(x_at + s * chunk, chunk), chunk)]
        return pltpu.make_async_copy(x4.at[k, xc], to, xsem.at[s])

    with scope("prep"):
        for k in range(3):
            xload(k).start()
        own = xc
        for j in range(2):
            def widen(r, j=j):
                od[0, j, r, :] = e_ref[pl.ds(j * ha + r.start, r.size), :].astype(F32)

            _loop_rows(ha, 16, widen)
        oext[...] = jnp.zeros_like(oext)
        oext[0 : rows - rm, :] = e_ref[rm:rows, :].astype(F32)
        cps = [local(od.at[0, j, pl.ds(0, ha)], eg.at[own, pl.ds(j * ha, ha)], esem.at[0, j]) for j in range(2)]
        cps.append(local(oext, eg.at[own, pl.ds(rm, 8)], esem.at[1, 0]))
        for cp in cps:
            cp.wait()
        pl.semaphore_wait(bar, 22)

    half_a, half_b = pl.ds(0, ha), pl.ds(ha, ha + 8)

    def piece(s, r, dev):
        return remote(eg.at[s, r], eg.at[s, r], dev)

    def slot(xx):
        return xx * 2 + c

    r_a, l_b = piece(own, half_a, xp), piece(own, half_b, xm)
    s_o = piece(own, pl.ds(0, dm.pad), sib)
    r_b, l_a = piece(own, half_b, xp), piece(own, half_a, xm)

    gain = g_ref[...]

    with scope("norm"):
        @pl.loop(0, 16)
        def _(k):
            @pl.when(k < 13)
            def _():
                xload(k + 3).start()

            xload(k).wait()

            def norm(r):
                v = dz[pl.ds(pl.multiple_of(x_at + lax.rem(k, 4) * chunk + r.start, r.size), r.size), :].astype(F32)
                inv = lax.rsqrt(jnp.mean(v * v, axis=-1, keepdims=True) + NORM_EPS)
                hv[pl.ds(pl.multiple_of(k * chunk + r.start, r.size), r.size), :] = (v * inv * gain).astype(BF16)

            _loop_rows(chunk, 16, norm)

    def product(lhs, lanes):
        v = lax.dot_general(lhs, hv[lanes, :], (((1,), (1,)), ((), ())), preferred_element_type=F32)
        return v * (LOG2E / LOGIT_SCALE)

    def add_stats(v, lanes):
        m_old, s_old = st[0:1, lanes], st[1:2, lanes]
        m = jnp.maximum(m_old, jnp.max(v, axis=0, keepdims=True))
        s = jnp.sum(jnp.exp2(v - m), axis=0, keepdims=True)
        st[0:1, lanes] = m
        st[1:2, lanes] = s_old * jnp.exp2(m_old - m) + s

    st[0:1, :] = jnp.full((1, tok), -1e30, F32)
    st[1:2, :] = jnp.zeros((1, tok), F32)
    segs = [(half, j) for half in range(2) for j in range(2)]

    def span(s):
        return (last_n, ha - last_n) if s else (0, last_n)

    def load(s, xx):
        r0, n = span(s)
        return [
            pltpu.make_async_copy(
                eg.at[xx[half] * 2 + j, pl.ds(half * ha + r0, n)], od.at[j, half, pl.ds(r0, n)], esem.at[s, half * 2 + j]
            )
            for half, j in segs
        ]

    def block(s, xx):
        r0, n = span(s)
        for cp in load(s, xx):
            cp.wait()
        for half, j in segs:
            def narrow(r, half=half, j=j):
                at = pl.multiple_of((half * 2 + j) * ha + r0 + r.start, r.size)
                dz[pl.ds(at, r.size), :] = od[j, half, pl.ds(pl.multiple_of(r0 + r.start, r.size), r.size), :].astype(BF16)

            _loop_rows(n, 16, narrow)
        left = [VOCAB_REAL - ((zy * 8 + xx[half] * 2 + j) * rows + half * ha + r0) for half, j in segs]
        w = nt // chunk
        deep = SLOTS // w

        def out(t):
            u = lax.rem(t, deep) * w
            return [
                pltpu.make_async_copy(
                    tst.at[u + i, pl.ds(m * n, n)],
                    zh.at[t * w + i, pl.ds(pl.multiple_of((xx[half] * 2 + half) * rm + j * ha + r0, 8), n)],
                    zsem.at[u + i, m],
                )
                for i in range(w)
                for m, (half, j) in enumerate(segs)
            ]

        @pl.loop(0, tok // nt)
        def _(t):
            @pl.when(t >= deep)
            def _():
                for cp in out(t - deep):
                    cp.wait()

            lanes = pl.ds(pl.multiple_of(t * nt, nt), nt)
            lhs = jnp.concatenate(
                [dz[(half * 2 + j) * ha + r0 : (half * 2 + j) * ha + r0 + n, :] for half, j in segs], axis=0
            )
            v = product(lhs, lanes)
            r = lax.broadcasted_iota(jnp.int32, (n, nt), 0)
            v = jnp.concatenate([jnp.where(r < left[m], v[m * n : (m + 1) * n], -jnp.inf) for m in range(4)], axis=0)
            u = lax.rem(t, deep) * w
            for i in range(w):
                tst[u + i, 0 : 4 * n, :] = v[:, i * chunk : (i + 1) * chunk]
            for cp in out(t):
                cp.start()
            add_stats(v, lanes)

        for t in range(deep):
            for cp in out(t + tok // nt - deep):
                cp.wait()

    def both(xx):
        for s in (1, 0):
            for cp in load(s, xx):
                cp.start()
        block(1, xx)
        block(0, xx)

    def turn(xx):
        for half in range(2):
            base = pl.multiple_of((xx[half] * 2 + half) * rm, rm)

            @pl.loop(0, dim // 128)
            def _(d, half=half, base=base):
                at = pl.ds(pl.multiple_of(d * 128, 128), 128)
                etv[at, pl.ds(base, rm)] = dz[half * rm : (half + 1) * rm, at].T

    with scope("own"):
        s_o.wait_recv()
        both((x, x))
        turn((x, x))

    with scope("labels"):
        total = jnp.sum(msk[...])
        for k in range(16):
            at = pl.ds(k * chunk, chunk)
            w_row[:, at] = msk[k, xc] / total
            q = lab[k, xc] - zy * (8 * rows)
            s = jnp.zeros_like(q)
            for i in range(1, 8):
                s = s + jnp.where(q >= i * rows, 1, 0)
            r = q - s * rows
            up = jnp.where(r >= ha, 1, 0)
            at_main = ((s // 2 * 2 + up) * 2 + s % 2) * ha + r - up * ha
            at_ext = dm.main + s * 8 + r - rm
            place = jnp.where(r < rm, at_main, at_ext)
            pos_row[:, at] = jnp.where((q >= 0) & (q < 8 * rows), place, -1).astype(F32)

    with scope("wait_1"):
        r_a.wait_recv()
        f1, f0 = pl.ds(last_n, ha - last_n), pl.ds(0, last_n)
        r_f1 = piece(slot(x_m), f1, xp)
        r_f0 = piece(slot(x_m), f0, xp)
        d = [piece(slot(x_m), half_a, sib)]
        l_b.wait_recv()
        g1, g0 = pl.ds(ha + last_n, ha - last_n + 8), pl.ds(ha, last_n)
        l_f1 = piece(slot(x_p), g1, xm)
        l_f0 = piece(slot(x_p), g0, xm)
        d.append(piece(slot(x_p), half_b, sib))
        for cp in d:
            cp.wait_recv()

    with scope("near_1"):
        both((x_m, x_p))
        turn((x_m, x_p))

    with scope("wait_2"):
        r_b.wait_recv()
        d = [piece(slot(x_m), half_b, sib)]
        l_a.wait_recv()
        d.append(piece(slot(x_p), half_a, sib))
        for cp in d:
            cp.wait_recv()

    with scope("near_2"):
        both((x_p, x_m))
        turn((x_p, x_m))

    with scope("wait_3"):
        r_f1.wait_recv()
        d = [piece(slot(x_far), f1, sib)]
        l_f1.wait_recv()
        d.append(piece(slot(x_far), g1, sib))
        for cp in d:
            cp.wait_recv()

    far = (x_far, x_far)
    with scope("far_1"):
        for cp in load(1, far):
            cp.start()
        ext_loads = [local(eg.at[s, pl.ds(rm, 8)], ext.at[pl.ds(s * 8, 8)], lsem.at[s]) for s in range(8)]
        block(1, far)
        for cp in ext_loads:
            cp.wait()
        dz[ext_at : ext_at + 64, :] = ext[...].astype(BF16)
        dz[ext_at + 64 : ext_at + 128, :] = jnp.zeros((64, dim), BF16)

        @pl.loop(0, tok // nt)
        def _(t):
            lanes = pl.ds(pl.multiple_of(t * nt, nt), nt)
            v = product(dz[ext_at : ext_at + 64, :], lanes)
            r = lax.broadcasted_iota(jnp.int32, v.shape, 0)
            ok = ((r & 7) < rows - rm) & ((zy * 8 + (r >> 3)) * rows + rm + (r & 7) < VOCAB_REAL)
            v = jnp.where(ok, v, -jnp.inf)
            zeh[:, lanes] = v
            add_stats(v, lanes)

    with scope("wait_4"):
        r_f0.wait_recv()
        d = [piece(slot(x_far), f0, sib)]
        l_f0.wait_recv()
        d.append(piece(slot(x_far), g0, sib))
        for cp in d:
            cp.wait_recv()

    with scope("far_0"):
        for cp in load(0, far):
            cp.start()
        block(0, far)

    with scope("turn_far"):
        scps = [remote(st, got.at[k], p) for k, p in enumerate(near)]
        turn(far)

        @pl.loop(0, dim // 128)
        def _(i):
            at = pl.ds(pl.multiple_of(i * 128, 128), 128)
            etv[at, dm.main : dm.wide] = dz[ext_at : ext_at + 128, at].T

    wide = 2 * rm

    def zload(first, i):
        at = pl.multiple_of(lax.rem(first + i // 16, 4) * wide, wide)
        s = lax.rem(i, SLOTS)
        return pltpu.make_async_copy(zh.at[lax.rem(i, 16), pl.ds(at, wide)], tst.at[s, pl.ds(0, wide)], tsem.at[s])

    def zahead(first):
        for i in range(SLOTS - 1):
            zload(first, i).start()

    with scope("stats"):
        zahead(x_far)
        xo_load = local(x4.at[zy, xc], xo, xsem.at[0])
        for cp in scps:
            cp.wait_recv()
        m = st[0:1, :]
        top = m
        for k in range(len(near)):
            top = jnp.maximum(top, got[k, 0:1, :])
        s = st[1:2, :] * jnp.exp2(m - top)
        for k in range(len(near)):
            s = s + got[k, 1:2, :] * jnp.exp2(got[k, 0:1, :] - top)
        lse_row[:, :] = top + jnp.log(s) * LOG2E
        tgt_row[:, :] = jnp.zeros((1, tok), F32)

    def dz_part(v, place, at, lanes):
        r = lax.broadcasted_iota(jnp.int32, v.shape, 0).astype(F32)
        hit = r == pos_row[:, lanes] - place.astype(F32)
        p = jnp.exp2(v - lse_row[:, lanes])
        dz[at, lanes] = (jnp.where(hit, p - 1.0, p) * w_row[:, lanes]).astype(BF16)
        tgt_row[:, lanes] += jnp.sum(jnp.where(hit, v, 0.0), axis=0, keepdims=True)

    step = min(128, wide)

    def dz_rows(first, start, stop, n):
        @pl.loop(start, stop)
        def _(i):
            @pl.when(i + SLOTS - 1 < n)
            def _():
                zload(first, i + SLOTS - 1).start()

            zload(first, i).wait()
            base = lax.rem(first + i // 16, 4) * wide
            lanes = pl.ds(pl.multiple_of(lax.rem(i, 16) * chunk, chunk), chunk)

            @pl.loop(0, wide // step)
            def _(j):
                at = pl.multiple_of(base + j * step, step)
                r = pl.ds(pl.multiple_of(j * step, step), step)
                dz_part(tst[lax.rem(i, SLOTS), r, :], at, pl.ds(at, step), lanes)

    with scope("dz_far"):
        dz_rows(x_far, 0, 16, 16)

    nd = min(1024, dim)

    def left_over():
        for l in range(0, tok, nt):
            lanes = pl.ds(l, nt)
            dz_part(zeh[:, lanes], jnp.int32(dm.main), pl.ds(dm.main, 64), lanes)
        dz[dm.main + 64 : dm.wide, :] = jnp.zeros((64, tok), BF16)

        @pl.loop(0, dim // nd)
        def _(i):
            lanes = pl.ds(pl.multiple_of(i * nd, nd), nd)
            dee[:, lanes] = jnp.dot(dz[dm.main : dm.main + 64, :], hv[:, lanes], preferred_element_type=F32)

    def de_block(xx, half, s):
        at = pl.ds(pl.multiple_of((xx * 2 + half) * rm, rm), rm)

        @pl.loop(0, dim // nd)
        def _(i):
            lanes = pl.ds(pl.multiple_of(i * nd, nd), nd)
            v = jnp.dot(dz[at, :], hv[:, lanes], preferred_element_type=F32)
            od[s, 0, 0:ha, lanes] = v[0:ha]
            od[s, 1, 0:ha, lanes] = v[ha:rm]

        n = ha + 8 * half
        if half:
            for j in range(2):
                od[s, j, ha : ha + 8, :] = dee[pl.ds(pl.multiple_of((xx * 2 + j) * 8, 8), 8), :]
        cp = _remote(od.at[s, 1 - c, pl.ds(0, n)], s_h.at[xx, pl.ds(half * ha, n)], send, recv, next(ids), sib)
        cp.start()
        return xx, half, s, n, cp

    def sum_load(blk):
        xx, half, s, n, cp = blk
        cp.wait_recv()
        return local(s_h.at[xx, pl.ds(half * ha, n)], sst.at[pl.ds(0, n)], dsem.at[s])

    def sum_add(blk, load_cp, to=None):
        xx, half, s, n, cp = blk
        there = pl.ds(half * ha, n)
        load_cp.wait()

        def add(r):
            od[s, c, r, :] = od[s, c, r, :] + sst[r, :]

        _loop_rows(n, 8, add)
        cp.wait_send()
        return local(od.at[s, c, pl.ds(0, n)], q_h.at[xx, there] if to is None else to.at[there], dsem.at[s])

    def ring_sum(xx, rows_, n, src, s, dst, dev):
        lds = [
            local(q_h.at[xx, rows_], od.at[s, 0, pl.ds(0, n)], lsem.at[0]),
            local(src, sst.at[pl.ds(0, n)], lsem.at[1]),
        ]
        for cp in lds:
            cp.wait()

        def add(r):
            od[s, 0, r, :] = od[s, 0, r, :] + sst[r, :]

        _loop_rows(n, 8, add)
        local(od.at[s, 0, pl.ds(0, n)], q_h.at[xx, rows_], lsem.at[0]).wait()
        return remote(q_h.at[xx, rows_], dst, dev)

    at_dht = SLOTS - 4

    def dh_group(q, n, where):
        def outs(i, s):
            p, ab = where(i)
            r = pl.ds(q * h, h)
            dsts = [dhp.at[ab * 2 + j, p, r] if q == 0 else dhp.at[p, ab * 2 + j, r] for j in range(2)]
            return [pltpu.make_async_copy(tst.at[at_dht + s * 2 + j, pl.ds(0, h)], dst, hsem.at[s * 2 + j]) for j, dst in enumerate(dsts)]

        @pl.loop(0, n)
        def _(i):
            s = lax.rem(i, 2)

            @pl.when(i >= 2)
            def _():
                for cp in outs(i, s):
                    cp.wait()

            p, ab = where(i)
            tiles = [(ab * 2 + j) * 4 + p if q == 0 else p * 4 + ab * 2 + j for j in range(2)]
            rhs = jnp.concatenate([dz[:, pl.ds(pl.multiple_of(k * chunk, chunk), chunk)] for k in tiles], axis=1)
            v = jnp.dot(etv[q * h : (q + 1) * h, :], rhs, preferred_element_type=F32)
            for j in range(2):
                tst[at_dht + s * 2 + j, 0:h, :] = v[:, j * chunk : (j + 1) * chunk]
            for cp in outs(i, s):
                cp.start()

        for s in range(2):
            for cp in outs(s, s):
                cp.wait()

    def part(q, p, lo, n):
        r = pl.ds(q * h, h)
        if q == 0:
            return dhp.at[pl.ds(lo, n), p, r]
        return dhp.at[p, pl.ds(lo, n), r]

    def one(q, p, i):
        r = pl.ds(q * h, h)
        return dhp.at[i, p, r] if q == 0 else dhp.at[p, i, r]

    ring1, ring2 = ((yp, ym), (zp, zm)), ((zp, zm), (yp, ym))
    pos1, pos2 = (y, z), (z, y)
    first, second = ({}, {}), ({}, {})

    def send_far(q):
        p, (rt, lt) = pos1[q], ring1[q]
        first[q]["far_r"] = remote(part(q, _mod4(p + 2), 0, 2), ya.at[q], rt)
        first[q]["far_l"] = remote(part(q, _mod4(p + 2), 2, 2), yb.at[q], lt)

    def send_near(q):
        p, (rt, lt) = pos1[q], ring1[q]
        first[q]["near_r"] = remote(part(q, _mod4(p + 1), 2, 2), yl.at[q, pl.ds(2, 2)], rt)
        first[q]["near_l"] = remote(part(q, _mod4(p - 1), 0, 2), yr.at[q, pl.ds(0, 2)], lt)

    def fetch(i, src):
        return local(src, tst.at[i, pl.ds(0, h)], tsem.at[i])

    def pass_on(q):
        p, (rt, lt) = pos1[q], ring1[q]
        lds = [fetch(i, one(q, _mod4(p + 1), i)) for i in range(2)]
        lds += [fetch(2 + i, one(q, _mod4(p - 1), 2 + i)) for i in range(2)]
        first[q]["far_r"].wait_recv()
        for i in range(2):
            lds[i].wait()
            _add_rows(ya.at[q, i], [tst.at[i, pl.ds(0, h)]], min(64, h))
        first[q]["sum_r"] = remote(ya.at[q], yl.at[q, pl.ds(0, 2)], rt)
        first[q]["far_l"].wait_recv()
        for i in range(2):
            lds[2 + i].wait()
            _add_rows(yb.at[q, i], [tst.at[2 + i, pl.ds(0, h)]], min(64, h))
        first[q]["sum_l"] = remote(yb.at[q], yr.at[q, pl.ds(2, 2)], lt)

    lo, hi = pl.ds(0, hc), pl.ds(hc, hc)

    def second_phase(q):
        r, (rt, lt) = pos2[q], ring2[q]
        r2, r1, rm1 = _mod4(r + 2), _mod4(r + 1), _mod4(r - 1)
        order = (r2, r1, rm1, r)
        lds = [fetch(i, one(q, pos1[q], k)) for i, k in enumerate(order)]
        for k in NEAR_KEYS:
            first[q][k].wait_recv()
        lds2 = [fetch(4 + i, yr.at[q, k]) for i, k in enumerate(order)]
        for i, k in enumerate(order):
            lds[i].wait()
            lds2[i].wait()
            _add_rows(yl.at[q, k], [tst.at[i, pl.ds(0, h)], tst.at[4 + i, pl.ds(0, h)]], min(64, h))
            if i == 0:
                second[q]["far_r"] = remote(yl.at[q, r2, lo], za.at[q], rt)
                second[q]["far_l"] = remote(yl.at[q, r2, hi], zb.at[q], lt)
            if i == 1:
                second[q]["near_r"] = remote(yl.at[q, r1, hi], zl.at[q, hi], rt)
            if i == 2:
                second[q]["near_l"] = remote(yl.at[q, rm1, lo], zr.at[q, lo], lt)

    def second_pass(q):
        r, (rt, lt) = pos2[q], ring2[q]
        r1, rm1 = _mod4(r + 1), _mod4(r - 1)
        second[q]["far_r"].wait_recv()
        _add_rows(yl.at[q, r1, lo], [za.at[q]], min(64, hc))
        second[q]["sum_r"] = remote(yl.at[q, r1, lo], zl.at[q, lo], rt)
        second[q]["far_l"].wait_recv()
        _add_rows(yl.at[q, rm1, hi], [zb.at[q]], min(64, hc))
        second[q]["sum_l"] = remote(yl.at[q, rm1, hi], zr.at[q, hi], lt)

    def last(q):
        r = pos2[q]
        for k in NEAR_KEYS:
            second[q][k].wait_recv()
        n = min(128, h)

        @pl.loop(0, h // n)
        def _(i):
            at = pl.ds(pl.multiple_of(i * n, n), n)
            v = yl[q, r, at, :] + zl[q, at, :] + zr[q, at, :]
            od[0, 0, 0:chunk, pl.ds(pl.multiple_of(q * h + i * n, n), n)] = (v * (1.0 / LOGIT_SCALE)).T

    rest = x_far + 1
    all_rest = 48
    with scope("de_far"):
        zahead(rest)
        b0 = de_block(x_far, 0, 0)
        left_over()
        b1 = de_block(x_far, 1, 1)
        c0 = sum_load(b0)
    with scope("dz_1"):
        dz_rows(rest, 0, 8, all_rest)
        c0 = sum_add(b0, c0)
        dz_rows(rest, 8, 16, all_rest)
        c0.wait()
        e0 = remote(q_h.at[x_far, half_a], xa, xp)
        c1 = sum_load(b1)
    with scope("dz_2"):
        dz_rows(rest, 16, 24, all_rest)
        c1 = sum_add(b1, c1)
        dz_rows(rest, 24, 32, all_rest)
        c1.wait()
        e1 = remote(q_h.at[x_far, half_b], xb, xm)
    with scope("dz_3"):
        dz_rows(rest, 32, all_rest, all_rest)

    def tiles_far(q):
        dh_group(q, 2, lambda i: (_mod4(pos1[q] + 2), i))
        send_far(q)

    def tiles_near(q):
        dh_group(q, 2, lambda i: (_mod4(pos1[q] + 1 + 2 * i), 1 - i))
        send_near(q)

    def tiles_pass(q):
        dh_group(q, 2, lambda i: (_mod4(pos1[q] + 1 + 2 * i), i))

    def tiles_own(q):
        dh_group(q, 2, lambda i: (pos1[q], i))

    with scope("dh_far"):
        tiles_far(1)
        tiles_far(0)
    with scope("dh_near"):
        tiles_near(1)
        tiles_near(0)
    with scope("de_2"):
        b2 = de_block(x_p, 1, 0)
        b3 = de_block(x_m, 0, 1)
        c2 = sum_load(b2)
    with scope("dh_pass"):
        tiles_pass(1)
        c2 = sum_add(b2, c2)
        c3 = sum_load(b3)
    with scope("pass_1"):
        pass_on(1)
        c2.wait()
        e2 = remote(q_h.at[x_p, half_b], xl.at[half_b], xp)
        c3 = sum_add(b3, c3)
    with scope("dh_pass0"):
        tiles_pass(0)
        c3.wait()
        e3 = remote(q_h.at[x_m, half_a], xr.at[half_a], xm)
    with scope("pass_0"):
        pass_on(0)
    with scope("de_4"):
        b4 = de_block(x_p, 0, 0)
        b5 = de_block(x_m, 1, 1)
        c4 = sum_load(b4)
    with scope("dh_own"):
        tiles_own(1)
        c4 = sum_add(b4, c4)
        c5 = sum_load(b5)
        tiles_own(0)
        c4.wait()
        c5 = sum_add(b5, c5)
    with scope("ring"):
        e0.wait_recv()
        e4 = ring_sum(x_p, half_a, ha, xa, 0, xl.at[half_a], xp)
        c5.wait()
        e1.wait_recv()
        e5 = ring_sum(x_m, half_b, ha + 8, xb, 1, xr.at[half_b], xm)
    with scope("de_6"):
        b6 = de_block(x, 0, 0)
        b7 = de_block(x, 1, 1)
        c6 = sum_load(b6)
    with scope("second_1"):
        second_phase(1)
    with scope("sum_6"):
        c6 = sum_add(b6, c6, q_o)
        c7 = sum_load(b7)
    with scope("second_0"):
        second_phase(0)
        c7 = sum_add(b7, c7, q_o)
        c6.wait()
        c7.wait()
    with scope("spass_1"):
        second_pass(1)
    with scope("spass_0"):
        second_pass(0)
    with scope("last_1"):
        last(1)
    with scope("last_0"):
        last(0)

    with scope("finish"):
        xo_load.wait()
        sm[...] = jnp.zeros_like(sm)

        def finish(r):
            v = xo[r, :].astype(F32)
            inv = lax.rsqrt(jnp.mean(v * v, axis=-1, keepdims=True) + NORM_EPS)
            x_hat = v * inv
            dh = od[0, 0, r, :]
            sm[:, 0:dim] += jnp.sum(dh * x_hat, axis=0, keepdims=True)
            u = dh * gain
            od[0, 1, r, :] = inv * (u - x_hat * jnp.mean(u * x_hat, axis=-1, keepdims=True))

        _loop_rows(chunk, 16, finish)
        lse = jnp.where(zy == 0, lse_row[:, :], 0.0)
        loss = jnp.sum(w_row[:, :] * (lse - tgt_row[:, :]))
        sm[:, dim : dim + 128] = jnp.full((1, 128), loss / LOG2E)

    with scope("small_1"):
        cps = [remote(sm, got1.at[k], p) for k, p in enumerate(near)]
        dx_copy = local(od.at[0, 1, pl.ds(0, chunk)], dx_out, osem.at[0])
        for cp in cps:
            cp.wait_recv()
    with scope("small_2"):
        tot = sm[...]
        for k in range(len(near)):
            tot = tot + got1[k]
        got2[len(line)] = tot
        cps = [remote(got2.at[len(line)], got2.at[k], p) for k, p in enumerate(line)]
    with scope("ring_end"):
        for cp in (e2, e3, e4, e5):
            cp.wait_recv()
    with scope("de_out"):
        dx_copy.wait()
        spans = [(pl.ds(i * ha, ha + 8 * i), pl.ds(0, ha + 8 * i)) for i in range(2)]
        own_rows = local(q_o.at[spans[0][0]], sst.at[spans[0][1]], dsem.at[0])
        lds = [
            [local(src.at[r], od.at[k, i, n], lsem.at[i * 2 + k]) for k, src in enumerate((xl, xr))]
            for i, (r, n) in enumerate(spans)
        ]
        outs = []
        for i, (r, n) in enumerate(spans):
            own_rows.wait()
            for cp in lds[i]:
                cp.wait()

            def total_up(r_, i=i):
                v = sst[r_, :] + od[0, i, r_, :] + od[1, i, r_, :]
                od[0, i, r_, :] = v * (1.0 / LOGIT_SCALE)

            _loop_rows(n.size, 8, total_up)
            outs.append(local(od.at[0, i, n], de_out.at[r], osem.at[i]))
            if i == 0:
                own_rows = local(q_o.at[spans[1][0]], sst.at[spans[1][1]], dsem.at[0])
    with scope("small_3"):
        for cp in cps:
            cp.wait_recv()
        for k in range(len(line)):
            tot = tot + got2[k]
        dg_out[...] = tot[:, 0:dim]
        loss_out[...] = tot[:, dim : dim + 128]
    for cp in outs:
        cp.wait()
    for cp in sent:
        cp.wait_send()


def _run(dm, x4, table, gain, labels, mask):
    hbm, vm = pl.BlockSpec(memory_space=HBM), pl.BlockSpec(memory_space=VMEM)
    sd = jax.ShapeDtypeStruct
    d, tok, h, ck, pad, ha = dm.dim, dm.tok, dm.h, dm.chunk, dm.pad, dm.ha
    line, quad, pair = VMEM((1, tok), F32), VMEM((2, 2, h, ck), F32), VMEM((2, h, ck), F32)
    part, shard = VMEM((2, h // 2, ck), F32), sd((pad, d), F32)
    out = pl.pallas_call(
        functools.partial(_kernel, dm),
        name="head",
        out_shape=(
            sd((ck, d), F32), shard, sd((1, d), F32), sd((1, 128), F32),
            shard, shard, shard,
            sd((8, pad, d), F32), sd((16, dm.main, ck), F32), sd((64, tok), F32),
            sd((4, pad, d), F32), sd((4, pad, d), F32), sd((ha, d), F32), sd((ha + 8, d), F32),
            sd((4, 4, d, ck), F32), sd((2, 4, h, ck), F32),
        ),
        in_specs=[hbm, vm, vm, vm, vm],
        out_specs=(hbm, hbm, vm, vm, hbm, hbm, hbm, hbm, hbm, vm, hbm, hbm, hbm, hbm, hbm, hbm),
        scratch_shapes=[
            VMEM((tok, d), BF16), VMEM((d, dm.wide), BF16), VMEM((dm.wide, tok), BF16),
            VMEM((2, 2, ha + 8, d), F32), VMEM((ha + 8, d), F32), VMEM((64, d), F32), VMEM((8, d), F32), VMEM((64, d), F32),
            quad, quad, VMEM((2, 4, h, ck), F32),
            part, part, pair, pair,
            VMEM((SLOTS, max(h, 2 * dm.rm), ck), F32), VMEM((ck, d), BF16),
            VMEM((2, tok), F32), line, line, line, line, VMEM((15, 2, tok), F32),
            VMEM((1, d + 128), F32), VMEM((15, 1, d + 128), F32), VMEM((8, 1, d + 128), F32),
            DMA((96,)), DMA((96,)),
            DMA((2, 4)), DMA((4,)), DMA((SLOTS, 4)), DMA((SLOTS,)), DMA((4,)), DMA((2,)), DMA((2,)), DMA((8,)),
        ],
        compiler_params=pltpu.CompilerParams(
            collective_id=0, has_side_effects=True, vmem_limit_bytes=67043328
        ),
    )(x4, table, gain, labels, mask)
    return out[:4]


def solution(mesh):
    group = mesh.shape[AXIS]

    def local_step(residual, labels, loss_mask, norm_gain, table_shard):
        tokens, dim = residual.shape
        rows = table_shard.shape[0]
        dm = Dims(tokens, dim, rows, group)
        x4 = residual.reshape(16, 8, dm.chunk, dim)
        lab = labels.reshape(16, 8, 1, dm.chunk)
        msk = loss_mask.reshape(16, 8, 1, dm.chunk)
        d_res, d_embed, d_gain, loss = _run(dm, x4, table_shard, norm_gain[None, :], lab, msk)
        return loss[0, 0], d_res, d_embed[:rows], d_gain[0]

    return jax.shard_map(
        local_step,
        mesh=mesh,
        in_specs=(P(), P(), P(), P(), P(AXIS, None)),
        out_specs=(P(), P(AXIS, None), P(AXIS, None), P()),
        check_vma=False,
    )
```

```python
import functools
import itertools
import math

import jax
import jax.numpy as jnp
from jax import lax
from jax.experimental import pallas as pl
from jax.experimental.pallas import tpu as pltpu
from jax.sharding import PartitionSpec as P

VOCAB_REAL = 49155
LOGIT_SCALE = 6.0
NORM_EPS = 1e-6

AXIS = "vp"
MESH = pl.DeviceIdType.MESH
F32 = jnp.float32
BF16 = jnp.bfloat16
HBM = pltpu.HBM
VMEM = pltpu.VMEM
DMA = pltpu.SemaphoreType.DMA


def _coords():
    me = lax.axis_index(AXIS)
    return me // 32, (me // 8) % 4, (me // 2) % 4, me % 2


def _dev(z, y, x, c):
    return ((z * 4 + y) * 4 + x) * 2 + c


def _mod4(v):
    return lax.rem(v + 8, 4)


def _barrier(peers):
    sem = pltpu.get_barrier_semaphore()
    for p in peers:
        pl.semaphore_signal(sem, inc=1, device_id=(p,), device_id_type=MESH)
    pl.semaphore_wait(sem, len(peers))


def _remote(src, dst, send, recv, k, dev):
    return pltpu.make_async_remote_copy(
        src_ref=src,
        dst_ref=dst,
        send_sem=send.at[k],
        recv_sem=recv.at[k],
        device_id=(dev,),
        device_id_type=MESH,
    )


class Dims:
    def __init__(self, tokens, dim, rows, group):
        self.dim, self.rows = dim, rows
        unit = 128 if rows >= 128 else 64
        self.rm = rows // unit * unit
        self.ha = self.rm // 2
        self.last = self.ha // 4
        self.pad = self.rm + 8
        self.chunk = tokens // group
        self.tok = 16 * self.chunk
        self.nt = 4 * self.chunk
        self.main = 8 * self.rm
        self.wide = self.main + 128
        self.h = dim // 2


def _loop_rows(rows, step, fn):
    @pl.loop(0, rows // step)
    def _(i):
        fn(pl.ds(pl.multiple_of(i * step, step), step))


def _add_rows(dst, srcs, step):
    def add(r):
        acc = dst[r, :]
        for s in srcs:
            acc = acc + s[r, :]
        dst[r, :] = acc

    _loop_rows(dst.shape[0], step, add)


SLOTS = 12
LOG2E = math.log2(math.e)
NEAR_KEYS = ("near_r", "near_l", "sum_r", "sum_l")
scope = jax.named_scope


def _kernel(
    dm, x4, e_ref, g_ref, lab, msk,
    dx_out, dg_out, loss_out, q_o, xl, xr, eg, zh, zeh, s_h, q_h, xa, xb, dhp, yr,
    hv, etv, dz, od, sst, dee, oext, ext, ya, yb, yl, za, zb, zl, zr, tst, xo,
    st, w_row, pos_row, lse_row, tgt_row, got, sm, got1, got2,
    send, recv,
    esem, xsem, zsem, tsem, hsem, dsem, osem, lsem,
):
    z, y, x, c = _coords()
    xc, zy = x * 2 + c, z * 4 + y
    rows, rm, ha, last_n, dim, h = dm.rows, dm.rm, dm.ha, dm.last, dm.dim, dm.h
    chunk, tok, nt, hc = dm.chunk, dm.tok, dm.nt, dm.h // 2
    x_far, x_p, x_m = _mod4(x + 2), _mod4(x + 1), _mod4(x - 1)
    xp, xm = _dev(z, y, x_p, c), _dev(z, y, x_m, c)
    yp, ym = _dev(z, _mod4(y + 1), x, c), _dev(z, _mod4(y - 1), x, c)
    zp, zm = _dev(_mod4(z + 1), y, x, c), _dev(_mod4(z - 1), y, x, c)
    sib = _dev(z, y, x, 1 - c)
    near = [_dev(_mod4(z + a), _mod4(y + b), x, c) for a in range(4) for b in range(4) if a or b]
    line = [_dev(z, y, _mod4(x + a), lax.rem(c + b, 2)) for a in range(4) for b in range(2) if a or b]
    bar = pltpu.get_barrier_semaphore()
    for p in (*near, *line):
        pl.semaphore_signal(bar, inc=1, device_id=(p,), device_id_type=MESH)
    sent = []
    ids = itertools.count()

    def remote(src, dst, dev):
        cp = _remote(src, dst, send, recv, next(ids), dev)
        cp.start()
        sent.append(cp)
        return cp

    def local(src, dst, sem):
        cp = pltpu.make_async_copy(src, dst, sem)
        cp.start()
        return cp

    x_at, ext_at = 2 * rm, 4 * rm

    def xload(k):
        s = lax.rem(k, 4)
        to = dz.at[pl.ds(pl.multiple_of(x_at + s * chunk, chunk), chunk)]
        return pltpu.make_async_copy(x4.at[k, xc], to, xsem.at[s])

    with scope("prep"):
        for k in range(3):
            xload(k).start()
        own = xc
        for j in range(2):
            def widen(r, j=j):
                od[0, j, r, :] = e_ref[pl.ds(j * ha + r.start, r.size), :].astype(F32)

            _loop_rows(ha, 16, widen)
        oext[...] = jnp.zeros_like(oext)
        oext[0 : rows - rm, :] = e_ref[rm:rows, :].astype(F32)
        cps = [local(od.at[0, j, pl.ds(0, ha)], eg.at[own, pl.ds(j * ha, ha)], esem.at[0, j]) for j in range(2)]
        cps.append(local(oext, eg.at[own, pl.ds(rm, 8)], esem.at[1, 0]))
        for cp in cps:
            cp.wait()
        pl.semaphore_wait(bar, 22)

    half_a, half_b = pl.ds(0, ha), pl.ds(ha, ha + 8)

    def piece(s, r, dev):
        return remote(eg.at[s, r], eg.at[s, r], dev)

    def slot(xx):
        return xx * 2 + c

    r_a, l_b = piece(own, half_a, xp), piece(own, half_b, xm)
    s_o = piece(own, pl.ds(0, dm.pad), sib)
    r_b, l_a = piece(own, half_b, xp), piece(own, half_a, xm)

    gain = g_ref[...]

    with scope("norm"):
        @pl.loop(0, 16)
        def _(k):
            @pl.when(k < 13)
            def _():
                xload(k + 3).start()

            xload(k).wait()

            def norm(r):
                v = dz[pl.ds(pl.multiple_of(x_at + lax.rem(k, 4) * chunk + r.start, r.size), r.size), :].astype(F32)
                inv = lax.rsqrt(jnp.mean(v * v, axis=-1, keepdims=True) + NORM_EPS)
                hv[pl.ds(pl.multiple_of(k * chunk + r.start, r.size), r.size), :] = (v * inv * gain).astype(BF16)

            _loop_rows(chunk, 16, norm)

    with scope("labels"):
        total = jnp.sum(msk[...])
        for k in range(16):
            at = pl.ds(k * chunk, chunk)
            w_row[:, at] = msk[k, xc] / total
            q = lab[k, xc] - zy * (8 * rows)
            s = jnp.zeros_like(q)
            for i in range(1, 8):
                s = s + jnp.where(q >= i * rows, 1, 0)
            r = q - s * rows
            up = jnp.where(r >= ha, 1, 0)
            at_main = ((s // 2 * 2 + up) * 2 + s % 2) * ha + r - up * ha
            at_ext = dm.main + s * 8 + r - rm
            place = jnp.where(r < rm, at_main, at_ext)
            pos_row[:, at] = jnp.where((q >= 0) & (q < 8 * rows), place, -1).astype(F32)

    def product(lhs, lanes):
        v = lax.dot_general(lhs, hv[lanes, :], (((1,), (1,)), ((), ())), preferred_element_type=F32)
        return v * (LOG2E / LOGIT_SCALE)

    def add_stats(v, lanes):
        m_old, s_old = st[0:1, lanes], st[1:2, lanes]
        m = jnp.maximum(m_old, jnp.max(v, axis=0, keepdims=True))
        s = jnp.sum(jnp.exp2(v - m), axis=0, keepdims=True)
        st[0:1, lanes] = m
        st[1:2, lanes] = s_old * jnp.exp2(m_old - m) + s

    def add_target(v, place, lanes):
        r = lax.broadcasted_iota(jnp.int32, v.shape, 0)
        hit = r.astype(F32) == pos_row[:, lanes] - place.astype(F32)
        tgt_row[:, lanes] += jnp.sum(jnp.where(hit, v, 0.0), axis=0, keepdims=True)

    st[0:1, :] = jnp.full((1, tok), -1e30, F32)
    st[1:2, :] = jnp.zeros((1, tok), F32)
    tgt_row[:, :] = jnp.zeros((1, tok), F32)
    segs = [(half, j) for half in range(2) for j in range(2)]

    def span(s):
        return (last_n, ha - last_n) if s else (0, last_n)

    def load(s, xx):
        r0, n = span(s)
        return [
            pltpu.make_async_copy(
                eg.at[xx[half] * 2 + j, pl.ds(half * ha + r0, n)], od.at[j, half, pl.ds(r0, n)], esem.at[s, half * 2 + j]
            )
            for half, j in segs
        ]

    def block(s, xx):
        r0, n = span(s)
        for cp in load(s, xx):
            cp.wait()
        for half, j in segs:
            def narrow(r, half=half, j=j):
                at = pl.multiple_of((half * 2 + j) * ha + r0 + r.start, r.size)
                dz[pl.ds(at, r.size), :] = od[j, half, pl.ds(pl.multiple_of(r0 + r.start, r.size), r.size), :].astype(BF16)

            _loop_rows(n, 16, narrow)
        left = [VOCAB_REAL - ((zy * 8 + xx[half] * 2 + j) * rows + half * ha + r0) for half, j in segs]
        w = nt // chunk
        deep = SLOTS // w

        def out(t):
            u = lax.rem(t, deep) * w
            return [
                pltpu.make_async_copy(
                    tst.at[u + i, pl.ds(m * n, n)],
                    zh.at[t * w + i, pl.ds(pl.multiple_of((xx[half] * 2 + half) * rm + j * ha + r0, 8), n)],
                    zsem.at[u + i, m],
                )
                for i in range(w)
                for m, (half, j) in enumerate(segs)
            ]

        @pl.loop(0, tok // nt)
        def _(t):
            @pl.when(t >= deep)
            def _():
                for cp in out(t - deep):
                    cp.wait()

            lanes = pl.ds(pl.multiple_of(t * nt, nt), nt)
            lhs = jnp.concatenate(
                [dz[(half * 2 + j) * ha + r0 : (half * 2 + j) * ha + r0 + n, :] for half, j in segs], axis=0
            )
            v = product(lhs, lanes)
            r = lax.broadcasted_iota(jnp.int32, (n, nt), 0)
            v = [jnp.where(r < left[m], v[m * n : (m + 1) * n], -jnp.inf) for m in range(len(segs))]
            for part_v, (half, j) in zip(v, segs):
                add_target(part_v, (xx[half] * 2 + half) * rm + j * ha + r0, lanes)
            v = jnp.concatenate(v, axis=0)
            u = lax.rem(t, deep) * w
            for i in range(w):
                tst[u + i, 0 : 4 * n, :] = v[:, i * chunk : (i + 1) * chunk]
            for cp in out(t):
                cp.start()
            add_stats(v, lanes)

        for t in range(deep):
            for cp in out(t + tok // nt - deep):
                cp.wait()

    def both(xx):
        for s in (1, 0):
            for cp in load(s, xx):
                cp.start()
        block(1, xx)
        block(0, xx)

    def turn(xx):
        for half in range(2):
            base = pl.multiple_of((xx[half] * 2 + half) * rm, rm)

            @pl.loop(0, dim // 128)
            def _(d, half=half, base=base):
                at = pl.ds(pl.multiple_of(d * 128, 128), 128)
                etv[at, pl.ds(base, rm)] = dz[half * rm : (half + 1) * rm, at].T

    with scope("own"):
        s_o.wait_recv()
        both((x, x))
        turn((x, x))

    with scope("wait_1"):
        r_a.wait_recv()
        f1, f0 = pl.ds(last_n, ha - last_n), pl.ds(0, last_n)
        r_f1 = piece(slot(x_m), f1, xp)
        r_f0 = piece(slot(x_m), f0, xp)
        d = [piece(slot(x_m), half_a, sib)]
        l_b.wait_recv()
        g1, g0 = pl.ds(ha + last_n, ha - last_n + 8), pl.ds(ha, last_n)
        l_f1 = piece(slot(x_p), g1, xm)
        l_f0 = piece(slot(x_p), g0, xm)
        d.append(piece(slot(x_p), half_b, sib))
        for cp in d:
            cp.wait_recv()

    with scope("near_1"):
        both((x_m, x_p))
        turn((x_m, x_p))

    with scope("wait_2"):
        r_b.wait_recv()
        d = [piece(slot(x_m), half_b, sib)]
        l_a.wait_recv()
        d.append(piece(slot(x_p), half_a, sib))
        for cp in d:
            cp.wait_recv()

    with scope("near_2"):
        both((x_p, x_m))
        turn((x_p, x_m))

    with scope("wait_3"):
        r_f1.wait_recv()
        d = [piece(slot(x_far), f1, sib)]
        l_f1.wait_recv()
        d.append(piece(slot(x_far), g1, sib))
        for cp in d:
            cp.wait_recv()

    far = (x_far, x_far)
    with scope("far_1"):
        for cp in load(1, far):
            cp.start()
        ext_loads = [local(eg.at[s, pl.ds(rm, 8)], ext.at[pl.ds(s * 8, 8)], lsem.at[s]) for s in range(8)]
        block(1, far)
    with scope("wait_4"):
        r_f0.wait_recv()
        d = [piece(slot(x_far), f0, sib)]
        l_f0.wait_recv()
        d.append(piece(slot(x_far), g0, sib))

    with scope("left"):
        for cp in ext_loads:
            cp.wait()
        dz[ext_at : ext_at + 64, :] = ext[...].astype(BF16)
        dz[ext_at + 64 : ext_at + 128, :] = jnp.zeros((64, dim), BF16)

        @pl.loop(0, tok // nt)
        def _(t):
            lanes = pl.ds(pl.multiple_of(t * nt, nt), nt)
            v = product(dz[ext_at : ext_at + 64, :], lanes)
            r = lax.broadcasted_iota(jnp.int32, v.shape, 0)
            ok = ((r & 7) < rows - rm) & ((zy * 8 + (r >> 3)) * rows + rm + (r & 7) < VOCAB_REAL)
            v = jnp.where(ok, v, -jnp.inf)
            zeh[:, lanes] = v
            add_target(v, jnp.int32(dm.main), lanes)
            add_stats(v, lanes)
        for cp in d:
            cp.wait_recv()

    with scope("far_0"):
        for cp in load(0, far):
            cp.start()
        block(0, far)

    with scope("turn_far"):
        scps = [remote(st, got.at[k], p) for k, p in enumerate(near)]
        turn(far)

        @pl.loop(0, dim // 128)
        def _(i):
            at = pl.ds(pl.multiple_of(i * 128, 128), 128)
            etv[at, dm.main : dm.wide] = dz[ext_at : ext_at + 128, at].T

    wide = 2 * rm

    def zload(first, i):
        at = pl.multiple_of(lax.rem(first + i // 16, 4) * wide, wide)
        s = lax.rem(i, SLOTS)
        return pltpu.make_async_copy(zh.at[lax.rem(i, 16), pl.ds(at, wide)], tst.at[s, pl.ds(0, wide)], tsem.at[s])

    def zahead(first):
        for i in range(SLOTS - 1):
            zload(first, i).start()

    with scope("stats"):
        zahead(x_far)
        xo_load = local(x4.at[zy, xc], xo, xsem.at[0])
        for cp in scps:
            cp.wait_recv()
        m = st[0:1, :]
        top = m
        for k in range(len(near)):
            top = jnp.maximum(top, got[k, 0:1, :])
        s = st[1:2, :] * jnp.exp2(m - top)
        for k in range(len(near)):
            s = s + got[k, 1:2, :] * jnp.exp2(got[k, 0:1, :] - top)
        lse_row[:, :] = top + jnp.log(s) * LOG2E

    def dz_part(v, place, at, lanes):
        r = lax.broadcasted_iota(jnp.int32, v.shape, 0).astype(F32)
        hit = r == pos_row[:, lanes] - place.astype(F32)
        p = jnp.exp2(v - lse_row[:, lanes])
        dz[at, lanes] = (jnp.where(hit, p - 1.0, p) * w_row[:, lanes]).astype(BF16)

    step = min(128, wide)

    def dz_rows(first, start, stop, n):
        @pl.loop(start, stop)
        def _(i):
            @pl.when(i + SLOTS - 1 < n)
            def _():
                zload(first, i + SLOTS - 1).start()

            zload(first, i).wait()
            base = lax.rem(first + i // 16, 4) * wide
            lanes = pl.ds(pl.multiple_of(lax.rem(i, 16) * chunk, chunk), chunk)

            @pl.loop(0, wide // step)
            def _(j):
                at = pl.multiple_of(base + j * step, step)
                r = pl.ds(pl.multiple_of(j * step, step), step)
                dz_part(tst[lax.rem(i, SLOTS), r, :], at, pl.ds(at, step), lanes)

    with scope("dz_far"):
        dz_rows(x_far, 0, 16, 16)

    nd = min(1024, dim)

    def left_over():
        for l in range(0, tok, nt):
            lanes = pl.ds(l, nt)
            dz_part(zeh[:, lanes], jnp.int32(dm.main), pl.ds(dm.main, 64), lanes)
        dz[dm.main + 64 : dm.wide, :] = jnp.zeros((64, tok), BF16)

        @pl.loop(0, dim // nd)
        def _(i):
            lanes = pl.ds(pl.multiple_of(i * nd, nd), nd)
            dee[:, lanes] = jnp.dot(dz[dm.main : dm.main + 64, :], hv[:, lanes], preferred_element_type=F32)

    def de_block(xx, half, s):
        at = pl.ds(pl.multiple_of((xx * 2 + half) * rm, rm), rm)

        @pl.loop(0, dim // nd)
        def _(i):
            lanes = pl.ds(pl.multiple_of(i * nd, nd), nd)
            v = jnp.dot(dz[at, :], hv[:, lanes], preferred_element_type=F32)
            od[s, 0, 0:ha, lanes] = v[0:ha]
            od[s, 1, 0:ha, lanes] = v[ha:rm]

        n = ha + 8 * half
        if half:
            for j in range(2):
                od[s, j, ha : ha + 8, :] = dee[pl.ds(pl.multiple_of((xx * 2 + j) * 8, 8), 8), :]
        cp = _remote(od.at[s, 1 - c, pl.ds(0, n)], s_h.at[xx, pl.ds(half * ha, n)], send, recv, next(ids), sib)
        cp.start()
        return xx, half, s, n, cp

    def sum_load(blk):
        xx, half, s, n, cp = blk
        cp.wait_recv()
        return local(s_h.at[xx, pl.ds(half * ha, n)], sst.at[pl.ds(0, n)], dsem.at[s])

    def sum_add(blk, load_cp, to=None):
        xx, half, s, n, cp = blk
        there = pl.ds(half * ha, n)
        load_cp.wait()

        def add(r):
            od[s, c, r, :] = od[s, c, r, :] + sst[r, :]

        _loop_rows(n, 8, add)
        cp.wait_send()
        return local(od.at[s, c, pl.ds(0, n)], q_h.at[xx, there] if to is None else to.at[there], dsem.at[s])

    def ring_sum(xx, rows_, n, src, s, dst, dev):
        lds = [
            local(q_h.at[xx, rows_], od.at[s, 0, pl.ds(0, n)], lsem.at[0]),
            local(src, sst.at[pl.ds(0, n)], lsem.at[1]),
        ]
        for cp in lds:
            cp.wait()

        def add(r):
            od[s, 0, r, :] = od[s, 0, r, :] + sst[r, :]

        _loop_rows(n, 8, add)
        local(od.at[s, 0, pl.ds(0, n)], q_h.at[xx, rows_], lsem.at[0]).wait()
        return remote(q_h.at[xx, rows_], dst, dev)

    at_dht = SLOTS - 4

    def dh_group(q, n, where):
        def outs(i, s):
            p, ab = where(i)
            r = pl.ds(q * h, h)
            dsts = [dhp.at[ab * 2 + j, p, r] if q == 0 else dhp.at[p, ab * 2 + j, r] for j in range(2)]
            return [pltpu.make_async_copy(tst.at[at_dht + s * 2 + j, pl.ds(0, h)], dst, hsem.at[s * 2 + j]) for j, dst in enumerate(dsts)]

        @pl.loop(0, n)
        def _(i):
            s = lax.rem(i, 2)

            @pl.when(i >= 2)
            def _():
                for cp in outs(i, s):
                    cp.wait()

            p, ab = where(i)
            tiles = [(ab * 2 + j) * 4 + p if q == 0 else p * 4 + ab * 2 + j for j in range(2)]
            rhs = jnp.concatenate([dz[:, pl.ds(pl.multiple_of(k * chunk, chunk), chunk)] for k in tiles], axis=1)
            v = jnp.dot(etv[q * h : (q + 1) * h, :], rhs, preferred_element_type=F32)
            for j in range(2):
                tst[at_dht + s * 2 + j, 0:h, :] = v[:, j * chunk : (j + 1) * chunk]
            for cp in outs(i, s):
                cp.start()

        for s in range(2):
            for cp in outs(s, s):
                cp.wait()

    def part(q, p, lo, n):
        r = pl.ds(q * h, h)
        if q == 0:
            return dhp.at[pl.ds(lo, n), p, r]
        return dhp.at[p, pl.ds(lo, n), r]

    def one(q, p, i):
        r = pl.ds(q * h, h)
        return dhp.at[i, p, r] if q == 0 else dhp.at[p, i, r]

    ring1, ring2 = ((yp, ym), (zp, zm)), ((zp, zm), (yp, ym))
    pos1, pos2 = (y, z), (z, y)
    first, second = ({}, {}), ({}, {})

    def send_far(q):
        p, (rt, lt) = pos1[q], ring1[q]
        first[q]["far_r"] = remote(part(q, _mod4(p + 2), 0, 2), ya.at[q], rt)
        first[q]["far_l"] = remote(part(q, _mod4(p + 2), 2, 2), yb.at[q], lt)

    def send_near(q):
        p, (rt, lt) = pos1[q], ring1[q]
        first[q]["near_r"] = remote(part(q, _mod4(p + 1), 2, 2), yl.at[q, pl.ds(2, 2)], rt)
        first[q]["near_l"] = remote(part(q, _mod4(p - 1), 0, 2), yr.at[q, pl.ds(0, 2)], lt)

    def fetch(i, src):
        return local(src, tst.at[i, pl.ds(0, h)], tsem.at[i])

    def pass_on(q):
        p, (rt, lt) = pos1[q], ring1[q]
        lds = [fetch(i, one(q, _mod4(p + 1), i)) for i in range(2)]
        lds += [fetch(2 + i, one(q, _mod4(p - 1), 2 + i)) for i in range(2)]
        first[q]["far_r"].wait_recv()
        for i in range(2):
            lds[i].wait()
            _add_rows(ya.at[q, i], [tst.at[i, pl.ds(0, h)]], min(64, h))
        first[q]["sum_r"] = remote(ya.at[q], yl.at[q, pl.ds(0, 2)], rt)
        first[q]["far_l"].wait_recv()
        for i in range(2):
            lds[2 + i].wait()
            _add_rows(yb.at[q, i], [tst.at[2 + i, pl.ds(0, h)]], min(64, h))
        first[q]["sum_l"] = remote(yb.at[q], yr.at[q, pl.ds(2, 2)], lt)

    lo, hi = pl.ds(0, hc), pl.ds(hc, hc)

    def second_phase(q):
        r, (rt, lt) = pos2[q], ring2[q]
        r2, r1, rm1 = _mod4(r + 2), _mod4(r + 1), _mod4(r - 1)
        order = (r2, r1, rm1, r)
        lds = [fetch(i, one(q, pos1[q], k)) for i, k in enumerate(order)]
        for k in NEAR_KEYS:
            first[q][k].wait_recv()
        lds2 = [fetch(4 + i, yr.at[q, k]) for i, k in enumerate(order)]
        for i, k in enumerate(order):
            lds[i].wait()
            lds2[i].wait()
            _add_rows(yl.at[q, k], [tst.at[i, pl.ds(0, h)], tst.at[4 + i, pl.ds(0, h)]], min(64, h))
            if i == 0:
                second[q]["far_r"] = remote(yl.at[q, r2, lo], za.at[q], rt)
                second[q]["far_l"] = remote(yl.at[q, r2, hi], zb.at[q], lt)
            if i == 1:
                second[q]["near_r"] = remote(yl.at[q, r1, hi], zl.at[q, hi], rt)
            if i == 2:
                second[q]["near_l"] = remote(yl.at[q, rm1, lo], zr.at[q, lo], lt)

    def second_pass(q):
        r, (rt, lt) = pos2[q], ring2[q]
        r1, rm1 = _mod4(r + 1), _mod4(r - 1)
        second[q]["far_r"].wait_recv()
        _add_rows(yl.at[q, r1, lo], [za.at[q]], min(64, hc))
        second[q]["sum_r"] = remote(yl.at[q, r1, lo], zl.at[q, lo], rt)
        second[q]["far_l"].wait_recv()
        _add_rows(yl.at[q, rm1, hi], [zb.at[q]], min(64, hc))
        second[q]["sum_l"] = remote(yl.at[q, rm1, hi], zr.at[q, hi], lt)

    def last(q):
        r = pos2[q]
        for k in NEAR_KEYS:
            second[q][k].wait_recv()
        n = min(128, h)

        @pl.loop(0, h // n)
        def _(i):
            at = pl.ds(pl.multiple_of(i * n, n), n)
            v = yl[q, r, at, :] + zl[q, at, :] + zr[q, at, :]
            od[0, 0, 0:chunk, pl.ds(pl.multiple_of(q * h + i * n, n), n)] = (v * (1.0 / LOGIT_SCALE)).T

    rest = x_far + 1
    all_rest = 48
    with scope("de_far"):
        zahead(rest)
        b0 = de_block(x_far, 0, 0)
        left_over()
        b1 = de_block(x_far, 1, 1)
        c0 = sum_load(b0)
    with scope("dz_1"):
        dz_rows(rest, 0, 8, all_rest)
        c0 = sum_add(b0, c0)
        dz_rows(rest, 8, 16, all_rest)
        c0.wait()
        e0 = remote(q_h.at[x_far, half_a], xa, xp)
        c1 = sum_load(b1)
    with scope("dz_2"):
        dz_rows(rest, 16, 24, all_rest)
        c1 = sum_add(b1, c1)
        dz_rows(rest, 24, 32, all_rest)
        c1.wait()
        e1 = remote(q_h.at[x_far, half_b], xb, xm)
    with scope("dz_3"):
        dz_rows(rest, 32, all_rest, all_rest)

    def tiles_far(q):
        dh_group(q, 2, lambda i: (_mod4(pos1[q] + 2), i))
        send_far(q)

    def tiles_near(q):
        dh_group(q, 2, lambda i: (_mod4(pos1[q] + 1 + 2 * i), 1 - i))
        send_near(q)

    def tiles_pass(q):
        dh_group(q, 2, lambda i: (_mod4(pos1[q] + 1 + 2 * i), i))

    def tiles_own(q):
        dh_group(q, 2, lambda i: (pos1[q], i))

    with scope("dh_far"):
        tiles_far(1)
        tiles_far(0)
    with scope("de_2"):
        b2 = de_block(x_p, 1, 0)
        b3 = de_block(x_m, 0, 1)
        c2 = sum_load(b2)
    with scope("dh_near"):
        tiles_near(1)
        c2 = sum_add(b2, c2)
        c3 = sum_load(b3)
        tiles_near(0)
        c2.wait()
        e2 = remote(q_h.at[x_p, half_b], xl.at[half_b], xp)
        c3 = sum_add(b3, c3)
    with scope("dh_pass"):
        tiles_pass(1)
        c3.wait()
        e3 = remote(q_h.at[x_m, half_a], xr.at[half_a], xm)
        pass_on(1)
        tiles_pass(0)
    with scope("pass_0"):
        pass_on(0)
    with scope("de_4"):
        b4 = de_block(x_p, 0, 0)
        b5 = de_block(x_m, 1, 1)
        c4 = sum_load(b4)
    with scope("dh_own"):
        tiles_own(1)
        c4 = sum_add(b4, c4)
        c5 = sum_load(b5)
        tiles_own(0)
        c4.wait()
        c5 = sum_add(b5, c5)
    with scope("ring"):
        e0.wait_recv()
        e4 = ring_sum(x_p, half_a, ha, xa, 0, xl.at[half_a], xp)
        c5.wait()
        e1.wait_recv()
        e5 = ring_sum(x_m, half_b, ha + 8, xb, 1, xr.at[half_b], xm)
    with scope("de_6"):
        b6 = de_block(x, 0, 0)
        b7 = de_block(x, 1, 1)
        c6 = sum_load(b6)
    with scope("second_1"):
        second_phase(1)
    with scope("sum_6"):
        c6 = sum_add(b6, c6, q_o)
        c7 = sum_load(b7)
    with scope("second_0"):
        second_phase(0)
        c7 = sum_add(b7, c7, q_o)
        c6.wait()
        c7.wait()
    with scope("spass_1"):
        second_pass(1)
    with scope("spass_0"):
        second_pass(0)
    with scope("last_1"):
        last(1)
    with scope("last_0"):
        last(0)

    with scope("finish"):
        xo_load.wait()
        sm[...] = jnp.zeros_like(sm)

        def finish(r):
            v = xo[r, :].astype(F32)
            inv = lax.rsqrt(jnp.mean(v * v, axis=-1, keepdims=True) + NORM_EPS)
            x_hat = v * inv
            dh = od[0, 0, r, :]
            sm[:, 0:dim] += jnp.sum(dh * x_hat, axis=0, keepdims=True)
            u = dh * gain
            od[0, 1, r, :] = inv * (u - x_hat * jnp.mean(u * x_hat, axis=-1, keepdims=True))

        _loop_rows(chunk, 16, finish)
        lse = jnp.where(zy == 0, lse_row[:, :], 0.0)
        loss = jnp.sum(w_row[:, :] * (lse - tgt_row[:, :]))
        sm[:, dim : dim + 128] = jnp.full((1, 128), loss / LOG2E)

    with scope("small_1"):
        cps = [remote(sm, got1.at[k], p) for k, p in enumerate(near)]
        dx_copy = local(od.at[0, 1, pl.ds(0, chunk)], dx_out, osem.at[0])
        for cp in cps:
            cp.wait_recv()
    with scope("small_2"):
        tot = sm[...]
        for k in range(len(near)):
            tot = tot + got1[k]
        got2[len(line)] = tot
        cps = [remote(got2.at[len(line)], got2.at[k], p) for k, p in enumerate(line)]
    with scope("small_3"):
        for cp in cps:
            cp.wait_recv()
        for k in range(len(line)):
            tot = tot + got2[k]
        dg_out[...] = tot[:, 0:dim]
        loss_out[...] = tot[:, dim : dim + 128]
    with scope("ring_end"):
        for cp in (e2, e3, e4, e5):
            cp.wait_recv()
        dx_copy.wait()
    for cp in sent:
        cp.wait_send()


def _run(dm, x4, table, gain, labels, mask):
    hbm, vm = pl.BlockSpec(memory_space=HBM), pl.BlockSpec(memory_space=VMEM)
    sd = jax.ShapeDtypeStruct
    d, tok, h, ck, pad, ha = dm.dim, dm.tok, dm.h, dm.chunk, dm.pad, dm.ha
    line, quad, pair = VMEM((1, tok), F32), VMEM((2, 2, h, ck), F32), VMEM((2, h, ck), F32)
    part, shard = VMEM((2, h // 2, ck), F32), sd((pad, d), F32)
    out = pl.pallas_call(
        functools.partial(_kernel, dm),
        name="head",
        out_shape=(
            sd((ck, d), F32), sd((1, d), F32), sd((1, 128), F32),
            shard, shard, shard,
            sd((8, pad, d), F32), sd((16, dm.main, ck), F32), sd((64, tok), F32),
            sd((4, pad, d), F32), sd((4, pad, d), F32), sd((ha, d), F32), sd((ha + 8, d), F32),
            sd((4, 4, d, ck), F32), sd((2, 4, h, ck), F32),
        ),
        in_specs=[hbm, vm, vm, vm, vm],
        out_specs=(hbm, vm, vm, hbm, hbm, hbm, hbm, hbm, vm, hbm, hbm, hbm, hbm, hbm, hbm),
        scratch_shapes=[
            VMEM((tok, d), BF16), VMEM((d, dm.wide), BF16), VMEM((dm.wide, tok), BF16),
            VMEM((2, 2, ha + 8, d), F32), VMEM((ha + 8, d), F32), VMEM((64, d), F32), VMEM((8, d), F32), VMEM((64, d), F32),
            quad, quad, VMEM((2, 4, h, ck), F32),
            part, part, pair, pair,
            VMEM((SLOTS, max(h, 2 * dm.rm), ck), F32), VMEM((ck, d), BF16),
            VMEM((2, tok), F32), line, line, line, line, VMEM((15, 2, tok), F32),
            VMEM((1, d + 128), F32), VMEM((15, 1, d + 128), F32), VMEM((8, 1, d + 128), F32),
            DMA((96,)), DMA((96,)),
            DMA((2, 4)), DMA((4,)), DMA((SLOTS, 4)), DMA((SLOTS,)), DMA((4,)), DMA((2,)), DMA((2,)), DMA((8,)),
        ],
        compiler_params=pltpu.CompilerParams(
            collective_id=0, has_side_effects=True, vmem_limit_bytes=67043328
        ),
    )(x4, table, gain, labels, mask)
    dx, dg, loss, *parts = out[:6]
    return _write_out(dm, parts, dx, dg, loss)


def _write_kernel(own, left, right, dx, dg, loss, de_o, dx_o, dg_o, loss_o):
    de_o[:, :] = (own[:, :] + left[:, :] + right[:, :]) * (1.0 / LOGIT_SCALE)
    dx_o[:, :] = dx[:, :]
    dg_o[:, :] = dg[:, :]
    loss_o[:, :] = loss[:, 0:1]


def _write_out(dm, parts, dx, dg, loss):
    d, step = dm.dim, 56 if dm.pad % 56 == 0 else 8
    blocks = dm.pad // step
    sd = jax.ShapeDtypeStruct
    some = pl.BlockSpec((step, d), lambda i: (i, 0))
    quarter = pl.BlockSpec((dm.chunk // 4, d), lambda i: (jnp.minimum(i, 3), 0))
    row, one = pl.BlockSpec((1, d), lambda i: (0, 0)), pl.BlockSpec((1, 1), lambda i: (0, 0))
    loss_row = pl.BlockSpec((1, 128), lambda i: (0, 0))
    return pl.pallas_call(
        _write_kernel,
        name="write_out",
        grid=(blocks,),
        out_shape=(sd((dm.rows, d), F32), sd((dm.chunk, d), F32), sd((1, d), F32), sd((1, 1), F32)),
        in_specs=[some, some, some, quarter, row, loss_row],
        out_specs=(some, quarter, row, one),
    )(*parts, dx, dg, loss)


def solution(mesh):
    group = mesh.shape[AXIS]

    def local_step(residual, labels, loss_mask, norm_gain, table_shard):
        tokens, dim = residual.shape
        rows = table_shard.shape[0]
        dm = Dims(tokens, dim, rows, group)
        x4 = residual.reshape(16, 8, dm.chunk, dim)
        lab = labels.reshape(16, 8, 1, dm.chunk)
        msk = loss_mask.reshape(16, 8, 1, dm.chunk)
        d_embed, d_res, d_gain, loss = _run(dm, x4, table_shard, norm_gain[None, :], lab, msk)
        return loss.reshape(()), d_res, d_embed, d_gain.reshape(dim)

    return jax.shard_map(
        local_step,
        mesh=mesh,
        in_specs=(P(), P(), P(), P(), P(AXIS, None)),
        out_specs=(P(), P(AXIS, None), P(AXIS, None), P()),
        check_vma=False,
    )
```

```python
import functools
import itertools
import math

import jax
import jax.numpy as jnp
from jax import lax
from jax.experimental import pallas as pl
from jax.experimental.pallas import tpu as pltpu
from jax.sharding import PartitionSpec as P

VOCAB_REAL = 49155
LOGIT_SCALE = 6.0
NORM_EPS = 1e-6

AXIS = "vp"
MESH = pl.DeviceIdType.MESH
F32 = jnp.float32
BF16 = jnp.bfloat16
HBM = pltpu.HBM
VMEM = pltpu.VMEM
DMA = pltpu.SemaphoreType.DMA


def _coords():
    me = lax.axis_index(AXIS)
    return me // 32, (me // 8) % 4, (me // 2) % 4, me % 2


def _dev(z, y, x, c):
    return ((z * 4 + y) * 4 + x) * 2 + c


def _mod4(v):
    return lax.rem(v + 8, 4)


def _barrier(peers):
    sem = pltpu.get_barrier_semaphore()
    for p in peers:
        pl.semaphore_signal(sem, inc=1, device_id=(p,), device_id_type=MESH)
    pl.semaphore_wait(sem, len(peers))


def _remote(src, dst, send, recv, k, dev):
    return pltpu.make_async_remote_copy(
        src_ref=src,
        dst_ref=dst,
        send_sem=send.at[k],
        recv_sem=recv.at[k],
        device_id=(dev,),
        device_id_type=MESH,
    )


class Dims:
    def __init__(self, tokens, dim, rows, group):
        self.dim, self.rows = dim, rows
        unit = 128 if rows >= 128 else 64
        self.rm = rows // unit * unit
        self.ha = self.rm // 2
        self.last = max(16, self.ha // 48 * 16)
        self.pad = self.rm + 8
        self.chunk = tokens // group
        self.tok = 16 * self.chunk
        self.nt = 4 * self.chunk
        self.main = 8 * self.rm
        self.wide = self.main + 128
        self.h = dim // 2


def _loop_rows(rows, step, fn):
    @pl.loop(0, rows // step)
    def _(i):
        fn(pl.ds(pl.multiple_of(i * step, step), step))


def _add_rows(dst, srcs, step):
    def add(r):
        acc = dst[r, :]
        for s in srcs:
            acc = acc + s[r, :]
        dst[r, :] = acc

    _loop_rows(dst.shape[0], step, add)


SLOTS = 12
TWO = range(2)
LOG2E = math.log2(math.e)
NEAR_KEYS = ("near_r", "near_l", "sum_r", "sum_l")
scope = jax.named_scope


def _kernel(
    dm, x4, e_ref, g_ref, lab, msk,
    dx_out, dg_out, loss_out, q_o, xs, xe, eg, zh, q_h, xa, xb, dhp, yr,
    hv, etv, dz, od, sst, few, oext, ya, yb, yl, za, zb, zl, zr, tst,
    st, w_row, pos_row, lse_row, tgt_row, got, sm, got1, got2,
    send, recv,
    free, esem, xsem, zsem, tsem, hsem, dsem, osem, lsem,
):
    z, y, x, c = _coords()
    xc, zy = x * 2 + c, z * 4 + y
    rows, rm, ha, last_n, dim, h = dm.rows, dm.rm, dm.ha, dm.last, dm.dim, dm.h
    chunk, tok, nt, hc = dm.chunk, dm.tok, dm.nt, dm.h // 2
    x_far, x_p, x_m = _mod4(x + 2), _mod4(x + 1), _mod4(x - 1)
    xp, xm = _dev(z, y, x_p, c), _dev(z, y, x_m, c)
    yp, ym = _dev(z, _mod4(y + 1), x, c), _dev(z, _mod4(y - 1), x, c)
    zp, zm = _dev(_mod4(z + 1), y, x, c), _dev(_mod4(z - 1), y, x, c)
    sib = _dev(z, y, x, 1 - c)
    near = [_dev(_mod4(z + a), _mod4(y + b), x, c) for a in range(4) for b in range(4) if a or b]
    line = [_dev(z, y, _mod4(x + a), lax.rem(c + b, 2)) for a in range(4) for b in TWO if a or b]
    bar = pltpu.get_barrier_semaphore()
    for p in (*near, *line):
        pl.semaphore_signal(bar, inc=1, device_id=(p,), device_id_type=MESH)
    sent = []
    ids = itertools.count()

    def remote(src, dst, dev):
        cp = _remote(src, dst, send, recv, next(ids), dev)
        cp.start()
        sent.append(cp)
        return cp

    def local(src, dst, sem):
        cp = pltpu.make_async_copy(src, dst, sem)
        cp.start()
        return cp

    x_at, ext_at = 2 * rm, 4 * rm

    def xload(k):
        s = lax.rem(k, 4)
        to = dz.at[pl.ds(pl.multiple_of(x_at + s * chunk, chunk), chunk)]
        return pltpu.make_async_copy(x4.at[k, xc], to, xsem.at[s])

    with scope("prep"):
        for k in range(3):
            xload(k).start()
        own = xc
        for j in TWO:
            def widen(r, j=j):
                od[0, j, r, :] = e_ref[pl.ds(j * ha + r.start, r.size), :].astype(F32)

            _loop_rows(ha, 16, widen)
        oext[...] = jnp.zeros_like(oext)
        oext[0 : rows - rm, :] = e_ref[rm:rows, :].astype(F32)
        cps = [local(od.at[0, j, pl.ds(0, ha)], eg.at[own, pl.ds(j * ha, ha)], esem.at[0, j]) for j in TWO]
        cps.append(local(oext, eg.at[own, pl.ds(rm, 8)], esem.at[1, 0]))
        for cp in cps:
            cp.wait()
        pl.semaphore_wait(bar, 22)

    half_a, half_b = pl.ds(0, ha), pl.ds(ha, ha + 8)

    def piece(s, r, dev):
        return remote(eg.at[s, r], eg.at[s, r], dev)

    def slot(xx):
        return xx * 2 + c

    r_a, l_b = piece(own, half_a, xp), piece(own, half_b, xm)
    s_o = piece(own, pl.ds(0, dm.pad), sib)
    r_b, l_a = piece(own, half_b, xp), piece(own, half_a, xm)

    gain = g_ref[...]

    with scope("norm"):
        @pl.loop(0, 16)
        def _(k):
            @pl.when(k < 13)
            def _():
                xload(k + 3).start()

            xload(k).wait()

            def norm(r):
                v = dz[pl.ds(pl.multiple_of(x_at + lax.rem(k, 4) * chunk + r.start, r.size), r.size), :].astype(F32)
                inv = lax.rsqrt(jnp.mean(v * v, axis=-1, keepdims=True) + NORM_EPS)
                hv[pl.ds(pl.multiple_of(k * chunk + r.start, r.size), r.size), :] = (v * inv * gain).astype(BF16)

            _loop_rows(chunk, 16, norm)

    with scope("labels"):
        total = jnp.sum(msk[...])
        for k in range(16):
            at = pl.ds(k * chunk, chunk)
            w_row[:, at] = msk[k, xc] / total
            q = lab[k, xc] - zy * (8 * rows)
            s = jnp.zeros_like(q)
            for i in range(1, 8):
                s = s + jnp.where(q >= i * rows, 1, 0)
            r = q - s * rows
            up = jnp.where(r >= ha, 1, 0)
            at_main = ((s // 2 * 2 + up) * 2 + s % 2) * ha + r - up * ha
            at_ext = dm.main + s * 8 + r - rm
            place = jnp.where(r < rm, at_main, at_ext)
            pos_row[:, at] = jnp.where((q >= 0) & (q < 8 * rows), place, -1).astype(F32)

    def product(lhs, lanes):
        v = lax.dot_general(lhs, hv[lanes, :], (((1,), (1,)), ((), ())), preferred_element_type=F32)
        return v * (LOG2E / LOGIT_SCALE)

    def add_stats(v, lanes):
        m_old, s_old = st[0:1, lanes], st[1:2, lanes]
        m = jnp.maximum(m_old, jnp.max(v, axis=0, keepdims=True))
        s = jnp.sum(jnp.exp2(v - m), axis=0, keepdims=True)
        st[0:1, lanes] = m
        st[1:2, lanes] = s_old * jnp.exp2(m_old - m) + s

    def add_target(v, place, lanes):
        r = lax.broadcasted_iota(jnp.int32, v.shape, 0)
        hit = r.astype(F32) == pos_row[:, lanes] - place.astype(F32)
        tgt_row[:, lanes] += jnp.sum(jnp.where(hit, v, 0.0), axis=0, keepdims=True)

    st[0:1, :] = jnp.full((1, tok), -1e30, F32)
    st[1:2, :] = jnp.zeros((1, tok), F32)
    tgt_row[:, :] = jnp.zeros((1, tok), F32)
    segs = [(half, j) for half in TWO for j in TWO]

    def span(s):
        return (last_n, ha - last_n) if s else (0, last_n)

    def load(s, xx):
        r0, n = span(s)
        return [
            pltpu.make_async_copy(
                eg.at[xx[half] * 2 + j, pl.ds(half * ha + r0, n)], od.at[j, half, pl.ds(r0, n)], esem.at[s, half * 2 + j]
            )
            for half, j in segs
        ]

    def block(s, xx):
        r0, n = span(s)
        for cp in load(s, xx):
            cp.wait()
        for half, j in segs:
            def narrow(r, half=half, j=j):
                at = pl.multiple_of((half * 2 + j) * ha + r0 + r.start, r.size)
                dz[pl.ds(at, r.size), :] = od[j, half, pl.ds(pl.multiple_of(r0 + r.start, r.size), r.size), :].astype(BF16)

            _loop_rows(n, 16, narrow)
        left = [VOCAB_REAL - ((zy * 8 + xx[half] * 2 + j) * rows + half * ha + r0) for half, j in segs]
        w = nt // chunk
        deep = SLOTS // w

        def out(t):
            u = lax.rem(t, deep) * w
            return [
                pltpu.make_async_copy(
                    tst.at[u + i, pl.ds(m * n, n)],
                    zh.at[t * w + i, pl.ds(pl.multiple_of((xx[half] * 2 + half) * rm + j * ha + r0, 8), n)],
                    zsem.at[u + i, m],
                )
                for i in range(w)
                for m, (half, j) in enumerate(segs)
            ]

        @pl.loop(0, tok // nt)
        def _(t):
            @pl.when(t >= deep)
            def _():
                for cp in out(t - deep):
                    cp.wait()

            lanes = pl.ds(pl.multiple_of(t * nt, nt), nt)
            lhs = jnp.concatenate(
                [dz[(half * 2 + j) * ha + r0 : (half * 2 + j) * ha + r0 + n, :] for half, j in segs], axis=0
            )
            v = product(lhs, lanes)
            r = lax.broadcasted_iota(jnp.int32, (n, nt), 0)
            v = [jnp.where(r < left[m], v[m * n : (m + 1) * n], -jnp.inf) for m in range(len(segs))]
            for part_v, (half, j) in zip(v, segs):
                add_target(part_v, (xx[half] * 2 + half) * rm + j * ha + r0, lanes)
            v = jnp.concatenate(v, axis=0)
            u = lax.rem(t, deep) * w
            for i in range(w):
                tst[u + i, 0 : 4 * n, :] = v[:, i * chunk : (i + 1) * chunk]
            for cp in out(t):
                cp.start()
            add_stats(v, lanes)

        for t in range(deep):
            for cp in out(t + tok // nt - deep):
                cp.wait()

    def both(xx):
        for s in (1, 0):
            for cp in load(s, xx):
                cp.start()
        block(1, xx)
        block(0, xx)

    def turn(xx):
        for half in TWO:
            base = pl.multiple_of((xx[half] * 2 + half) * rm, rm)

            @pl.loop(0, dim // 128)
            def _(d, half=half, base=base):
                at = pl.ds(pl.multiple_of(d * 128, 128), 128)
                etv[at, pl.ds(base, rm)] = dz[half * rm : (half + 1) * rm, at].T

    with scope("own"):
        s_o.wait_recv()
        both((x, x))
        turn((x, x))

    with scope("wait_1"):
        r_a.wait_recv()
        f1, f0 = pl.ds(last_n, ha - last_n), pl.ds(0, last_n)
        r_f1 = piece(slot(x_m), f1, xp)
        r_f0 = piece(slot(x_m), f0, xp)
        d = [piece(slot(x_m), half_a, sib)]
        l_b.wait_recv()
        g1, g0 = pl.ds(ha + last_n, ha - last_n + 8), pl.ds(ha, last_n)
        l_f1 = piece(slot(x_p), g1, xm)
        l_f0 = piece(slot(x_p), g0, xm)
        d.append(piece(slot(x_p), half_b, sib))
        for cp in d:
            cp.wait_recv()

    with scope("near_1"):
        both((x_m, x_p))
        turn((x_m, x_p))

    with scope("wait_2"):
        r_b.wait_recv()
        d = [piece(slot(x_m), half_b, sib)]
        l_a.wait_recv()
        d.append(piece(slot(x_p), half_a, sib))
        for cp in d:
            cp.wait_recv()

    with scope("near_2"):
        both((x_p, x_m))
        turn((x_p, x_m))

    with scope("wait_3"):
        r_f1.wait_recv()
        d = [piece(slot(x_far), f1, sib)]
        l_f1.wait_recv()
        d.append(piece(slot(x_far), g1, sib))
        for cp in d:
            cp.wait_recv()

    far = (x_far, x_far)
    with scope("far_1"):
        for cp in load(1, far):
            cp.start()
        ext_loads = [local(eg.at[s, pl.ds(rm, 8)], few.at[pl.ds(s * 8, 8)], lsem.at[s]) for s in range(8)]
        block(1, far)
    with scope("wait_4"):
        r_f0.wait_recv()
        d = [piece(slot(x_far), f0, sib)]
        l_f0.wait_recv()
        d.append(piece(slot(x_far), g0, sib))

    with scope("left"):
        for cp in ext_loads:
            cp.wait()
        dz[ext_at : ext_at + 64, :] = few[...].astype(BF16)
        dz[ext_at + 64 : ext_at + 128, :] = jnp.zeros((64, dim), BF16)

        @pl.loop(0, tok // nt)
        def _(t):
            lanes = pl.ds(pl.multiple_of(t * nt, nt), nt)
            v = product(dz[ext_at : ext_at + 64, :], lanes)
            r = lax.broadcasted_iota(jnp.int32, v.shape, 0)
            ok = ((r & 7) < rows - rm) & ((zy * 8 + (r >> 3)) * rows + rm + (r & 7) < VOCAB_REAL)
            v = jnp.where(ok, v, -jnp.inf)
            few[:, lanes] = v
            add_target(v, jnp.int32(dm.main), lanes)
            add_stats(v, lanes)
        for cp in d:
            cp.wait_recv()

    with scope("far_0"):
        for cp in load(0, far):
            cp.start()
        block(0, far)

    with scope("turn_far"):
        scps = [remote(st, got.at[k], p) for k, p in enumerate(near)]
        turn(far)

        @pl.loop(0, dim // 128)
        def _(i):
            at = pl.ds(pl.multiple_of(i * 128, 128), 128)
            etv[at, dm.main : dm.wide] = dz[ext_at : ext_at + 128, at].T

    wide = 2 * rm

    at_dht = SLOTS - 4

    def chunk_of(zz, yy):
        return _mod4(zz) * 4 + _mod4(yy)

    def all_far(i):
        return x_far, i

    def in_order(i):
        n = i // 3
        m = n - 7
        k = jnp.where(n < 7, chunk_of(z + n - 1, y + 2), chunk_of(z + 3 + m // 3, y + 3 + lax.rem(m + 9, 3)))
        return _mod4(x + 3 + lax.rem(i, 3)), jnp.where(n < 4, chunk_of(z + 2, n), k)

    def zload(where, i, ring):
        xx, k = where(i)
        s = lax.rem(i, ring)
        at = pl.multiple_of(xx * wide, wide)
        return pltpu.make_async_copy(zh.at[k, pl.ds(at, wide)], tst.at[s, pl.ds(0, wide)], tsem.at[s])

    def zahead(where, ring):
        for i in range(ring - 1):
            zload(where, i, ring).start()

    with scope("stats"):
        zahead(all_far, SLOTS)
        for cp in scps:
            cp.wait_recv()
        m = st[0:1, :]
        top = m
        for k in range(len(near)):
            top = jnp.maximum(top, got[k, 0:1, :])
        s = st[1:2, :] * jnp.exp2(m - top)
        for k in range(len(near)):
            s = s + got[k, 1:2, :] * jnp.exp2(got[k, 0:1, :] - top)
        lse_row[:, :] = top + jnp.log(s) * LOG2E

    def dz_part(v, place, at, lanes):
        r = lax.broadcasted_iota(jnp.int32, v.shape, 0).astype(F32)
        hit = r == pos_row[:, lanes] - place.astype(F32)
        p = jnp.exp2(v - lse_row[:, lanes])
        dz[at, lanes] = (jnp.where(hit, p - 1.0, p) * w_row[:, lanes]).astype(BF16)

    step = min(128, wide)

    def dz_rows(where, start, stop, n, ring):
        @pl.loop(start, stop)
        def _(i):
            @pl.when(i + ring - 1 < n)
            def _():
                zload(where, i + ring - 1, ring).start()

            zload(where, i, ring).wait()
            xx, k = where(i)
            lanes = pl.ds(pl.multiple_of(k * chunk, chunk), chunk)

            @pl.loop(0, wide // step)
            def _(j):
                at = pl.multiple_of(xx * wide + j * step, step)
                r = pl.ds(pl.multiple_of(j * step, step), step)
                dz_part(tst[lax.rem(i, ring), r, :], at, pl.ds(at, step), lanes)

    with scope("dz_far"):
        dz_rows(all_far, 0, 16, 16, SLOTS)

    nd = min(1024, dim)
    few_rows = pl.ds(dm.main, 64)

    used = set()

    def de_block(xx, half, s, with_few=False):
        at = pl.ds(pl.multiple_of((xx * 2 + half) * rm, rm), rm)

        @pl.loop(0, dim // nd)
        def _(i):
            lanes = pl.ds(pl.multiple_of(i * nd, nd), nd)
            lhs = jnp.concatenate([dz[at, :], dz[few_rows, :]], axis=0) if with_few else dz[at, :]
            v = jnp.dot(lhs, hv[:, lanes], preferred_element_type=F32)
            for j in TWO:
                od[s, j, 0:ha, lanes] = v[j * ha : (j + 1) * ha]
            if with_few:
                few[:, lanes] = v[rm:]

        n = ha + 8 * half
        if half:
            for j in TWO:
                od[s, j, ha : ha + 8, :] = few[pl.ds(pl.multiple_of((xx * 2 + j) * 8, 8), 8), :]
        if s in used:
            pl.semaphore_wait(free.at[s], 1)
        used.add(s)
        cp = _remote(od.at[s, 1 - c, pl.ds(0, n)], sst.at[s, pl.ds(0, n)], send, recv, next(ids), sib)
        cp.start()
        return half, s, n, cp

    def early(blk, src):
        half, s, n, cp = blk
        cp.wait_send()
        return local(src.at[pl.ds(half * ha, n)], od.at[s, 1 - c, pl.ds(0, n)], lsem.at[s])

    def sum_add(blk, to, more=None):
        half, s, n, cp = blk
        cp.wait_recv()
        if more is not None:
            more.wait()

        def add(r):
            v = od[s, c, r, :] + sst[s, r, :]
            od[s, c, r, :] = v if more is None else v + od[s, 1 - c, r, :]

        _loop_rows(n, 8, add)
        if more is None:
            pl.semaphore_signal(free.at[s], inc=1, device_id=(sib,), device_id_type=MESH)
            cp.wait_send()
        return local(od.at[s, c, pl.ds(0, n)], to.at[pl.ds(half * ha, n)], dsem.at[s])

    def ring_sum(xx, rows_, n, src, s, dst, dev):
        lds = [
            local(q_h.at[xx, rows_], od.at[s, 0, pl.ds(0, n)], lsem.at[0]),
            local(src, od.at[s, 1, pl.ds(0, n)], lsem.at[1]),
        ]
        for cp in lds:
            cp.wait()
        _add_rows(od.at[s, 0, pl.ds(0, n)], [od.at[s, 1, pl.ds(0, n)]], 8)
        local(od.at[s, 0, pl.ds(0, n)], q_h.at[xx, rows_], lsem.at[0]).wait()
        return remote(q_h.at[xx, rows_], dst, dev)

    stores = []

    def flush():
        while stores:
            stores.pop().wait()

    def tiles(q, where):
        flush()

        def outs(i):
            p, ab = where(i)
            r = pl.ds(q * h, h)
            dsts = [dhp.at[ab * 2 + j, p, r] if q == 0 else dhp.at[p, ab * 2 + j, r] for j in TWO]
            return [
                pltpu.make_async_copy(tst.at[at_dht + i * 2 + j, pl.ds(0, h)], dst, hsem.at[i * 2 + j])
                for j, dst in enumerate(dsts)
            ]

        @pl.loop(0, 2)
        def _(i):
            p, ab = where(i)
            ks = [(ab * 2 + j) * 4 + p if q == 0 else p * 4 + ab * 2 + j for j in TWO]
            rhs = jnp.concatenate([dz[:, pl.ds(pl.multiple_of(k * chunk, chunk), chunk)] for k in ks], axis=1)
            v = jnp.dot(etv[q * h : (q + 1) * h, :], rhs, preferred_element_type=F32)
            for j in TWO:
                tst[at_dht + i * 2 + j, 0:h, :] = v[:, j * chunk : (j + 1) * chunk]
            for cp in outs(i):
                cp.start()

        for i in TWO:
            stores.extend(outs(i))

    def part(q, p, lo, n):
        r = pl.ds(q * h, h)
        if q == 0:
            return dhp.at[pl.ds(lo, n), p, r]
        return dhp.at[p, pl.ds(lo, n), r]

    def one(q, p, i):
        r = pl.ds(q * h, h)
        return dhp.at[i, p, r] if q == 0 else dhp.at[p, i, r]

    ring1, ring2 = ((yp, ym), (zp, zm)), ((zp, zm), (yp, ym))
    pos1, pos2 = (y, z), (z, y)
    first, second = ({}, {}), ({}, {})

    def send_far(q):
        flush()
        p, (rt, lt) = pos1[q], ring1[q]
        first[q]["far_r"] = remote(part(q, _mod4(p + 2), 0, 2), ya.at[q], rt)
        first[q]["far_l"] = remote(part(q, _mod4(p + 2), 2, 2), yb.at[q], lt)

    def send_near(q):
        flush()
        p, (rt, lt) = pos1[q], ring1[q]
        first[q]["near_r"] = remote(part(q, _mod4(p + 1), 2, 2), yl.at[q, pl.ds(2, 2)], rt)
        first[q]["near_l"] = remote(part(q, _mod4(p - 1), 0, 2), yr.at[q, pl.ds(0, 2)], lt)

    def fetch(i, src):
        return local(src, tst.at[i, pl.ds(0, h)], tsem.at[i])

    def pass_on(q):
        flush()
        p, (rt, lt) = pos1[q], ring1[q]
        lds = [fetch(i, one(q, _mod4(p + 1), i)) for i in TWO]
        lds += [fetch(2 + i, one(q, _mod4(p - 1), 2 + i)) for i in TWO]
        first[q]["far_r"].wait_recv()
        for i in TWO:
            lds[i].wait()
            _add_rows(ya.at[q, i], [tst.at[i, pl.ds(0, h)]], min(64, h))
        first[q]["sum_r"] = remote(ya.at[q], yl.at[q, pl.ds(0, 2)], rt)
        first[q]["far_l"].wait_recv()
        for i in TWO:
            lds[2 + i].wait()
            _add_rows(yb.at[q, i], [tst.at[2 + i, pl.ds(0, h)]], min(64, h))
        first[q]["sum_l"] = remote(yb.at[q], yr.at[q, pl.ds(2, 2)], lt)

    lo, hi = pl.ds(0, hc), pl.ds(hc, hc)

    def second_phase(q):
        flush()
        r, (rt, lt) = pos2[q], ring2[q]
        r2, r1, rm1 = _mod4(r + 2), _mod4(r + 1), _mod4(r - 1)
        order = (r2, r1, rm1, r)
        lds = [fetch(i, one(q, pos1[q], k)) for i, k in enumerate(order)]
        for k in NEAR_KEYS:
            first[q][k].wait_recv()
        lds2 = [fetch(4 + i, yr.at[q, k]) for i, k in enumerate(order)]
        for i, k in enumerate(order):
            lds[i].wait()
            lds2[i].wait()
            _add_rows(yl.at[q, k], [tst.at[i, pl.ds(0, h)], tst.at[4 + i, pl.ds(0, h)]], min(64, h))
            if i == 0:
                second[q]["far_r"] = remote(yl.at[q, r2, lo], za.at[q], rt)
                second[q]["far_l"] = remote(yl.at[q, r2, hi], zb.at[q], lt)
            if i == 1:
                second[q]["near_r"] = remote(yl.at[q, r1, hi], zl.at[q, hi], rt)
            if i == 2:
                second[q]["near_l"] = remote(yl.at[q, rm1, lo], zr.at[q, lo], lt)

    def second_pass(q):
        r, (rt, lt) = pos2[q], ring2[q]
        r1, rm1 = _mod4(r + 1), _mod4(r - 1)
        second[q]["far_r"].wait_recv()
        _add_rows(yl.at[q, r1, lo], [za.at[q]], min(64, hc))
        second[q]["sum_r"] = remote(yl.at[q, r1, lo], zl.at[q, lo], rt)
        second[q]["far_l"].wait_recv()
        _add_rows(yl.at[q, rm1, hi], [zb.at[q]], min(64, hc))
        second[q]["sum_l"] = remote(yl.at[q, rm1, hi], zr.at[q, hi], lt)

    def last(q):
        r = pos2[q]
        for k in NEAR_KEYS:
            second[q][k].wait_recv()
        n = min(128, h)

        @pl.loop(0, h // n)
        def _(i):
            at = pl.ds(pl.multiple_of(i * n, n), n)
            v = yl[q, r, at, :] + zl[q, at, :] + zr[q, at, :]
            od[0, 0, 0:chunk, pl.ds(pl.multiple_of(q * h + i * n, n), n)] = (v * (1.0 / LOGIT_SCALE)).T

    def tiles_far(q):
        tiles(q, lambda i: (_mod4(pos1[q] + 2), i))

    def tiles_near(q):
        tiles(q, lambda i: (_mod4(pos1[q] + 1 + 2 * i), 1 - i))

    def tiles_pass(q):
        tiles(q, lambda i: (_mod4(pos1[q] + 1 + 2 * i), i))

    def tiles_own(q):
        tiles(q, lambda i: (pos1[q], i))

    all_rest = 48

    def dz_rest(start, stop):
        dz_rows(in_order, start, stop, all_rest, at_dht)

    with scope("de_far"):
        zahead(in_order, at_dht)
        b0 = de_block(x_far, 0, 0)
        for l in range(0, tok, nt):
            lanes = pl.ds(l, nt)
            dz_part(few[:, lanes], jnp.int32(dm.main), few_rows, lanes)
        dz[dm.main + 64 : dm.wide, :] = jnp.zeros((64, tok), BF16)
        b1 = de_block(x_far, 1, 1, True)
    with scope("dz_1"):
        c0 = sum_add(b0, q_h.at[x_far])
        dz_rest(0, 8)
        c0.wait()
        e0 = remote(q_h.at[x_far, half_a], xa, xp)
        dz_rest(8, 12)
        c1 = sum_add(b1, q_h.at[x_far])
    with scope("dh_far1"):
        tiles_far(1)
        c1.wait()
        e1 = remote(q_h.at[x_far, half_b], xb, xm)
    with scope("dz_2"):
        dz_rest(12, 21)
        send_far(1)
    with scope("dh_far0"):
        tiles_far(0)
    with scope("dz_3"):
        dz_rest(21, 25)
        send_far(0)
        dz_rest(25, all_rest)
    with scope("de_2"):
        b2 = de_block(x_p, 1, 0)
        b3 = de_block(x_m, 0, 1)
        c2 = sum_add(b2, q_h.at[x_p])
    with scope("dh_near"):
        tiles_near(1)
        c2.wait()
        e2 = remote(q_h.at[x_p, half_b], xe.at[half_b], xp)
        c3 = sum_add(b3, q_h.at[x_m])
        send_near(1)
        tiles_near(0)
        c3.wait()
        e3 = remote(q_h.at[x_m, half_a], xe.at[half_a], xm)
        send_near(0)
    with scope("dh_pass"):
        tiles_pass(1)
        tiles_pass(0)
        pass_on(1)
    with scope("de_4"):
        b4 = de_block(x_p, 0, 0)
        pass_on(0)
        b5 = de_block(x_m, 1, 1)
        c4 = sum_add(b4, q_h.at[x_p])
    with scope("dh_own"):
        tiles_own(1)
        c5 = sum_add(b5, q_h.at[x_m])
        tiles_own(0)
        c4.wait()
        c5.wait()
    with scope("ring"):
        e0.wait_recv()
        e4 = ring_sum(x_p, half_a, ha, xa, 0, xs.at[half_a], xp)
        e1.wait_recv()
        e5 = ring_sum(x_m, half_b, ha + 8, xb, 1, xs.at[half_b], xm)
    with scope("de_6"):
        b6 = de_block(x, 0, 0)
    with scope("second_1"):
        second_phase(1)
    with scope("de_7"):
        b7 = de_block(x, 1, 1)
        xo_load = local(x4.at[zy, xc], dz.at[pl.ds(0, chunk)], xsem.at[0])
    with scope("second_0"):
        second_phase(0)
    with scope("spass_1"):
        second_pass(1)
    with scope("sum_6"):
        e3.wait_recv()
        c6 = early(b6, xe)
        e2.wait_recv()
        c7 = early(b7, xe)
        c6 = sum_add(b6, q_o, c6)
        c7 = sum_add(b7, q_o, c7)
    with scope("spass_0"):
        second_pass(0)
        c6.wait()
        c7.wait()
    with scope("last_1"):
        last(1)
    with scope("last_0"):
        last(0)

    with scope("finish"):
        xo_load.wait()
        sm[...] = jnp.zeros_like(sm)

        def finish(r):
            v = dz[r, :].astype(F32)
            inv = lax.rsqrt(jnp.mean(v * v, axis=-1, keepdims=True) + NORM_EPS)
            x_hat = v * inv
            dh = od[0, 0, r, :]
            sm[:, 0:dim] += jnp.sum(dh * x_hat, axis=0, keepdims=True)
            u = dh * gain
            od[0, 1, r, :] = inv * (u - x_hat * jnp.mean(u * x_hat, axis=-1, keepdims=True))

        _loop_rows(chunk, 16, finish)
        lse = jnp.where(zy == 0, lse_row[:, :], 0.0)
        loss = jnp.sum(w_row[:, :] * (lse - tgt_row[:, :]))
        sm[:, dim : dim + 128] = jnp.full((1, 128), loss / LOG2E)

    with scope("small_1"):
        cps = [remote(sm, got1.at[k], p) for k, p in enumerate(near)]
        dx_copy = local(od.at[0, 1, pl.ds(0, chunk)], dx_out, osem.at[0])
        for cp in cps:
            cp.wait_recv()
    with scope("small_2"):
        tot = sm[...]
        for k in range(len(near)):
            tot = tot + got1[k]
        got2[len(line)] = tot
        cps = [remote(got2.at[len(line)], got2.at[k], p) for k, p in enumerate(line)]
    with scope("small_3"):
        for cp in cps:
            cp.wait_recv()
        for k in range(len(line)):
            tot = tot + got2[k]
        dg_out[...] = tot[:, 0:dim]
        loss_out[...] = tot[:, dim : dim + 128]
    with scope("ring_end"):
        for cp in (e4, e5):
            cp.wait_recv()
        dx_copy.wait()
    for cp in sent:
        cp.wait_send()


def _run(dm, x4, table, gain, labels, mask):
    hbm, vm = pl.BlockSpec(memory_space=HBM), pl.BlockSpec(memory_space=VMEM)
    sd = jax.ShapeDtypeStruct
    d, tok, h, ck, pad, ha = dm.dim, dm.tok, dm.h, dm.chunk, dm.pad, dm.ha
    line, quad, pair = VMEM((1, tok), F32), VMEM((2, 2, h, ck), F32), VMEM((2, h, ck), F32)
    part, shard = VMEM((2, h // 2, ck), F32), sd((pad, d), F32)
    out = pl.pallas_call(
        functools.partial(_kernel, dm),
        name="head",
        out_shape=(
            sd((ck, d), F32), sd((1, d), F32), sd((1, 128), F32),
            shard, shard, shard,
            sd((8, pad, d), F32), sd((16, dm.main, ck), F32),
            sd((4, pad, d), F32), sd((ha, d), F32), sd((ha + 8, d), F32),
            sd((4, 4, d, ck), F32), sd((2, 4, h, ck), F32),
        ),
        in_specs=[hbm, vm, vm, vm, vm],
        out_specs=(hbm, vm, vm, *[hbm] * 10),
        scratch_shapes=[
            VMEM((tok, d), BF16), VMEM((d, dm.wide), BF16), VMEM((dm.wide, tok), BF16),
            VMEM((2, 2, ha + 8, d), F32), VMEM((2, ha + 8, d), F32), VMEM((64, d), F32), VMEM((8, d), F32),
            quad, quad, VMEM((2, 4, h, ck), F32),
            part, part, pair, pair,
            VMEM((SLOTS, max(h, 2 * dm.rm), ck), F32),
            VMEM((2, tok), F32), line, line, line, line, VMEM((15, 2, tok), F32),
            VMEM((1, d + 128), F32), VMEM((15, 1, d + 128), F32), VMEM((8, 1, d + 128), F32),
            DMA((96,)), DMA((96,)), pltpu.SemaphoreType.REGULAR((2,)),
            DMA((2, 4)), DMA((4,)), DMA((SLOTS, 4)), DMA((SLOTS,)), DMA((4,)), DMA((2,)), DMA((2,)), DMA((8,)),
        ],
        compiler_params=pltpu.CompilerParams(
            collective_id=0, has_side_effects=True, vmem_limit_bytes=67043328
        ),
    )(x4, table, gain, labels, mask)
    dx, dg, loss, *parts = out[:5]
    return _write_out(dm, parts, dx, dg, loss)


def _write_kernel(own, ring, dx, dg, loss, de_o, dx_o, dg_o, loss_o):
    de_o[:, :] = (own[:, :] + ring[:, :]) * (1.0 / LOGIT_SCALE)
    dx_o[:, :] = dx[:, :]
    dg_o[:, :] = dg[:, :]
    loss_o[:, :] = loss[:, 0:1]


def _write_out(dm, parts, dx, dg, loss):
    d, step, blocks = dm.dim, dm.ha + 8, 2
    sd = jax.ShapeDtypeStruct
    some = pl.BlockSpec((step, d), lambda i: (i, 0))
    quarter = pl.BlockSpec((dm.chunk // blocks, d), lambda i: (i, 0))
    row, one = pl.BlockSpec((1, d), lambda i: (0, 0)), pl.BlockSpec((1, 1), lambda i: (0, 0))
    loss_row = pl.BlockSpec((1, 128), lambda i: (0, 0))
    return pl.pallas_call(
        _write_kernel,
        name="write_out",
        grid=(blocks,),
        out_shape=(sd((dm.rows, d), F32), sd((dm.chunk, d), F32), sd((1, d), F32), sd((1, 1), F32)),
        in_specs=[some, some, quarter, row, loss_row],
        out_specs=(some, quarter, row, one),
    )(*parts, dx, dg, loss)


def solution(mesh):
    group = mesh.shape[AXIS]

    def local_step(residual, labels, loss_mask, norm_gain, table_shard):
        tokens, dim = residual.shape
        rows = table_shard.shape[0]
        dm = Dims(tokens, dim, rows, group)
        x4 = residual.reshape(16, 8, dm.chunk, dim)
        lab = labels.reshape(16, 8, 1, dm.chunk)
        msk = loss_mask.reshape(16, 8, 1, dm.chunk)
        d_embed, d_res, d_gain, loss = _run(dm, x4, table_shard, norm_gain[None, :], lab, msk)
        return loss.reshape(()), d_res, d_embed, d_gain.reshape(dim)

    return jax.shard_map(
        local_step,
        mesh=mesh,
        in_specs=(P(), P(), P(), P(), P(AXIS, None)),
        out_specs=(P(), P(AXIS, None), P(AXIS, None), P()),
        check_vma=False,
    )
```

```python
import functools
import itertools
import math

import jax
import jax.numpy as jnp
from jax import lax
from jax.experimental import pallas as pl
from jax.experimental.pallas import tpu as pltpu
from jax.sharding import PartitionSpec as P

VOCAB_REAL = 49155
LOGIT_SCALE = 6.0
NORM_EPS = 1e-6

AXIS = "vp"
MESH = pl.DeviceIdType.MESH
F32 = jnp.float32
BF16 = jnp.bfloat16
HBM = pltpu.HBM
VMEM = pltpu.VMEM
DMA = pltpu.SemaphoreType.DMA


def _coords():
    me = lax.axis_index(AXIS)
    return me // 32, (me // 8) % 4, (me // 2) % 4, me % 2


def _dev(z, y, x, c):
    return ((z * 4 + y) * 4 + x) * 2 + c


def _mod4(v):
    return lax.rem(v + 8, 4)


def _barrier(peers):
    sem = pltpu.get_barrier_semaphore()
    for p in peers:
        pl.semaphore_signal(sem, inc=1, device_id=(p,), device_id_type=MESH)
    pl.semaphore_wait(sem, len(peers))


def _remote(src, dst, send, recv, k, dev):
    return pltpu.make_async_remote_copy(
        src_ref=src,
        dst_ref=dst,
        send_sem=send.at[k],
        recv_sem=recv.at[k],
        device_id=(dev,),
        device_id_type=MESH,
    )


class Dims:
    def __init__(self, tokens, dim, rows, group):
        self.dim, self.rows = dim, rows
        unit = 128 if rows >= 128 else 64
        self.rm = rows // unit * unit
        self.ha = self.rm // 2
        self.last = max(16, self.ha // 48 * 16)
        self.pad = self.rm + 8
        self.chunk = tokens // group
        self.tok = 16 * self.chunk
        self.nt = 4 * self.chunk
        self.main = 8 * self.rm
        self.wide = self.main + 128
        self.h = dim // 2


def _loop_rows(rows, step, fn):
    @pl.loop(0, rows // step)
    def _(i):
        fn(pl.ds(pl.multiple_of(i * step, step), step))


def _add_rows(dst, srcs, step):
    def add(r):
        acc = dst[r, :]
        for s in srcs:
            acc = acc + s[r, :]
        dst[r, :] = acc

    _loop_rows(dst.shape[0], step, add)


SLOTS = 12
FEW = 64
TWO = range(2)
LOG2E = math.log2(math.e)
NEAR_KEYS = ("near_r", "near_l", "sum_r", "sum_l")
scope = jax.named_scope


def _kernel(
    dm, x4, e_ref, g_ref, lab, msk,
    dx_out, dg_out, loss_out, q_o, xs, xe, eg, zh, q_h, xa, xb, dhp, yr,
    hv, etv, dz, od, sst, few, oext, ya, yb, yl, za, zb, zl, zr, tst,
    st, w_row, pos_row, lse_row, tgt_row, got, sm, got1, got2,
    send, recv,
    free, esem, xsem, zsem, tsem, hsem, dsem, osem, lsem,
):
    z, y, x, c = _coords()
    xc, zy = x * 2 + c, z * 4 + y
    rows, rm, ha, last_n, dim, h = dm.rows, dm.rm, dm.ha, dm.last, dm.dim, dm.h
    chunk, tok, nt, hc = dm.chunk, dm.tok, dm.nt, dm.h // 2
    x_far, x_p, x_m = _mod4(x + 2), _mod4(x + 1), _mod4(x - 1)
    xp, xm = _dev(z, y, x_p, c), _dev(z, y, x_m, c)
    yp, ym = _dev(z, _mod4(y + 1), x, c), _dev(z, _mod4(y - 1), x, c)
    zp, zm = _dev(_mod4(z + 1), y, x, c), _dev(_mod4(z - 1), y, x, c)
    sib = _dev(z, y, x, 1 - c)
    near = [_dev(_mod4(z + a), _mod4(y + b), x, c) for a in range(4) for b in range(4) if a or b]
    line = [_dev(z, y, _mod4(x + a), lax.rem(c + b, 2)) for a in range(4) for b in TWO if a or b]
    bar = pltpu.get_barrier_semaphore()
    for p in (*near, *line):
        pl.semaphore_signal(bar, inc=1, device_id=(p,), device_id_type=MESH)
    sent = []
    ids = itertools.count()

    def remote(src, dst, dev):
        cp = _remote(src, dst, send, recv, next(ids), dev)
        cp.start()
        sent.append(cp)
        return cp

    def local(src, dst, sem):
        cp = pltpu.make_async_copy(src, dst, sem)
        cp.start()
        return cp

    x_at, ext_at = 2 * rm, 4 * rm

    def xload(k):
        s = lax.rem(k, 4)
        to = dz.at[pl.ds(pl.multiple_of(x_at + s * chunk, chunk), chunk)]
        return pltpu.make_async_copy(x4.at[k, xc], to, xsem.at[s])

    with scope("prep"):
        for k in range(3):
            xload(k).start()
        own = xc
        for j in TWO:
            def widen(r, j=j):
                od[0, j, r, :] = e_ref[pl.ds(j * ha + r.start, r.size), :].astype(F32)

            _loop_rows(ha, 16, widen)
        oext[...] = jnp.zeros_like(oext)
        oext[0 : rows - rm, :] = e_ref[rm:rows, :].astype(F32)
        cps = [local(od.at[0, j, pl.ds(0, ha)], eg.at[own, pl.ds(j * ha, ha)], esem.at[0, j]) for j in TWO]
        cps.append(local(oext, eg.at[own, pl.ds(rm, 8)], esem.at[1, 0]))
        for cp in cps:
            cp.wait()
        pl.semaphore_wait(bar, 22)

    half_a, half_b = pl.ds(0, ha), pl.ds(ha, ha + 8)

    def piece(s, r, dev):
        return remote(eg.at[s, r], eg.at[s, r], dev)

    def slot(xx):
        return xx * 2 + c

    r_a, l_b = piece(own, half_a, xp), piece(own, half_b, xm)
    s_o = piece(own, pl.ds(0, dm.pad), sib)
    r_b, l_a = piece(own, half_b, xp), piece(own, half_a, xm)

    gain = g_ref[...]

    with scope("norm"):
        @pl.loop(0, 16)
        def _(k):
            @pl.when(k < 13)
            def _():
                xload(k + 3).start()

            xload(k).wait()

            def norm(r):
                v = dz[pl.ds(pl.multiple_of(x_at + lax.rem(k, 4) * chunk + r.start, r.size), r.size), :].astype(F32)
                inv = lax.rsqrt(jnp.mean(v * v, axis=-1, keepdims=True) + NORM_EPS)
                hv[pl.ds(pl.multiple_of(k * chunk + r.start, r.size), r.size), :] = (v * inv * gain).astype(BF16)

            _loop_rows(chunk, 16, norm)

    with scope("labels"):
        total = jnp.sum(msk[...])
        for k in range(16):
            at = pl.ds(k * chunk, chunk)
            w_row[:, at] = msk[k, xc] / total
            q = lab[k, xc] - zy * (8 * rows)
            s = jnp.zeros_like(q)
            for i in range(1, 8):
                s = s + jnp.where(q >= i * rows, 1, 0)
            r = q - s * rows
            up = jnp.where(r >= ha, 1, 0)
            at_main = ((s // 2 * 2 + up) * 2 + s % 2) * ha + r - up * ha
            at_ext = dm.main + s * 8 + r - rm
            place = jnp.where(r < rm, at_main, at_ext)
            pos_row[:, at] = jnp.where((q >= 0) & (q < 8 * rows), place, -1).astype(F32)

    def product(lhs, lanes):
        v = lax.dot_general(lhs, hv[lanes, :], (((1,), (1,)), ((), ())), preferred_element_type=F32)
        return v * (LOG2E / LOGIT_SCALE)

    def add_stats(v, lanes):
        m_old, s_old = st[0:1, lanes], st[1:2, lanes]
        m = jnp.maximum(m_old, jnp.max(v, axis=0, keepdims=True))
        s = jnp.sum(jnp.exp2(v - m), axis=0, keepdims=True)
        st[0:1, lanes] = m
        st[1:2, lanes] = s_old * jnp.exp2(m_old - m) + s

    def add_target(v, place, lanes):
        r = lax.broadcasted_iota(jnp.int32, v.shape, 0)
        hit = r.astype(F32) == pos_row[:, lanes] - place.astype(F32)
        tgt_row[:, lanes] += jnp.sum(jnp.where(hit, v, 0.0), axis=0, keepdims=True)

    st[0:1, :] = jnp.full((1, tok), -1e30, F32)
    st[1:2, :] = jnp.zeros((1, tok), F32)
    tgt_row[:, :] = jnp.zeros((1, tok), F32)
    segs = [(half, j) for half in TWO for j in TWO]

    def span(s):
        return (last_n, ha - last_n) if s else (0, last_n)

    def load(s, xx):
        r0, n = span(s)
        return [
            pltpu.make_async_copy(
                eg.at[xx[half] * 2 + j, pl.ds(half * ha + r0, n)], od.at[j, half, pl.ds(r0, n)], esem.at[s, half * 2 + j]
            )
            for half, j in segs
        ]

    def narrow_all(s, src):
        r0, n = span(s)
        for half, j in segs:
            def narrow(r, half=half, j=j):
                at = pl.multiple_of((half * 2 + j) * ha + r0 + r.start, r.size)
                dz[pl.ds(at, r.size), :] = src(half, j)[r, :].astype(BF16)

            _loop_rows(n, 16, narrow)

    def block(s, xx, loaded=False, with_few=False):
        r0, n = span(s)
        if not loaded:
            for cp in load(s, xx):
                cp.wait()
            narrow_all(s, lambda half, j: od.at[j, half, pl.ds(r0, n)])
        left = [VOCAB_REAL - ((zy * 8 + xx[half] * 2 + j) * rows + half * ha + r0) for half, j in segs]
        w = nt // chunk
        deep = SLOTS // w

        def out(t):
            u = lax.rem(t, deep) * w
            return [
                pltpu.make_async_copy(
                    tst.at[u + i, pl.ds(m * n, n)],
                    zh.at[t * w + i, pl.ds(pl.multiple_of((xx[half] * 2 + half) * rm + j * ha + r0, 8), n)],
                    zsem.at[u + i, m],
                )
                for i in range(w)
                for m, (half, j) in enumerate(segs)
            ]

        @pl.loop(0, tok // nt)
        def _(t):
            @pl.when(t >= deep)
            def _():
                for cp in out(t - deep):
                    cp.wait()

            lanes = pl.ds(pl.multiple_of(t * nt, nt), nt)
            lhs = [dz[(half * 2 + j) * ha + r0 : (half * 2 + j) * ha + r0 + n, :] for half, j in segs]
            if with_few:
                lhs.append(dz[ext_at : ext_at + FEW, :])
            v = product(jnp.concatenate(lhs, axis=0), lanes)
            v, v_few = v[: 4 * n], v[4 * n :]
            r = lax.broadcasted_iota(jnp.int32, (n, nt), 0)
            v = [jnp.where(r < left[m], v[m * n : (m + 1) * n], -jnp.inf) for m in range(len(segs))]
            for part_v, (half, j) in zip(v, segs):
                add_target(part_v, (xx[half] * 2 + half) * rm + j * ha + r0, lanes)
            u = lax.rem(t, deep) * w
            for i in range(w):
                for m in range(len(segs)):
                    tst[u + i, m * n : (m + 1) * n, :] = v[m][:, i * chunk : (i + 1) * chunk]
            if with_few:
                r = lax.broadcasted_iota(jnp.int32, v_few.shape, 0)
                ok = ((r & 7) < rows - rm) & ((zy * 8 + (r >> 3)) * rows + rm + (r & 7) < VOCAB_REAL)
                v_few = jnp.where(ok, v_few, -jnp.inf)
                few[:, lanes] = v_few
                add_target(v_few, jnp.int32(dm.main), lanes)
                v.append(v_few)
            v = jnp.concatenate(v, axis=0)
            for cp in out(t):
                cp.start()
            add_stats(v, lanes)

        for t in range(deep):
            for cp in out(t + tok // nt - deep):
                cp.wait()

    def both(xx):
        for s in (1, 0):
            for cp in load(s, xx):
                cp.start()
        block(1, xx)
        block(0, xx)

    def turn(xx):
        for half in TWO:
            base = pl.multiple_of((xx[half] * 2 + half) * rm, rm)

            @pl.loop(0, dim // 128)
            def _(d, half=half, base=base):
                at = pl.ds(pl.multiple_of(d * 128, 128), 128)
                etv[at, pl.ds(base, rm)] = dz[half * rm : (half + 1) * rm, at].T

    with scope("own"):
        s_o.wait_recv()
        both((x, x))
        turn((x, x))

    with scope("wait_1"):
        r_a.wait_recv()
        f1, f0 = pl.ds(last_n, ha - last_n), pl.ds(0, last_n)
        r_f1 = piece(slot(x_m), f1, xp)
        r_f0 = remote(eg.at[slot(x_m), f0], sst.at[c, f0], xp)
        d = [piece(slot(x_m), half_a, sib)]
        l_b.wait_recv()
        g1, g0 = pl.ds(ha + last_n, ha - last_n + 8), pl.ds(ha, last_n)
        l_f1 = piece(slot(x_p), g1, xm)
        l_f0 = remote(eg.at[slot(x_p), g0], sst.at[c, pl.ds(last_n, last_n)], xm)
        d.append(piece(slot(x_p), half_b, sib))
        for cp in d:
            cp.wait_recv()

    with scope("near_1"):
        both((x_m, x_p))
        turn((x_m, x_p))

    with scope("wait_2"):
        r_b.wait_recv()
        d = [piece(slot(x_m), half_b, sib)]
        l_a.wait_recv()
        d.append(piece(slot(x_p), half_a, sib))
        for cp in d:
            cp.wait_recv()

    with scope("near_2"):
        both((x_p, x_m))
        turn((x_p, x_m))

    with scope("wait_3"):
        r_f1.wait_recv()
        d = [piece(slot(x_far), f1, sib)]
        l_f1.wait_recv()
        d.append(piece(slot(x_far), g1, sib))
        for cp in d:
            cp.wait_recv()

    far = (x_far, x_far)
    with scope("far_1"):
        for cp in load(1, far):
            cp.start()
        ext_loads = [local(eg.at[s, pl.ds(rm, 8)], few.at[pl.ds(s * 8, 8)], lsem.at[s]) for s in range(8)]
        for cp in ext_loads:
            cp.wait()
        dz[ext_at : ext_at + FEW, :] = few[...].astype(BF16)
        dz[ext_at + FEW : ext_at + 128, :] = jnp.zeros((FEW, dim), BF16)
        block(1, far, with_few=True)

    with scope("wait_4"):
        r_f0.wait_recv()
        l_f0.wait_recv()
        both_last = sst.at[c, pl.ds(0, 2 * last_n)]
        over = _remote(both_last, both_last, send, recv, next(ids), sib)
        over.start()
        over.wait_recv()

    with scope("far_0"):
        narrow_all(0, lambda half, j: sst.at[j, pl.ds(half * last_n, last_n)])
        over.wait_send()
        for s in TWO:
            pl.semaphore_signal(free.at[s], inc=1, device_id=(sib,), device_id_type=MESH)
        block(0, far, loaded=True)

    with scope("turn_far"):
        scps = [remote(st, got.at[k], p) for k, p in enumerate(near)]
        turn(far)

        @pl.loop(0, dim // 128)
        def _(i):
            at = pl.ds(pl.multiple_of(i * 128, 128), 128)
            etv[at, dm.main : dm.wide] = dz[ext_at : ext_at + 128, at].T

    wide = 2 * rm

    at_dht = SLOTS - 4

    def chunk_of(zz, yy):
        return _mod4(zz) * 4 + _mod4(yy)

    def all_far(i):
        return x_far * wide + i // 16 * rm, lax.rem(i, 16)

    def in_order(i):
        n = i // 3
        m = n - 7
        k = jnp.where(n < 7, chunk_of(z + n - 1, y + 2), chunk_of(z + 3 + m // 3, y + 3 + lax.rem(m + 9, 3)))
        return _mod4(x + 3 + lax.rem(i, 3)) * wide, jnp.where(n < 4, chunk_of(z + 2, n), k)

    def zload(where, i, ring, n):
        at, k = where(i)
        s = lax.rem(i, ring)
        src = zh.at[k, pl.ds(pl.multiple_of(at, rm), n)]
        return pltpu.make_async_copy(src, tst.at[s, pl.ds(0, n)], tsem.at[s])

    def zahead(where, ring, n):
        for i in range(ring - 1):
            zload(where, i, ring, n).start()

    with scope("stats"):
        zahead(all_far, SLOTS, rm)
        for cp in scps:
            cp.wait_recv()
        m = st[0:1, :]
        top = m
        for k in range(len(near)):
            top = jnp.maximum(top, got[k, 0:1, :])
        s = st[1:2, :] * jnp.exp2(m - top)
        for k in range(len(near)):
            s = s + got[k, 1:2, :] * jnp.exp2(got[k, 0:1, :] - top)
        lse_row[:, :] = top + jnp.log(s) * LOG2E

    def dz_part(v, place, at, lanes):
        r = lax.broadcasted_iota(jnp.int32, v.shape, 0).astype(F32)
        hit = r == pos_row[:, lanes] - place.astype(F32)
        p = jnp.exp2(v - lse_row[:, lanes])
        dz[at, lanes] = (jnp.where(hit, p - 1.0, p) * w_row[:, lanes]).astype(BF16)

    step = min(128, rm)

    def dz_rows(where, start, stop, last_tile, ring, n):
        @pl.loop(start, stop)
        def _(i):
            @pl.when(i + ring - 1 < last_tile)
            def _():
                zload(where, i + ring - 1, ring, n).start()

            zload(where, i, ring, n).wait()
            row, k = where(i)
            lanes = pl.ds(pl.multiple_of(k * chunk, chunk), chunk)

            @pl.loop(0, n // step)
            def _(j):
                at = pl.multiple_of(row + j * step, step)
                r = pl.ds(pl.multiple_of(j * step, step), step)
                dz_part(tst[lax.rem(i, ring), r, :], at, pl.ds(at, step), lanes)

    def dz_far(start, stop):
        dz_rows(all_far, start, stop, 32, SLOTS, rm)

    with scope("dz_far"):
        dz_far(0, 16)

    nd = min(1024, dim)
    few_rows = pl.ds(dm.main, FEW)

    def de_block(xx, half, s, with_few=False):
        at = pl.ds(pl.multiple_of((xx * 2 + half) * rm, rm), rm)

        @pl.loop(0, dim // nd)
        def _(i):
            lanes = pl.ds(pl.multiple_of(i * nd, nd), nd)
            lhs = jnp.concatenate([dz[at, :], dz[few_rows, :]], axis=0) if with_few else dz[at, :]
            v = jnp.dot(lhs, hv[:, lanes], preferred_element_type=F32)
            for j in TWO:
                od[s, j, 0:ha, lanes] = v[j * ha : (j + 1) * ha]
            if with_few:
                few[:, lanes] = v[rm:]

        n = ha + 8 * half
        if half:
            for j in TWO:
                od[s, j, ha : ha + 8, :] = few[pl.ds(pl.multiple_of((xx * 2 + j) * 8, 8), 8), :]
        pl.semaphore_wait(free.at[s], 1)
        cp = _remote(od.at[s, 1 - c, pl.ds(0, n)], sst.at[s, pl.ds(0, n)], send, recv, next(ids), sib)
        cp.start()
        return half, s, n, cp

    def early(blk, src):
        half, s, n, cp = blk
        cp.wait_send()
        return local(src.at[pl.ds(half * ha, n)], od.at[s, 1 - c, pl.ds(0, n)], lsem.at[s])

    def sum_add(blk, to, more=None):
        half, s, n, cp = blk
        cp.wait_recv()
        if more is not None:
            more.wait()

        def add(r):
            v = od[s, c, r, :] + sst[s, r, :]
            od[s, c, r, :] = v if more is None else v + od[s, 1 - c, r, :]

        _loop_rows(n, 8, add)
        if more is None:
            pl.semaphore_signal(free.at[s], inc=1, device_id=(sib,), device_id_type=MESH)
            cp.wait_send()
        return local(od.at[s, c, pl.ds(0, n)], to.at[pl.ds(half * ha, n)], dsem.at[s])

    def ring_sum(xx, rows_, n, src, s, dst, dev):
        lds = [
            local(q_h.at[xx, rows_], od.at[s, 0, pl.ds(0, n)], lsem.at[0]),
            local(src, od.at[s, 1, pl.ds(0, n)], lsem.at[1]),
        ]
        for cp in lds:
            cp.wait()
        _add_rows(od.at[s, 0, pl.ds(0, n)], [od.at[s, 1, pl.ds(0, n)]], 8)
        local(od.at[s, 0, pl.ds(0, n)], q_h.at[xx, rows_], lsem.at[0]).wait()
        return remote(q_h.at[xx, rows_], dst, dev)

    stores = []

    def flush():
        while stores:
            stores.pop().wait()

    def tiles(q, where):
        flush()

        def outs(i):
            p, ab = where(i)
            r = pl.ds(q * h, h)
            dsts = [dhp.at[ab * 2 + j, p, r] if q == 0 else dhp.at[p, ab * 2 + j, r] for j in TWO]
            return [
                pltpu.make_async_copy(tst.at[at_dht + i * 2 + j, pl.ds(0, h)], dst, hsem.at[i * 2 + j])
                for j, dst in enumerate(dsts)
            ]

        @pl.loop(0, 2)
        def _(i):
            p, ab = where(i)
            ks = [(ab * 2 + j) * 4 + p if q == 0 else p * 4 + ab * 2 + j for j in TWO]
            rhs = jnp.concatenate([dz[:, pl.ds(pl.multiple_of(k * chunk, chunk), chunk)] for k in ks], axis=1)
            v = jnp.dot(etv[q * h : (q + 1) * h, :], rhs, preferred_element_type=F32)
            for j in TWO:
                tst[at_dht + i * 2 + j, 0:h, :] = v[:, j * chunk : (j + 1) * chunk]
            for cp in outs(i):
                cp.start()

        for i in TWO:
            stores.extend(outs(i))

    def part(q, p, lo, n):
        r = pl.ds(q * h, h)
        if q == 0:
            return dhp.at[pl.ds(lo, n), p, r]
        return dhp.at[p, pl.ds(lo, n), r]

    def one(q, p, i):
        r = pl.ds(q * h, h)
        return dhp.at[i, p, r] if q == 0 else dhp.at[p, i, r]

    ring1, ring2 = ((yp, ym), (zp, zm)), ((zp, zm), (yp, ym))
    pos1, pos2 = (y, z), (z, y)
    first, second = ({}, {}), ({}, {})

    def send_far(q):
        flush()
        p, (rt, lt) = pos1[q], ring1[q]
        first[q]["far_r"] = remote(part(q, _mod4(p + 2), 0, 2), ya.at[q], rt)
        first[q]["far_l"] = remote(part(q, _mod4(p + 2), 2, 2), yb.at[q], lt)

    def send_near(q):
        flush()
        p, (rt, lt) = pos1[q], ring1[q]
        first[q]["near_r"] = remote(part(q, _mod4(p + 1), 2, 2), yl.at[q, pl.ds(2, 2)], rt)
        first[q]["near_l"] = remote(part(q, _mod4(p - 1), 0, 2), yr.at[q, pl.ds(0, 2)], lt)

    def fetch(i, src):
        return local(src, tst.at[i, pl.ds(0, h)], tsem.at[i])

    def pass_on(q):
        flush()
        p, (rt, lt) = pos1[q], ring1[q]
        lds = [fetch(i, one(q, _mod4(p + 1), i)) for i in TWO]
        lds += [fetch(2 + i, one(q, _mod4(p - 1), 2 + i)) for i in TWO]
        first[q]["far_r"].wait_recv()
        for i in TWO:
            lds[i].wait()
            _add_rows(ya.at[q, i], [tst.at[i, pl.ds(0, h)]], min(FEW, h))
        first[q]["sum_r"] = remote(ya.at[q], yl.at[q, pl.ds(0, 2)], rt)
        first[q]["far_l"].wait_recv()
        for i in TWO:
            lds[2 + i].wait()
            _add_rows(yb.at[q, i], [tst.at[2 + i, pl.ds(0, h)]], min(FEW, h))
        first[q]["sum_l"] = remote(yb.at[q], yr.at[q, pl.ds(2, 2)], lt)

    lo, hi = pl.ds(0, hc), pl.ds(hc, hc)

    def second_phase(q):
        flush()
        r, (rt, lt) = pos2[q], ring2[q]
        r2, r1, rm1 = _mod4(r + 2), _mod4(r + 1), _mod4(r - 1)
        order = (r2, r1, rm1, r)
        lds = [fetch(i, one(q, pos1[q], k)) for i, k in enumerate(order)]
        for k in NEAR_KEYS:
            first[q][k].wait_recv()
        lds2 = [fetch(4 + i, yr.at[q, k]) for i, k in enumerate(order)]
        for i, k in enumerate(order):
            lds[i].wait()
            lds2[i].wait()
            _add_rows(yl.at[q, k], [tst.at[i, pl.ds(0, h)], tst.at[4 + i, pl.ds(0, h)]], min(FEW, h))
            if i == 0:
                second[q]["far_r"] = remote(yl.at[q, r2, lo], za.at[q], rt)
                second[q]["far_l"] = remote(yl.at[q, r2, hi], zb.at[q], lt)
            if i == 1:
                second[q]["near_r"] = remote(yl.at[q, r1, hi], zl.at[q, hi], rt)
            if i == 2:
                second[q]["near_l"] = remote(yl.at[q, rm1, lo], zr.at[q, lo], lt)

    def second_pass(q):
        r, (rt, lt) = pos2[q], ring2[q]
        r1, rm1 = _mod4(r + 1), _mod4(r - 1)
        second[q]["far_r"].wait_recv()
        _add_rows(yl.at[q, r1, lo], [za.at[q]], min(FEW, hc))
        second[q]["sum_r"] = remote(yl.at[q, r1, lo], zl.at[q, lo], rt)
        second[q]["far_l"].wait_recv()
        _add_rows(yl.at[q, rm1, hi], [zb.at[q]], min(FEW, hc))
        second[q]["sum_l"] = remote(yl.at[q, rm1, hi], zr.at[q, hi], lt)

    def last(q):
        r = pos2[q]
        for k in NEAR_KEYS:
            second[q][k].wait_recv()
        n = min(128, h)

        @pl.loop(0, h // n)
        def _(i):
            at = pl.ds(pl.multiple_of(i * n, n), n)
            v = yl[q, r, at, :] + zl[q, at, :] + zr[q, at, :]
            od[0, 0, 0:chunk, pl.ds(pl.multiple_of(q * h + i * n, n), n)] = (v * (1.0 / LOGIT_SCALE)).T

    def tiles_far(q):
        tiles(q, lambda i: (_mod4(pos1[q] + 2), i))

    def tiles_near(q):
        tiles(q, lambda i: (_mod4(pos1[q] + 1 + 2 * i), 1 - i))

    def tiles_pass(q):
        tiles(q, lambda i: (_mod4(pos1[q] + 1 + 2 * i), i))

    def tiles_own(q):
        tiles(q, lambda i: (pos1[q], i))

    all_rest = 48

    def dz_rest(start, stop):
        dz_rows(in_order, start, stop, all_rest, at_dht, wide)

    with scope("de_far"):
        b0 = de_block(x_far, 0, 0)
        dz_far(16, 32)
        zahead(in_order, at_dht, wide)
        for l in range(0, tok, nt):
            lanes = pl.ds(l, nt)
            dz_part(few[:, lanes], jnp.int32(dm.main), few_rows, lanes)
        dz[dm.main + FEW : dm.wide, :] = jnp.zeros((FEW, tok), BF16)
        b1 = de_block(x_far, 1, 1, True)
    with scope("dz_1"):
        c0 = sum_add(b0, q_h.at[x_far])
        dz_rest(0, 8)
        c0.wait()
        e0 = remote(q_h.at[x_far, half_a], xa, xp)
        dz_rest(8, 12)
        c1 = sum_add(b1, q_h.at[x_far])
    with scope("dh_far1"):
        tiles_far(1)
        c1.wait()
        e1 = remote(q_h.at[x_far, half_b], xb, xm)
    with scope("dz_2"):
        dz_rest(12, 21)
        send_far(1)
    with scope("dh_far0"):
        tiles_far(0)
    with scope("dz_3"):
        dz_rest(21, 25)
        send_far(0)
        dz_rest(25, all_rest)
    with scope("de_2"):
        b2 = de_block(x_p, 1, 0)
        b3 = de_block(x_m, 0, 1)
        c2 = sum_add(b2, q_h.at[x_p])
    with scope("dh_near"):
        tiles_near(1)
        c2.wait()
        e2 = remote(q_h.at[x_p, half_b], xe.at[half_b], xp)
        c3 = sum_add(b3, q_h.at[x_m])
        send_near(1)
        tiles_near(0)
        c3.wait()
        e3 = remote(q_h.at[x_m, half_a], xe.at[half_a], xm)
        send_near(0)
    with scope("dh_pass"):
        tiles_pass(1)
        tiles_pass(0)
        pass_on(1)
    with scope("de_4"):
        b4 = de_block(x_p, 0, 0)
        pass_on(0)
        b5 = de_block(x_m, 1, 1)
        c4 = sum_add(b4, q_h.at[x_p])
    with scope("dh_own"):
        tiles_own(1)
        c5 = sum_add(b5, q_h.at[x_m])
        tiles_own(0)
        c4.wait()
        c5.wait()
    old = list(sent)
    sent.clear()
    with scope("ring"):
        e0.wait_recv()
        e4 = ring_sum(x_p, half_a, ha, xa, 0, xs.at[half_a], xp)
        e1.wait_recv()
        e5 = ring_sum(x_m, half_b, ha + 8, xb, 1, xs.at[half_b], xm)
    with scope("de_6"):
        b6 = de_block(x, 0, 0)
    with scope("de_7"):
        b7 = de_block(x, 1, 1)
        xo_load = local(x4.at[zy, xc], dz.at[pl.ds(0, chunk)], xsem.at[0])
    with scope("second_1"):
        second_phase(1)
    with scope("second_0"):
        second_phase(0)
    with scope("spass_1"):
        second_pass(1)
    with scope("sum_6"):
        e3.wait_recv()
        c6 = early(b6, xe)
        e2.wait_recv()
        c7 = early(b7, xe)
        c6 = sum_add(b6, q_o, c6)
        c7 = sum_add(b7, q_o, c7)
    with scope("spass_0"):
        second_pass(0)
        c6.wait()
        c7.wait()
    with scope("last_1"):
        for cp in old:
            cp.wait_send()
        last(1)
    with scope("last_0"):
        last(0)

    with scope("finish"):
        xo_load.wait()
        sm[...] = jnp.zeros_like(sm)

        def finish(r):
            v = dz[r, :].astype(F32)
            inv = lax.rsqrt(jnp.mean(v * v, axis=-1, keepdims=True) + NORM_EPS)
            x_hat = v * inv
            dh = od[0, 0, r, :]
            sm[:, 0:dim] += jnp.sum(dh * x_hat, axis=0, keepdims=True)
            u = dh * gain
            od[0, 1, r, :] = inv * (u - x_hat * jnp.mean(u * x_hat, axis=-1, keepdims=True))

        _loop_rows(chunk, 16, finish)
        lse = jnp.where(zy == 0, lse_row[:, :], 0.0)
        loss = jnp.sum(w_row[:, :] * (lse - tgt_row[:, :]))
        sm[:, dim : dim + 128] = jnp.full((1, 128), loss / LOG2E)

    with scope("small_1"):
        cps = [remote(sm, got1.at[k], p) for k, p in enumerate(near)]
        dx_copy = local(od.at[0, 1, pl.ds(0, chunk)], dx_out, osem.at[0])
        for cp in cps:
            cp.wait_recv()
    with scope("small_2"):
        tot = sm[...]
        for k in range(len(near)):
            tot = tot + got1[k]
        got2[len(line)] = tot
        cps = [remote(got2.at[len(line)], got2.at[k], p) for k, p in enumerate(line)]
    with scope("small_3"):
        for cp in cps:
            cp.wait_recv()
        for k in range(len(line)):
            tot = tot + got2[k]
        dg_out[...] = tot[:, 0:dim]
        loss_out[...] = tot[:, dim : dim + 128]
    with scope("ring_end"):
        for cp in (e4, e5):
            cp.wait_recv()
        dx_copy.wait()
    for cp in sent:
        cp.wait_send()


def _run(dm, x4, table, gain, labels, mask):
    hbm, vm = pl.BlockSpec(memory_space=HBM), pl.BlockSpec(memory_space=VMEM)
    sd = jax.ShapeDtypeStruct
    d, tok, h, ck, pad, ha = dm.dim, dm.tok, dm.h, dm.chunk, dm.pad, dm.ha
    line, quad, pair = VMEM((1, tok), F32), VMEM((2, 2, h, ck), F32), VMEM((2, h, ck), F32)
    part, shard = VMEM((2, h // 2, ck), F32), sd((pad, d), F32)
    out = pl.pallas_call(
        functools.partial(_kernel, dm),
        name="head",
        out_shape=(
            sd((ck, d), F32), sd((1, d), F32), sd((1, 128), F32),
            shard, shard, shard,
            sd((8, pad, d), F32), sd((16, dm.main, ck), F32),
            sd((4, pad, d), F32), sd((ha, d), F32), sd((ha + 8, d), F32),
            sd((4, 4, d, ck), F32), sd((2, 4, h, ck), F32),
        ),
        in_specs=[hbm, vm, vm, vm, vm],
        out_specs=(hbm, vm, vm, *[hbm] * 10),
        scratch_shapes=[
            VMEM((tok, d), BF16), VMEM((d, dm.wide), BF16), VMEM((dm.wide, tok), BF16),
            VMEM((2, 2, ha + 8, d), F32), VMEM((2, ha + 8, d), F32), VMEM((FEW, d), F32), VMEM((8, d), F32),
            quad, quad, VMEM((2, 4, h, ck), F32),
            part, part, pair, pair,
            VMEM((SLOTS, max(h, 2 * dm.rm), ck), F32),
            VMEM((2, tok), F32), line, line, line, line, VMEM((15, 2, tok), F32),
            VMEM((1, d + 128), F32), VMEM((15, 1, d + 128), F32), VMEM((8, 1, d + 128), F32),
            DMA((96,)), DMA((96,)), pltpu.SemaphoreType.REGULAR((2,)),
            DMA((2, 4)), DMA((4,)), DMA((SLOTS, 4)), DMA((SLOTS,)), DMA((4,)), DMA((2,)), DMA((2,)), DMA((8,)),
        ],
        compiler_params=pltpu.CompilerParams(
            collective_id=0, has_side_effects=True, vmem_limit_bytes=67043328
        ),
    )(x4, table, gain, labels, mask)
    dx, dg, loss, *parts = out[:5]
    return _write_out(dm, parts, dx, dg, loss)


def _write_kernel(own, ring, dx, dg, loss, de_o, dx_o, dg_o, loss_o):
    de_o[:, :] = (own[:, :] + ring[:, :]) * (1.0 / LOGIT_SCALE)
    dx_o[:, :] = dx[:, :]
    dg_o[:, :] = dg[:, :]
    loss_o[:, :] = loss[:, 0:1]


def _write_out(dm, parts, dx, dg, loss):
    d, step, blocks = dm.dim, dm.ha + 8, 2
    sd = jax.ShapeDtypeStruct
    some = pl.BlockSpec((step, d), lambda i: (i, 0))
    quarter = pl.BlockSpec((dm.chunk // blocks, d), lambda i: (i, 0))
    row, one = pl.BlockSpec((1, d), lambda i: (0, 0)), pl.BlockSpec((1, 1), lambda i: (0, 0))
    loss_row = pl.BlockSpec((1, 128), lambda i: (0, 0))
    return pl.pallas_call(
        _write_kernel,
        name="write_out",
        grid=(blocks,),
        out_shape=(sd((dm.rows, d), F32), sd((dm.chunk, d), F32), sd((1, d), F32), sd((1, 1), F32)),
        in_specs=[some, some, quarter, row, loss_row],
        out_specs=(some, quarter, row, one),
    )(*parts, dx, dg, loss)


def solution(mesh):
    group = mesh.shape[AXIS]

    def local_step(residual, labels, loss_mask, norm_gain, table_shard):
        tokens, dim = residual.shape
        rows = table_shard.shape[0]
        dm = Dims(tokens, dim, rows, group)
        x4 = residual.reshape(16, 8, dm.chunk, dim)
        lab = labels.reshape(16, 8, 1, dm.chunk)
        msk = loss_mask.reshape(16, 8, 1, dm.chunk)
        d_embed, d_res, d_gain, loss = _run(dm, x4, table_shard, norm_gain[None, :], lab, msk)
        return loss.reshape(()), d_res, d_embed, d_gain.reshape(dim)

    return jax.shard_map(
        local_step,
        mesh=mesh,
        in_specs=(P(), P(), P(), P(), P(AXIS, None)),
        out_specs=(P(), P(AXIS, None), P(AXIS, None), P()),
        check_vma=False,
    )
```

```python
import functools
import itertools
import math

import jax
import jax.numpy as jnp
from jax import lax
from jax.experimental import pallas as pl
from jax.experimental.pallas import tpu as pltpu
from jax.sharding import PartitionSpec as P

VOCAB_REAL = 49155
LOGIT_SCALE = 6.0
NORM_EPS = 1e-6

AXIS = "vp"
MESH = pl.DeviceIdType.MESH
F32 = jnp.float32
BF16 = jnp.bfloat16
HBM = pltpu.HBM
VMEM = pltpu.VMEM
DMA = pltpu.SemaphoreType.DMA


def _coords():
    me = lax.axis_index(AXIS)
    return me // 32, (me // 8) % 4, (me // 2) % 4, me % 2


def _dev(z, y, x, c):
    return ((z * 4 + y) * 4 + x) * 2 + c


def _mod4(v):
    return lax.rem(v + 8, 4)


def _barrier(peers):
    sem = pltpu.get_barrier_semaphore()
    for p in peers:
        pl.semaphore_signal(sem, inc=1, device_id=(p,), device_id_type=MESH)
    pl.semaphore_wait(sem, len(peers))


def _remote(src, dst, send, recv, k, dev):
    return pltpu.make_async_remote_copy(
        src_ref=src,
        dst_ref=dst,
        send_sem=send.at[k],
        recv_sem=recv.at[k],
        device_id=(dev,),
        device_id_type=MESH,
    )


class Dims:
    def __init__(self, tokens, dim, rows, group):
        self.dim, self.rows = dim, rows
        unit = 128 if rows >= 128 else 64
        self.rm = rows // unit * unit
        self.ha = self.rm // 2
        self.last = max(16, self.ha // 48 * 16)
        self.pad = self.rm + 8
        self.chunk = tokens // group
        self.tok = 16 * self.chunk
        self.nt = 4 * self.chunk
        self.main = 8 * self.rm
        self.wide = self.main + 128
        self.h = dim // 2


def _rem(a, b):
    return a % b if isinstance(a, int) else lax.rem(a, b)


def _pick(test, a, b):
    return (a if test else b) if isinstance(test, bool) else jnp.where(test, a, b)


def _loop_rows(rows, step, fn):
    @pl.loop(0, rows // step)
    def _(i):
        fn(pl.ds(pl.multiple_of(i * step, step), step))


def _add_rows(dst, srcs, step):
    def add(r):
        acc = dst[r, :]
        for s in srcs:
            acc = acc + s[r, :]
        dst[r, :] = acc

    _loop_rows(dst.shape[0], step, add)


SLOTS = 12
FEW = 64
TWO = range(2)
LOG2E = math.log2(math.e)
NEAR_KEYS = ("near_r", "near_l", "sum_r", "sum_l")
scope = jax.named_scope


def _kernel(
    dm, x4, e_ref, g_ref, lab, msk,
    dx_out, got2, q_o, xs, xe, eg, zh, q_h, xa, xb, dhp, yr,
    hv, etv, dz, od, sst, few, oext, ya, yb, yl, za, zb, zl, zr, tst,
    m_row, s_row, w_row, pos_row, lse_row, tgt_row, got, sm, got1, total_v,
    send, recv,
    free, esem, xsem, zsem, tsem, hsem, dsem, osem, lsem,
):
    z, y, x, c = _coords()
    xc, zy = x * 2 + c, z * 4 + y
    rows, rm, ha, last_n, dim, h = dm.rows, dm.rm, dm.ha, dm.last, dm.dim, dm.h
    chunk, tok, nt, hc = dm.chunk, dm.tok, dm.nt, dm.h // 2
    x_far, x_p, x_m = _mod4(x + 2), _mod4(x + 1), _mod4(x - 1)
    xp, xm = _dev(z, y, x_p, c), _dev(z, y, x_m, c)
    yp, ym = _dev(z, _mod4(y + 1), x, c), _dev(z, _mod4(y - 1), x, c)
    zp, zm = _dev(_mod4(z + 1), y, x, c), _dev(_mod4(z - 1), y, x, c)
    sib = _dev(z, y, x, 1 - c)
    near = [_dev(_mod4(z + a), _mod4(y + b), x, c) for a in range(4) for b in range(4) if a or b]
    line = [_dev(z, y, _mod4(x + a), lax.rem(c + b, 2)) for a in range(4) for b in TWO if a or b]
    bar = pltpu.get_barrier_semaphore()
    for p in (*near, *line):
        pl.semaphore_signal(bar, inc=1, device_id=(p,), device_id_type=MESH)
    sent = []
    ids = itertools.count()

    def remote(src, dst, dev):
        cp = _remote(src, dst, send, recv, next(ids), dev)
        cp.start()
        sent.append(cp)
        return cp

    def local(src, dst, sem):
        cp = pltpu.make_async_copy(src, dst, sem)
        cp.start()
        return cp

    x_at, ext_at = 2 * rm, 4 * rm

    def xload(k):
        s = lax.rem(k, 4)
        to = dz.at[pl.ds(pl.multiple_of(x_at + s * chunk, chunk), chunk)]
        return pltpu.make_async_copy(x4.at[k, xc], to, xsem.at[s])

    with scope("prep"):
        for k in range(3):
            xload(k).start()
        own = xc
        for j in TWO:
            def widen(r, j=j):
                od[0, j, r, :] = e_ref[pl.ds(j * ha + r.start, r.size), :].astype(F32)

            _loop_rows(ha, 16, widen)
        oext[...] = jnp.zeros_like(oext)
        oext[0 : rows - rm, :] = e_ref[rm:rows, :].astype(F32)
        cps = [local(od.at[0, j, pl.ds(0, ha)], eg.at[own, pl.ds(j * ha, ha)], esem.at[0, j]) for j in TWO]
        cps.append(local(oext, eg.at[own, pl.ds(rm, 8)], esem.at[1, 0]))
        for cp in cps:
            cp.wait()
        pl.semaphore_wait(bar, 22)

    half_a, half_b = pl.ds(0, ha), pl.ds(ha, ha + 8)

    def piece(s, r, dev):
        return remote(eg.at[s, r], eg.at[s, r], dev)

    def slot(xx):
        return xx * 2 + c

    r_a, l_b = piece(own, half_a, xp), piece(own, half_b, xm)
    s_o = piece(own, pl.ds(0, dm.pad), sib)
    r_b, l_a = piece(own, half_b, xp), piece(own, half_a, xm)

    gain = g_ref[...]

    with scope("norm"):
        @pl.loop(0, 16)
        def _(k):
            @pl.when(k < 13)
            def _():
                xload(k + 3).start()

            xload(k).wait()

            def norm(r):
                v = dz[pl.ds(pl.multiple_of(x_at + lax.rem(k, 4) * chunk + r.start, r.size), r.size), :].astype(F32)
                inv = lax.rsqrt(jnp.mean(v * v, axis=-1, keepdims=True) + NORM_EPS)
                hv[pl.ds(pl.multiple_of(k * chunk + r.start, r.size), r.size), :] = (v * inv * gain).astype(BF16)

            _loop_rows(chunk, 16, norm)

    with scope("labels"):
        total = jnp.sum(msk[...])
        for k in range(16):
            at = pl.ds(k * chunk, chunk)
            w_row[:, at] = msk[k, xc] / total
            q = lab[k, xc] - zy * (8 * rows)
            s = jnp.zeros_like(q)
            for i in range(1, 8):
                s = s + jnp.where(q >= i * rows, 1, 0)
            r = q - s * rows
            up = jnp.where(r >= ha, 1, 0)
            at_main = ((s // 2 * 2 + up) * 2 + s % 2) * ha + r - up * ha
            at_ext = dm.main + s * 8 + r - rm
            place = jnp.where(r < rm, at_main, at_ext)
            pos_row[:, at] = jnp.where((q >= 0) & (q < 8 * rows), place, -1).astype(F32)

    def product(lhs, lanes):
        v = lax.dot_general(lhs, hv[lanes, :], (((1,), (1,)), ((), ())), preferred_element_type=F32)
        return v * (LOG2E / LOGIT_SCALE)

    def add_stats(v, lanes):
        m_old, s_old = m_row[:, lanes], s_row[:, lanes]
        m = jnp.maximum(m_old, jnp.max(v, axis=0, keepdims=True))
        s = jnp.sum(jnp.exp2(v - m), axis=0, keepdims=True)
        m_row[:, lanes] = m
        s_row[:, lanes] = s_old * jnp.exp2(m_old - m) + s

    def add_target(v, place, lanes):
        r = lax.broadcasted_iota(jnp.int32, v.shape, 0)
        hit = r.astype(F32) == pos_row[:, lanes] - place.astype(F32)
        tgt_row[:, lanes] += jnp.sum(jnp.where(hit, v, 0.0), axis=0, keepdims=True)

    m_row[:, :] = jnp.full((1, tok), -1e30, F32)
    s_row[:, :] = jnp.zeros((1, tok), F32)
    tgt_row[:, :] = jnp.zeros((1, tok), F32)
    segs = [(half, j) for half in TWO for j in TWO]

    def span(s):
        return (last_n, ha - last_n) if s else (0, last_n)

    def load(s, xx):
        r0, n = span(s)
        return [
            pltpu.make_async_copy(
                eg.at[xx[half] * 2 + j, pl.ds(half * ha + r0, n)], od.at[j, half, pl.ds(r0, n)], esem.at[s, half * 2 + j]
            )
            for half, j in segs
        ]

    def narrow_all(s, src):
        r0, n = span(s)
        for half, j in segs:
            def narrow(r, half=half, j=j):
                at = pl.multiple_of((half * 2 + j) * ha + r0 + r.start, r.size)
                dz[pl.ds(at, r.size), :] = src(half, j)[r, :].astype(BF16)

            _loop_rows(n, 16, narrow)

    def block(s, xx, loaded=False, with_few=False):
        r0, n = span(s)
        if not loaded:
            for cp in load(s, xx):
                cp.wait()
            narrow_all(s, lambda half, j: od.at[j, half, pl.ds(r0, n)])
        left = [VOCAB_REAL - ((zy * 8 + xx[half] * 2 + j) * rows + half * ha + r0) for half, j in segs]
        w = nt // chunk
        deep = SLOTS // w

        def out(t):
            u = lax.rem(t, deep) * w
            return [
                pltpu.make_async_copy(
                    tst.at[u + i, pl.ds(m * n, n)],
                    zh.at[t * w + i, pl.ds(pl.multiple_of((xx[half] * 2 + half) * rm + j * ha + r0, 8), n)],
                    zsem.at[u + i, m],
                )
                for i in range(w)
                for m, (half, j) in enumerate(segs)
            ]

        @pl.loop(0, tok // nt)
        def _(t):
            @pl.when(t >= deep)
            def _():
                for cp in out(t - deep):
                    cp.wait()

            lanes = pl.ds(pl.multiple_of(t * nt, nt), nt)
            lhs = [dz[(half * 2 + j) * ha + r0 : (half * 2 + j) * ha + r0 + n, :] for half, j in segs]
            if with_few:
                lhs.append(dz[ext_at : ext_at + FEW, :])
            v = product(jnp.concatenate(lhs, axis=0), lanes)
            v, v_few = v[: 4 * n], v[4 * n :]
            r = lax.broadcasted_iota(jnp.int32, (n, nt), 0)
            v = [jnp.where(r < left[m], v[m * n : (m + 1) * n], -jnp.inf) for m in range(len(segs))]
            for part_v, (half, j) in zip(v, segs):
                add_target(part_v, (xx[half] * 2 + half) * rm + j * ha + r0, lanes)
            u = lax.rem(t, deep) * w
            for i in range(w):
                for m in range(len(segs)):
                    tst[u + i, m * n : (m + 1) * n, :] = v[m][:, i * chunk : (i + 1) * chunk]
            if with_few:
                r = lax.broadcasted_iota(jnp.int32, v_few.shape, 0)
                ok = ((r & 7) < rows - rm) & ((zy * 8 + (r >> 3)) * rows + rm + (r & 7) < VOCAB_REAL)
                v_few = jnp.where(ok, v_few, -jnp.inf)
                few[:, lanes] = v_few
                add_target(v_few, jnp.int32(dm.main), lanes)
                v.append(v_few)
            v = jnp.concatenate(v, axis=0)
            for cp in out(t):
                cp.start()
            add_stats(v, lanes)

        for t in range(deep):
            for cp in out(t + tok // nt - deep):
                cp.wait()

    def both(xx):
        for s in (1, 0):
            for cp in load(s, xx):
                cp.start()
        block(1, xx)
        block(0, xx)

    def turn(xx):
        for half in TWO:
            base = pl.multiple_of((xx[half] * 2 + half) * rm, rm)

            @pl.loop(0, dim // 128)
            def _(d, half=half, base=base):
                at = pl.ds(pl.multiple_of(d * 128, 128), 128)
                etv[at, pl.ds(base, rm)] = dz[half * rm : (half + 1) * rm, at].T

    with scope("own"):
        s_o.wait_recv()
        both((x, x))
        turn((x, x))

    with scope("wait_1"):
        r_a.wait_recv()
        f1, f0 = pl.ds(last_n, ha - last_n), pl.ds(0, last_n)
        r_f1 = piece(slot(x_m), f1, xp)
        r_f0 = remote(eg.at[slot(x_m), f0], sst.at[c, f0], xp)
        d = [piece(slot(x_m), half_a, sib)]
        l_b.wait_recv()
        g1, g0 = pl.ds(ha + last_n, ha - last_n + 8), pl.ds(ha, last_n)
        l_f1 = piece(slot(x_p), g1, xm)
        l_f0 = remote(eg.at[slot(x_p), g0], sst.at[c, pl.ds(last_n, last_n)], xm)
        d.append(piece(slot(x_p), half_b, sib))
        for cp in d:
            cp.wait_recv()

    with scope("near_1"):
        both((x_m, x_p))
        turn((x_m, x_p))

    with scope("wait_2"):
        r_b.wait_recv()
        d = [piece(slot(x_m), half_b, sib)]
        l_a.wait_recv()
        d.append(piece(slot(x_p), half_a, sib))
        for cp in d:
            cp.wait_recv()

    with scope("near_2"):
        both((x_p, x_m))
        turn((x_p, x_m))

    with scope("wait_3"):
        r_f1.wait_recv()
        d = [piece(slot(x_far), f1, sib)]
        l_f1.wait_recv()
        d.append(piece(slot(x_far), g1, sib))
        for cp in d:
            cp.wait_recv()

    far = (x_far, x_far)
    with scope("far_1"):
        for cp in load(1, far):
            cp.start()
        ext_loads = [local(eg.at[s, pl.ds(rm, 8)], few.at[pl.ds(s * 8, 8)], lsem.at[s]) for s in range(8)]
        for cp in ext_loads:
            cp.wait()
        dz[ext_at : ext_at + FEW, :] = few[...].astype(BF16)
        dz[ext_at + FEW : ext_at + 128, :] = jnp.zeros((FEW, dim), BF16)
        block(1, far, with_few=True)

    with scope("wait_4"):
        r_f0.wait_recv()
        l_f0.wait_recv()
        both_last = sst.at[c, pl.ds(0, 2 * last_n)]
        over = _remote(both_last, both_last, send, recv, next(ids), sib)
        over.start()
        over.wait_recv()

    with scope("far_0"):
        narrow_all(0, lambda half, j: sst.at[j, pl.ds(half * last_n, last_n)])
        over.wait_send()
        for s in TWO:
            pl.semaphore_signal(free.at[s], inc=1, device_id=(sib,), device_id_type=MESH)
        block(0, far, loaded=True)

    with scope("turn_far"):
        lse_row[:, :] = m_row[:, :] + jnp.log(s_row[:, :]) * LOG2E
        scps = [_remote(lse_row, got.at[k], send, recv, next(ids), p) for k, p in enumerate(near)]
        for cp in scps:
            cp.start()
        turn(far)

        @pl.loop(0, dim // 128)
        def _(i):
            at = pl.ds(pl.multiple_of(i * 128, 128), 128)
            etv[at, dm.main : dm.wide] = dz[ext_at : ext_at + 128, at].T

    wide = 2 * rm

    at_dht = SLOTS - 4

    def chunk_of(zz, yy):
        return _mod4(zz) * 4 + _rem(yy + 8, 4)

    def all_far(i):
        return x_far * wide + i // 16 * rm, _rem(i, 16)

    def in_order(i):
        n = i // 3
        m = n - 7
        k = _pick(n < 7, chunk_of(z + n - 1, y + 2), chunk_of(z + 3 + m // 3, y + 3 + _rem(m + 9, 3)))
        return _mod4(x + 3 + _rem(i, 3)) * wide, _pick(n < 4, chunk_of(z + 2, n), k)

    def later(i):
        return in_order(i + SLOTS)

    def zload(where, i, ring, n):
        at, k = where(i)
        s = _rem(i, ring)
        src = zh.at[k, pl.ds(pl.multiple_of(at, rm), n)]
        return pltpu.make_async_copy(src, tst.at[s, pl.ds(0, n)], tsem.at[s])

    def zahead(where, ring, n):
        for i in range(ring):
            zload(where, i, ring, n).start()

    with scope("stats"):
        zahead(all_far, SLOTS, rm)
        for cp in scps:
            cp.wait_recv()
            cp.wait_send()
        top = lse_row[:, :]
        for k in range(len(near)):
            top = jnp.maximum(top, got[k])
        s = jnp.exp2(lse_row[:, :] - top)
        for k in range(len(near)):
            s = s + jnp.exp2(got[k] - top)
        lse_row[:, :] = top + jnp.log(s) * LOG2E

    def dz_part(v, place, at, lanes):
        r = lax.broadcasted_iota(jnp.int32, v.shape, 0).astype(F32)
        hit = r == pos_row[:, lanes] - place.astype(F32)
        p = jnp.exp2(v - lse_row[:, lanes])
        dz[at, lanes] = (jnp.where(hit, p - 1.0, p) * w_row[:, lanes]).astype(BF16)

    step = min(128, rm)

    def dz_rows(where, start, stop, last_tile, ring, n):
        @pl.loop(start, stop)
        def _(i):
            @pl.when((i > 0) & (i + ring - 1 < last_tile))
            def _():
                zload(where, i + ring - 1, ring, n).start()

            zload(where, i, ring, n).wait()
            row, k = where(i)
            lanes = pl.ds(pl.multiple_of(k * chunk, chunk), chunk)

            @pl.loop(0, n // step)
            def _(j):
                at = pl.multiple_of(row + j * step, step)
                r = pl.ds(pl.multiple_of(j * step, step), step)
                dz_part(tst[lax.rem(i, ring), r, :], at, pl.ds(at, step), lanes)

    def dz_far(start, stop):
        dz_rows(all_far, start, stop, 32, SLOTS, rm)

    with scope("dz_far"):
        dz_far(0, 16)

    nd = min(1024, dim)
    few_rows = pl.ds(dm.main, FEW)

    def de_block(xx, half, s, with_few=False):
        at = pl.ds(pl.multiple_of((xx * 2 + half) * rm, rm), rm)

        @pl.loop(0, dim // nd)
        def _(i):
            lanes = pl.ds(pl.multiple_of(i * nd, nd), nd)
            lhs = jnp.concatenate([dz[at, :], dz[few_rows, :]], axis=0) if with_few else dz[at, :]
            v = jnp.dot(lhs, hv[:, lanes], preferred_element_type=F32)
            for j in TWO:
                od[s, j, 0:ha, lanes] = v[j * ha : (j + 1) * ha]
            if with_few:
                few[:, lanes] = v[rm:]

        n = ha + 8 * half
        if half:
            for j in TWO:
                od[s, j, ha : ha + 8, :] = few[pl.ds(pl.multiple_of((xx * 2 + j) * 8, 8), 8), :]
        pl.semaphore_wait(free.at[s], 1)
        cp = _remote(od.at[s, 1 - c, pl.ds(0, n)], sst.at[s, pl.ds(0, n)], send, recv, next(ids), sib)
        cp.start()
        return half, s, n, cp

    def early(blk, src):
        half, s, n, cp = blk
        cp.wait_send()
        return local(src.at[pl.ds(half * ha, n)], od.at[s, 1 - c, pl.ds(0, n)], lsem.at[s])

    def sum_add(blk, to, more=None):
        half, s, n, cp = blk
        cp.wait_recv()
        if more is not None:
            more.wait()

        def add(r):
            v = od[s, c, r, :] + sst[s, r, :]
            od[s, c, r, :] = v if more is None else v + od[s, 1 - c, r, :]

        _loop_rows(n, 8, add)
        if more is None:
            pl.semaphore_signal(free.at[s], inc=1, device_id=(sib,), device_id_type=MESH)
            cp.wait_send()
        return local(od.at[s, c, pl.ds(0, n)], to.at[pl.ds(half * ha, n)], dsem.at[s])

    def ring_sum(xx, rows_, n, src, s, dst, dev):
        lds = [
            local(q_h.at[xx, rows_], od.at[s, 0, pl.ds(0, n)], lsem.at[0]),
            local(src, od.at[s, 1, pl.ds(0, n)], lsem.at[1]),
        ]
        for cp in lds:
            cp.wait()
        _add_rows(od.at[s, 0, pl.ds(0, n)], [od.at[s, 1, pl.ds(0, n)]], 8)
        local(od.at[s, 0, pl.ds(0, n)], q_h.at[xx, rows_], lsem.at[0]).wait()
        return remote(q_h.at[xx, rows_], dst, dev)

    stores = []

    def flush():
        while stores:
            stores.pop().wait()

    def tiles(q, where, between=None):
        flush()

        def outs(i):
            p, ab = where(i)
            r = pl.ds(q * h, h)
            dsts = [dhp.at[ab * 2 + j, p, r] if q == 0 else dhp.at[p, ab * 2 + j, r] for j in TWO]
            return [
                pltpu.make_async_copy(tst.at[at_dht + i * 2 + j, pl.ds(0, h)], dst, hsem.at[i * 2 + j])
                for j, dst in enumerate(dsts)
            ]

        @pl.loop(0, 2)
        def _(i):
            if between is not None:
                pl.when(i > 0)(between)
            p, ab = where(i)
            ks = [(ab * 2 + j) * 4 + p if q == 0 else p * 4 + ab * 2 + j for j in TWO]
            rhs = jnp.concatenate([dz[:, pl.ds(pl.multiple_of(k * chunk, chunk), chunk)] for k in ks], axis=1)
            v = jnp.dot(etv[q * h : (q + 1) * h, :], rhs, preferred_element_type=F32)
            for j in TWO:
                tst[at_dht + i * 2 + j, 0:h, :] = v[:, j * chunk : (j + 1) * chunk]
            for cp in outs(i):
                cp.start()

        for i in TWO:
            stores.extend(outs(i))

    def part(q, p, lo, n):
        r = pl.ds(q * h, h)
        if q == 0:
            return dhp.at[pl.ds(lo, n), p, r]
        return dhp.at[p, pl.ds(lo, n), r]

    def one(q, p, i):
        r = pl.ds(q * h, h)
        return dhp.at[i, p, r] if q == 0 else dhp.at[p, i, r]

    ring1, ring2 = ((yp, ym), (zp, zm)), ((zp, zm), (yp, ym))
    pos1, pos2 = (y, z), (z, y)
    first, second = ({}, {}), ({}, {})

    def send_far(q):
        flush()
        p, (rt, lt) = pos1[q], ring1[q]
        first[q]["far_r"] = remote(part(q, _mod4(p + 2), 0, 2), ya.at[q], rt)
        first[q]["far_l"] = remote(part(q, _mod4(p + 2), 2, 2), yb.at[q], lt)

    def send_near(q):
        flush()
        p, (rt, lt) = pos1[q], ring1[q]
        first[q]["near_r"] = remote(part(q, _mod4(p + 1), 2, 2), yl.at[q, pl.ds(2, 2)], rt)
        first[q]["near_l"] = remote(part(q, _mod4(p - 1), 0, 2), yr.at[q, pl.ds(0, 2)], lt)

    def fetch(i, src):
        return local(src, tst.at[i, pl.ds(0, h)], tsem.at[i])

    def pass_on(q):
        flush()
        p, (rt, lt) = pos1[q], ring1[q]
        lds = [fetch(i, one(q, _mod4(p + 1), i)) for i in TWO]
        lds += [fetch(2 + i, one(q, _mod4(p - 1), 2 + i)) for i in TWO]
        first[q]["far_r"].wait_recv()
        for i in TWO:
            lds[i].wait()
            _add_rows(ya.at[q, i], [tst.at[i, pl.ds(0, h)]], min(FEW, h))
        first[q]["sum_r"] = remote(ya.at[q], yl.at[q, pl.ds(0, 2)], rt)
        first[q]["far_l"].wait_recv()
        for i in TWO:
            lds[2 + i].wait()
            _add_rows(yb.at[q, i], [tst.at[2 + i, pl.ds(0, h)]], min(FEW, h))
        first[q]["sum_l"] = remote(yb.at[q], yr.at[q, pl.ds(2, 2)], lt)

    lo, hi = pl.ds(0, hc), pl.ds(hc, hc)

    def second_phase(q):
        flush()
        r, (rt, lt) = pos2[q], ring2[q]
        r2, r1, rm1 = _mod4(r + 2), _mod4(r + 1), _mod4(r - 1)
        order = (r2, r1, rm1, r)
        lds = [fetch(i, one(q, pos1[q], k)) for i, k in enumerate(order)]
        for k in NEAR_KEYS:
            first[q][k].wait_recv()
        lds2 = [fetch(4 + i, yr.at[q, k]) for i, k in enumerate(order)]
        for i, k in enumerate(order):
            lds[i].wait()
            lds2[i].wait()
            _add_rows(yl.at[q, k], [tst.at[i, pl.ds(0, h)], tst.at[4 + i, pl.ds(0, h)]], min(FEW, h))
            if i == 0:
                second[q]["far_r"] = remote(yl.at[q, r2, lo], za.at[q], rt)
                second[q]["far_l"] = remote(yl.at[q, r2, hi], zb.at[q], lt)
            if i == 1:
                second[q]["near_r"] = remote(yl.at[q, r1, hi], zl.at[q, hi], rt)
            if i == 2:
                second[q]["near_l"] = remote(yl.at[q, rm1, lo], zr.at[q, lo], lt)

    def second_pass(q):
        r, (rt, lt) = pos2[q], ring2[q]
        r1, rm1 = _mod4(r + 1), _mod4(r - 1)
        second[q]["far_r"].wait_recv()
        _add_rows(yl.at[q, r1, lo], [za.at[q]], min(FEW, hc))
        second[q]["sum_r"] = remote(yl.at[q, r1, lo], zl.at[q, lo], rt)
        second[q]["far_l"].wait_recv()
        _add_rows(yl.at[q, rm1, hi], [zb.at[q]], min(FEW, hc))
        second[q]["sum_l"] = remote(yl.at[q, rm1, hi], zr.at[q, hi], lt)

    def last(q):
        r = pos2[q]
        for k in NEAR_KEYS:
            second[q][k].wait_recv()
        n = min(128, h)

        @pl.loop(0, h // n)
        def _(i):
            at = pl.ds(pl.multiple_of(i * n, n), n)
            v = yl[q, r, at, :] + zl[q, at, :] + zr[q, at, :]
            od[0, 0, 0:chunk, pl.ds(pl.multiple_of(q * h + i * n, n), n)] = (v * (1.0 / LOGIT_SCALE)).T

    def tiles_far(q, between=None):
        tiles(q, lambda i: (_mod4(pos1[q] + 2), i), between)

    def tiles_near(q):
        tiles(q, lambda i: (_mod4(pos1[q] + 1 + 2 * i), 1 - i))

    def tiles_pass(q):
        tiles(q, lambda i: (_mod4(pos1[q] + 1 + 2 * i), i))

    def tiles_own(q):
        tiles(q, lambda i: (pos1[q], i))

    all_later = 48 - SLOTS

    def dz_first(start, stop):
        dz_rows(in_order, start, stop, SLOTS, SLOTS, wide)

    def dz_later(start, stop):
        dz_rows(later, start, stop, all_later, at_dht, wide)

    with scope("de_far"):
        b0 = de_block(x_far, 0, 0)
        dz_far(16, 32)
        zahead(in_order, SLOTS, wide)
        for l in range(0, tok, nt):
            lanes = pl.ds(l, nt)
            dz_part(few[:, lanes], jnp.int32(dm.main), few_rows, lanes)
        dz[dm.main + FEW : dm.wide, :] = jnp.zeros((FEW, tok), BF16)
        b1 = de_block(x_far, 1, 1, True)
    with scope("dz_1"):
        c0 = sum_add(b0, q_h.at[x_far])
        dz_first(0, 8)
        c0.wait()
        e0 = remote(q_h.at[x_far, half_a], xa, xp)
        dz_first(8, SLOTS)
        zahead(later, at_dht, wide)
        c1 = sum_add(b1, q_h.at[x_far])
    with scope("dh_far1"):
        e1 = _remote(q_h.at[x_far, half_b], xb, send, recv, next(ids), xm)
        sent.append(e1)

        def send_e1():
            c1.wait()
            e1.start()

        tiles_far(1, send_e1)
    with scope("dz_2"):
        dz_later(0, 9)
        send_far(1)
    with scope("dh_far0"):
        tiles_far(0)
    with scope("dz_3"):
        dz_later(9, 13)
        send_far(0)
        dz_later(13, all_later)
    with scope("de_2"):
        b2 = de_block(x_p, 1, 0)
        b3 = de_block(x_m, 0, 1)
        c2 = sum_add(b2, q_h.at[x_p])
    with scope("dh_near"):
        tiles_near(1)
        c2.wait()
        e2 = remote(q_h.at[x_p, half_b], xe.at[half_b], xp)
        c3 = sum_add(b3, q_h.at[x_m])
        send_near(1)
        tiles_near(0)
        c3.wait()
        e3 = remote(q_h.at[x_m, half_a], xe.at[half_a], xm)
        send_near(0)
    with scope("dh_pass"):
        tiles_pass(1)
        tiles_pass(0)
        pass_on(1)
    with scope("de_4"):
        b4 = de_block(x_p, 0, 0)
        pass_on(0)
        b5 = de_block(x_m, 1, 1)
        c4 = sum_add(b4, q_h.at[x_p])
    with scope("dh_own"):
        tiles_own(1)
        c5 = sum_add(b5, q_h.at[x_m])
        tiles_own(0)
        c4.wait()
        c5.wait()
    old = list(sent)
    sent.clear()
    with scope("ring"):
        e0.wait_recv()
        e4 = ring_sum(x_p, half_a, ha, xa, 0, xs.at[half_a], xp)
        e1.wait_recv()
        e5 = ring_sum(x_m, half_b, ha + 8, xb, 1, xs.at[half_b], xm)
    with scope("de_6"):
        b6 = de_block(x, 0, 0)
    with scope("de_7"):
        b7 = de_block(x, 1, 1)
        xo_load = local(x4.at[zy, xc], dz.at[pl.ds(0, chunk)], xsem.at[0])
    with scope("second_1"):
        second_phase(1)
    with scope("second_0"):
        second_phase(0)
    with scope("spass_1"):
        second_pass(1)
    with scope("sum_6"):
        e3.wait_recv()
        c6 = early(b6, xe)
        e2.wait_recv()
        c7 = early(b7, xe)
        c6 = sum_add(b6, q_o, c6)
        c7 = sum_add(b7, q_o, c7)
    with scope("spass_0"):
        second_pass(0)
        c6.wait()
        c7.wait()
    with scope("last_1"):
        for cp in old:
            cp.wait_send()
        last(1)
    with scope("last_0"):
        last(0)

    with scope("finish"):
        xo_load.wait()
        sm[...] = jnp.zeros_like(sm)

        def finish(r):
            v = dz[r, :].astype(F32)
            inv = lax.rsqrt(jnp.mean(v * v, axis=-1, keepdims=True) + NORM_EPS)
            x_hat = v * inv
            dh = od[0, 0, r, :]
            sm[:, 0:dim] += jnp.sum(dh * x_hat, axis=0, keepdims=True)
            u = dh * gain
            od[0, 1, r, :] = inv * (u - x_hat * jnp.mean(u * x_hat, axis=-1, keepdims=True))

        _loop_rows(chunk, 16, finish)
        lse = jnp.where(zy == 0, lse_row[:, :], 0.0)
        loss = jnp.sum(w_row[:, :] * (lse - tgt_row[:, :]))
        sm[:, dim : dim + 128] = jnp.full((1, 128), loss / LOG2E)

    with scope("small_1"):
        cps = [remote(sm, got1.at[k], p) for k, p in enumerate(near)]
        dx_copy = local(od.at[0, 1, pl.ds(0, chunk)], dx_out, osem.at[0])
        for cp in cps:
            cp.wait_recv()
    with scope("small_2"):
        tot = sm[...]
        for k in range(len(near)):
            tot = tot + got1[k]
        total_v[...] = tot
        cps = [remote(total_v, got2.at[k], p) for k, p in enumerate(line)]
        mine = local(total_v, got2.at[len(line)], osem.at[1])
    with scope("small_3"):
        for cp in cps:
            cp.wait_recv()
        mine.wait()
    with scope("ring_end"):
        for cp in (e4, e5):
            cp.wait_recv()
        dx_copy.wait()
    for cp in sent:
        cp.wait_send()


def _run(dm, x4, table, gain, labels, mask):
    hbm, vm = pl.BlockSpec(memory_space=HBM), pl.BlockSpec(memory_space=VMEM)
    sd = jax.ShapeDtypeStruct
    d, tok, h, ck, pad, ha = dm.dim, dm.tok, dm.h, dm.chunk, dm.pad, dm.ha
    line, quad, pair = VMEM((1, tok), F32), VMEM((2, 2, h, ck), F32), VMEM((2, h, ck), F32)
    part, shard = VMEM((2, h // 2, ck), F32), sd((pad, d), F32)
    out = pl.pallas_call(
        functools.partial(_kernel, dm),
        name="head",
        out_shape=(
            sd((ck, d), F32), sd((8, 1, d + 128), F32),
            shard, shard, shard,
            sd((8, pad, d), F32), sd((16, dm.main, ck), F32),
            sd((4, pad, d), F32), sd((ha, d), F32), sd((ha + 8, d), F32),
            sd((4, 4, d, ck), F32), sd((2, 4, h, ck), F32),
        ),
        in_specs=[hbm, vm, vm, vm, vm],
        out_specs=[hbm] * 12,
        scratch_shapes=[
            VMEM((tok, d), BF16), VMEM((d, dm.wide), BF16), VMEM((dm.wide, tok), BF16),
            VMEM((2, 2, ha + 8, d), F32), VMEM((2, ha + 8, d), F32), VMEM((FEW, d), F32), VMEM((8, d), F32),
            quad, quad, VMEM((2, 4, h, ck), F32),
            part, part, pair, pair,
            VMEM((SLOTS, max(h, 2 * dm.rm), ck), F32),
            line, line, line, line, line, line, VMEM((15, 1, tok), F32),
            VMEM((1, d + 128), F32), VMEM((15, 1, d + 128), F32), VMEM((1, d + 128), F32),
            DMA((96,)), DMA((96,)), pltpu.SemaphoreType.REGULAR((2,)),
            DMA((2, 4)), DMA((4,)), DMA((SLOTS, 4)), DMA((SLOTS,)), DMA((4,)), DMA((2,)), DMA((2,)), DMA((8,)),
        ],
        compiler_params=pltpu.CompilerParams(
            collective_id=0, has_side_effects=True, vmem_limit_bytes=67043328
        ),
    )(x4, table, gain, labels, mask)
    return _write_out(dm, out[2:4], *out[:2])


def _write_kernel(own, ring, dx, small, de_o, dx_o, dg_o, loss_o):
    de_o[:, :] = (own[:, :] + ring[:, :]) * (1.0 / LOGIT_SCALE)
    dx_o[:, :] = dx[:, :]
    total = jnp.sum(small[:, :, :], axis=0)
    d = dg_o.shape[1]
    dg_o[:, :] = total[:, :d]
    loss_o[:, :] = total[:, d : d + 1]


def _write_out(dm, parts, dx, small):
    d, step, blocks = dm.dim, dm.ha + 8, 2
    sd = jax.ShapeDtypeStruct
    some = pl.BlockSpec((step, d), lambda i: (i, 0))
    half = pl.BlockSpec((dm.chunk // blocks, d), lambda i: (i, 0))
    row, one = pl.BlockSpec((1, d), lambda i: (0, 0)), pl.BlockSpec((1, 1), lambda i: (0, 0))
    rows = pl.BlockSpec(small.shape, lambda i: (0, 0, 0))
    return pl.pallas_call(
        _write_kernel,
        name="write_out",
        grid=(blocks,),
        out_shape=(sd((dm.rows, d), F32), sd((dm.chunk, d), F32), sd((1, d), F32), sd((1, 1), F32)),
        in_specs=[some, some, half, rows],
        out_specs=(some, half, row, one),
    )(*parts, dx, small)


def solution(mesh):
    group = mesh.shape[AXIS]

    def local_step(residual, labels, loss_mask, norm_gain, table_shard):
        tokens, dim = residual.shape
        rows = table_shard.shape[0]
        dm = Dims(tokens, dim, rows, group)
        x4 = residual.reshape(16, 8, dm.chunk, dim)
        lab = labels.reshape(16, 8, 1, dm.chunk)
        msk = loss_mask.reshape(16, 8, 1, dm.chunk)
        d_embed, d_res, d_gain, loss = _run(dm, x4, table_shard, norm_gain[None, :], lab, msk)
        return loss.reshape(()), d_res, d_embed, d_gain.reshape(dim)

    return jax.shard_map(
        local_step,
        mesh=mesh,
        in_specs=(P(), P(), P(), P(), P(AXIS, None)),
        out_specs=(P(), P(AXIS, None), P(AXIS, None), P()),
        check_vma=False,
    )
```

```python
import functools
import itertools
import math

import jax
import jax.numpy as jnp
from jax import lax
from jax.experimental import pallas as pl
from jax.experimental.pallas import tpu as pltpu
from jax.sharding import PartitionSpec as P

VOCAB_REAL = 49155
LOGIT_SCALE = 6.0
NORM_EPS = 1e-6

AXIS = "vp"
MESH = pl.DeviceIdType.MESH
F32 = jnp.float32
BF16 = jnp.bfloat16
HBM = pltpu.HBM
VMEM = pltpu.VMEM
DMA = pltpu.SemaphoreType.DMA


def _coords():
    me = lax.axis_index(AXIS)
    return me // 32, (me // 8) % 4, (me // 2) % 4, me % 2


def _dev(z, y, x, c):
    return ((z * 4 + y) * 4 + x) * 2 + c


def _mod4(v):
    return lax.rem(v + 8, 4)


def _barrier(peers):
    sem = pltpu.get_barrier_semaphore()
    for p in peers:
        pl.semaphore_signal(sem, inc=1, device_id=(p,), device_id_type=MESH)
    pl.semaphore_wait(sem, len(peers))


def _remote(src, dst, send, recv, k, dev):
    return pltpu.make_async_remote_copy(
        src_ref=src,
        dst_ref=dst,
        send_sem=send.at[k],
        recv_sem=recv.at[k],
        device_id=(dev,),
        device_id_type=MESH,
    )


class Dims:
    def __init__(self, tokens, dim, rows, group):
        self.dim, self.rows = dim, rows
        unit = 128 if rows >= 128 else 64
        self.rm = rows // unit * unit
        self.ha = self.rm // 2
        mid, low = self.ha // 2, self.ha // 96 * 16
        self.cuts = ((mid, self.ha - mid), (low, mid - low), (0, low))
        self.pad = self.rm + 8
        self.chunk = tokens // group
        self.tok = 16 * self.chunk
        self.nt = 4 * self.chunk
        self.main = 8 * self.rm
        self.wide = self.main + 128
        self.h = dim // 2


def _rem(a, b):
    return a % b if isinstance(a, int) else lax.rem(a, b)


def _pick(test, a, b):
    return (a if test else b) if isinstance(test, bool) else jnp.where(test, a, b)


def _loop_rows(rows, step, fn):
    @pl.loop(0, rows // step)
    def _(i):
        fn(pl.ds(pl.multiple_of(i * step, step), step))


def _add_rows(dst, srcs, step):
    def add(r):
        acc = dst[r, :]
        for s in srcs:
            acc = acc + s[r, :]
        dst[r, :] = acc

    _loop_rows(dst.shape[0], step, add)


SLOTS = 12
FEW = 64
TWO = range(2)
LOG2E = math.log2(math.e)
NEAR_KEYS = ("near_r", "near_l", "sum_r", "sum_l")
scope = jax.named_scope


def _kernel(
    dm, x4, e_ref, g_ref, lab, msk,
    dx_out, got2, q_o, xs, xe, eg, zh, q_h, xa, xb, dhp, yr,
    hv, etv, dz, od, sst, few, oext, ya, yb, yl, za, zb, zl, zr, tst,
    m_row, s_row, w_row, pos_row, lse_row, tgt_row, got, sm, got1, total_v,
    send, recv,
    free, esem, xsem, zsem, tsem, hsem, dsem, osem, lsem,
):
    z, y, x, c = _coords()
    xc, zy = x * 2 + c, z * 4 + y
    rows, rm, ha, dim, h = dm.rows, dm.rm, dm.ha, dm.dim, dm.h
    chunk, tok, nt, hc = dm.chunk, dm.tok, dm.nt, dm.h // 2
    x_far, x_p, x_m = _mod4(x + 2), _mod4(x + 1), _mod4(x - 1)
    xp, xm = _dev(z, y, x_p, c), _dev(z, y, x_m, c)
    yp, ym = _dev(z, _mod4(y + 1), x, c), _dev(z, _mod4(y - 1), x, c)
    zp, zm = _dev(_mod4(z + 1), y, x, c), _dev(_mod4(z - 1), y, x, c)
    sib = _dev(z, y, x, 1 - c)
    near = [_dev(_mod4(z + a), _mod4(y + b), x, c) for a in range(4) for b in range(4) if a or b]
    line = [_dev(z, y, _mod4(x + a), lax.rem(c + b, 2)) for a in range(4) for b in TWO if a or b]
    bar = pltpu.get_barrier_semaphore()
    for p in (*near, *line):
        pl.semaphore_signal(bar, inc=1, device_id=(p,), device_id_type=MESH)
    sent = []
    ids = itertools.count()

    def remote(src, dst, dev):
        cp = _remote(src, dst, send, recv, next(ids), dev)
        cp.start()
        sent.append(cp)
        return cp

    def local(src, dst, sem):
        cp = pltpu.make_async_copy(src, dst, sem)
        cp.start()
        return cp

    x_at, ext_at = 2 * rm, 4 * rm

    def xload(k):
        s = lax.rem(k, 4)
        to = dz.at[pl.ds(pl.multiple_of(x_at + s * chunk, chunk), chunk)]
        return pltpu.make_async_copy(x4.at[k, xc], to, xsem.at[s])

    with scope("prep"):
        for k in range(3):
            xload(k).start()
        own = xc
        for j in TWO:
            def widen(r, j=j):
                od[0, j, r, :] = e_ref[pl.ds(j * ha + r.start, r.size), :].astype(F32)

            _loop_rows(ha, 16, widen)
        oext[...] = jnp.zeros_like(oext)
        oext[0 : rows - rm, :] = e_ref[rm:rows, :].astype(F32)
        cps = [local(od.at[0, j, pl.ds(0, ha)], eg.at[own, pl.ds(j * ha, ha)], esem.at[j]) for j in TWO]
        cps.append(local(oext, eg.at[own, pl.ds(rm, 8)], esem.at[2]))
        for cp in cps:
            cp.wait()
        pl.semaphore_wait(bar, 22)

    half_a, half_b = pl.ds(0, ha), pl.ds(ha, ha + 8)

    def piece(s, r, dev):
        return remote(eg.at[s, r], eg.at[s, r], dev)

    def slot(xx):
        return xx * 2 + c

    r_a, l_b = piece(own, half_a, xp), piece(own, half_b, xm)
    s_o = piece(own, pl.ds(0, dm.pad), sib)
    r_b, l_a = piece(own, half_b, xp), piece(own, half_a, xm)

    gain = g_ref[...]

    with scope("norm"):
        @pl.loop(0, 16)
        def _(k):
            @pl.when(k < 13)
            def _():
                xload(k + 3).start()

            xload(k).wait()

            def norm(r):
                v = dz[pl.ds(pl.multiple_of(x_at + lax.rem(k, 4) * chunk + r.start, r.size), r.size), :].astype(F32)
                inv = lax.rsqrt(jnp.mean(v * v, axis=-1, keepdims=True) + NORM_EPS)
                hv[pl.ds(pl.multiple_of(k * chunk + r.start, r.size), r.size), :] = (v * inv * gain).astype(BF16)

            _loop_rows(chunk, 16, norm)

    with scope("labels"):
        total = jnp.sum(msk[...])
        for k in range(16):
            at = pl.ds(k * chunk, chunk)
            w_row[:, at] = msk[k, xc] / total
            q = lab[k, xc] - zy * (8 * rows)
            s = jnp.zeros_like(q)
            for i in range(1, 8):
                s = s + jnp.where(q >= i * rows, 1, 0)
            r = q - s * rows
            up = jnp.where(r >= ha, 1, 0)
            at_main = ((s // 2 * 2 + up) * 2 + s % 2) * ha + r - up * ha
            at_ext = dm.main + s * 8 + r - rm
            place = jnp.where(r < rm, at_main, at_ext)
            pos_row[:, at] = jnp.where((q >= 0) & (q < 8 * rows), place, -1).astype(F32)

    def product(lhs, lanes):
        v = lax.dot_general(lhs, hv[lanes, :], (((1,), (1,)), ((), ())), preferred_element_type=F32)
        return v * (LOG2E / LOGIT_SCALE)

    def add_stats(v, lanes):
        m_old, s_old = m_row[:, lanes], s_row[:, lanes]
        m = jnp.maximum(m_old, jnp.max(v, axis=0, keepdims=True))
        s = jnp.sum(jnp.exp2(v - m), axis=0, keepdims=True)
        m_row[:, lanes] = m
        s_row[:, lanes] = s_old * jnp.exp2(m_old - m) + s

    def add_target(v, place, lanes):
        r = lax.broadcasted_iota(jnp.int32, v.shape, 0)
        hit = r.astype(F32) == pos_row[:, lanes] - place.astype(F32)
        tgt_row[:, lanes] += jnp.sum(jnp.where(hit, v, 0.0), axis=0, keepdims=True)

    m_row[:, :] = jnp.full((1, tok), -1e30, F32)
    s_row[:, :] = jnp.zeros((1, tok), F32)
    tgt_row[:, :] = jnp.zeros((1, tok), F32)
    segs = [(half, j) for half in TWO for j in TWO]

    def load(r0, n, xx):
        return [
            local(
                eg.at[xx[half] * 2 + j, pl.ds(half * ha + r0, n)], od.at[j, half, pl.ds(r0, n)], esem.at[half * 2 + j]
            )
            for half, j in segs
        ]

    def narrow_all(r0, n, src):
        for half, j in segs:
            def narrow(r, half=half, j=j):
                at = pl.multiple_of((half * 2 + j) * ha + r0 + r.start, r.size)
                dz[pl.ds(at, r.size), :] = src(half, j)[r, :].astype(BF16)

            _loop_rows(n, 16, narrow)

    def block(r0, n, xx, loads=(), with_few=False):
        if loads:
            for cp in loads:
                cp.wait()
            narrow_all(r0, n, lambda half, j: od.at[j, half, pl.ds(r0, n)])
        left = [VOCAB_REAL - ((zy * 8 + xx[half] * 2 + j) * rows + half * ha + r0) for half, j in segs]
        w = nt // chunk
        deep = SLOTS // w

        def out(t):
            u = lax.rem(t, deep) * w
            return [
                pltpu.make_async_copy(
                    tst.at[u + i, pl.ds(m * n, n)],
                    zh.at[t * w + i, pl.ds(pl.multiple_of((xx[half] * 2 + half) * rm + j * ha + r0, 8), n)],
                    zsem.at[u + i, m],
                )
                for i in range(w)
                for m, (half, j) in enumerate(segs)
            ]

        @pl.loop(0, tok // nt)
        def _(t):
            @pl.when(t >= deep)
            def _():
                for cp in out(t - deep):
                    cp.wait()

            lanes = pl.ds(pl.multiple_of(t * nt, nt), nt)
            lhs = [dz[(half * 2 + j) * ha + r0 : (half * 2 + j) * ha + r0 + n, :] for half, j in segs]
            if with_few:
                lhs.append(dz[ext_at : ext_at + FEW, :])
            v = product(jnp.concatenate(lhs, axis=0), lanes)
            v, v_few = v[: 4 * n], v[4 * n :]
            r = lax.broadcasted_iota(jnp.int32, (n, nt), 0)
            v = [jnp.where(r < left[m], v[m * n : (m + 1) * n], -jnp.inf) for m in range(len(segs))]
            for part_v, (half, j) in zip(v, segs):
                add_target(part_v, (xx[half] * 2 + half) * rm + j * ha + r0, lanes)
            u = lax.rem(t, deep) * w
            for i in range(w):
                for m in range(len(segs)):
                    tst[u + i, m * n : (m + 1) * n, :] = v[m][:, i * chunk : (i + 1) * chunk]
            if with_few:
                r = lax.broadcasted_iota(jnp.int32, v_few.shape, 0)
                ok = ((r & 7) < rows - rm) & ((zy * 8 + (r >> 3)) * rows + rm + (r & 7) < VOCAB_REAL)
                v_few = jnp.where(ok, v_few, -jnp.inf)
                few[:, lanes] = v_few
                add_target(v_few, jnp.int32(dm.main), lanes)
                v.append(v_few)
            v = jnp.concatenate(v, axis=0)
            for cp in out(t):
                cp.start()
            add_stats(v, lanes)

        for t in range(deep):
            for cp in out(t + tok // nt - deep):
                cp.wait()

    def both(xx):
        block(0, ha, xx, load(0, ha, xx))

    def turn(xx):
        for half in TWO:
            base = pl.multiple_of((xx[half] * 2 + half) * rm, rm)

            @pl.loop(0, dim // 128)
            def _(d, half=half, base=base):
                at = pl.ds(pl.multiple_of(d * 128, 128), 128)
                etv[at, pl.ds(base, rm)] = dz[half * rm : (half + 1) * rm, at].T

    with scope("own"):
        s_o.wait_recv()
        both((x, x))
        turn((x, x))

    with scope("wait_1"):
        r_a.wait_recv()
        last_n = dm.cuts[-1][1]
        spans = [(pl.ds(r0, n), pl.ds(ha + r0, n + 8 * (r0 + n == ha))) for r0, n in dm.cuts]

        def far_pieces(xx, half, to):
            cps = [piece(slot(xx), pair[half], to) for pair in spans[:-1]]
            cps.append(remote(eg.at[slot(xx), spans[-1][half]], sst.at[c, pl.ds(half * last_n, last_n)], to))
            return cps

        r_f = far_pieces(x_m, 0, xp)
        d = [piece(slot(x_m), half_a, sib)]
        l_b.wait_recv()
        l_f = far_pieces(x_p, 1, xm)
        d.append(piece(slot(x_p), half_b, sib))
        for cp in d:
            cp.wait_recv()

    with scope("near_1"):
        both((x_m, x_p))
        turn((x_m, x_p))

    with scope("wait_2"):
        r_b.wait_recv()
        d = [piece(slot(x_m), half_b, sib)]
        l_a.wait_recv()
        d.append(piece(slot(x_p), half_a, sib))
        for cp in d:
            cp.wait_recv()

    with scope("near_2"):
        both((x_p, x_m))
        turn((x_p, x_m))

    far = (x_far, x_far)

    def far_arrived(i):
        d = []
        for cp, r in zip((r_f[i], l_f[i]), spans[i]):
            cp.wait_recv()
            d.append(piece(slot(x_far), r, sib))
        for cp in d:
            cp.wait_recv()

    with scope("wait_3"):
        far_arrived(0)
    with scope("far_a"):
        loads = load(*dm.cuts[0], far)
        ext_loads = [local(eg.at[s, pl.ds(rm, 8)], few.at[pl.ds(s * 8, 8)], lsem.at[s]) for s in range(8)]
        for cp in ext_loads:
            cp.wait()
        dz[ext_at : ext_at + FEW, :] = few[...].astype(BF16)
        dz[ext_at + FEW : ext_at + 128, :] = jnp.zeros((FEW, dim), BF16)
        block(*dm.cuts[0], far, loads, True)
    with scope("wait_4"):
        far_arrived(1)
    with scope("far_b"):
        block(*dm.cuts[1], far, load(*dm.cuts[1], far))

    with scope("wait_5"):
        r_f[-1].wait_recv()
        l_f[-1].wait_recv()
        both_last = sst.at[c, pl.ds(0, 2 * last_n)]
        over = _remote(both_last, both_last, send, recv, next(ids), sib)
        over.start()
        over.wait_recv()

    with scope("far_c"):
        narrow_all(0, last_n, lambda half, j: sst.at[j, pl.ds(half * last_n, last_n)])
        over.wait_send()
        for s in TWO:
            pl.semaphore_signal(free.at[s], inc=1, device_id=(sib,), device_id_type=MESH)
        block(0, last_n, far)

    with scope("turn_far"):
        lse_row[:, :] = m_row[:, :] + jnp.log(s_row[:, :]) * LOG2E
        scps = [_remote(lse_row, got.at[k], send, recv, next(ids), p) for k, p in enumerate(near)]
        for cp in scps:
            cp.start()
        turn(far)

        @pl.loop(0, dim // 128)
        def _(i):
            at = pl.ds(pl.multiple_of(i * 128, 128), 128)
            etv[at, dm.main : dm.wide] = dz[ext_at : ext_at + 128, at].T

    wide = 2 * rm

    at_dht = SLOTS - 4

    def chunk_of(zz, yy):
        return _mod4(zz) * 4 + _rem(yy + 8, 4)

    def all_far(i):
        return x_far * wide + i // 16 * rm, _rem(i, 16)

    def in_order(i):
        n = i // 3
        m = n - 7
        k = _pick(n < 7, chunk_of(z + n - 1, y + 2), chunk_of(z + 3 + m // 3, y + 3 + _rem(m + 9, 3)))
        return _mod4(x + 3 + _rem(i, 3)) * wide, _pick(n < 4, chunk_of(z + 2, n), k)

    def later(i):
        return in_order(i + SLOTS)

    def zload(where, i, ring, n):
        at, k = where(i)
        s = _rem(i, ring)
        src = zh.at[k, pl.ds(pl.multiple_of(at, rm), n)]
        return pltpu.make_async_copy(src, tst.at[s, pl.ds(0, n)], tsem.at[s])

    def zahead(where, ring, n):
        for i in range(ring):
            zload(where, i, ring, n).start()

    with scope("stats"):
        zahead(all_far, SLOTS, rm)
        for cp in scps:
            cp.wait_recv()
            cp.wait_send()
        top = lse_row[:, :]
        for k in range(len(near)):
            top = jnp.maximum(top, got[k])
        s = jnp.exp2(lse_row[:, :] - top)
        for k in range(len(near)):
            s = s + jnp.exp2(got[k] - top)
        lse_row[:, :] = top + jnp.log(s) * LOG2E

    def dz_part(v, place, at, lanes):
        r = lax.broadcasted_iota(jnp.int32, v.shape, 0).astype(F32)
        hit = r == pos_row[:, lanes] - place.astype(F32)
        p = jnp.exp2(v - lse_row[:, lanes])
        dz[at, lanes] = (jnp.where(hit, p - 1.0, p) * w_row[:, lanes]).astype(BF16)

    step = min(128, rm)

    def dz_rows(where, start, stop, last_tile, ring, n):
        @pl.loop(start, stop)
        def _(i):
            @pl.when((i > 0) & (i + ring - 1 < last_tile))
            def _():
                zload(where, i + ring - 1, ring, n).start()

            zload(where, i, ring, n).wait()
            row, k = where(i)
            lanes = pl.ds(pl.multiple_of(k * chunk, chunk), chunk)

            @pl.loop(0, n // step)
            def _(j):
                at = pl.multiple_of(row + j * step, step)
                r = pl.ds(pl.multiple_of(j * step, step), step)
                dz_part(tst[lax.rem(i, ring), r, :], at, pl.ds(at, step), lanes)

    def dz_far(start, stop):
        dz_rows(all_far, start, stop, 32, SLOTS, rm)

    with scope("dz_far"):
        dz_far(0, 16)

    nd = min(1024, dim)
    few_rows = pl.ds(dm.main, FEW)

    def de_block(xx, half, s, with_few=False):
        at = pl.ds(pl.multiple_of((xx * 2 + half) * rm, rm), rm)

        @pl.loop(0, dim // nd)
        def _(i):
            lanes = pl.ds(pl.multiple_of(i * nd, nd), nd)
            lhs = jnp.concatenate([dz[at, :], dz[few_rows, :]], axis=0) if with_few else dz[at, :]
            v = jnp.dot(lhs, hv[:, lanes], preferred_element_type=F32)
            for j in TWO:
                od[s, j, 0:ha, lanes] = v[j * ha : (j + 1) * ha]
            if with_few:
                few[:, lanes] = v[rm:]

        n = ha + 8 * half
        if half:
            for j in TWO:
                od[s, j, ha : ha + 8, :] = few[pl.ds(pl.multiple_of((xx * 2 + j) * 8, 8), 8), :]
        pl.semaphore_wait(free.at[s], 1)
        cp = _remote(od.at[s, 1 - c, pl.ds(0, n)], sst.at[s, pl.ds(0, n)], send, recv, next(ids), sib)
        cp.start()
        return half, s, n, cp

    def stored(blk, to):
        half, s, n, _ = blk
        return pltpu.make_async_copy(od.at[s, c, pl.ds(0, n)], to.at[pl.ds(half * ha, n)], dsem.at[s])

    def early(blk, src):
        half, s, n, cp = blk
        cp.wait_send()
        return local(src.at[pl.ds(half * ha, n)], od.at[s, 1 - c, pl.ds(0, n)], lsem.at[s])

    def sum_add(blk, to, more=None):
        half, s, n, cp = blk
        cp.wait_recv()
        if more is not None:
            more.wait()

        def add(r):
            v = od[s, c, r, :] + sst[s, r, :]
            od[s, c, r, :] = v if more is None else v + od[s, 1 - c, r, :]

        _loop_rows(n, 8, add)
        if more is None:
            pl.semaphore_signal(free.at[s], inc=1, device_id=(sib,), device_id_type=MESH)
            cp.wait_send()
        cp = stored(blk, to)
        cp.start()
        return cp

    def ring_sum(xx, rows_, n, src, s, dst, dev):
        lds = [
            local(q_h.at[xx, rows_], od.at[s, 0, pl.ds(0, n)], lsem.at[0]),
            local(src, od.at[s, 1, pl.ds(0, n)], lsem.at[1]),
        ]
        for cp in lds:
            cp.wait()
        _add_rows(od.at[s, 0, pl.ds(0, n)], [od.at[s, 1, pl.ds(0, n)]], 8)
        local(od.at[s, 0, pl.ds(0, n)], q_h.at[xx, rows_], lsem.at[0]).wait()
        return remote(q_h.at[xx, rows_], dst, dev)

    stores = []

    def flush():
        while stores:
            stores.pop().wait()

    def tiles(q, where, between=None):
        flush()

        def outs(i):
            p, ab = where(i)
            r = pl.ds(q * h, h)
            dsts = [dhp.at[ab * 2 + j, p, r] if q == 0 else dhp.at[p, ab * 2 + j, r] for j in TWO]
            return [
                pltpu.make_async_copy(tst.at[at_dht + i * 2 + j, pl.ds(0, h)], dst, hsem.at[i * 2 + j])
                for j, dst in enumerate(dsts)
            ]

        @pl.loop(0, 2)
        def _(i):
            if between is not None:
                pl.when(i > 0)(between)
            p, ab = where(i)
            ks = [(ab * 2 + j) * 4 + p if q == 0 else p * 4 + ab * 2 + j for j in TWO]
            rhs = jnp.concatenate([dz[:, pl.ds(pl.multiple_of(k * chunk, chunk), chunk)] for k in ks], axis=1)
            v = jnp.dot(etv[q * h : (q + 1) * h, :], rhs, preferred_element_type=F32)
            for j in TWO:
                tst[at_dht + i * 2 + j, 0:h, :] = v[:, j * chunk : (j + 1) * chunk]
            for cp in outs(i):
                cp.start()

        for i in TWO:
            stores.extend(outs(i))

    def part(q, p, lo, n):
        r = pl.ds(q * h, h)
        if q == 0:
            return dhp.at[pl.ds(lo, n), p, r]
        return dhp.at[p, pl.ds(lo, n), r]

    def one(q, p, i):
        r = pl.ds(q * h, h)
        return dhp.at[i, p, r] if q == 0 else dhp.at[p, i, r]

    ring1, ring2 = ((yp, ym), (zp, zm)), ((zp, zm), (yp, ym))
    pos1, pos2 = (y, z), (z, y)
    first, second = ({}, {}), ({}, {})

    def send_far(q):
        flush()
        p, (rt, lt) = pos1[q], ring1[q]
        first[q]["far_r"] = remote(part(q, _mod4(p + 2), 0, 2), ya.at[q], rt)
        first[q]["far_l"] = remote(part(q, _mod4(p + 2), 2, 2), yb.at[q], lt)

    def send_near(q):
        flush()
        p, (rt, lt) = pos1[q], ring1[q]
        first[q]["near_r"] = remote(part(q, _mod4(p + 1), 2, 2), yl.at[q, pl.ds(2, 2)], rt)
        first[q]["near_l"] = remote(part(q, _mod4(p - 1), 0, 2), yr.at[q, pl.ds(0, 2)], lt)

    def fetch(i, src):
        return local(src, tst.at[i, pl.ds(0, h)], tsem.at[i])

    def pass_on(q):
        flush()
        p, (rt, lt) = pos1[q], ring1[q]
        lds = [fetch(i, one(q, _mod4(p + 1), i)) for i in TWO]
        lds += [fetch(2 + i, one(q, _mod4(p - 1), 2 + i)) for i in TWO]
        first[q]["far_r"].wait_recv()
        for i in TWO:
            lds[i].wait()
            _add_rows(ya.at[q, i], [tst.at[i, pl.ds(0, h)]], min(FEW, h))
        first[q]["sum_r"] = remote(ya.at[q], yl.at[q, pl.ds(0, 2)], rt)
        first[q]["far_l"].wait_recv()
        for i in TWO:
            lds[2 + i].wait()
            _add_rows(yb.at[q, i], [tst.at[2 + i, pl.ds(0, h)]], min(FEW, h))
        first[q]["sum_l"] = remote(yb.at[q], yr.at[q, pl.ds(2, 2)], lt)

    lo, hi = pl.ds(0, hc), pl.ds(hc, hc)

    def second_phase(q):
        flush()
        r, (rt, lt) = pos2[q], ring2[q]
        r2, r1, rm1 = _mod4(r + 2), _mod4(r + 1), _mod4(r - 1)
        order = (r2, r1, rm1, r)
        lds = [fetch(i, one(q, pos1[q], k)) for i, k in enumerate(order)]
        for k in NEAR_KEYS:
            first[q][k].wait_recv()
        lds2 = [fetch(4 + i, yr.at[q, k]) for i, k in enumerate(order)]
        for i, k in enumerate(order):
            lds[i].wait()
            lds2[i].wait()
            _add_rows(yl.at[q, k], [tst.at[i, pl.ds(0, h)], tst.at[4 + i, pl.ds(0, h)]], min(FEW, h))
            if i == 0:
                second[q]["far_r"] = remote(yl.at[q, r2, lo], za.at[q], rt)
                second[q]["far_l"] = remote(yl.at[q, r2, hi], zb.at[q], lt)
            if i == 1:
                second[q]["near_r"] = remote(yl.at[q, r1, hi], zl.at[q, hi], rt)
            if i == 2:
                second[q]["near_l"] = remote(yl.at[q, rm1, lo], zr.at[q, lo], lt)

    def second_pass(q):
        r, (rt, lt) = pos2[q], ring2[q]
        r1, rm1 = _mod4(r + 1), _mod4(r - 1)
        second[q]["far_r"].wait_recv()
        _add_rows(yl.at[q, r1, lo], [za.at[q]], min(FEW, hc))
        second[q]["sum_r"] = remote(yl.at[q, r1, lo], zl.at[q, lo], rt)
        second[q]["far_l"].wait_recv()
        _add_rows(yl.at[q, rm1, hi], [zb.at[q]], min(FEW, hc))
        second[q]["sum_l"] = remote(yl.at[q, rm1, hi], zr.at[q, hi], lt)

    def last(q):
        r = pos2[q]
        for k in NEAR_KEYS:
            second[q][k].wait_recv()
        n = min(128, h)

        @pl.loop(0, h // n)
        def _(i):
            at = pl.ds(pl.multiple_of(i * n, n), n)
            v = yl[q, r, at, :] + zl[q, at, :] + zr[q, at, :]
            od[0, 0, 0:chunk, pl.ds(pl.multiple_of(q * h + i * n, n), n)] = (v * (1.0 / LOGIT_SCALE)).T

    def tiles_far(q, between=None):
        tiles(q, lambda i: (_mod4(pos1[q] + 2), i), between)

    def tiles_near(q):
        tiles(q, lambda i: (_mod4(pos1[q] + 1 + 2 * i), 1 - i))

    def tiles_pass(q):
        tiles(q, lambda i: (_mod4(pos1[q] + 1 + 2 * i), i))

    def tiles_own(q):
        tiles(q, lambda i: (pos1[q], i))

    all_later = 48 - SLOTS

    def dz_first(start, stop):
        dz_rows(in_order, start, stop, SLOTS, SLOTS, wide)

    def dz_later(start, stop):
        dz_rows(later, start, stop, all_later, at_dht, wide)

    with scope("de_far"):
        b0 = de_block(x_far, 0, 0)
        dz_far(16, 32)
        zahead(in_order, SLOTS, wide)
        for l in range(0, tok, nt):
            lanes = pl.ds(l, nt)
            dz_part(few[:, lanes], jnp.int32(dm.main), few_rows, lanes)
        dz[dm.main + FEW : dm.wide, :] = jnp.zeros((FEW, tok), BF16)
        b1 = de_block(x_far, 1, 1, True)
    with scope("dz_1"):
        c0 = sum_add(b0, q_h.at[x_far])
        dz_first(0, 8)
        c0.wait()
        e0 = remote(q_h.at[x_far, half_a], xa, xp)
        dz_first(8, SLOTS)
        zahead(later, at_dht, wide)
    with scope("dh_far1"):
        def between():
            sum_add(b1, q_h.at[x_far])

        tiles_far(1, between)
        c1 = stored(b1, q_h.at[x_far])
        c1.wait()
        e1 = remote(q_h.at[x_far, half_b], xb, xm)
    with scope("dz_2"):
        dz_later(0, 9)
        send_far(1)
    with scope("dh_far0"):
        tiles_far(0)
    with scope("dz_3"):
        dz_later(9, 13)
        send_far(0)
        dz_later(13, all_later)
    with scope("de_2"):
        b2 = de_block(x_p, 1, 0)
        b3 = de_block(x_m, 0, 1)
        c2 = sum_add(b2, q_h.at[x_p])
    with scope("dh_near"):
        tiles_near(1)
        c2.wait()
        e2 = remote(q_h.at[x_p, half_b], xe.at[half_b], xp)
        c3 = sum_add(b3, q_h.at[x_m])
        send_near(1)
        tiles_near(0)
        c3.wait()
        e3 = remote(q_h.at[x_m, half_a], xe.at[half_a], xm)
        send_near(0)
    with scope("dh_pass"):
        tiles_pass(1)
        tiles_pass(0)
        pass_on(1)
    with scope("de_4"):
        b4 = de_block(x_p, 0, 0)
        pass_on(0)
        b5 = de_block(x_m, 1, 1)
        c4 = sum_add(b4, q_h.at[x_p])
    with scope("dh_own"):
        tiles_own(1)
        c5 = sum_add(b5, q_h.at[x_m])
        tiles_own(0)
        c4.wait()
        c5.wait()
    old = list(sent)
    sent.clear()
    with scope("ring"):
        e0.wait_recv()
        e4 = ring_sum(x_p, half_a, ha, xa, 0, xs.at[half_a], xp)
        e1.wait_recv()
        e5 = ring_sum(x_m, half_b, ha + 8, xb, 1, xs.at[half_b], xm)
    with scope("de_6"):
        b6 = de_block(x, 0, 0)
    with scope("de_7"):
        b7 = de_block(x, 1, 1)
        xo_load = local(x4.at[zy, xc], dz.at[pl.ds(0, chunk)], xsem.at[0])
    with scope("second_1"):
        second_phase(1)
    with scope("second_0"):
        second_phase(0)
    with scope("spass_1"):
        second_pass(1)
    with scope("sum_6"):
        e3.wait_recv()
        c6 = early(b6, xe)
        e2.wait_recv()
        c7 = early(b7, xe)
        c6 = sum_add(b6, q_o, c6)
        c7 = sum_add(b7, q_o, c7)
    with scope("spass_0"):
        second_pass(0)
        c6.wait()
        c7.wait()
    with scope("last_1"):
        for cp in old:
            cp.wait_send()
        last(1)
    with scope("last_0"):
        last(0)

    with scope("finish"):
        xo_load.wait()
        sm[...] = jnp.zeros_like(sm)

        def finish(r):
            v = dz[r, :].astype(F32)
            inv = lax.rsqrt(jnp.mean(v * v, axis=-1, keepdims=True) + NORM_EPS)
            x_hat = v * inv
            dh = od[0, 0, r, :]
            sm[:, 0:dim] += jnp.sum(dh * x_hat, axis=0, keepdims=True)
            u = dh * gain
            od[0, 1, r, :] = inv * (u - x_hat * jnp.mean(u * x_hat, axis=-1, keepdims=True))

        _loop_rows(chunk, 16, finish)
        lse = jnp.where(zy == 0, lse_row[:, :], 0.0)
        loss = jnp.sum(w_row[:, :] * (lse - tgt_row[:, :]))
        sm[:, dim : dim + 128] = jnp.full((1, 128), loss / LOG2E)

    with scope("small_1"):
        cps = [remote(sm, got1.at[k], p) for k, p in enumerate(near)]
        dx_copy = local(od.at[0, 1, pl.ds(0, chunk)], dx_out, osem.at[0])
        for cp in cps:
            cp.wait_recv()
    with scope("small_2"):
        tot = sm[...]
        for k in range(len(near)):
            tot = tot + got1[k]
        total_v[...] = tot
        cps = [remote(total_v, got2.at[k], p) for k, p in enumerate(line)]
        mine = local(total_v, got2.at[len(line)], osem.at[1])
    with scope("small_3"):
        for cp in cps:
            cp.wait_recv()
        mine.wait()
    with scope("ring_end"):
        for cp in (e4, e5):
            cp.wait_recv()
        dx_copy.wait()
    for cp in sent:
        cp.wait_send()


def _run(dm, x4, table, gain, labels, mask):
    hbm, vm = pl.BlockSpec(memory_space=HBM), pl.BlockSpec(memory_space=VMEM)
    sd = jax.ShapeDtypeStruct
    d, tok, h, ck, pad, ha = dm.dim, dm.tok, dm.h, dm.chunk, dm.pad, dm.ha
    line, quad, pair = VMEM((1, tok), F32), VMEM((2, 2, h, ck), F32), VMEM((2, h, ck), F32)
    part, shard = VMEM((2, h // 2, ck), F32), sd((pad, d), F32)
    out = pl.pallas_call(
        functools.partial(_kernel, dm),
        name="head",
        out_shape=(
            sd((ck, d), F32), sd((8, 1, d + 128), F32),
            shard, shard, shard,
            sd((8, pad, d), F32), sd((16, dm.main, ck), F32),
            sd((4, pad, d), F32), sd((ha, d), F32), sd((ha + 8, d), F32),
            sd((4, 4, d, ck), F32), sd((2, 4, h, ck), F32),
        ),
        in_specs=[hbm, vm, vm, vm, vm],
        out_specs=[hbm] * 12,
        scratch_shapes=[
            VMEM((tok, d), BF16), VMEM((d, dm.wide), BF16), VMEM((dm.wide, tok), BF16),
            VMEM((2, 2, ha + 8, d), F32), VMEM((2, ha + 8, d), F32), VMEM((FEW, d), F32), VMEM((8, d), F32),
            quad, quad, VMEM((2, 4, h, ck), F32),
            part, part, pair, pair,
            VMEM((SLOTS, max(h, 2 * dm.rm), ck), F32),
            line, line, line, line, line, line, VMEM((15, 1, tok), F32),
            VMEM((1, d + 128), F32), VMEM((15, 1, d + 128), F32), VMEM((1, d + 128), F32),
            DMA((96,)), DMA((96,)), pltpu.SemaphoreType.REGULAR((2,)),
            DMA((4,)), DMA((4,)), DMA((SLOTS, 4)), DMA((SLOTS,)), DMA((4,)), DMA((2,)), DMA((2,)), DMA((8,)),
        ],
        compiler_params=pltpu.CompilerParams(
            collective_id=0, has_side_effects=True, vmem_limit_bytes=67043328
        ),
    )(x4, table, gain, labels, mask)
    return _write_out(dm, out[2:4], *out[:2])


def _write_kernel(own, ring, dx, small, de_o, dx_o, dg_o, loss_o):
    de_o[:, :] = (own[:, :] + ring[:, :]) * (1.0 / LOGIT_SCALE)
    dx_o[:, :] = dx[:, :]
    total = jnp.sum(small[:, :, :], axis=0)
    d = dg_o.shape[1]
    dg_o[:, :] = total[:, :d]
    loss_o[:, :] = total[:, d : d + 1]


def _write_out(dm, parts, dx, small):
    d, step, blocks = dm.dim, dm.ha + 8, 2
    sd = jax.ShapeDtypeStruct
    some = pl.BlockSpec((step, d), lambda i: (i, 0))
    half = pl.BlockSpec((dm.chunk // blocks, d), lambda i: (i, 0))
    row, one = pl.BlockSpec((1, d), lambda i: (0, 0)), pl.BlockSpec((1, 1), lambda i: (0, 0))
    rows = pl.BlockSpec(small.shape, lambda i: (0, 0, 0))
    return pl.pallas_call(
        _write_kernel,
        name="write_out",
        grid=(blocks,),
        out_shape=(sd((dm.rows, d), F32), sd((dm.chunk, d), F32), sd((1, d), F32), sd((1, 1), F32)),
        in_specs=[some, some, half, rows],
        out_specs=(some, half, row, one),
    )(*parts, dx, small)


def solution(mesh):
    group = mesh.shape[AXIS]

    def local_step(residual, labels, loss_mask, norm_gain, table_shard):
        tokens, dim = residual.shape
        rows = table_shard.shape[0]
        dm = Dims(tokens, dim, rows, group)
        x4 = residual.reshape(16, 8, dm.chunk, dim)
        lab = labels.reshape(16, 8, 1, dm.chunk)
        msk = loss_mask.reshape(16, 8, 1, dm.chunk)
        d_embed, d_res, d_gain, loss = _run(dm, x4, table_shard, norm_gain[None, :], lab, msk)
        return loss.reshape(()), d_res, d_embed, d_gain.reshape(dim)

    return jax.shard_map(
        local_step,
        mesh=mesh,
        in_specs=(P(), P(), P(), P(), P(AXIS, None)),
        out_specs=(P(), P(AXIS, None), P(AXIS, None), P()),
        check_vma=False,
    )
```

```python
import functools
import itertools
import math

import jax
import jax.numpy as jnp
from jax import lax
from jax.experimental import pallas as pl
from jax.experimental.pallas import tpu as pltpu
from jax.sharding import PartitionSpec as P

VOCAB_REAL = 49155
LOGIT_SCALE = 6.0
NORM_EPS = 1e-6

AXIS = "vp"
MESH = pl.DeviceIdType.MESH
F32 = jnp.float32
BF16 = jnp.bfloat16
HBM = pltpu.HBM
VMEM = pltpu.VMEM
DMA = pltpu.SemaphoreType.DMA


def _coords():
    me = lax.axis_index(AXIS)
    return me // 32, (me // 8) % 4, (me // 2) % 4, me % 2


def _dev(z, y, x, c):
    return ((z * 4 + y) * 4 + x) * 2 + c


def _mod4(v):
    return lax.rem(v + 8, 4)


def _barrier(peers):
    sem = pltpu.get_barrier_semaphore()
    for p in peers:
        pl.semaphore_signal(sem, inc=1, device_id=(p,), device_id_type=MESH)
    pl.semaphore_wait(sem, len(peers))


def _remote(src, dst, send, recv, k, dev):
    return pltpu.make_async_remote_copy(
        src_ref=src,
        dst_ref=dst,
        send_sem=send.at[k],
        recv_sem=recv.at[k],
        device_id=(dev,),
        device_id_type=MESH,
    )


class Dims:
    def __init__(self, tokens, dim, rows, group):
        self.dim, self.rows = dim, rows
        unit = 128 if rows >= 128 else 64
        self.rm = rows // unit * unit
        self.ha = self.rm // 2
        low = max(16, self.ha // 48 * 16)
        self.cuts = ((low, self.ha - low), (0, low))
        self.pad = self.rm + 8
        self.chunk = tokens // group
        self.tok = 16 * self.chunk
        self.nt = 4 * self.chunk
        self.main = 8 * self.rm
        self.wide = self.main + 128
        self.h = dim // 2


def _rem(a, b):
    return a % b if isinstance(a, int) else lax.rem(a, b)


def _pick(test, a, b):
    return (a if test else b) if isinstance(test, bool) else jnp.where(test, a, b)


def _loop_rows(rows, step, fn):
    @pl.loop(0, rows // step)
    def _(i):
        fn(pl.ds(pl.multiple_of(i * step, step), step))


def _add_rows(dst, srcs, step):
    def add(r):
        acc = dst[r, :]
        for s in srcs:
            acc = acc + s[r, :]
        dst[r, :] = acc

    _loop_rows(dst.shape[0], step, add)


SLOTS = 12
FEW = 64
TWO = range(2)
LOG2E = math.log2(math.e)
NEAR_KEYS = ("near_r", "near_l", "sum_r", "sum_l")
scope = jax.named_scope


def _kernel(
    dm, x4, e_ref, g_ref, lab, msk,
    dx_out, got2, q_o, xs, xe, eg, zh, q_h, xa, xb, dhp, yr,
    hv, etv, dz, od, sst, few, oext, ya, yb, yl, za, zb, zl, zr, tst,
    m_row, s_row, w_row, pos_row, lse_row, tgt_row, got, sm, got1, total_v,
    send, recv,
    free, esem, xsem, zsem, tsem, hsem, dsem, osem, lsem,
):
    z, y, x, c = _coords()
    xc, zy = x * 2 + c, z * 4 + y
    rows, rm, ha, dim, h = dm.rows, dm.rm, dm.ha, dm.dim, dm.h
    chunk, tok, nt, hc = dm.chunk, dm.tok, dm.nt, dm.h // 2
    x_far, x_p, x_m = _mod4(x + 2), _mod4(x + 1), _mod4(x - 1)
    xp, xm = _dev(z, y, x_p, c), _dev(z, y, x_m, c)
    yp, ym = _dev(z, _mod4(y + 1), x, c), _dev(z, _mod4(y - 1), x, c)
    zp, zm = _dev(_mod4(z + 1), y, x, c), _dev(_mod4(z - 1), y, x, c)
    sib = _dev(z, y, x, 1 - c)
    near = [_dev(_mod4(z + a), _mod4(y + b), x, c) for a in range(4) for b in range(4) if a or b]
    line = [_dev(z, y, _mod4(x + a), lax.rem(c + b, 2)) for a in range(4) for b in TWO if a or b]
    bar = pltpu.get_barrier_semaphore()
    for p in (*near, *line):
        pl.semaphore_signal(bar, inc=1, device_id=(p,), device_id_type=MESH)
    sent = []
    ids = itertools.count()

    def remote(src, dst, dev):
        cp = _remote(src, dst, send, recv, next(ids), dev)
        cp.start()
        sent.append(cp)
        return cp

    def local(src, dst, sem):
        cp = pltpu.make_async_copy(src, dst, sem)
        cp.start()
        return cp

    x_at, ext_at = 2 * rm, 4 * rm

    def xload(k):
        s = lax.rem(k, 4)
        to = dz.at[pl.ds(pl.multiple_of(x_at + s * chunk, chunk), chunk)]
        return pltpu.make_async_copy(x4.at[k, xc], to, xsem.at[s])

    with scope("prep"):
        for k in range(3):
            xload(k).start()
        own = xc
        for j in TWO:
            def widen(r, j=j):
                od[0, j, r, :] = e_ref[pl.ds(j * ha + r.start, r.size), :].astype(F32)

            _loop_rows(ha, 16, widen)
        oext[...] = jnp.zeros_like(oext)
        oext[0 : rows - rm, :] = e_ref[rm:rows, :].astype(F32)
        cps = [local(od.at[0, j, pl.ds(0, ha)], eg.at[own, pl.ds(j * ha, ha)], esem.at[j]) for j in TWO]
        cps.append(local(oext, eg.at[own, pl.ds(rm, 8)], esem.at[2]))
        for cp in cps:
            cp.wait()
        pl.semaphore_wait(bar, 22)

    half_a, half_b = pl.ds(0, ha), pl.ds(ha, ha + 8)

    def piece(s, r, dev):
        return remote(eg.at[s, r], eg.at[s, r], dev)

    def slot(xx):
        return xx * 2 + c

    r_a, l_b = piece(own, half_a, xp), piece(own, half_b, xm)
    s_o = piece(own, pl.ds(0, dm.pad), sib)
    r_b, l_a = piece(own, half_b, xp), piece(own, half_a, xm)

    gain = g_ref[...]

    with scope("norm"):
        @pl.loop(0, 16)
        def _(k):
            @pl.when(k < 13)
            def _():
                xload(k + 3).start()

            xload(k).wait()

            def norm(r):
                v = dz[pl.ds(pl.multiple_of(x_at + lax.rem(k, 4) * chunk + r.start, r.size), r.size), :].astype(F32)
                inv = lax.rsqrt(jnp.mean(v * v, axis=-1, keepdims=True) + NORM_EPS)
                hv[pl.ds(pl.multiple_of(k * chunk + r.start, r.size), r.size), :] = (v * inv * gain).astype(BF16)

            _loop_rows(chunk, 16, norm)

    with scope("labels"):
        total = jnp.sum(msk[...])
        for k in range(16):
            at = pl.ds(k * chunk, chunk)
            w_row[:, at] = msk[k, xc] / total
            q = lab[k, xc] - zy * (8 * rows)
            s = jnp.zeros_like(q)
            for i in range(1, 8):
                s = s + jnp.where(q >= i * rows, 1, 0)
            r = q - s * rows
            up = jnp.where(r >= ha, 1, 0)
            at_main = ((s // 2 * 2 + up) * 2 + s % 2) * ha + r - up * ha
            at_ext = dm.main + s * 8 + r - rm
            place = jnp.where(r < rm, at_main, at_ext)
            pos_row[:, at] = jnp.where((q >= 0) & (q < 8 * rows), place, -1).astype(F32)

    def product(lhs, lanes):
        v = lax.dot_general(lhs, hv[lanes, :], (((1,), (1,)), ((), ())), preferred_element_type=F32)
        return v * (LOG2E / LOGIT_SCALE)

    def add_stats(v, lanes):
        m_old, s_old = m_row[:, lanes], s_row[:, lanes]
        m = jnp.maximum(m_old, jnp.max(v, axis=0, keepdims=True))
        s = jnp.sum(jnp.exp2(v - m), axis=0, keepdims=True)
        m_row[:, lanes] = m
        s_row[:, lanes] = s_old * jnp.exp2(m_old - m) + s

    def add_target(v, place, lanes):
        r = lax.broadcasted_iota(jnp.int32, v.shape, 0)
        hit = r.astype(F32) == pos_row[:, lanes] - place.astype(F32)
        tgt_row[:, lanes] += jnp.sum(jnp.where(hit, v, 0.0), axis=0, keepdims=True)

    m_row[:, :] = jnp.full((1, tok), -1e30, F32)
    s_row[:, :] = jnp.zeros((1, tok), F32)
    tgt_row[:, :] = jnp.zeros((1, tok), F32)
    segs = [(half, j) for half in TWO for j in TWO]

    def load(r0, n, xx):
        return [
            local(
                eg.at[xx[half] * 2 + j, pl.ds(half * ha + r0, n)], od.at[j, half, pl.ds(r0, n)], esem.at[half * 2 + j]
            )
            for half, j in segs
        ]

    def narrow_all(r0, n, src):
        for half, j in segs:
            def narrow(r, half=half, j=j):
                at = pl.multiple_of((half * 2 + j) * ha + r0 + r.start, r.size)
                dz[pl.ds(at, r.size), :] = src(half, j)[r, :].astype(BF16)

            _loop_rows(n, 16, narrow)

    def block(r0, n, xx, loads=(), with_few=False):
        if loads:
            for cp in loads:
                cp.wait()
            narrow_all(r0, n, lambda half, j: od.at[j, half, pl.ds(r0, n)])
        left = [VOCAB_REAL - ((zy * 8 + xx[half] * 2 + j) * rows + half * ha + r0) for half, j in segs]
        w = nt // chunk
        deep = SLOTS // w

        def out(t):
            u = lax.rem(t, deep) * w
            return [
                pltpu.make_async_copy(
                    tst.at[u + i, pl.ds(m * n, n)],
                    zh.at[t * w + i, pl.ds(pl.multiple_of((xx[half] * 2 + half) * rm + j * ha + r0, 8), n)],
                    zsem.at[u + i, m],
                )
                for i in range(w)
                for m, (half, j) in enumerate(segs)
            ]

        @pl.loop(0, tok // nt)
        def _(t):
            @pl.when(t >= deep)
            def _():
                for cp in out(t - deep):
                    cp.wait()

            lanes = pl.ds(pl.multiple_of(t * nt, nt), nt)
            lhs = [dz[(half * 2 + j) * ha + r0 : (half * 2 + j) * ha + r0 + n, :] for half, j in segs]
            if with_few:
                lhs.append(dz[ext_at : ext_at + FEW, :])
            v = product(jnp.concatenate(lhs, axis=0), lanes)
            v, v_few = v[: 4 * n], v[4 * n :]
            r = lax.broadcasted_iota(jnp.int32, (n, nt), 0)
            v = [jnp.where(r < left[m], v[m * n : (m + 1) * n], -jnp.inf) for m in range(len(segs))]
            for part_v, (half, j) in zip(v, segs):
                add_target(part_v, (xx[half] * 2 + half) * rm + j * ha + r0, lanes)
            u = lax.rem(t, deep) * w
            for i in range(w):
                for m in range(len(segs)):
                    tst[u + i, m * n : (m + 1) * n, :] = v[m][:, i * chunk : (i + 1) * chunk]
            if with_few:
                r = lax.broadcasted_iota(jnp.int32, v_few.shape, 0)
                ok = ((r & 7) < rows - rm) & ((zy * 8 + (r >> 3)) * rows + rm + (r & 7) < VOCAB_REAL)
                v_few = jnp.where(ok, v_few, -jnp.inf)
                few[:, lanes] = v_few
                add_target(v_few, jnp.int32(dm.main), lanes)
                v.append(v_few)
            v = jnp.concatenate(v, axis=0)
            for cp in out(t):
                cp.start()
            add_stats(v, lanes)

        for t in range(deep):
            for cp in out(t + tok // nt - deep):
                cp.wait()

    def both(xx):
        block(0, ha, xx, load(0, ha, xx))

    def turn(xx):
        for half in TWO:
            base = pl.multiple_of((xx[half] * 2 + half) * rm, rm)

            @pl.loop(0, dim // 128)
            def _(d, half=half, base=base):
                at = pl.ds(pl.multiple_of(d * 128, 128), 128)
                etv[at, pl.ds(base, rm)] = dz[half * rm : (half + 1) * rm, at].T

    with scope("own"):
        s_o.wait_recv()
        both((x, x))
        turn((x, x))

    with scope("wait_1"):
        r_a.wait_recv()
        last_n = dm.cuts[-1][1]
        spans = [(pl.ds(r0, n), pl.ds(ha + r0, n + 8 * (r0 + n == ha))) for r0, n in dm.cuts]

        def far_pieces(xx, half, to):
            cps = [piece(slot(xx), pair[half], to) for pair in spans[:-1]]
            cps.append(remote(eg.at[slot(xx), spans[-1][half]], sst.at[c, pl.ds(half * last_n, last_n)], to))
            return cps

        r_f = far_pieces(x_m, 0, xp)
        d = [piece(slot(x_m), half_a, sib)]
        l_b.wait_recv()
        l_f = far_pieces(x_p, 1, xm)
        d.append(piece(slot(x_p), half_b, sib))
        for cp in d:
            cp.wait_recv()

    with scope("near_1"):
        both((x_m, x_p))
        turn((x_m, x_p))

    with scope("wait_2"):
        r_b.wait_recv()
        d = [piece(slot(x_m), half_b, sib)]
        l_a.wait_recv()
        d.append(piece(slot(x_p), half_a, sib))
        for cp in d:
            cp.wait_recv()

    with scope("near_2"):
        both((x_p, x_m))
        turn((x_p, x_m))

    far = (x_far, x_far)

    def far_arrived(i):
        d = []
        for cp, r in zip((r_f[i], l_f[i]), spans[i]):
            cp.wait_recv()
            d.append(piece(slot(x_far), r, sib))
        for cp in d:
            cp.wait_recv()

    with scope("wait_3"):
        far_arrived(0)
    with scope("far_a"):
        loads = load(*dm.cuts[0], far)
        ext_loads = [local(eg.at[s, pl.ds(rm, 8)], few.at[pl.ds(s * 8, 8)], lsem.at[s]) for s in range(8)]
        for cp in ext_loads:
            cp.wait()
        dz[ext_at : ext_at + FEW, :] = few[...].astype(BF16)
        dz[ext_at + FEW : ext_at + 128, :] = jnp.zeros((FEW, dim), BF16)
        block(*dm.cuts[0], far, loads, True)
    with scope("wait_5"):
        r_f[-1].wait_recv()
        l_f[-1].wait_recv()
        both_last = sst.at[c, pl.ds(0, 2 * last_n)]
        over = _remote(both_last, both_last, send, recv, next(ids), sib)
        over.start()
        over.wait_recv()

    with scope("far_c"):
        narrow_all(0, last_n, lambda half, j: sst.at[j, pl.ds(half * last_n, last_n)])
        over.wait_send()
        for s in TWO:
            pl.semaphore_signal(free.at[s], inc=1, device_id=(sib,), device_id_type=MESH)
        block(0, last_n, far)

    with scope("turn_far"):
        lse_row[:, :] = m_row[:, :] + jnp.log(s_row[:, :]) * LOG2E
        scps = [_remote(lse_row, got.at[k], send, recv, next(ids), p) for k, p in enumerate(near)]
        for cp in scps:
            cp.start()
        turn(far)

        @pl.loop(0, dim // 128)
        def _(i):
            at = pl.ds(pl.multiple_of(i * 128, 128), 128)
            etv[at, dm.main : dm.wide] = dz[ext_at : ext_at + 128, at].T

    wide = 2 * rm

    at_dht = SLOTS - 4

    def chunk_of(zz, yy):
        return _mod4(zz) * 4 + _rem(yy + 8, 4)

    def all_far(i):
        return x_far * wide + i // 16 * rm, _rem(i, 16)

    def in_order(i):
        n = i // 3
        m = n - 7
        k = _pick(n < 7, chunk_of(z + n - 1, y + 2), chunk_of(z + 3 + m // 3, y + 3 + _rem(m + 9, 3)))
        return _mod4(x + 3 + _rem(i, 3)) * wide, _pick(n < 4, chunk_of(z + 2, n), k)

    def later(i):
        return in_order(i + SLOTS)

    def zload(where, i, ring, n):
        at, k = where(i)
        s = _rem(i, ring)
        src = zh.at[k, pl.ds(pl.multiple_of(at, rm), n)]
        return pltpu.make_async_copy(src, tst.at[s, pl.ds(0, n)], tsem.at[s])

    def zahead(where, ring, n):
        for i in range(ring):
            zload(where, i, ring, n).start()

    with scope("stats"):
        zahead(all_far, SLOTS, rm)
        for cp in scps:
            cp.wait_recv()
            cp.wait_send()
        top = lse_row[:, :]
        for k in range(len(near)):
            top = jnp.maximum(top, got[k])
        s = jnp.exp2(lse_row[:, :] - top)
        for k in range(len(near)):
            s = s + jnp.exp2(got[k] - top)
        lse_row[:, :] = top + jnp.log(s) * LOG2E

    def dz_part(v, place, at, lanes):
        r = lax.broadcasted_iota(jnp.int32, v.shape, 0).astype(F32)
        hit = r == pos_row[:, lanes] - place.astype(F32)
        p = jnp.exp2(v - lse_row[:, lanes])
        dz[at, lanes] = (jnp.where(hit, p - 1.0, p) * w_row[:, lanes]).astype(BF16)

    step = min(128, rm)

    def dz_rows(where, start, stop, last_tile, ring, n):
        @pl.loop(start, stop)
        def _(i):
            @pl.when((i > 0) & (i + ring - 1 < last_tile))
            def _():
                zload(where, i + ring - 1, ring, n).start()

            zload(where, i, ring, n).wait()
            row, k = where(i)
            lanes = pl.ds(pl.multiple_of(k * chunk, chunk), chunk)

            @pl.loop(0, n // step)
            def _(j):
                at = pl.multiple_of(row + j * step, step)
                r = pl.ds(pl.multiple_of(j * step, step), step)
                dz_part(tst[lax.rem(i, ring), r, :], at, pl.ds(at, step), lanes)

    def dz_far(start, stop):
        dz_rows(all_far, start, stop, 32, SLOTS, rm)

    with scope("dz_far"):
        dz_far(0, 16)

    nd = min(1024, dim)
    few_rows = pl.ds(dm.main, FEW)

    def de_block(xx, half, s, with_few=False):
        at = pl.ds(pl.multiple_of((xx * 2 + half) * rm, rm), rm)

        @pl.loop(0, dim // nd)
        def _(i):
            lanes = pl.ds(pl.multiple_of(i * nd, nd), nd)
            lhs = jnp.concatenate([dz[at, :], dz[few_rows, :]], axis=0) if with_few else dz[at, :]
            v = jnp.dot(lhs, hv[:, lanes], preferred_element_type=F32)
            for j in TWO:
                od[s, j, 0:ha, lanes] = v[j * ha : (j + 1) * ha]
            if with_few:
                few[:, lanes] = v[rm:]

        n = ha + 8 * half
        if half:
            for j in TWO:
                od[s, j, ha : ha + 8, :] = few[pl.ds(pl.multiple_of((xx * 2 + j) * 8, 8), 8), :]
        pl.semaphore_wait(free.at[s], 1)
        cp = _remote(od.at[s, 1 - c, pl.ds(0, n)], sst.at[s, pl.ds(0, n)], send, recv, next(ids), sib)
        cp.start()
        return half, s, n, cp

    def stored(blk, to):
        half, s, n, _ = blk
        return pltpu.make_async_copy(od.at[s, c, pl.ds(0, n)], to.at[pl.ds(half * ha, n)], dsem.at[s])

    def early(blk, src):
        half, s, n, cp = blk
        cp.wait_send()
        return local(src.at[pl.ds(half * ha, n)], od.at[s, 1 - c, pl.ds(0, n)], lsem.at[s])

    def sum_add(blk, to, more=None):
        half, s, n, cp = blk
        cp.wait_recv()
        if more is not None:
            more.wait()

        def add(r):
            v = od[s, c, r, :] + sst[s, r, :]
            od[s, c, r, :] = v if more is None else v + od[s, 1 - c, r, :]

        _loop_rows(n, 8, add)
        if more is None:
            pl.semaphore_signal(free.at[s], inc=1, device_id=(sib,), device_id_type=MESH)
            cp.wait_send()
        cp = stored(blk, to)
        cp.start()
        return cp

    def ring_sum(xx, rows_, n, src, s, dst, dev):
        lds = [
            local(q_h.at[xx, rows_], od.at[s, 0, pl.ds(0, n)], lsem.at[0]),
            local(src, od.at[s, 1, pl.ds(0, n)], lsem.at[1]),
        ]
        for cp in lds:
            cp.wait()
        _add_rows(od.at[s, 0, pl.ds(0, n)], [od.at[s, 1, pl.ds(0, n)]], 8)
        local(od.at[s, 0, pl.ds(0, n)], q_h.at[xx, rows_], lsem.at[0]).wait()
        return remote(q_h.at[xx, rows_], dst, dev)

    stores = []

    def flush():
        while stores:
            stores.pop().wait()

    def tiles(q, where, between=None):
        flush()

        def outs(i):
            p, ab = where(i)
            r = pl.ds(q * h, h)
            dsts = [dhp.at[ab * 2 + j, p, r] if q == 0 else dhp.at[p, ab * 2 + j, r] for j in TWO]
            return [
                pltpu.make_async_copy(tst.at[at_dht + i * 2 + j, pl.ds(0, h)], dst, hsem.at[i * 2 + j])
                for j, dst in enumerate(dsts)
            ]

        @pl.loop(0, 2)
        def _(i):
            if between is not None:
                pl.when(i > 0)(between)
            p, ab = where(i)
            ks = [(ab * 2 + j) * 4 + p if q == 0 else p * 4 + ab * 2 + j for j in TWO]
            rhs = jnp.concatenate([dz[:, pl.ds(pl.multiple_of(k * chunk, chunk), chunk)] for k in ks], axis=1)
            v = jnp.dot(etv[q * h : (q + 1) * h, :], rhs, preferred_element_type=F32)
            for j in TWO:
                tst[at_dht + i * 2 + j, 0:h, :] = v[:, j * chunk : (j + 1) * chunk]
            for cp in outs(i):
                cp.start()

        for i in TWO:
            stores.extend(outs(i))

    def part(q, p, lo, n):
        r = pl.ds(q * h, h)
        if q == 0:
            return dhp.at[pl.ds(lo, n), p, r]
        return dhp.at[p, pl.ds(lo, n), r]

    def one(q, p, i):
        r = pl.ds(q * h, h)
        return dhp.at[i, p, r] if q == 0 else dhp.at[p, i, r]

    ring1, ring2 = ((yp, ym), (zp, zm)), ((zp, zm), (yp, ym))
    pos1, pos2 = (y, z), (z, y)
    first, second = ({}, {}), ({}, {})

    def send_far(q):
        flush()
        p, (rt, lt) = pos1[q], ring1[q]
        first[q]["far_r"] = remote(part(q, _mod4(p + 2), 0, 2), ya.at[q], rt)
        first[q]["far_l"] = remote(part(q, _mod4(p + 2), 2, 2), yb.at[q], lt)

    def send_near(q):
        flush()
        p, (rt, lt) = pos1[q], ring1[q]
        first[q]["near_r"] = remote(part(q, _mod4(p + 1), 2, 2), yl.at[q, pl.ds(2, 2)], rt)
        first[q]["near_l"] = remote(part(q, _mod4(p - 1), 0, 2), yr.at[q, pl.ds(0, 2)], lt)

    def fetch(i, src):
        return local(src, tst.at[i, pl.ds(0, h)], tsem.at[i])

    def pass_on(q):
        flush()
        p, (rt, lt) = pos1[q], ring1[q]
        lds = [fetch(i, one(q, _mod4(p + 1), i)) for i in TWO]
        lds += [fetch(2 + i, one(q, _mod4(p - 1), 2 + i)) for i in TWO]
        first[q]["far_r"].wait_recv()
        for i in TWO:
            lds[i].wait()
            _add_rows(ya.at[q, i], [tst.at[i, pl.ds(0, h)]], min(FEW, h))
        first[q]["sum_r"] = remote(ya.at[q], yl.at[q, pl.ds(0, 2)], rt)
        first[q]["far_l"].wait_recv()
        for i in TWO:
            lds[2 + i].wait()
            _add_rows(yb.at[q, i], [tst.at[2 + i, pl.ds(0, h)]], min(FEW, h))
        first[q]["sum_l"] = remote(yb.at[q], yr.at[q, pl.ds(2, 2)], lt)

    lo, hi = pl.ds(0, hc), pl.ds(hc, hc)

    def second_phase(q):
        flush()
        r, (rt, lt) = pos2[q], ring2[q]
        r2, r1, rm1 = _mod4(r + 2), _mod4(r + 1), _mod4(r - 1)
        order = (r2, r1, rm1, r)
        lds = [fetch(i, one(q, pos1[q], k)) for i, k in enumerate(order)]
        for k in NEAR_KEYS:
            first[q][k].wait_recv()
        lds2 = [fetch(4 + i, yr.at[q, k]) for i, k in enumerate(order)]
        for i, k in enumerate(order):
            lds[i].wait()
            lds2[i].wait()
            _add_rows(yl.at[q, k], [tst.at[i, pl.ds(0, h)], tst.at[4 + i, pl.ds(0, h)]], min(FEW, h))
            if i == 0:
                second[q]["far_r"] = remote(yl.at[q, r2, lo], za.at[q], rt)
                second[q]["far_l"] = remote(yl.at[q, r2, hi], zb.at[q], lt)
            if i == 1:
                second[q]["near_r"] = remote(yl.at[q, r1, hi], zl.at[q, hi], rt)
            if i == 2:
                second[q]["near_l"] = remote(yl.at[q, rm1, lo], zr.at[q, lo], lt)

    def second_pass(q):
        r, (rt, lt) = pos2[q], ring2[q]
        r1, rm1 = _mod4(r + 1), _mod4(r - 1)
        second[q]["far_r"].wait_recv()
        _add_rows(yl.at[q, r1, lo], [za.at[q]], min(FEW, hc))
        second[q]["sum_r"] = remote(yl.at[q, r1, lo], zl.at[q, lo], rt)
        second[q]["far_l"].wait_recv()
        _add_rows(yl.at[q, rm1, hi], [zb.at[q]], min(FEW, hc))
        second[q]["sum_l"] = remote(yl.at[q, rm1, hi], zr.at[q, hi], lt)

    def last(q):
        r = pos2[q]
        for k in NEAR_KEYS:
            second[q][k].wait_recv()
        n = min(128, h)

        @pl.loop(0, h // n)
        def _(i):
            at = pl.ds(pl.multiple_of(i * n, n), n)
            v = yl[q, r, at, :] + zl[q, at, :] + zr[q, at, :]
            od[0, 0, 0:chunk, pl.ds(pl.multiple_of(q * h + i * n, n), n)] = (v * (1.0 / LOGIT_SCALE)).T

    def tiles_far(q, between=None):
        tiles(q, lambda i: (_mod4(pos1[q] + 2), i), between)

    def tiles_near(q):
        tiles(q, lambda i: (_mod4(pos1[q] + 1 + 2 * i), 1 - i))

    def tiles_pass(q):
        tiles(q, lambda i: (_mod4(pos1[q] + 1 + 2 * i), i))

    def tiles_own(q):
        tiles(q, lambda i: (pos1[q], i))

    all_later = 48 - SLOTS

    def dz_first(start, stop):
        dz_rows(in_order, start, stop, SLOTS, SLOTS, wide)

    def dz_later(start, stop):
        dz_rows(later, start, stop, all_later, at_dht, wide)

    with scope("de_far"):
        b0 = de_block(x_far, 0, 0)
        dz_far(16, 32)
        zahead(in_order, SLOTS, wide)
        for l in range(0, tok, nt):
            lanes = pl.ds(l, nt)
            dz_part(few[:, lanes], jnp.int32(dm.main), few_rows, lanes)
        dz[dm.main + FEW : dm.wide, :] = jnp.zeros((FEW, tok), BF16)
        b1 = de_block(x_far, 1, 1, True)
    with scope("dz_1"):
        c0 = sum_add(b0, q_h.at[x_far])
        dz_first(0, 8)
        c0.wait()
        e0 = remote(q_h.at[x_far, half_a], xa, xp)
        dz_first(8, SLOTS)
        zahead(later, at_dht, wide)
    with scope("dh_far1"):
        def between():
            sum_add(b1, q_h.at[x_far])

        tiles_far(1, between)
        c1 = stored(b1, q_h.at[x_far])
        c1.wait()
        e1 = remote(q_h.at[x_far, half_b], xb, xm)
    with scope("dz_2"):
        dz_later(0, 9)
        send_far(1)
    with scope("dh_far0"):
        tiles_far(0)
    with scope("dz_3"):
        dz_later(9, 13)
        send_far(0)
        dz_later(13, all_later)
    with scope("de_2"):
        b2 = de_block(x_p, 1, 0)
        b3 = de_block(x_m, 0, 1)
        c2 = sum_add(b2, q_h.at[x_p])
    with scope("dh_near"):
        tiles_near(1)
        c2.wait()
        e2 = remote(q_h.at[x_p, half_b], xe.at[half_b], xp)
        c3 = sum_add(b3, q_h.at[x_m])
        send_near(1)
        tiles_near(0)
        c3.wait()
        e3 = remote(q_h.at[x_m, half_a], xe.at[half_a], xm)
        send_near(0)
    with scope("dh_pass"):
        tiles_pass(1)
        tiles_pass(0)
        pass_on(1)
    with scope("de_4"):
        b4 = de_block(x_p, 0, 0)
        pass_on(0)
        b5 = de_block(x_m, 1, 1)
        c4 = sum_add(b4, q_h.at[x_p])
    with scope("dh_own"):
        tiles_own(1)
        c5 = sum_add(b5, q_h.at[x_m])
        tiles_own(0)
        c4.wait()
        c5.wait()
    old = list(sent)
    sent.clear()
    with scope("ring"):
        e0.wait_recv()
        e4 = ring_sum(x_p, half_a, ha, xa, 0, xs.at[half_a], xp)
        e1.wait_recv()
        e5 = ring_sum(x_m, half_b, ha + 8, xb, 1, xs.at[half_b], xm)
    with scope("de_6"):
        b6 = de_block(x, 0, 0)
    with scope("de_7"):
        b7 = de_block(x, 1, 1)
        xo_load = local(x4.at[zy, xc], dz.at[pl.ds(0, chunk)], xsem.at[0])
    with scope("second_1"):
        second_phase(1)
    with scope("second_0"):
        second_phase(0)
    with scope("spass_1"):
        second_pass(1)
    with scope("sum_6"):
        e3.wait_recv()
        c6 = early(b6, xe)
        e2.wait_recv()
        c7 = early(b7, xe)
        c6 = sum_add(b6, q_o, c6)
        c7 = sum_add(b7, q_o, c7)
    with scope("spass_0"):
        second_pass(0)
        c6.wait()
        c7.wait()
    def drain(cps):
        while cps:
            cps.pop().wait_send()

    with scope("last_1"):
        drain(old)
        last(1)
    with scope("last_0"):
        last(0)

    with scope("finish"):
        xo_load.wait()
        sm[...] = jnp.zeros_like(sm)

        def finish(r):
            v = dz[r, :].astype(F32)
            inv = lax.rsqrt(jnp.mean(v * v, axis=-1, keepdims=True) + NORM_EPS)
            x_hat = v * inv
            dh = od[0, 0, r, :]
            sm[:, 0:dim] += jnp.sum(dh * x_hat, axis=0, keepdims=True)
            u = dh * gain
            od[0, 1, r, :] = inv * (u - x_hat * jnp.mean(u * x_hat, axis=-1, keepdims=True))

        _loop_rows(chunk, 16, finish)
        lse = jnp.where(zy == 0, lse_row[:, :], 0.0)
        loss = jnp.sum(w_row[:, :] * (lse - tgt_row[:, :]))
        sm[:, dim : dim + 128] = jnp.full((1, 128), loss / LOG2E)

    with scope("small_1"):
        old = [cp for cp in sent if cp is not e4 and cp is not e5]
        sent.clear()
        cps = [remote(sm, got1.at[k], p) for k, p in enumerate(near)]
        dx_copy = local(od.at[0, 1, pl.ds(0, chunk)], dx_out, osem.at[0])
        drain(old)
        for cp in cps:
            cp.wait_recv()
    with scope("small_2"):
        tot = sm[...]
        for k in range(len(near)):
            tot = tot + got1[k]
        total_v[...] = tot
        drain(sent)
        cps = [remote(total_v, got2.at[k], p) for k, p in enumerate(line)]
        mine = local(total_v, got2.at[len(line)], osem.at[1])
    with scope("small_3"):
        dx_copy.wait()
        mine.wait()
        for cp in cps:
            cp.wait_recv()
    with scope("ring_end"):
        for cp in (e4, e5):
            cp.wait()
        drain(sent)


def _run(dm, x4, table, gain, labels, mask):
    hbm, vm = pl.BlockSpec(memory_space=HBM), pl.BlockSpec(memory_space=VMEM)
    sd = jax.ShapeDtypeStruct
    d, tok, h, ck, pad, ha = dm.dim, dm.tok, dm.h, dm.chunk, dm.pad, dm.ha
    line, quad, pair = VMEM((1, tok), F32), VMEM((2, 2, h, ck), F32), VMEM((2, h, ck), F32)
    part, shard = VMEM((2, h // 2, ck), F32), sd((pad, d), F32)
    out = pl.pallas_call(
        functools.partial(_kernel, dm),
        name="head",
        out_shape=(
            sd((ck, d), F32), sd((8, 1, d + 128), F32),
            shard, shard, shard,
            sd((8, pad, d), F32), sd((16, dm.main, ck), F32),
            sd((4, pad, d), F32), sd((ha, d), F32), sd((ha + 8, d), F32),
            sd((4, 4, d, ck), F32), sd((2, 4, h, ck), F32),
        ),
        in_specs=[hbm, vm, vm, vm, vm],
        out_specs=[hbm] * 12,
        scratch_shapes=[
            VMEM((tok, d), BF16), VMEM((d, dm.wide), BF16), VMEM((dm.wide, tok), BF16),
            VMEM((2, 2, ha + 8, d), F32), VMEM((2, ha + 8, d), F32), VMEM((FEW, d), F32), VMEM((8, d), F32),
            quad, quad, VMEM((2, 4, h, ck), F32),
            part, part, pair, pair,
            VMEM((SLOTS, max(h, 2 * dm.rm), ck), F32),
            line, line, line, line, line, line, VMEM((15, 1, tok), F32),
            VMEM((1, d + 128), F32), VMEM((15, 1, d + 128), F32), VMEM((1, d + 128), F32),
            DMA((96,)), DMA((96,)), pltpu.SemaphoreType.REGULAR((2,)),
            DMA((4,)), DMA((4,)), DMA((SLOTS, 4)), DMA((SLOTS,)), DMA((4,)), DMA((2,)), DMA((2,)), DMA((8,)),
        ],
        compiler_params=pltpu.CompilerParams(
            collective_id=0, has_side_effects=True, vmem_limit_bytes=67043328
        ),
    )(x4, table, gain, labels, mask)
    return _write_out(dm, out[2:4], *out[:2])


def _write_kernel(own, ring, dx, small, de_o, dx_o, dg_o, loss_o):
    de_o[:, :] = (own[:, :] + ring[:, :]) * (1.0 / LOGIT_SCALE)
    dx_o[:, :] = dx[:, :]
    total = jnp.sum(small[:, :, :], axis=0)
    d = dg_o.shape[1]
    dg_o[:, :] = total[:, :d]
    loss_o[:, :] = total[:, d : d + 1]


def _write_out(dm, parts, dx, small):
    d, step, blocks = dm.dim, dm.ha + 8, 2
    sd = jax.ShapeDtypeStruct
    some = pl.BlockSpec((step, d), lambda i: (i, 0))
    half = pl.BlockSpec((dm.chunk // blocks, d), lambda i: (i, 0))
    row, one = pl.BlockSpec((1, d), lambda i: (0, 0)), pl.BlockSpec((1, 1), lambda i: (0, 0))
    rows = pl.BlockSpec(small.shape, lambda i: (0, 0, 0))
    return pl.pallas_call(
        _write_kernel,
        name="write_out",
        grid=(blocks,),
        out_shape=(sd((dm.rows, d), F32), sd((dm.chunk, d), F32), sd((1, d), F32), sd((1, 1), F32)),
        in_specs=[some, some, half, rows],
        out_specs=(some, half, row, one),
    )(*parts, dx, small)


def solution(mesh):
    group = mesh.shape[AXIS]

    def local_step(residual, labels, loss_mask, norm_gain, table_shard):
        tokens, dim = residual.shape
        rows = table_shard.shape[0]
        dm = Dims(tokens, dim, rows, group)
        x4 = residual.reshape(16, 8, dm.chunk, dim)
        lab = labels.reshape(16, 8, 1, dm.chunk)
        msk = loss_mask.reshape(16, 8, 1, dm.chunk)
        d_embed, d_res, d_gain, loss = _run(dm, x4, table_shard, norm_gain[None, :], lab, msk)
        return loss.reshape(()), d_res, d_embed, d_gain.reshape(dim)

    return jax.shard_map(
        local_step,
        mesh=mesh,
        in_specs=(P(), P(), P(), P(), P(AXIS, None)),
        out_specs=(P(), P(AXIS, None), P(AXIS, None), P()),
        check_vma=False,
    )
```

```python
import functools
import itertools
import math

import jax
import jax.numpy as jnp
from jax import lax
from jax.experimental import pallas as pl
from jax.experimental.pallas import tpu as pltpu
from jax.sharding import PartitionSpec as P

VOCAB_REAL = 49155
LOGIT_SCALE = 6.0
NORM_EPS = 1e-6

AXIS = "vp"
MESH = pl.DeviceIdType.MESH
F32 = jnp.float32
BF16 = jnp.bfloat16
HBM = pltpu.HBM
VMEM = pltpu.VMEM
DMA = pltpu.SemaphoreType.DMA


def _coords():
    me = lax.axis_index(AXIS)
    return me // 32, (me // 8) % 4, (me // 2) % 4, me % 2


def _dev(z, y, x, c):
    return ((z * 4 + y) * 4 + x) * 2 + c


def _mod4(v):
    return lax.rem(v + 8, 4)


def _barrier(peers):
    sem = pltpu.get_barrier_semaphore()
    for p in peers:
        pl.semaphore_signal(sem, inc=1, device_id=(p,), device_id_type=MESH)
    pl.semaphore_wait(sem, len(peers))


def _remote(src, dst, send, recv, k, dev):
    return pltpu.make_async_remote_copy(
        src_ref=src,
        dst_ref=dst,
        send_sem=send.at[k],
        recv_sem=recv.at[k],
        device_id=(dev,),
        device_id_type=MESH,
    )


class Dims:
    def __init__(self, tokens, dim, rows, group):
        self.dim, self.rows = dim, rows
        unit = 128 if rows >= 128 else 64
        self.rm = rows // unit * unit
        self.ha = self.rm // 2
        low = max(16, self.ha // 48 * 16)
        self.cuts = ((low, self.ha - low), (0, low))
        self.pad = self.rm + 8
        self.chunk = tokens // group
        self.tok = 16 * self.chunk
        self.nt = 4 * self.chunk
        self.main = 8 * self.rm
        self.wide = self.main + 128
        self.h = dim // 2


def _top(n):
    return pl.ds(0, n)


def _rem(a, b):
    return a % b if isinstance(a, int) else lax.rem(a, b)


def _pick(test, a, b):
    return (a if test else b) if isinstance(test, bool) else jnp.where(test, a, b)


def _loop_rows(rows, step, fn):
    @pl.loop(0, rows // step)
    def _(i):
        fn(pl.ds(pl.multiple_of(i * step, step), step))


def _add_rows(dst, srcs, step):
    def add(r):
        acc = dst[r, :]
        for s in srcs:
            acc = acc + s[r, :]
        dst[r, :] = acc

    _loop_rows(dst.shape[0], step, add)


SLOTS = 12
FEW = 64
TWO = range(2)
LOG2E = math.log2(math.e)
NEAR_KEYS = ("near_r", "near_l", "sum_r", "sum_l")
scope = jax.named_scope


def _kernel(
    dm, x4, e_ref, g_ref, lab, msk,
    dx_out, got2, q_o, xs, xe, eg, zh, q_h, xa, xb, dhp, yr,
    hv, etv, dz, od, sst, few, oext, ya, yb, yl, za, zb, zl, zr, tst,
    m_row, s_row, w_row, pos_row, lse_row, tgt_row, got, sm, got1, total_v,
    send, recv,
    free, tsem, hsem, dsem, osem, lsem,
):
    z, y, x, c = _coords()
    xc, zy = x * 2 + c, z * 4 + y
    rows, rm, ha, dim, h = dm.rows, dm.rm, dm.ha, dm.dim, dm.h
    chunk, tok, nt, hc = dm.chunk, dm.tok, dm.nt, dm.h // 2
    x_far, x_p, x_m = _mod4(x + 2), _mod4(x + 1), _mod4(x - 1)
    xp, xm = _dev(z, y, x_p, c), _dev(z, y, x_m, c)
    yp, ym = _dev(z, _mod4(y + 1), x, c), _dev(z, _mod4(y - 1), x, c)
    zp, zm = _dev(_mod4(z + 1), y, x, c), _dev(_mod4(z - 1), y, x, c)
    sib = _dev(z, y, x, 1 - c)
    near = [_dev(_mod4(z + a), _mod4(y + b), x, c) for a in range(4) for b in range(4) if a or b]
    line = [_dev(z, y, _mod4(x + a), lax.rem(c + b, 2)) for a in range(4) for b in TWO if a or b]
    bar = pltpu.get_barrier_semaphore()
    for p in (*near, *line):
        pl.semaphore_signal(bar, inc=1, device_id=(p,), device_id_type=MESH)
    sent = []
    ids = itertools.count()

    def remote(src, dst, dev):
        cp = _remote(src, dst, send, recv, next(ids), dev)
        cp.start()
        sent.append(cp)
        return cp

    def exchange(src, dst, devs):
        k = next(ids)
        for i, dev in enumerate(devs):
            _remote(src, dst.at[i], send, recv, k, dev).start()
        whole = dst.at[_top(len(devs))]
        return pltpu.make_async_copy(whole, whole, recv.at[k]), pltpu.make_async_copy(whole, whole, send.at[k])

    def local(src, dst, sem):
        cp = pltpu.make_async_copy(src, dst, sem)
        cp.start()
        return cp

    x_at, ext_at = 2 * rm, 4 * rm

    def xload(k):
        s = lax.rem(k, 4)
        to = dz.at[pl.ds(pl.multiple_of(x_at + s * chunk, chunk), chunk)]
        return pltpu.make_async_copy(x4.at[k, xc], to, tsem.at[s])

    with scope("prep"):
        for k in range(3):
            xload(k).start()
        own = xc
        for j in TWO:
            def widen(r, j=j):
                od[0, j, r, :] = e_ref[pl.ds(j * ha + r.start, r.size), :].astype(F32)

            _loop_rows(ha, 16, widen)
        oext[...] = jnp.zeros_like(oext)
        oext[0 : rows - rm, :] = e_ref[rm:rows, :].astype(F32)
        cps = [local(od.at[0, j, _top(ha)], eg.at[own, pl.ds(j * ha, ha)], hsem.at[j]) for j in TWO]
        cps.append(local(oext, eg.at[own, pl.ds(rm, 8)], hsem.at[2]))
        for cp in cps:
            cp.wait()
        pl.semaphore_wait(bar, 22)

    half_a, half_b = _top(ha), pl.ds(ha, ha + 8)

    def piece(s, r, dev):
        return remote(eg.at[s, r], eg.at[s, r], dev)

    def slot(xx):
        return xx * 2 + c

    r_a, l_b = piece(own, half_a, xp), piece(own, half_b, xm)
    s_o = piece(own, _top(dm.pad), sib)
    r_b, l_a = piece(own, half_b, xp), piece(own, half_a, xm)

    gain = g_ref[...]

    with scope("norm"):
        @pl.loop(0, 16)
        def _(k):
            @pl.when(k < 13)
            def _():
                xload(k + 3).start()

            xload(k).wait()

            def norm(r):
                v = dz[pl.ds(pl.multiple_of(x_at + lax.rem(k, 4) * chunk + r.start, r.size), r.size), :].astype(F32)
                inv = lax.rsqrt(jnp.mean(v * v, axis=-1, keepdims=True) + NORM_EPS)
                hv[pl.ds(pl.multiple_of(k * chunk + r.start, r.size), r.size), :] = (v * inv * gain).astype(BF16)

            _loop_rows(chunk, 16, norm)

    with scope("labels"):
        total = jnp.sum(msk[...])
        for k in range(16):
            at = pl.ds(k * chunk, chunk)
            w_row[:, at] = msk[k, xc] / total
            q = lab[k, xc] - zy * (8 * rows)
            s = jnp.zeros_like(q)
            for i in range(1, 8):
                s = s + jnp.where(q >= i * rows, 1, 0)
            r = q - s * rows
            up = jnp.where(r >= ha, 1, 0)
            at_main = ((s // 2 * 2 + up) * 2 + s % 2) * ha + r - up * ha
            at_ext = dm.main + s * 8 + r - rm
            place = jnp.where(r < rm, at_main, at_ext)
            pos_row[:, at] = jnp.where((q >= 0) & (q < 8 * rows), place, -1).astype(F32)

    def product(lhs, lanes):
        v = lax.dot_general(lhs, hv[lanes, :], (((1,), (1,)), ((), ())), preferred_element_type=F32)
        return v * (LOG2E / LOGIT_SCALE)

    def add_stats(v, lanes):
        m_old, s_old = m_row[:, lanes], s_row[:, lanes]
        m = jnp.maximum(m_old, jnp.max(v, axis=0, keepdims=True))
        s = jnp.sum(jnp.exp2(v - m), axis=0, keepdims=True)
        m_row[:, lanes] = m
        s_row[:, lanes] = s_old * jnp.exp2(m_old - m) + s

    def add_target(v, place, lanes):
        r = lax.broadcasted_iota(jnp.int32, v.shape, 0)
        hit = r.astype(F32) == pos_row[:, lanes] - place.astype(F32)
        tgt_row[:, lanes] += jnp.sum(jnp.where(hit, v, 0.0), axis=0, keepdims=True)

    m_row[:, :] = jnp.full((1, tok), -1e30, F32)
    s_row[:, :] = jnp.zeros((1, tok), F32)
    tgt_row[:, :] = jnp.zeros((1, tok), F32)
    segs = [(half, j) for half in TWO for j in TWO]

    def load(r0, n, xx):
        return [
            local(
                eg.at[xx[half] * 2 + j, pl.ds(half * ha + r0, n)], od.at[j, half, pl.ds(r0, n)], hsem.at[half * 2 + j]
            )
            for half, j in segs
        ]

    def narrow_all(r0, n, src):
        for half, j in segs:
            def narrow(r, half=half, j=j):
                at = pl.multiple_of((half * 2 + j) * ha + r0 + r.start, r.size)
                dz[pl.ds(at, r.size), :] = src(half, j)[r, :].astype(BF16)

            _loop_rows(n, 16, narrow)

    def block(r0, n, xx, loads=(), with_few=False):
        if loads:
            for cp in loads:
                cp.wait()
            narrow_all(r0, n, lambda half, j: od.at[j, half, pl.ds(r0, n)])
        left = [VOCAB_REAL - ((zy * 8 + xx[half] * 2 + j) * rows + half * ha + r0) for half, j in segs]
        w = nt // chunk
        deep = SLOTS // w

        def out(t):
            u = lax.rem(t, deep) * w
            return [
                pltpu.make_async_copy(
                    tst.at[u + i, pl.ds(m * n, n)],
                    zh.at[t * w + i, pl.ds(pl.multiple_of((xx[half] * 2 + half) * rm + j * ha + r0, 8), n)],
                    tsem.at[u + i],
                )
                for i in range(w)
                for m, (half, j) in enumerate(segs)
            ]

        def out_wait(t):
            u = lax.rem(t, deep) * w
            for i in range(w):
                whole = tst.at[u + i, _top(4 * n)]
                pltpu.make_async_copy(whole, zh.at[t * w + i, _top(4 * n)], tsem.at[u + i]).wait()

        @pl.loop(0, tok // nt)
        def _(t):
            @pl.when(t >= deep)
            def _():
                out_wait(t - deep)

            lanes = pl.ds(pl.multiple_of(t * nt, nt), nt)
            lhs = [dz[(half * 2 + j) * ha + r0 : (half * 2 + j) * ha + r0 + n, :] for half, j in segs]
            if with_few:
                lhs.append(dz[ext_at : ext_at + FEW, :])
            v = product(jnp.concatenate(lhs, axis=0), lanes)
            v, v_few = v[: 4 * n], v[4 * n :]
            r = lax.broadcasted_iota(jnp.int32, (n, nt), 0)
            v = [jnp.where(r < left[m], v[m * n : (m + 1) * n], -jnp.inf) for m in range(len(segs))]
            for part_v, (half, j) in zip(v, segs):
                add_target(part_v, (xx[half] * 2 + half) * rm + j * ha + r0, lanes)
            u = lax.rem(t, deep) * w
            for i in range(w):
                for m in range(len(segs)):
                    tst[u + i, m * n : (m + 1) * n, :] = v[m][:, i * chunk : (i + 1) * chunk]
            if with_few:
                r = lax.broadcasted_iota(jnp.int32, v_few.shape, 0)
                ok = ((r & 7) < rows - rm) & ((zy * 8 + (r >> 3)) * rows + rm + (r & 7) < VOCAB_REAL)
                v_few = jnp.where(ok, v_few, -jnp.inf)
                few[:, lanes] = v_few
                add_target(v_few, jnp.int32(dm.main), lanes)
                v.append(v_few)
            v = jnp.concatenate(v, axis=0)
            for cp in out(t):
                cp.start()
            add_stats(v, lanes)

        for t in range(deep):
            out_wait(t + tok // nt - deep)

    def both(xx):
        block(0, ha, xx, load(0, ha, xx))

    def turn(xx):
        for half in TWO:
            base = pl.multiple_of((xx[half] * 2 + half) * rm, rm)

            @pl.loop(0, dim // 128)
            def _(d, half=half, base=base):
                at = pl.ds(pl.multiple_of(d * 128, 128), 128)
                etv[at, pl.ds(base, rm)] = dz[half * rm : (half + 1) * rm, at].T

    with scope("own"):
        s_o.wait_recv()
        both((x, x))
        turn((x, x))

    with scope("wait_1"):
        r_a.wait_recv()
        last_n = dm.cuts[-1][1]
        spans = [(pl.ds(r0, n), pl.ds(ha + r0, n + 8 * (r0 + n == ha))) for r0, n in dm.cuts]

        def far_pieces(xx, half, to):
            cps = [piece(slot(xx), pair[half], to) for pair in spans[:-1]]
            cps.append(remote(eg.at[slot(xx), spans[-1][half]], sst.at[c, pl.ds(half * last_n, last_n)], to))
            return cps

        r_f = far_pieces(x_m, 0, xp)
        d = [piece(slot(x_m), half_a, sib)]
        l_b.wait_recv()
        l_f = far_pieces(x_p, 1, xm)
        d.append(piece(slot(x_p), half_b, sib))
        for cp in d:
            cp.wait_recv()

    with scope("near_1"):
        both((x_m, x_p))
        turn((x_m, x_p))

    with scope("wait_2"):
        r_b.wait_recv()
        d = [piece(slot(x_m), half_b, sib)]
        l_a.wait_recv()
        d.append(piece(slot(x_p), half_a, sib))
        for cp in d:
            cp.wait_recv()

    with scope("near_2"):
        both((x_p, x_m))
        turn((x_p, x_m))

    far = (x_far, x_far)

    def far_arrived(i):
        d = []
        for cp, r in zip((r_f[i], l_f[i]), spans[i]):
            cp.wait_recv()
            d.append(piece(slot(x_far), r, sib))
        for cp in d:
            cp.wait_recv()

    with scope("wait_3"):
        far_arrived(0)
    with scope("far_a"):
        loads = load(*dm.cuts[0], far)
        ext_loads = [local(eg.at[s, pl.ds(rm, 8)], few.at[pl.ds(s * 8, 8)], lsem.at[s]) for s in range(8)]
        for cp in ext_loads:
            cp.wait()
        dz[ext_at : ext_at + FEW, :] = few[...].astype(BF16)
        dz[ext_at + FEW : ext_at + 128, :] = jnp.zeros((FEW, dim), BF16)
        block(*dm.cuts[0], far, loads, True)
    with scope("wait_5"):
        r_f[-1].wait_recv()
        l_f[-1].wait_recv()
        both_last = sst.at[c, _top(2 * last_n)]
        over = _remote(both_last, both_last, send, recv, next(ids), sib)
        over.start()
        over.wait_recv()

    with scope("far_c"):
        narrow_all(0, last_n, lambda half, j: sst.at[j, pl.ds(half * last_n, last_n)])
        over.wait_send()
        for s in TWO:
            pl.semaphore_signal(free.at[s], inc=1, device_id=(sib,), device_id_type=MESH)
        block(0, last_n, far)

    with scope("turn_far"):
        lse_row[:, :] = m_row[:, :] + jnp.log(s_row[:, :]) * LOG2E
        stats = exchange(lse_row, got, near)
        turn(far)

        @pl.loop(0, dim // 128)
        def _(i):
            at = pl.ds(pl.multiple_of(i * 128, 128), 128)
            etv[at, dm.main : dm.wide] = dz[ext_at : ext_at + 128, at].T

    wide = 2 * rm

    at_dht = SLOTS - 4

    def chunk_of(zz, yy):
        return _mod4(zz) * 4 + _rem(yy + 8, 4)

    def all_far(i):
        return x_far * wide + i // 16 * rm, _rem(i, 16)

    def in_order(i):
        n = i // 3
        m = n - 7
        k = _pick(n < 7, chunk_of(z + n - 1, y + 2), chunk_of(z + 3 + m // 3, y + 3 + _rem(m + 9, 3)))
        return _mod4(x + 3 + _rem(i, 3)) * wide, _pick(n < 4, chunk_of(z + 2, n), k)

    def later(i):
        return in_order(i + SLOTS)

    def zload(where, i, ring, n):
        at, k = where(i)
        s = _rem(i, ring)
        src = zh.at[k, pl.ds(pl.multiple_of(at, rm), n)]
        return pltpu.make_async_copy(src, tst.at[s, _top(n)], tsem.at[s])

    def zahead(where, ring, n):
        for i in range(ring):
            zload(where, i, ring, n).start()

    with scope("stats"):
        zahead(all_far, SLOTS, rm)
        for cp in stats:
            cp.wait()
        top = lse_row[:, :]
        for k in range(len(near)):
            top = jnp.maximum(top, got[k])
        s = jnp.exp2(lse_row[:, :] - top)
        for k in range(len(near)):
            s = s + jnp.exp2(got[k] - top)
        lse_row[:, :] = top + jnp.log(s) * LOG2E

    def dz_part(v, place, at, lanes):
        r = lax.broadcasted_iota(jnp.int32, v.shape, 0).astype(F32)
        hit = r == pos_row[:, lanes] - place.astype(F32)
        p = jnp.exp2(v - lse_row[:, lanes])
        dz[at, lanes] = (jnp.where(hit, p - 1.0, p) * w_row[:, lanes]).astype(BF16)

    step = min(128, rm)

    def dz_rows(where, start, stop, last_tile, ring, n):
        @pl.loop(start, stop)
        def _(i):
            @pl.when((i > 0) & (i + ring - 1 < last_tile))
            def _():
                zload(where, i + ring - 1, ring, n).start()

            zload(where, i, ring, n).wait()
            row, k = where(i)
            lanes = pl.ds(pl.multiple_of(k * chunk, chunk), chunk)

            @pl.loop(0, n // step)
            def _(j):
                at = pl.multiple_of(row + j * step, step)
                r = pl.ds(pl.multiple_of(j * step, step), step)
                dz_part(tst[lax.rem(i, ring), r, :], at, pl.ds(at, step), lanes)

    def dz_far(start, stop):
        dz_rows(all_far, start, stop, 32, SLOTS, rm)

    with scope("dz_far"):
        dz_far(0, 16)

    nd = dim // 2
    few_rows = pl.ds(dm.main, FEW)
    pair_ids = [(next(ids), next(ids)) for _ in TWO]

    def over_d2d(s, n, i):
        lanes = pl.ds(pl.multiple_of(i * nd, nd), nd)
        there = sst.at[s, _top(n), lanes]
        return _remote(od.at[s, 1 - c, _top(n), lanes], there, send, recv, pair_ids[s][0] + i, sib)

    def de_block(xx, half, s, with_few=False):
        at = pl.ds(pl.multiple_of((xx * 2 + half) * rm, rm), rm)
        n = ha + 8 * half
        pl.semaphore_wait(free.at[s], 1)

        @pl.loop(0, 2)
        def _(i):
            lanes = pl.ds(pl.multiple_of(i * nd, nd), nd)
            lhs = jnp.concatenate([dz[at, :], dz[few_rows, :]], axis=0) if with_few else dz[at, :]
            v = jnp.dot(lhs, hv[:, lanes], preferred_element_type=F32)
            if with_few:
                few[:, lanes] = v[rm:]
            for j in TWO:
                od[s, j, 0:ha, lanes] = v[j * ha : (j + 1) * ha]
                if half:
                    od[s, j, ha:n, lanes] = few[pl.ds(pl.multiple_of((xx * 2 + j) * 8, 8), 8), lanes]
            over_d2d(s, n, i).start()

        return half, s, n

    def stored(blk, to):
        half, s, n = blk
        return pltpu.make_async_copy(od.at[s, c, _top(n)], to.at[pl.ds(half * ha, n)], dsem.at[s])

    def early(blk, src):
        half, s, n = blk
        for i in TWO:
            over_d2d(s, n, i).wait_send()
        return local(src.at[pl.ds(half * ha, n)], od.at[s, 1 - c, _top(n)], lsem.at[s])

    def sum_add(blk, to, more=None):
        half, s, n = blk
        for i in TWO:
            over_d2d(s, n, i).wait_recv()
        if more is not None:
            more.wait()

        def add(r):
            v = od[s, c, r, :] + sst[s, r, :]
            od[s, c, r, :] = v if more is None else v + od[s, 1 - c, r, :]

        _loop_rows(n, 8, add)
        if more is None:
            pl.semaphore_signal(free.at[s], inc=1, device_id=(sib,), device_id_type=MESH)
            for i in TWO:
                over_d2d(s, n, i).wait_send()
        cp = stored(blk, to)
        cp.start()
        return cp

    def ring_sum(xx, rows_, n, src, s, dst, dev):
        lds = [
            local(q_h.at[xx, rows_], od.at[s, 0, _top(n)], lsem.at[0]),
            local(src, od.at[s, 1, _top(n)], lsem.at[1]),
        ]
        for cp in lds:
            cp.wait()
        _add_rows(od.at[s, 0, _top(n)], [od.at[s, 1, _top(n)]], 8)
        local(od.at[s, 0, _top(n)], q_h.at[xx, rows_], lsem.at[0]).wait()
        return remote(q_h.at[xx, rows_], dst, dev)

    stores = []

    def flush():
        while stores:
            stores.pop().wait()

    def tiles(q, where, between=None):
        flush()

        def outs(i):
            p, ab = where(i)
            r = pl.ds(q * h, h)
            dsts = [dhp.at[ab * 2 + j, p, r] if q == 0 else dhp.at[p, ab * 2 + j, r] for j in TWO]
            return [
                pltpu.make_async_copy(tst.at[at_dht + i * 2 + j, _top(h)], dst, hsem.at[i * 2 + j])
                for j, dst in enumerate(dsts)
            ]

        @pl.loop(0, 2)
        def _(i):
            if between is not None:
                pl.when(i > 0)(between)
            p, ab = where(i)
            ks = [(ab * 2 + j) * 4 + p if q == 0 else p * 4 + ab * 2 + j for j in TWO]
            rhs = jnp.concatenate([dz[:, pl.ds(pl.multiple_of(k * chunk, chunk), chunk)] for k in ks], axis=1)
            v = jnp.dot(etv[q * h : (q + 1) * h, :], rhs, preferred_element_type=F32)
            for j in TWO:
                tst[at_dht + i * 2 + j, 0:h, :] = v[:, j * chunk : (j + 1) * chunk]
            for cp in outs(i):
                cp.start()

        for i in TWO:
            stores.extend(outs(i))

    def part(q, p, lo, n):
        r = pl.ds(q * h, h)
        if q == 0:
            return dhp.at[pl.ds(lo, n), p, r]
        return dhp.at[p, pl.ds(lo, n), r]

    def one(q, p, i):
        r = pl.ds(q * h, h)
        return dhp.at[i, p, r] if q == 0 else dhp.at[p, i, r]

    ring1, ring2 = ((yp, ym), (zp, zm)), ((zp, zm), (yp, ym))
    pos1, pos2 = (y, z), (z, y)
    first, second = ({}, {}), ({}, {})

    def send_far(q):
        flush()
        p, (rt, lt) = pos1[q], ring1[q]
        first[q]["far_r"] = remote(part(q, _mod4(p + 2), 0, 2), ya.at[q], rt)
        first[q]["far_l"] = remote(part(q, _mod4(p + 2), 2, 2), yb.at[q], lt)

    def send_near(q):
        flush()
        p, (rt, lt) = pos1[q], ring1[q]
        first[q]["near_r"] = remote(part(q, _mod4(p + 1), 2, 2), yl.at[q, pl.ds(2, 2)], rt)
        first[q]["near_l"] = remote(part(q, _mod4(p - 1), 0, 2), yr.at[q, _top(2)], lt)

    def fetch(i, src):
        return local(src, tst.at[i, _top(h)], tsem.at[i])

    def pass_on(q):
        flush()
        p, (rt, lt) = pos1[q], ring1[q]
        lds = [fetch(i, one(q, _mod4(p + 1), i)) for i in TWO]
        lds += [fetch(2 + i, one(q, _mod4(p - 1), 2 + i)) for i in TWO]
        first[q]["far_r"].wait_recv()
        for i in TWO:
            lds[i].wait()
            _add_rows(ya.at[q, i], [tst.at[i, _top(h)]], min(FEW, h))
        first[q]["sum_r"] = remote(ya.at[q], yl.at[q, _top(2)], rt)
        first[q]["far_l"].wait_recv()
        for i in TWO:
            lds[2 + i].wait()
            _add_rows(yb.at[q, i], [tst.at[2 + i, _top(h)]], min(FEW, h))
        first[q]["sum_l"] = remote(yb.at[q], yr.at[q, pl.ds(2, 2)], lt)

    lo, hi = _top(hc), pl.ds(hc, hc)

    def second_phase(q):
        flush()
        r, (rt, lt) = pos2[q], ring2[q]
        r2, r1, rm1 = _mod4(r + 2), _mod4(r + 1), _mod4(r - 1)
        order = (r2, r1, rm1, r)
        lds = [fetch(i, one(q, pos1[q], k)) for i, k in enumerate(order)]
        for k in NEAR_KEYS:
            first[q][k].wait_recv()
        lds2 = [fetch(4 + i, yr.at[q, k]) for i, k in enumerate(order)]
        for i, k in enumerate(order):
            lds[i].wait()
            lds2[i].wait()
            _add_rows(yl.at[q, k], [tst.at[i, _top(h)], tst.at[4 + i, _top(h)]], min(FEW, h))
            if i == 0:
                second[q]["far_r"] = remote(yl.at[q, r2, lo], za.at[q], rt)
                second[q]["far_l"] = remote(yl.at[q, r2, hi], zb.at[q], lt)
            if i == 1:
                second[q]["near_r"] = remote(yl.at[q, r1, hi], zl.at[q, hi], rt)
            if i == 2:
                second[q]["near_l"] = remote(yl.at[q, rm1, lo], zr.at[q, lo], lt)

    def second_pass(q):
        r, (rt, lt) = pos2[q], ring2[q]
        r1, rm1 = _mod4(r + 1), _mod4(r - 1)
        second[q]["far_r"].wait_recv()
        _add_rows(yl.at[q, r1, lo], [za.at[q]], min(FEW, hc))
        second[q]["sum_r"] = remote(yl.at[q, r1, lo], zl.at[q, lo], rt)
        second[q]["far_l"].wait_recv()
        _add_rows(yl.at[q, rm1, hi], [zb.at[q]], min(FEW, hc))
        second[q]["sum_l"] = remote(yl.at[q, rm1, hi], zr.at[q, hi], lt)

    def last(q):
        r = pos2[q]
        for k in NEAR_KEYS:
            second[q][k].wait_recv()
        n = min(128, h)

        @pl.loop(0, h // n)
        def _(i):
            at = pl.ds(pl.multiple_of(i * n, n), n)
            v = yl[q, r, at, :] + zl[q, at, :] + zr[q, at, :]
            od[0, 0, 0:chunk, pl.ds(pl.multiple_of(q * h + i * n, n), n)] = (v * (1.0 / LOGIT_SCALE)).T

    def tiles_far(q, between=None):
        tiles(q, lambda i: (_mod4(pos1[q] + 2), i), between)

    def tiles_near(q):
        tiles(q, lambda i: (_mod4(pos1[q] + 1 + 2 * i), 1 - i))

    def tiles_pass(q):
        tiles(q, lambda i: (_mod4(pos1[q] + 1 + 2 * i), i))

    def tiles_own(q):
        tiles(q, lambda i: (pos1[q], i))

    all_later = 48 - SLOTS

    def dz_first(start, stop):
        dz_rows(in_order, start, stop, SLOTS, SLOTS, wide)

    def dz_later(start, stop):
        dz_rows(later, start, stop, all_later, at_dht, wide)

    with scope("de_far"):
        b0 = de_block(x_far, 0, 0)
        dz_far(16, 32)
        zahead(in_order, SLOTS, wide)
        for l in range(0, tok, nt):
            lanes = pl.ds(l, nt)
            dz_part(few[:, lanes], jnp.int32(dm.main), few_rows, lanes)
        dz[dm.main + FEW : dm.wide, :] = jnp.zeros((FEW, tok), BF16)
        b1 = de_block(x_far, 1, 1, True)
    with scope("dz_1"):
        c0 = sum_add(b0, q_h.at[x_far])
        dz_first(0, 8)
        c0.wait()
        e0 = remote(q_h.at[x_far, half_a], xa, xp)
        dz_first(8, SLOTS)
        zahead(later, at_dht, wide)
    with scope("dh_far1"):
        def between():
            sum_add(b1, q_h.at[x_far])

        tiles_far(1, between)
        c1 = stored(b1, q_h.at[x_far])
        c1.wait()
        e1 = remote(q_h.at[x_far, half_b], xb, xm)
    with scope("dz_2"):
        dz_later(0, 9)
        send_far(1)
    with scope("dh_far0"):
        tiles_far(0)
    with scope("dz_3"):
        dz_later(9, 13)
        send_far(0)
        dz_later(13, all_later)
    with scope("de_2"):
        b2 = de_block(x_p, 1, 0)
        b3 = de_block(x_m, 0, 1)
        c2 = sum_add(b2, q_h.at[x_p])
    with scope("dh_near"):
        tiles_near(1)
        c2.wait()
        e2 = remote(q_h.at[x_p, half_b], xe.at[half_b], xp)
        c3 = sum_add(b3, q_h.at[x_m])
        send_near(1)
        tiles_near(0)
        c3.wait()
        e3 = remote(q_h.at[x_m, half_a], xe.at[half_a], xm)
        send_near(0)
    with scope("dh_pass"):
        tiles_pass(1)
        tiles_pass(0)
        pass_on(1)
    with scope("de_4"):
        b4 = de_block(x_p, 0, 0)
        pass_on(0)
        b5 = de_block(x_m, 1, 1)
        c4 = sum_add(b4, q_h.at[x_p])
    with scope("dh_own"):
        tiles_own(1)
        c5 = sum_add(b5, q_h.at[x_m])
        tiles_own(0)
        c4.wait()
        c5.wait()
    old = list(sent)
    sent.clear()
    with scope("ring"):
        e0.wait_recv()
        e4 = ring_sum(x_p, half_a, ha, xa, 0, xs.at[half_a], xp)
        e1.wait_recv()
        e5 = ring_sum(x_m, half_b, ha + 8, xb, 1, xs.at[half_b], xm)
    with scope("de_6"):
        b6 = de_block(x, 0, 0)
    with scope("de_7"):
        b7 = de_block(x, 1, 1)
        xo_load = local(x4.at[zy, xc], dz.at[_top(chunk)], osem.at[0])
    with scope("second_1"):
        second_phase(1)
    with scope("second_0"):
        second_phase(0)
    with scope("spass_1"):
        second_pass(1)
    with scope("sum_6"):
        e3.wait_recv()
        c6 = early(b6, xe)
        e2.wait_recv()
        c7 = early(b7, xe)
        c6 = sum_add(b6, q_o, c6)
        c7 = sum_add(b7, q_o, c7)
    with scope("spass_0"):
        second_pass(0)
        c6.wait()
        c7.wait()
    def drain(cps):
        while cps:
            cps.pop().wait_send()

    def own_x(r):
        v = dz[r, :].astype(F32)
        inv = lax.rsqrt(jnp.mean(v * v, axis=-1, keepdims=True) + NORM_EPS)
        od[1, 0, r, :] = v * inv
        od[1, 1, r, 0:128] = jnp.broadcast_to(inv, (r.size, 128))

    def own_dg(q):
        lanes = pl.ds(q * h, h)

        def add(i, acc):
            r = pl.ds(pl.multiple_of(i * 8, 8), 8)
            return acc + od[0, 0, r, lanes] * od[1, 0, r, lanes]

        acc = lax.fori_loop(0, chunk // 8, add, jnp.zeros((8, h), F32))
        sm[:, lanes] = jnp.sum(acc, axis=0, keepdims=True)

    def own_dx(r):
        x_hat, u = od[1, 0, r, :], od[0, 0, r, :] * gain
        od[0, 1, r, :] = od[1, 1, r, 0:1] * (u - x_hat * jnp.mean(u * x_hat, axis=-1, keepdims=True))

    with scope("own_x"):
        xo_load.wait()
        _loop_rows(chunk, 16, own_x)
        lse = jnp.where(zy == 0, lse_row[:, :], 0.0)
        loss = jnp.sum(w_row[:, :] * (lse - tgt_row[:, :]))
        sm[:, dim : dim + 128] = jnp.full((1, 128), loss / LOG2E)
        drain(old)
    with scope("last_1"):
        last(1)
        own_dg(1)
    with scope("last_0"):
        last(0)
        own_dg(0)

    with scope("small_1"):
        old = [cp for cp in sent if cp is not e4 and cp is not e5]
        near_sums = exchange(sm, got1, near)
        _loop_rows(chunk, 16, own_dx)
        dx_copy = local(od.at[0, 1, _top(chunk)], dx_out, osem.at[0])
        drain(old)
        for cp in near_sums:
            cp.wait()
    with scope("small_2"):
        tot = sm[...]
        for k in range(len(near)):
            tot = tot + got1[k]
        total_v[...] = tot
        all_sums = exchange(total_v, got2, line)
        mine = local(total_v, got2.at[len(line)], osem.at[1])
    with scope("ring_end"):
        for cp in (e4, e5):
            cp.wait()
        dx_copy.wait()
        mine.wait()
    with scope("small_3"):
        for cp in all_sums:
            cp.wait()


def _run(dm, x4, table, gain, labels, mask):
    hbm, vm = pl.BlockSpec(memory_space=HBM), pl.BlockSpec(memory_space=VMEM)
    sd = jax.ShapeDtypeStruct
    d, tok, h, ck, pad, ha = dm.dim, dm.tok, dm.h, dm.chunk, dm.pad, dm.ha
    line, quad, pair = VMEM((1, tok), F32), VMEM((2, 2, h, ck), F32), VMEM((2, h, ck), F32)
    part, shard = VMEM((2, h // 2, ck), F32), sd((pad, d), F32)
    out = pl.pallas_call(
        functools.partial(_kernel, dm),
        name="head",
        out_shape=(
            sd((ck, d), F32), sd((8, 1, d + 128), F32),
            shard, shard, shard,
            sd((8, pad, d), F32), sd((16, dm.main, ck), F32),
            sd((4, pad, d), F32), sd((ha, d), F32), sd((ha + 8, d), F32),
            sd((4, 4, d, ck), F32), sd((2, 4, h, ck), F32),
        ),
        in_specs=[hbm, vm, vm, vm, vm],
        out_specs=[hbm] * 12,
        scratch_shapes=[
            VMEM((tok, d), BF16), VMEM((d, dm.wide), BF16), VMEM((dm.wide, tok), BF16),
            VMEM((2, 2, ha + 8, d), F32), VMEM((2, ha + 8, d), F32), VMEM((FEW, d), F32), VMEM((8, d), F32),
            quad, quad, VMEM((2, 4, h, ck), F32),
            part, part, pair, pair,
            VMEM((SLOTS, max(h, 2 * dm.rm), ck), F32),
            line, line, line, line, line, line, VMEM((15, 1, tok), F32),
            VMEM((1, d + 128), F32), VMEM((15, 1, d + 128), F32), VMEM((1, d + 128), F32),
            DMA((53,)), DMA((53,)), pltpu.SemaphoreType.REGULAR((2,)),
            DMA((SLOTS,)), DMA((4,)), DMA((2,)), DMA((2,)), DMA((8,)),
        ],
        compiler_params=pltpu.CompilerParams(
            collective_id=0, has_side_effects=True, vmem_limit_bytes=67043328
        ),
    )(x4, table, gain, labels, mask)
    return _write_out(dm, out[2:4], *out[:2])


def _write_kernel(own, ring, dx, small, de_o, dx_o, dg_o, loss_o):
    de_o[:, :] = (own[:, :] + ring[:, :]) * (1.0 / LOGIT_SCALE)
    dx_o[:, :] = dx[:, :]
    total = jnp.sum(small[:, :, :], axis=0)
    d = dg_o.shape[1]
    dg_o[:, :] = total[:, :d]
    loss_o[:, :] = total[:, d : d + 1]


def _write_out(dm, parts, dx, small):
    d, step, blocks = dm.dim, dm.ha + 8, 2
    sd = jax.ShapeDtypeStruct
    some = pl.BlockSpec((step, d), lambda i: (i, 0))
    half = pl.BlockSpec((dm.chunk // blocks, d), lambda i: (i, 0))
    row, one = pl.BlockSpec((1, d), lambda i: (0, 0)), pl.BlockSpec((1, 1), lambda i: (0, 0))
    rows = pl.BlockSpec(small.shape, lambda i: (0, 0, 0))
    return pl.pallas_call(
        _write_kernel,
        name="write_out",
        grid=(blocks,),
        out_shape=(sd((dm.rows, d), F32), sd((dm.chunk, d), F32), sd((1, d), F32), sd((1, 1), F32)),
        in_specs=[some, some, half, rows],
        out_specs=(some, half, row, one),
    )(*parts, dx, small)


def solution(mesh):
    group = mesh.shape[AXIS]

    def local_step(residual, labels, loss_mask, norm_gain, table_shard):
        tokens, dim = residual.shape
        rows = table_shard.shape[0]
        dm = Dims(tokens, dim, rows, group)
        x4 = residual.reshape(16, 8, dm.chunk, dim)
        lab = labels.reshape(16, 8, 1, dm.chunk)
        msk = loss_mask.reshape(16, 8, 1, dm.chunk)
        d_embed, d_res, d_gain, loss = _run(dm, x4, table_shard, norm_gain[None, :], lab, msk)
        return loss.reshape(()), d_res, d_embed, d_gain.reshape(dim)

    return jax.shard_map(
        local_step,
        mesh=mesh,
        in_specs=(P(), P(), P(), P(), P(AXIS, None)),
        out_specs=(P(), P(AXIS, None), P(AXIS, None), P()),
        check_vma=False,
    )
```

```python
import functools
import itertools
import math

import jax
import jax.numpy as jnp
from jax import lax
from jax.experimental import pallas as pl
from jax.experimental.pallas import tpu as pltpu
from jax.sharding import PartitionSpec as P

VOCAB_REAL = 49155
LOGIT_SCALE = 6.0
NORM_EPS = 1e-6

AXIS = "vp"
MESH = pl.DeviceIdType.MESH
F32 = jnp.float32
BF16 = jnp.bfloat16
HBM = pltpu.HBM
VMEM = pltpu.VMEM
DMA = pltpu.SemaphoreType.DMA


def _coords():
    me = lax.axis_index(AXIS)
    return me // 32, (me // 8) % 4, (me // 2) % 4, me % 2


def _dev(z, y, x, c):
    return ((z * 4 + y) * 4 + x) * 2 + c


def _mod4(v):
    return lax.rem(v + 8, 4)


def _barrier(peers):
    sem = pltpu.get_barrier_semaphore()
    for p in peers:
        pl.semaphore_signal(sem, inc=1, device_id=(p,), device_id_type=MESH)
    pl.semaphore_wait(sem, len(peers))


def _remote(src, dst, send, recv, k, dev):
    return pltpu.make_async_remote_copy(
        src_ref=src,
        dst_ref=dst,
        send_sem=send.at[k],
        recv_sem=recv.at[k],
        device_id=(dev,),
        device_id_type=MESH,
    )


LANES = 128


class Dims:
    def __init__(self, tokens, dim, rows, group):
        self.dim, self.rows = dim, rows
        unit = LANES if rows >= LANES else 64
        self.rm = rows // unit * unit
        self.ha = self.rm // 2
        low = max(16, self.ha // 48 * 16)
        self.cuts = ((low, self.ha - low), (0, low))
        self.pad = self.rm + 8
        self.chunk = tokens // group
        self.tok = 16 * self.chunk
        self.nt = 4 * self.chunk
        self.main = 8 * self.rm
        self.wide = self.main + LANES
        self.h = dim // 2


def _top(n):
    return pl.ds(0, n)


def _rem(a, b):
    return a % b if isinstance(a, int) else lax.rem(a, b)


def _pick(test, a, b):
    return (a if test else b) if isinstance(test, bool) else jnp.where(test, a, b)


def _loop_rows(rows, step, fn):
    @pl.loop(0, rows // step)
    def _(i):
        fn(pl.ds(pl.multiple_of(i * step, step), step))


def _add_rows(dst, srcs, step):
    def add(r):
        acc = dst[r, :]
        for s in srcs:
            acc = acc + s[r, :]
        dst[r, :] = acc

    _loop_rows(dst.shape[0], step, add)


SLOTS = 12
FEW = 64
TWO = range(2)
LOG2E = math.log2(math.e)
NEAR_KEYS = ("near_r", "near_l", "sum_r", "sum_l")
scope = jax.named_scope


def _kernel(
    dm, x4, e_ref, g_ref, lab, msk,
    dx_out, got2, q_o, xs, xe, eg, zh, q_h, xa, xb, dhp, yr,
    hv, etv, dz, od, sst, few, oext, ya, yb, yl, za, zb, zl, zr, tst,
    m_row, s_row, w_row, pos_row, lse_row, tgt_row, got, sm, got1, total_v,
    send, recv,
    free, tsem, hsem, dsem, osem, lsem,
):
    z, y, x, c = _coords()
    xc, zy = x * 2 + c, z * 4 + y
    rows, rm, ha, dim, h = dm.rows, dm.rm, dm.ha, dm.dim, dm.h
    chunk, tok, nt, hc = dm.chunk, dm.tok, dm.nt, dm.h // 2
    x_far, x_p, x_m = _mod4(x + 2), _mod4(x + 1), _mod4(x - 1)
    xp, xm = _dev(z, y, x_p, c), _dev(z, y, x_m, c)
    yp, ym = _dev(z, _mod4(y + 1), x, c), _dev(z, _mod4(y - 1), x, c)
    zp, zm = _dev(_mod4(z + 1), y, x, c), _dev(_mod4(z - 1), y, x, c)
    sib = _dev(z, y, x, 1 - c)
    near = [_dev(_mod4(z + a), _mod4(y + b), x, c) for a in range(4) for b in range(4) if a or b]
    line = [_dev(z, y, _mod4(x + a), lax.rem(c + b, 2)) for a in range(4) for b in TWO if a or b]
    bar = pltpu.get_barrier_semaphore()
    for p in (*near, *line):
        pl.semaphore_signal(bar, inc=1, device_id=(p,), device_id_type=MESH)
    sent = []
    ids = itertools.count()

    def remote(src, dst, dev):
        cp = _remote(src, dst, send, recv, next(ids), dev)
        cp.start()
        sent.append(cp)
        return cp

    def exchange(src, dst, devs):
        k = next(ids)
        for i, dev in enumerate(devs):
            _remote(src, dst.at[i], send, recv, k, dev).start()
        whole = dst.at[_top(len(devs))]
        return pltpu.make_async_copy(whole, whole, recv.at[k]), pltpu.make_async_copy(whole, whole, send.at[k])

    def local(src, dst, sem):
        cp = pltpu.make_async_copy(src, dst, sem)
        cp.start()
        return cp

    x_at, ext_at = 2 * rm, 4 * rm

    def xload(k):
        s = lax.rem(k, 4)
        to = dz.at[pl.ds(pl.multiple_of(x_at + s * chunk, chunk), chunk)]
        return pltpu.make_async_copy(x4.at[k, xc], to, tsem.at[s])

    with scope("prep"):
        for k in range(3):
            xload(k).start()
        own = xc
        for j in TWO:
            def widen(r, j=j):
                od[0, j, r, :] = e_ref[pl.ds(j * ha + r.start, r.size), :].astype(F32)

            _loop_rows(ha, 16, widen)
        oext[...] = jnp.zeros_like(oext)
        oext[0 : rows - rm, :] = e_ref[rm:rows, :].astype(F32)
        cps = [local(od.at[0, j, _top(ha)], eg.at[own, pl.ds(j * ha, ha)], hsem.at[j]) for j in TWO]
        cps.append(local(oext, eg.at[own, pl.ds(rm, 8)], hsem.at[2]))
        for cp in cps:
            cp.wait()
        pl.semaphore_wait(bar, 22)

    half_a, half_b = _top(ha), pl.ds(ha, ha + 8)

    def piece(s, r, dev):
        return remote(eg.at[s, r], eg.at[s, r], dev)

    def slot(xx):
        return xx * 2 + c

    r_a, l_b = piece(own, half_a, xp), piece(own, half_b, xm)
    s_o = piece(own, _top(dm.pad), sib)
    r_b, l_a = piece(own, half_b, xp), piece(own, half_a, xm)

    gain = g_ref[...]

    with scope("norm"):
        @pl.loop(0, 16)
        def _(k):
            @pl.when(k < 13)
            def _():
                xload(k + 3).start()

            xload(k).wait()

            def norm(r):
                v = dz[pl.ds(pl.multiple_of(x_at + lax.rem(k, 4) * chunk + r.start, r.size), r.size), :].astype(F32)
                inv = lax.rsqrt(jnp.mean(v * v, axis=-1, keepdims=True) + NORM_EPS)
                hv[pl.ds(pl.multiple_of(k * chunk + r.start, r.size), r.size), :] = (v * inv * gain).astype(BF16)

            _loop_rows(chunk, 16, norm)

    with scope("labels"):
        total = jnp.sum(msk[...])
        for k in range(16):
            at = pl.ds(k * chunk, chunk)
            w_row[:, at] = msk[k, xc] / total
            q = lab[k, xc] - zy * (8 * rows)
            s = jnp.zeros_like(q)
            for i in range(1, 8):
                s = s + jnp.where(q >= i * rows, 1, 0)
            r = q - s * rows
            up = jnp.where(r >= ha, 1, 0)
            at_main = ((s // 2 * 2 + up) * 2 + s % 2) * ha + r - up * ha
            at_ext = dm.main + s * 8 + r - rm
            place = jnp.where(r < rm, at_main, at_ext)
            pos_row[:, at] = jnp.where((q >= 0) & (q < 8 * rows), place, -1).astype(F32)

    def product(lhs, lanes):
        v = lax.dot_general(lhs, hv[lanes, :], (((1,), (1,)), ((), ())), preferred_element_type=F32)
        return v * (LOG2E / LOGIT_SCALE)

    def add_stats(v, lanes):
        m_old, s_old = m_row[:, lanes], s_row[:, lanes]
        m = jnp.maximum(m_old, jnp.max(v, axis=0, keepdims=True))
        s = jnp.sum(jnp.exp2(v - m), axis=0, keepdims=True)
        m_row[:, lanes] = m
        s_row[:, lanes] = s_old * jnp.exp2(m_old - m) + s

    def add_target(v, place, lanes):
        r = lax.broadcasted_iota(jnp.int32, v.shape, 0)
        hit = r.astype(F32) == pos_row[:, lanes] - place.astype(F32)
        tgt_row[:, lanes] += jnp.sum(jnp.where(hit, v, 0.0), axis=0, keepdims=True)

    m_row[:, :] = jnp.full((1, tok), -1e30, F32)
    s_row[:, :] = jnp.zeros((1, tok), F32)
    tgt_row[:, :] = jnp.zeros((1, tok), F32)
    segs = [(half, j) for half in TWO for j in TWO]

    def load(r0, n, xx):
        return [
            local(
                eg.at[xx[half] * 2 + j, pl.ds(half * ha + r0, n)], od.at[j, half, pl.ds(r0, n)], hsem.at[half * 2 + j]
            )
            for half, j in segs
        ]

    def narrow_all(r0, n, src):
        for half, j in segs:
            def narrow(r, half=half, j=j):
                at = pl.multiple_of((half * 2 + j) * ha + r0 + r.start, r.size)
                dz[pl.ds(at, r.size), :] = src(half, j)[r, :].astype(BF16)

            _loop_rows(n, 16, narrow)

    def block(r0, n, xx, loads=(), with_few=False):
        if loads:
            for cp in loads:
                cp.wait()
            narrow_all(r0, n, lambda half, j: od.at[j, half, pl.ds(r0, n)])
        left = [VOCAB_REAL - ((zy * 8 + xx[half] * 2 + j) * rows + half * ha + r0) for half, j in segs]
        w = nt // chunk
        deep = SLOTS // w

        def out(t):
            u = lax.rem(t, deep) * w
            return [
                pltpu.make_async_copy(
                    tst.at[u + i, pl.ds(m * n, n)],
                    zh.at[t * w + i, pl.ds(pl.multiple_of((xx[half] * 2 + half) * rm + j * ha + r0, 8), n)],
                    tsem.at[u + i],
                )
                for i in range(w)
                for m, (half, j) in enumerate(segs)
            ]

        def out_wait(t):
            u = lax.rem(t, deep) * w
            for i in range(w):
                whole = tst.at[u + i, _top(4 * n)]
                pltpu.make_async_copy(whole, zh.at[t * w + i, _top(4 * n)], tsem.at[u + i]).wait()

        @pl.loop(0, tok // nt)
        def _(t):
            @pl.when(t >= deep)
            def _():
                out_wait(t - deep)

            lanes = pl.ds(pl.multiple_of(t * nt, nt), nt)
            lhs = [dz[(half * 2 + j) * ha + r0 : (half * 2 + j) * ha + r0 + n, :] for half, j in segs]
            if with_few:
                lhs.append(dz[ext_at : ext_at + FEW, :])
            v = product(jnp.concatenate(lhs, axis=0), lanes)
            v, v_few = v[: 4 * n], v[4 * n :]
            r = lax.broadcasted_iota(jnp.int32, (n, nt), 0)
            v = [jnp.where(r < left[m], v[m * n : (m + 1) * n], -jnp.inf) for m in range(len(segs))]
            for part_v, (half, j) in zip(v, segs):
                add_target(part_v, (xx[half] * 2 + half) * rm + j * ha + r0, lanes)
            u = lax.rem(t, deep) * w
            for i in range(w):
                for m in range(len(segs)):
                    tst[u + i, m * n : (m + 1) * n, :] = v[m][:, i * chunk : (i + 1) * chunk]
            if with_few:
                r = lax.broadcasted_iota(jnp.int32, v_few.shape, 0)
                ok = ((r & 7) < rows - rm) & ((zy * 8 + (r >> 3)) * rows + rm + (r & 7) < VOCAB_REAL)
                v_few = jnp.where(ok, v_few, -jnp.inf)
                few[:, lanes] = v_few
                add_target(v_few, jnp.int32(dm.main), lanes)
                v.append(v_few)
            v = jnp.concatenate(v, axis=0)
            for cp in out(t):
                cp.start()
            add_stats(v, lanes)

        for t in range(deep):
            out_wait(t + tok // nt - deep)

    def both(xx):
        block(0, ha, xx, load(0, ha, xx))

    def turn(xx):
        for half in TWO:
            base = pl.multiple_of((xx[half] * 2 + half) * rm, rm)

            @pl.loop(0, dim // LANES)
            def _(d, half=half, base=base):
                at = pl.ds(pl.multiple_of(d * LANES, LANES), LANES)
                etv[at, pl.ds(base, rm)] = dz[half * rm : (half + 1) * rm, at].T

    with scope("own"):
        s_o.wait_recv()
        both((x, x))
        turn((x, x))

    with scope("wait_1"):
        r_a.wait_recv()
        last_n = dm.cuts[-1][1]
        spans = [(pl.ds(r0, n), pl.ds(ha + r0, n + 8 * (r0 + n == ha))) for r0, n in dm.cuts]

        def far_pieces(xx, half, to):
            cps = [piece(slot(xx), pair[half], to) for pair in spans[:-1]]
            cps.append(remote(eg.at[slot(xx), spans[-1][half]], sst.at[c, pl.ds(half * last_n, last_n)], to))
            return cps

        r_f = far_pieces(x_m, 0, xp)
        d = [piece(slot(x_m), half_a, sib)]
        l_b.wait_recv()
        l_f = far_pieces(x_p, 1, xm)
        d.append(piece(slot(x_p), half_b, sib))
        for cp in d:
            cp.wait_recv()

    with scope("near_1"):
        both((x_m, x_p))
        turn((x_m, x_p))

    with scope("wait_2"):
        r_b.wait_recv()
        d = [piece(slot(x_m), half_b, sib)]
        l_a.wait_recv()
        d.append(piece(slot(x_p), half_a, sib))
        for cp in d:
            cp.wait_recv()

    with scope("near_2"):
        both((x_p, x_m))
        turn((x_p, x_m))

    far = (x_far, x_far)

    def far_arrived(i):
        d = []
        for cp, r in zip((r_f[i], l_f[i]), spans[i]):
            cp.wait_recv()
            d.append(piece(slot(x_far), r, sib))
        for cp in d:
            cp.wait_recv()

    with scope("wait_3"):
        far_arrived(0)
    with scope("far_a"):
        loads = load(*dm.cuts[0], far)
        ext_loads = [local(eg.at[s, pl.ds(rm, 8)], few.at[pl.ds(s * 8, 8)], lsem.at[s]) for s in range(8)]
        for cp in ext_loads:
            cp.wait()
        dz[ext_at : ext_at + FEW, :] = few[...].astype(BF16)
        dz[ext_at + FEW : ext_at + LANES, :] = jnp.zeros((FEW, dim), BF16)
        block(*dm.cuts[0], far, loads, True)
    with scope("wait_5"):
        @pl.loop(0, dim // LANES)
        def _(i):
            at = pl.ds(pl.multiple_of(i * LANES, LANES), LANES)
            etv[at, dm.main : dm.wide] = dz[ext_at : ext_at + LANES, at].T

        r_f[-1].wait_recv()
        l_f[-1].wait_recv()
        both_last = sst.at[c, _top(2 * last_n)]
        over = _remote(both_last, both_last, send, recv, next(ids), sib)
        over.start()
        over.wait_recv()

    with scope("far_c"):
        narrow_all(0, last_n, lambda half, j: sst.at[j, pl.ds(half * last_n, last_n)])
        block(0, last_n, far)
        over.wait_send()
        for s in TWO:
            pl.semaphore_signal(free.at[s], inc=1, device_id=(sib,), device_id_type=MESH)

    with scope("turn_far"):
        lse_row[:, :] = m_row[:, :] + jnp.log(s_row[:, :]) * LOG2E
        stats = exchange(lse_row, got, near)
        turn(far)

    wide = 2 * rm

    at_dht = SLOTS - 4

    def chunk_of(zz, yy):
        return _mod4(zz) * 4 + _rem(yy + 8, 4)

    def all_far(i):
        return x_far * wide + i // 16 * rm, _rem(i, 16)

    def in_order(i):
        n = i // 3
        m = n - 7
        k = _pick(n < 7, chunk_of(z + n - 1, y + 2), chunk_of(z + 3 + m // 3, y + 3 + _rem(m + 9, 3)))
        return _mod4(x + 3 + _rem(i, 3)) * wide, _pick(n < 4, chunk_of(z + 2, n), k)

    def later(i):
        return in_order(i + SLOTS)

    def zload(where, i, ring, n):
        at, k = where(i)
        s = _rem(i, ring)
        src = zh.at[k, pl.ds(pl.multiple_of(at, rm), n)]
        return pltpu.make_async_copy(src, tst.at[s, _top(n)], tsem.at[s])

    def zahead(where, ring, n):
        for i in range(ring):
            zload(where, i, ring, n).start()

    with scope("stats"):
        zahead(all_far, SLOTS, rm)
        for cp in stats:
            cp.wait()
        top = lse_row[:, :]
        for k in range(len(near)):
            top = jnp.maximum(top, got[k])
        s = jnp.exp2(lse_row[:, :] - top)
        for k in range(len(near)):
            s = s + jnp.exp2(got[k] - top)
        lse_row[:, :] = top + jnp.log(s) * LOG2E

    def dz_part(v, place, at, lanes):
        r = lax.broadcasted_iota(jnp.int32, v.shape, 0).astype(F32)
        hit = r == pos_row[:, lanes] - place.astype(F32)
        p = jnp.exp2(v - lse_row[:, lanes])
        dz[at, lanes] = (jnp.where(hit, p - 1.0, p) * w_row[:, lanes]).astype(BF16)

    step = min(LANES, rm)

    def dz_rows(where, start, stop, last_tile, ring, n):
        @pl.loop(start, stop)
        def _(i):
            @pl.when((i > 0) & (i + ring - 1 < last_tile))
            def _():
                zload(where, i + ring - 1, ring, n).start()

            zload(where, i, ring, n).wait()
            row, k = where(i)
            lanes = pl.ds(pl.multiple_of(k * chunk, chunk), chunk)

            @pl.loop(0, n // step)
            def _(j):
                at = pl.multiple_of(row + j * step, step)
                r = pl.ds(pl.multiple_of(j * step, step), step)
                dz_part(tst[lax.rem(i, ring), r, :], at, pl.ds(at, step), lanes)

    def dz_far(start, stop):
        dz_rows(all_far, start, stop, 32, SLOTS, rm)

    with scope("dz_far"):
        dz_far(0, 16)

    nd = dim // 2
    few_rows = pl.ds(dm.main, FEW)
    pair_ids = [(next(ids), next(ids)) for _ in TWO]

    def over_d2d(s, n, i):
        lanes = pl.ds(pl.multiple_of(i * nd, nd), nd)
        there = sst.at[s, _top(n), lanes]
        return _remote(od.at[s, 1 - c, _top(n), lanes], there, send, recv, pair_ids[s][0] + i, sib)

    def de_block(xx, half, s, with_few=False, between=None):
        at = pl.ds(pl.multiple_of((xx * 2 + half) * rm, rm), rm)
        n = ha + 8 * half
        pl.semaphore_wait(free.at[s], 1)

        @pl.loop(0, 2)
        def _(i):
            lanes = pl.ds(pl.multiple_of(i * nd, nd), nd)
            if between is not None:
                pl.when(i > 0)(between)
            lhs = jnp.concatenate([dz[at, :], dz[few_rows, :]], axis=0) if with_few else dz[at, :]
            v = jnp.dot(lhs, hv[:, lanes], preferred_element_type=F32)
            if with_few:
                few[:, lanes] = v[rm:]
            for j in TWO:
                od[s, j, 0:ha, lanes] = v[j * ha : (j + 1) * ha]
                if half:
                    od[s, j, ha:n, lanes] = few[pl.ds(pl.multiple_of((xx * 2 + j) * 8, 8), 8), lanes]
            over_d2d(s, n, i).start()

        return half, s, n

    def stored(blk, to):
        half, s, n = blk
        return pltpu.make_async_copy(od.at[s, c, _top(n)], to.at[pl.ds(half * ha, n)], dsem.at[s])

    def credit(s, n):
        pl.semaphore_signal(free.at[s], inc=1, device_id=(sib,), device_id_type=MESH)
        for i in TWO:
            over_d2d(s, n, i).wait_send()

    def sum_half(blk, i, to):
        half, s, n = blk
        lanes = pl.ds(i * nd, nd)
        over_d2d(s, n, i).wait_recv()

        def add(r):
            od[s, c, r, lanes] = od[s, c, r, lanes] + sst[s, r, lanes]

        _loop_rows(n, 8, add)
        if i:
            credit(s, n)
        return local(od.at[s, c, _top(n), lanes], to.at[pl.ds(half * ha, n), lanes], lsem.at[4 + s * 2 + i])

    def far_sends(r, dst, dev):
        cps = []
        for i in TWO:
            lanes = pl.ds(i * nd, nd)
            cps.append(_remote(q_h.at[x_far, r, lanes], dst.at[:, lanes], send, recv, next(ids), dev))
        sent.extend(cps)
        return cps

    def early(blk, src):
        half, s, n = blk
        for i in TWO:
            over_d2d(s, n, i).wait_send()
        return local(src.at[pl.ds(half * ha, n)], od.at[s, 1 - c, _top(n)], lsem.at[s])

    def sum_add(blk, to, more=None):
        half, s, n = blk
        for i in TWO:
            over_d2d(s, n, i).wait_recv()
        if more is not None:
            more.wait()

        def add(r):
            v = od[s, c, r, :] + sst[s, r, :]
            od[s, c, r, :] = v if more is None else v + od[s, 1 - c, r, :]

        _loop_rows(n, 8, add)
        if more is None:
            credit(s, n)
        cp = stored(blk, to)
        cp.start()
        return cp

    def ring_sum(xx, rows_, n, src, s, dst, dev):
        lds = [
            local(q_h.at[xx, rows_], od.at[s, 0, _top(n)], lsem.at[0]),
            local(src, od.at[s, 1, _top(n)], lsem.at[1]),
        ]
        for cp in lds:
            cp.wait()
        _add_rows(od.at[s, 0, _top(n)], [od.at[s, 1, _top(n)]], 8)
        local(od.at[s, 0, _top(n)], q_h.at[xx, rows_], lsem.at[0]).wait()
        return remote(q_h.at[xx, rows_], dst, dev)

    stores = []

    def flush():
        while stores:
            stores.pop().wait()

    def tiles(q, where, between=None):
        flush()

        def outs(i):
            p, ab = where(i)
            r = pl.ds(q * h, h)
            dsts = [dhp.at[ab * 2 + j, p, r] if q == 0 else dhp.at[p, ab * 2 + j, r] for j in TWO]
            return [
                pltpu.make_async_copy(tst.at[at_dht + i * 2 + j, _top(h)], dst, hsem.at[i * 2 + j])
                for j, dst in enumerate(dsts)
            ]

        @pl.loop(0, 2)
        def _(i):
            if between is not None:
                pl.when(i > 0)(between)
            p, ab = where(i)
            ks = [(ab * 2 + j) * 4 + p if q == 0 else p * 4 + ab * 2 + j for j in TWO]
            rhs = jnp.concatenate([dz[:, pl.ds(pl.multiple_of(k * chunk, chunk), chunk)] for k in ks], axis=1)
            v = jnp.dot(etv[q * h : (q + 1) * h, :], rhs, preferred_element_type=F32)
            for j in TWO:
                tst[at_dht + i * 2 + j, 0:h, :] = v[:, j * chunk : (j + 1) * chunk]
            for cp in outs(i):
                cp.start()

        for i in TWO:
            stores.extend(outs(i))

    def part(q, p, lo, n):
        r = pl.ds(q * h, h)
        if q == 0:
            return dhp.at[pl.ds(lo, n), p, r]
        return dhp.at[p, pl.ds(lo, n), r]

    def one(q, p, i):
        r = pl.ds(q * h, h)
        return dhp.at[i, p, r] if q == 0 else dhp.at[p, i, r]

    ring1, ring2 = ((yp, ym), (zp, zm)), ((zp, zm), (yp, ym))
    pos1, pos2 = (y, z), (z, y)
    first, second = ({}, {}), ({}, {})

    def send_far(q):
        flush()
        p, (rt, lt) = pos1[q], ring1[q]
        first[q]["far_r"] = remote(part(q, _mod4(p + 2), 0, 2), ya.at[q], rt)
        first[q]["far_l"] = remote(part(q, _mod4(p + 2), 2, 2), yb.at[q], lt)

    def send_near(q):
        flush()
        p, (rt, lt) = pos1[q], ring1[q]
        first[q]["near_r"] = remote(part(q, _mod4(p + 1), 2, 2), yl.at[q, pl.ds(2, 2)], rt)
        first[q]["near_l"] = remote(part(q, _mod4(p - 1), 0, 2), yr.at[q, _top(2)], lt)

    def fetch(i, src):
        return local(src, tst.at[i, _top(h)], tsem.at[i])

    def pass_on(q):
        flush()
        p, (rt, lt) = pos1[q], ring1[q]
        lds = [fetch(i, one(q, _mod4(p + 1), i)) for i in TWO]
        lds += [fetch(2 + i, one(q, _mod4(p - 1), 2 + i)) for i in TWO]
        first[q]["far_r"].wait_recv()
        for i in TWO:
            lds[i].wait()
            _add_rows(ya.at[q, i], [tst.at[i, _top(h)]], min(FEW, h))
        first[q]["sum_r"] = remote(ya.at[q], yl.at[q, _top(2)], rt)
        first[q]["far_l"].wait_recv()
        for i in TWO:
            lds[2 + i].wait()
            _add_rows(yb.at[q, i], [tst.at[2 + i, _top(h)]], min(FEW, h))
        first[q]["sum_l"] = remote(yb.at[q], yr.at[q, pl.ds(2, 2)], lt)

    lo, hi = _top(hc), pl.ds(hc, hc)

    def second_phase(q):
        flush()
        r, (rt, lt) = pos2[q], ring2[q]
        r2, r1, rm1 = _mod4(r + 2), _mod4(r + 1), _mod4(r - 1)
        order = (r2, r1, rm1, r)
        lds = [fetch(i, one(q, pos1[q], k)) for i, k in enumerate(order)]
        for k in NEAR_KEYS:
            first[q][k].wait_recv()
        lds2 = [fetch(4 + i, yr.at[q, k]) for i, k in enumerate(order)]
        for i, k in enumerate(order):
            lds[i].wait()
            lds2[i].wait()
            _add_rows(yl.at[q, k], [tst.at[i, _top(h)], tst.at[4 + i, _top(h)]], min(FEW, h))
            if i == 0:
                second[q]["far_r"] = remote(yl.at[q, r2, lo], za.at[q], rt)
                second[q]["far_l"] = remote(yl.at[q, r2, hi], zb.at[q], lt)
            if i == 1:
                second[q]["near_r"] = remote(yl.at[q, r1, hi], zl.at[q, hi], rt)
            if i == 2:
                second[q]["near_l"] = remote(yl.at[q, rm1, lo], zr.at[q, lo], lt)

    def second_pass(q):
        r, (rt, lt) = pos2[q], ring2[q]
        r1, rm1 = _mod4(r + 1), _mod4(r - 1)
        second[q]["far_r"].wait_recv()
        _add_rows(yl.at[q, r1, lo], [za.at[q]], min(FEW, hc))
        second[q]["sum_r"] = remote(yl.at[q, r1, lo], zl.at[q, lo], rt)
        second[q]["far_l"].wait_recv()
        _add_rows(yl.at[q, rm1, hi], [zb.at[q]], min(FEW, hc))
        second[q]["sum_l"] = remote(yl.at[q, rm1, hi], zr.at[q, hi], lt)

    def last(q):
        r = pos2[q]
        for k in NEAR_KEYS:
            second[q][k].wait_recv()
        n = min(LANES, h)

        @pl.loop(0, h // n)
        def _(i):
            at = pl.ds(pl.multiple_of(i * n, n), n)
            v = yl[q, r, at, :] + zl[q, at, :] + zr[q, at, :]
            od[0, 0, 0:chunk, pl.ds(pl.multiple_of(q * h + i * n, n), n)] = (v * (1.0 / LOGIT_SCALE)).T

    def tiles_far(q, between=None):
        tiles(q, lambda i: (_mod4(pos1[q] + 2), i), between)

    def tiles_near(q, between=None):
        tiles(q, lambda i: (_mod4(pos1[q] + 1 + 2 * i), 1 - i), between)

    def tiles_pass(q):
        tiles(q, lambda i: (_mod4(pos1[q] + 1 + 2 * i), i))

    def tiles_own(q):
        tiles(q, lambda i: (pos1[q], i))

    all_later = 48 - SLOTS

    def dz_first(start, stop):
        dz_rows(in_order, start, stop, SLOTS, SLOTS, wide)

    def dz_later(start, stop):
        dz_rows(later, start, stop, all_later, at_dht, wide)

    with scope("de_far"):
        to_far = q_h.at[x_far]
        e0, e1 = far_sends(half_a, xa, xp), far_sends(half_b, xb, xm)
        b0 = de_block(x_far, 0, 0)
        dz_far(16, 24)
        c0 = [sum_half(b0, 0, to_far)]
        dz_far(24, 32)
        c0[0].wait()
        e0[0].start()
        c0.append(sum_half(b0, 1, to_far))
        zahead(in_order, SLOTS, wide)
        for l in range(0, tok, nt):
            lanes = pl.ds(l, nt)
            dz_part(few[:, lanes], jnp.int32(dm.main), few_rows, lanes)
        dz[dm.main + FEW : dm.wide, :] = jnp.zeros((FEW, tok), BF16)

        def rest_of_e0():
            c0[1].wait()
            e0[1].start()

        b1 = de_block(x_far, 1, 1, True, rest_of_e0)
    with scope("dz_1"):
        dz_first(0, 8)
        c1 = sum_half(b1, 0, to_far)
        dz_first(8, SLOTS)
        zahead(later, at_dht, wide)
        c1.wait()
        e1[0].start()
    with scope("dh_far1"):
        def rest_of_b1():
            sum_half(b1, 1, to_far)

        tiles_far(1, rest_of_b1)
        n = ha + 8
        rest = pl.ds(nd, nd)
        pltpu.make_async_copy(od.at[1, c, _top(n), rest], to_far.at[half_b, rest], lsem.at[7]).wait()
        e1[1].start()
    with scope("dz_2"):
        dz_later(0, 9)
        send_far(1)
    with scope("dh_far0"):
        tiles_far(0)
    with scope("dz_3"):
        dz_later(9, 13)
        send_far(0)
        dz_later(13, all_later)
    with scope("dh_near1"):
        tiles_near(1)
    with scope("de_2"):
        b2 = de_block(x_p, 1, 0)
        send_near(1)
        b3 = de_block(x_m, 0, 1)
        c2 = sum_add(b2, q_h.at[x_p])
        e2 = _remote(q_h.at[x_p, half_b], xe.at[half_b], send, recv, next(ids), xp)
        sent.append(e2)
    with scope("dh_near0"):
        def send_e2():
            c2.wait()
            e2.start()

        tiles_near(0, send_e2)
        c3 = sum_add(b3, q_h.at[x_m])
        send_near(0)
        c3.wait()
        e3 = remote(q_h.at[x_m, half_a], xe.at[half_a], xm)
    with scope("dh_pass"):
        tiles_pass(1)
        tiles_pass(0)
        pass_on(1)
    with scope("de_4"):
        b4 = de_block(x_p, 0, 0)
        pass_on(0)
        b5 = de_block(x_m, 1, 1)
        c4 = sum_add(b4, q_h.at[x_p])
    with scope("dh_own"):
        tiles_own(1)
        c5 = sum_add(b5, q_h.at[x_m])
        tiles_own(0)
        c4.wait()
        c5.wait()
    old = list(sent)
    sent.clear()
    with scope("ring"):
        for cp in e0:
            cp.wait_recv()
        e4 = ring_sum(x_p, half_a, ha, xa, 0, xs.at[half_a], xp)
        for cp in e1:
            cp.wait_recv()
        e5 = ring_sum(x_m, half_b, ha + 8, xb, 1, xs.at[half_b], xm)
    with scope("de_6"):
        b6 = de_block(x, 0, 0)
    with scope("de_7"):
        b7 = de_block(x, 1, 1)
        xo_load = local(x4.at[zy, xc], dz.at[_top(chunk)], osem.at[0])
    with scope("second_1"):
        second_phase(1)
    with scope("second_0"):
        second_phase(0)
    with scope("spass_1"):
        second_pass(1)
    with scope("sum_6"):
        e3.wait_recv()
        c6 = early(b6, xe)
        e2.wait_recv()
        c7 = early(b7, xe)
        c6 = sum_add(b6, q_o, c6)
        c7 = sum_add(b7, q_o, c7)
    with scope("spass_0"):
        second_pass(0)
        c6.wait()
        c7.wait()
    def drain(cps):
        while cps:
            cps.pop().wait_send()

    def own_x(r):
        v = dz[r, :].astype(F32)
        inv = lax.rsqrt(jnp.mean(v * v, axis=-1, keepdims=True) + NORM_EPS)
        od[1, 0, r, :] = v * inv
        od[1, 1, r, 0:LANES] = jnp.broadcast_to(inv, (r.size, LANES))

    def own_dg(q):
        lanes = pl.ds(q * h, h)

        def add(i, acc):
            r = pl.ds(pl.multiple_of(i * 8, 8), 8)
            return acc + od[0, 0, r, lanes] * od[1, 0, r, lanes]

        acc = lax.fori_loop(0, chunk // 8, add, jnp.zeros((8, h), F32))
        sm[:, lanes] = jnp.sum(acc, axis=0, keepdims=True)

    def own_dx(r):
        x_hat, u = od[1, 0, r, :], od[0, 0, r, :] * gain
        od[0, 1, r, :] = od[1, 1, r, 0:1] * (u - x_hat * jnp.mean(u * x_hat, axis=-1, keepdims=True))

    with scope("own_x"):
        xo_load.wait()
        _loop_rows(chunk, 16, own_x)
        lse = jnp.where(zy == 0, lse_row[:, :], 0.0)
        loss = jnp.sum(w_row[:, :] * (lse - tgt_row[:, :]))
        sm[:, dim : dim + LANES] = jnp.full((1, LANES), loss / LOG2E)
        drain(old)
    with scope("last_1"):
        last(1)
        own_dg(1)
    with scope("last_0"):
        last(0)
        own_dg(0)

    with scope("small_1"):
        old = [cp for cp in sent if cp is not e4 and cp is not e5]
        near_sums = exchange(sm, got1, near)
        _loop_rows(chunk, 16, own_dx)
        dx_copy = local(od.at[0, 1, _top(chunk)], dx_out, osem.at[0])
        drain(old)
        for cp in near_sums:
            cp.wait()
    with scope("small_2"):
        tot = sm[...]
        for k in range(len(near)):
            tot = tot + got1[k]
        total_v[...] = tot
        all_sums = exchange(total_v, got2, line)
        mine = local(total_v, got2.at[len(line)], osem.at[1])
    with scope("ring_end"):
        for cp in (e4, e5):
            cp.wait()
        dx_copy.wait()
        mine.wait()
    with scope("small_3"):
        for cp in all_sums:
            cp.wait()


def _run(dm, x4, table, gain, labels, mask):
    hbm, vm = pl.BlockSpec(memory_space=HBM), pl.BlockSpec(memory_space=VMEM)
    sd = jax.ShapeDtypeStruct
    d, tok, h, ck, pad, ha = dm.dim, dm.tok, dm.h, dm.chunk, dm.pad, dm.ha
    line, quad, pair = VMEM((1, tok), F32), VMEM((2, 2, h, ck), F32), VMEM((2, h, ck), F32)
    part, shard = VMEM((2, h // 2, ck), F32), sd((pad, d), F32)
    out = pl.pallas_call(
        functools.partial(_kernel, dm),
        name="head",
        out_shape=(
            sd((ck, d), F32), sd((8, 1, d + LANES), F32),
            shard, shard, shard,
            sd((8, pad, d), F32), sd((16, dm.main, ck), F32),
            sd((4, pad, d), F32), sd((ha, d), F32), sd((ha + 8, d), F32),
            sd((4, 4, d, ck), F32), sd((2, 4, h, ck), F32),
        ),
        in_specs=[hbm, vm, vm, vm, vm],
        out_specs=[hbm] * 12,
        scratch_shapes=[
            VMEM((tok, d), BF16), VMEM((d, dm.wide), BF16), VMEM((dm.wide, tok), BF16),
            VMEM((2, 2, ha + 8, d), F32), VMEM((2, ha + 8, d), F32), VMEM((FEW, d), F32), VMEM((8, d), F32),
            quad, quad, VMEM((2, 4, h, ck), F32),
            part, part, pair, pair,
            VMEM((SLOTS, max(h, 2 * dm.rm), ck), F32),
            line, line, line, line, line, line, VMEM((15, 1, tok), F32),
            VMEM((1, d + LANES), F32), VMEM((15, 1, d + LANES), F32), VMEM((1, d + LANES), F32),
            DMA((55,)), DMA((55,)), pltpu.SemaphoreType.REGULAR((2,)),
            DMA((SLOTS,)), DMA((4,)), DMA((2,)), DMA((2,)), DMA((8,)),
        ],
        compiler_params=pltpu.CompilerParams(
            collective_id=0, has_side_effects=True, vmem_limit_bytes=67043328
        ),
    )(x4, table, gain, labels, mask)
    return _write_out(dm, out[2:4], *out[:2])


def _write_kernel(own, ring, dx, small, de_o, dx_o, dg_o, loss_o):
    de_o[:, :] = (own[:, :] + ring[:, :]) * (1.0 / LOGIT_SCALE)
    dx_o[:, :] = dx[:, :]
    total = jnp.sum(small[:, :, :], axis=0)
    d = dg_o.shape[1]
    dg_o[:, :] = total[:, :d]
    loss_o[:, :] = total[:, d : d + 1]


def _write_out(dm, parts, dx, small):
    d, step, blocks = dm.dim, dm.ha + 8, 2
    sd = jax.ShapeDtypeStruct
    some = pl.BlockSpec((step, d), lambda i: (i, 0))
    half = pl.BlockSpec((dm.chunk // blocks, d), lambda i: (i, 0))
    row, one = pl.BlockSpec((1, d), lambda i: (0, 0)), pl.BlockSpec((1, 1), lambda i: (0, 0))
    rows = pl.BlockSpec(small.shape, lambda i: (0, 0, 0))
    return pl.pallas_call(
        _write_kernel,
        name="write_out",
        grid=(blocks,),
        out_shape=(sd((dm.rows, d), F32), sd((dm.chunk, d), F32), sd((1, d), F32), sd((1, 1), F32)),
        in_specs=[some, some, half, rows],
        out_specs=(some, half, row, one),
    )(*parts, dx, small)


def solution(mesh):
    group = mesh.shape[AXIS]

    def local_step(residual, labels, loss_mask, norm_gain, table_shard):
        tokens, dim = residual.shape
        rows = table_shard.shape[0]
        dm = Dims(tokens, dim, rows, group)
        x4 = residual.reshape(16, 8, dm.chunk, dim)
        lab = labels.reshape(16, 8, 1, dm.chunk)
        msk = loss_mask.reshape(16, 8, 1, dm.chunk)
        d_embed, d_res, d_gain, loss = _run(dm, x4, table_shard, norm_gain[None, :], lab, msk)
        return loss.reshape(()), d_res, d_embed, d_gain.reshape(dim)

    return jax.shard_map(
        local_step,
        mesh=mesh,
        in_specs=(P(), P(), P(), P(), P(AXIS, None)),
        out_specs=(P(), P(AXIS, None), P(AXIS, None), P()),
        check_vma=False,
    )
```

```python
import functools
import itertools
import math

import jax
import jax.numpy as jnp
from jax import lax
from jax.experimental import pallas as pl
from jax.experimental.pallas import tpu as pltpu
from jax.sharding import PartitionSpec as P

VOCAB_REAL = 49155
LOGIT_SCALE = 6.0
NORM_EPS = 1e-6

AXIS = "vp"
MESH = pl.DeviceIdType.MESH
F32 = jnp.float32
BF16 = jnp.bfloat16
HBM = pltpu.HBM
VMEM = pltpu.VMEM
DMA = pltpu.SemaphoreType.DMA


def _coords():
    me = lax.axis_index(AXIS)
    return me // 32, (me // 8) % 4, (me // 2) % 4, me % 2


def _dev(z, y, x, c):
    return ((z * 4 + y) * 4 + x) * 2 + c


def _mod4(v):
    return lax.rem(v + 8, 4)


def _barrier(peers):
    sem = pltpu.get_barrier_semaphore()
    for p in peers:
        pl.semaphore_signal(sem, inc=1, device_id=(p,), device_id_type=MESH)
    pl.semaphore_wait(sem, len(peers))


def _remote(src, dst, send, recv, k, dev):
    return pltpu.make_async_remote_copy(
        src_ref=src,
        dst_ref=dst,
        send_sem=send.at[k],
        recv_sem=recv.at[k],
        device_id=(dev,),
        device_id_type=MESH,
    )


LANES = 128


class Dims:
    def __init__(self, tokens, dim, rows, group):
        self.dim, self.rows = dim, rows
        unit = LANES if rows >= LANES else 64
        self.rm = rows // unit * unit
        self.ha = self.rm // 2
        low = max(16, self.ha // 48 * 16)
        self.cuts = ((low, self.ha - low), (0, low))
        self.pad = self.rm + 8
        self.chunk = tokens // group
        self.tok = 16 * self.chunk
        self.nt = 4 * self.chunk
        self.main = 8 * self.rm
        self.wide = self.main + LANES
        self.h = dim // 2


def _top(n):
    return pl.ds(0, n)


def _rem(a, b):
    return a % b if isinstance(a, int) else lax.rem(a, b)


def _pick(test, a, b):
    return (a if test else b) if isinstance(test, bool) else jnp.where(test, a, b)


def _loop_rows(rows, step, fn):
    @pl.loop(0, rows // step)
    def _(i):
        fn(pl.ds(pl.multiple_of(i * step, step), step))


def _add_rows(dst, srcs, step):
    def add(r):
        acc = dst[r, :]
        for s in srcs:
            acc = acc + s[r, :]
        dst[r, :] = acc

    _loop_rows(dst.shape[0], step, add)


SLOTS = 12
FEW = 64
TWO = range(2)
LOG2E = math.log2(math.e)
NEAR_KEYS = ("near_r", "near_l", "sum_r", "sum_l")
scope = jax.named_scope


def _kernel(
    dm, x4, e_ref, g_ref, lab, msk,
    dx_out, got2, q_o, xs, xe, eg, zh, q_h, xa, xb, dhp, yr,
    hv, etv, dz, od, sst, few, oext, ya, yb, yl, za, zb, zl, zr, tst,
    m_row, s_row, w_row, pos_row, lse_row, tgt_row, got, sm, got1, total_v,
    send, recv,
    free, tsem, hsem, dsem, osem, lsem,
):
    z, y, x, c = _coords()
    xc, zy = x * 2 + c, z * 4 + y
    rows, rm, ha, dim, h = dm.rows, dm.rm, dm.ha, dm.dim, dm.h
    chunk, tok, nt, hc = dm.chunk, dm.tok, dm.nt, dm.h // 2
    x_far, x_p, x_m = _mod4(x + 2), _mod4(x + 1), _mod4(x - 1)
    xp, xm = _dev(z, y, x_p, c), _dev(z, y, x_m, c)
    yp, ym = _dev(z, _mod4(y + 1), x, c), _dev(z, _mod4(y - 1), x, c)
    zp, zm = _dev(_mod4(z + 1), y, x, c), _dev(_mod4(z - 1), y, x, c)
    sib = _dev(z, y, x, 1 - c)
    near = [_dev(_mod4(z + a), _mod4(y + b), x, c) for a in range(4) for b in range(4) if a or b]
    line = [_dev(z, y, _mod4(x + a), lax.rem(c + b, 2)) for a in range(4) for b in TWO if a or b]
    bar = pltpu.get_barrier_semaphore()
    for p in (*near, *line):
        pl.semaphore_signal(bar, inc=1, device_id=(p,), device_id_type=MESH)
    sent = []
    ids = itertools.count()

    def remote(src, dst, dev):
        cp = _remote(src, dst, send, recv, next(ids), dev)
        cp.start()
        sent.append(cp)
        return cp

    def exchange(src, dst, devs):
        k = next(ids)
        for i, dev in enumerate(devs):
            _remote(src, dst.at[i], send, recv, k, dev).start()
        whole = dst.at[_top(len(devs))]
        return pltpu.make_async_copy(whole, whole, recv.at[k]), pltpu.make_async_copy(whole, whole, send.at[k])

    def local(src, dst, sem):
        cp = pltpu.make_async_copy(src, dst, sem)
        cp.start()
        return cp

    x_at, ext_at = 2 * rm, 4 * rm

    def xload(k):
        s = lax.rem(k, 4)
        to = dz.at[pl.ds(pl.multiple_of(x_at + s * chunk, chunk), chunk)]
        return pltpu.make_async_copy(x4.at[k, xc], to, tsem.at[s])

    with scope("prep"):
        for k in range(3):
            xload(k).start()
        own = xc
        for j in TWO:
            def widen(r, j=j):
                od[0, j, r, :] = e_ref[pl.ds(j * ha + r.start, r.size), :].astype(F32)

            _loop_rows(ha, 16, widen)
        oext[...] = jnp.zeros_like(oext)
        oext[0 : rows - rm, :] = e_ref[rm:rows, :].astype(F32)
        cps = [local(od.at[0, j, _top(ha)], eg.at[own, pl.ds(j * ha, ha)], hsem.at[j]) for j in TWO]
        cps.append(local(oext, eg.at[own, pl.ds(rm, 8)], hsem.at[2]))
        for cp in cps:
            cp.wait()
        pl.semaphore_wait(bar, 22)

    half_a, half_b = _top(ha), pl.ds(ha, ha + 8)

    def piece(s, r, dev):
        return remote(eg.at[s, r], eg.at[s, r], dev)

    def slot(xx):
        return xx * 2 + c

    r_a, l_b = piece(own, half_a, xp), piece(own, half_b, xm)
    s_o = piece(own, _top(dm.pad), sib)
    r_b, l_a = piece(own, half_b, xp), piece(own, half_a, xm)

    gain = g_ref[...]

    with scope("norm"):
        @pl.loop(0, 16)
        def _(k):
            @pl.when(k < 13)
            def _():
                xload(k + 3).start()

            xload(k).wait()

            def norm(r):
                v = dz[pl.ds(pl.multiple_of(x_at + lax.rem(k, 4) * chunk + r.start, r.size), r.size), :].astype(F32)
                inv = lax.rsqrt(jnp.mean(v * v, axis=-1, keepdims=True) + NORM_EPS)
                hv[pl.ds(pl.multiple_of(k * chunk + r.start, r.size), r.size), :] = (v * inv * gain).astype(BF16)

            _loop_rows(chunk, 16, norm)

    with scope("labels"):
        total = jnp.sum(msk[...])
        for k in range(16):
            at = pl.ds(k * chunk, chunk)
            w_row[:, at] = msk[k, xc] / total
            q = lab[k, xc] - zy * (8 * rows)
            s = jnp.zeros_like(q)
            for i in range(1, 8):
                s = s + jnp.where(q >= i * rows, 1, 0)
            r = q - s * rows
            up = jnp.where(r >= ha, 1, 0)
            at_main = ((s // 2 * 2 + up) * 2 + s % 2) * ha + r - up * ha
            at_ext = dm.main + s * 8 + r - rm
            place = jnp.where(r < rm, at_main, at_ext)
            pos_row[:, at] = jnp.where((q >= 0) & (q < 8 * rows), place, -1).astype(F32)

    def product(lhs, lanes):
        v = lax.dot_general(lhs, hv[lanes, :], (((1,), (1,)), ((), ())), preferred_element_type=F32)
        return v * (LOG2E / LOGIT_SCALE)

    def add_stats(v, lanes):
        m_old, s_old = m_row[:, lanes], s_row[:, lanes]
        m = jnp.maximum(m_old, jnp.max(v, axis=0, keepdims=True))
        s = jnp.sum(jnp.exp2(v - m), axis=0, keepdims=True)
        m_row[:, lanes] = m
        s_row[:, lanes] = s_old * jnp.exp2(m_old - m) + s

    def add_target(v, place, lanes):
        r = lax.broadcasted_iota(jnp.int32, v.shape, 0)
        hit = r.astype(F32) == pos_row[:, lanes] - place.astype(F32)
        tgt_row[:, lanes] += jnp.sum(jnp.where(hit, v, 0.0), axis=0, keepdims=True)

    m_row[:, :] = jnp.full((1, tok), -1e30, F32)
    s_row[:, :] = jnp.zeros((1, tok), F32)
    tgt_row[:, :] = jnp.zeros((1, tok), F32)
    segs = [(half, j) for half in TWO for j in TWO]

    def load(r0, n, xx, cores=TWO):
        return [
            local(
                eg.at[xx[half] * 2 + j, pl.ds(half * ha + r0, n)],
                od.at[j, half, pl.ds(r0, n)],
                hsem.at[half * len(cores) + k],
            )
            for half in TWO
            for k, j in enumerate(cores)
        ]

    def narrow_all(r0, n, src, cores=TWO):
        for half in TWO:
            for j in cores:
                def narrow(r, half=half, j=j):
                    at = pl.multiple_of((half * 2 + j) * ha + r0 + r.start, r.size)
                    dz[pl.ds(at, r.size), :] = src(half, j)[r, :].astype(BF16)

                _loop_rows(n, 16, narrow)

    def load_narrow(r0, n, xx, core):
        for cp in load(r0, n, xx, (core,)):
            cp.wait()
        narrow_all(r0, n, lambda half, j: od.at[j, half, pl.ds(r0, n)], (core,))

    def block(r0, n, xx, loads=(), with_few=False):
        if loads:
            for cp in loads:
                cp.wait()
            narrow_all(r0, n, lambda half, j: od.at[j, half, pl.ds(r0, n)])
        left = [VOCAB_REAL - ((zy * 8 + xx[half] * 2 + j) * rows + half * ha + r0) for half, j in segs]
        w = nt // chunk
        deep = SLOTS // w

        def out(t):
            u = lax.rem(t, deep) * w
            return [
                pltpu.make_async_copy(
                    tst.at[u + i, pl.ds(m * n, n)],
                    zh.at[t * w + i, pl.ds(pl.multiple_of((xx[half] * 2 + half) * rm + j * ha + r0, 8), n)],
                    tsem.at[u + i],
                )
                for i in range(w)
                for m, (half, j) in enumerate(segs)
            ]

        def out_wait(t):
            u = lax.rem(t, deep) * w
            for i in range(w):
                whole = tst.at[u + i, _top(4 * n)]
                pltpu.make_async_copy(whole, zh.at[t * w + i, _top(4 * n)], tsem.at[u + i]).wait()

        @pl.loop(0, tok // nt)
        def _(t):
            @pl.when(t >= deep)
            def _():
                out_wait(t - deep)

            lanes = pl.ds(pl.multiple_of(t * nt, nt), nt)
            lhs = [dz[(half * 2 + j) * ha + r0 : (half * 2 + j) * ha + r0 + n, :] for half, j in segs]
            if with_few:
                lhs.append(dz[ext_at : ext_at + FEW, :])
            v = product(jnp.concatenate(lhs, axis=0), lanes)
            v, v_few = v[: 4 * n], v[4 * n :]
            r = lax.broadcasted_iota(jnp.int32, (n, nt), 0)
            v = [jnp.where(r < left[m], v[m * n : (m + 1) * n], -jnp.inf) for m in range(len(segs))]
            for part_v, (half, j) in zip(v, segs):
                add_target(part_v, (xx[half] * 2 + half) * rm + j * ha + r0, lanes)
            u = lax.rem(t, deep) * w
            for i in range(w):
                for m in range(len(segs)):
                    tst[u + i, m * n : (m + 1) * n, :] = v[m][:, i * chunk : (i + 1) * chunk]
            if with_few:
                r = lax.broadcasted_iota(jnp.int32, v_few.shape, 0)
                ok = ((r & 7) < rows - rm) & ((zy * 8 + (r >> 3)) * rows + rm + (r & 7) < VOCAB_REAL)
                v_few = jnp.where(ok, v_few, -jnp.inf)
                few[:, lanes] = v_few
                add_target(v_few, jnp.int32(dm.main), lanes)
                v.append(v_few)
            v = jnp.concatenate(v, axis=0)
            for cp in out(t):
                cp.start()
            add_stats(v, lanes)

        for t in range(deep):
            out_wait(t + tok // nt - deep)

    def both(xx):
        block(0, ha, xx, load(0, ha, xx))

    def turn(xx):
        for half in TWO:
            base = pl.multiple_of((xx[half] * 2 + half) * rm, rm)

            @pl.loop(0, dim // LANES)
            def _(d, half=half, base=base):
                at = pl.ds(pl.multiple_of(d * LANES, LANES), LANES)
                etv[at, pl.ds(base, rm)] = dz[half * rm : (half + 1) * rm, at].T

    with scope("own"):
        s_o.wait_recv()
        both((x, x))
        turn((x, x))

    with scope("wait_1"):
        r_a.wait_recv()
        last_n = dm.cuts[-1][1]
        spans = [(pl.ds(r0, n), pl.ds(ha + r0, n + 8 * (r0 + n == ha))) for r0, n in dm.cuts]

        def far_pieces(xx, half, to):
            cps = [piece(slot(xx), pair[half], to) for pair in spans[:-1]]
            cps.append(remote(eg.at[slot(xx), spans[-1][half]], sst.at[c, pl.ds(half * last_n, last_n)], to))
            return cps

        r_f = far_pieces(x_m, 0, xp)
        d = [piece(slot(x_m), half_a, sib)]
        l_b.wait_recv()
        l_f = far_pieces(x_p, 1, xm)
        d.append(piece(slot(x_p), half_b, sib))
        for cp in d:
            cp.wait_recv()

    with scope("near_1"):
        both((x_m, x_p))
        turn((x_m, x_p))

    with scope("wait_2"):
        r_b.wait_recv()
        d = [piece(slot(x_m), half_b, sib)]
        l_a.wait_recv()
        d.append(piece(slot(x_p), half_a, sib))
        for cp in d:
            cp.wait_recv()

    with scope("near_2"):
        both((x_p, x_m))
        turn((x_p, x_m))

    far = (x_far, x_far)

    with scope("wait_3"):
        d = []
        for cp, r in zip((r_f[0], l_f[0]), spans[0]):
            cp.wait_recv()
            d.append(piece(slot(x_far), r, sib))
        load_narrow(*dm.cuts[0], far, c)
        for cp in d:
            cp.wait_recv()
    with scope("far_a"):
        ext_loads = [local(eg.at[s, pl.ds(rm, 8)], few.at[pl.ds(s * 8, 8)], lsem.at[s]) for s in range(8)]
        load_narrow(*dm.cuts[0], far, 1 - c)
        for cp in ext_loads:
            cp.wait()
        dz[ext_at : ext_at + FEW, :] = few[...].astype(BF16)
        dz[ext_at + FEW : ext_at + LANES, :] = jnp.zeros((FEW, dim), BF16)
        block(*dm.cuts[0], far, with_few=True)
    with scope("wait_5"):
        r_f[-1].wait_recv()
        l_f[-1].wait_recv()
        both_last = sst.at[c, _top(2 * last_n)]
        over = _remote(both_last, both_last, send, recv, next(ids), sib)
        over.start()

        @pl.loop(0, dim // LANES)
        def _(i):
            at = pl.ds(pl.multiple_of(i * LANES, LANES), LANES)
            etv[at, dm.main : dm.wide] = dz[ext_at : ext_at + LANES, at].T

        def last_rows(half, j):
            return sst.at[j, pl.ds(half * last_n, last_n)]

        narrow_all(0, last_n, last_rows, (c,))
        over.wait_recv()

    with scope("far_c"):
        narrow_all(0, last_n, last_rows, (1 - c,))
        block(0, last_n, far)
        over.wait_send()
        for s in TWO:
            pl.semaphore_signal(free.at[s], inc=1, device_id=(sib,), device_id_type=MESH)

    with scope("turn_far"):
        lse_row[:, :] = m_row[:, :] + jnp.log(s_row[:, :]) * LOG2E
        stats = exchange(lse_row, got, near)
        turn(far)

    wide = 2 * rm

    at_dht = SLOTS - 4

    def chunk_of(zz, yy):
        return _mod4(zz) * 4 + _rem(yy + 8, 4)

    def all_far(i):
        return x_far * wide + i // 16 * rm, _rem(i, 16)

    def in_order(i):
        n = i // 3
        m = n - 7
        k = _pick(n < 7, chunk_of(z + n - 1, y + 2), chunk_of(z + 3 + m // 3, y + 3 + _rem(m + 9, 3)))
        return _mod4(x + 3 + _rem(i, 3)) * wide, _pick(n < 4, chunk_of(z + 2, n), k)

    def later(i):
        return in_order(i + SLOTS)

    def zload(where, i, ring, n):
        at, k = where(i)
        s = _rem(i, ring)
        src = zh.at[k, pl.ds(pl.multiple_of(at, rm), n)]
        return pltpu.make_async_copy(src, tst.at[s, _top(n)], tsem.at[s])

    def zahead(where, ring, n):
        for i in range(ring):
            zload(where, i, ring, n).start()

    with scope("stats"):
        zahead(all_far, SLOTS, rm)
        for cp in stats:
            cp.wait()
        top = lse_row[:, :]
        for k in range(len(near)):
            top = jnp.maximum(top, got[k])
        s = jnp.exp2(lse_row[:, :] - top)
        for k in range(len(near)):
            s = s + jnp.exp2(got[k] - top)
        lse_row[:, :] = top + jnp.log(s) * LOG2E

    def dz_part(v, place, at, lanes):
        r = lax.broadcasted_iota(jnp.int32, v.shape, 0).astype(F32)
        hit = r == pos_row[:, lanes] - place.astype(F32)
        p = jnp.exp2(v - lse_row[:, lanes])
        dz[at, lanes] = (jnp.where(hit, p - 1.0, p) * w_row[:, lanes]).astype(BF16)

    step = min(LANES, rm)

    def dz_rows(where, start, stop, last_tile, ring, n):
        @pl.loop(start, stop)
        def _(i):
            @pl.when((i > 0) & (i + ring - 1 < last_tile))
            def _():
                zload(where, i + ring - 1, ring, n).start()

            zload(where, i, ring, n).wait()
            row, k = where(i)
            lanes = pl.ds(pl.multiple_of(k * chunk, chunk), chunk)

            @pl.loop(0, n // step)
            def _(j):
                at = pl.multiple_of(row + j * step, step)
                r = pl.ds(pl.multiple_of(j * step, step), step)
                dz_part(tst[lax.rem(i, ring), r, :], at, pl.ds(at, step), lanes)

    def dz_far(start, stop):
        dz_rows(all_far, start, stop, 32, SLOTS, rm)

    with scope("dz_far"):
        dz_far(0, 16)

    nd = dim // 2
    few_rows = pl.ds(dm.main, FEW)
    pair_ids = [(next(ids), next(ids)) for _ in TWO]

    def over_d2d(s, n, i):
        lanes = pl.ds(pl.multiple_of(i * nd, nd), nd)
        there = sst.at[s, _top(n), lanes]
        return _remote(od.at[s, 1 - c, _top(n), lanes], there, send, recv, pair_ids[s][0] + i, sib)

    def de_block(xx, half, s, with_few=False):
        at = pl.ds(pl.multiple_of((xx * 2 + half) * rm, rm), rm)
        n = ha + 8 * half
        pl.semaphore_wait(free.at[s], 1)

        @pl.loop(0, 2)
        def _(i):
            lanes = pl.ds(pl.multiple_of(i * nd, nd), nd)
            lhs = jnp.concatenate([dz[at, :], dz[few_rows, :]], axis=0) if with_few else dz[at, :]
            v = jnp.dot(lhs, hv[:, lanes], preferred_element_type=F32)
            if with_few:
                few[:, lanes] = v[rm:]
            for j in TWO:
                od[s, j, 0:ha, lanes] = v[j * ha : (j + 1) * ha]
                if half:
                    od[s, j, ha:n, lanes] = few[pl.ds(pl.multiple_of((xx * 2 + j) * 8, 8), 8), lanes]
            over_d2d(s, n, i).start()

        return half, s, n

    def stored(blk, to):
        half, s, n = blk
        return pltpu.make_async_copy(od.at[s, c, _top(n)], to.at[pl.ds(half * ha, n)], dsem.at[s])

    def early(blk, src):
        half, s, n = blk
        for i in TWO:
            over_d2d(s, n, i).wait_send()
        return local(src.at[pl.ds(half * ha, n)], od.at[s, 1 - c, _top(n)], lsem.at[s])

    def sum_add(blk, to, more=None):
        half, s, n = blk
        for i in TWO:
            over_d2d(s, n, i).wait_recv()
        if more is not None:
            more.wait()

        def add(r):
            v = od[s, c, r, :] + sst[s, r, :]
            od[s, c, r, :] = v if more is None else v + od[s, 1 - c, r, :]

        _loop_rows(n, 8, add)
        if more is None:
            pl.semaphore_signal(free.at[s], inc=1, device_id=(sib,), device_id_type=MESH)
            for i in TWO:
                over_d2d(s, n, i).wait_send()
        cp = stored(blk, to)
        cp.start()
        return cp

    def ring_sum(xx, rows_, n, src, s, dst, dev):
        lds = [
            local(q_h.at[xx, rows_], od.at[s, 0, _top(n)], lsem.at[0]),
            local(src, od.at[s, 1, _top(n)], lsem.at[1]),
        ]
        for cp in lds:
            cp.wait()
        _add_rows(od.at[s, 0, _top(n)], [od.at[s, 1, _top(n)]], 8)
        local(od.at[s, 0, _top(n)], q_h.at[xx, rows_], lsem.at[0]).wait()
        return remote(q_h.at[xx, rows_], dst, dev)

    stores = []

    def flush():
        while stores:
            stores.pop().wait()

    def tiles(q, where, between=None):
        flush()

        def outs(i):
            p, ab = where(i)
            r = pl.ds(q * h, h)
            dsts = [dhp.at[ab * 2 + j, p, r] if q == 0 else dhp.at[p, ab * 2 + j, r] for j in TWO]
            return [
                pltpu.make_async_copy(tst.at[at_dht + i * 2 + j, _top(h)], dst, hsem.at[i * 2 + j])
                for j, dst in enumerate(dsts)
            ]

        @pl.loop(0, 2)
        def _(i):
            if between is not None:
                pl.when(i > 0)(between)
            p, ab = where(i)
            ks = [(ab * 2 + j) * 4 + p if q == 0 else p * 4 + ab * 2 + j for j in TWO]
            rhs = jnp.concatenate([dz[:, pl.ds(pl.multiple_of(k * chunk, chunk), chunk)] for k in ks], axis=1)
            v = jnp.dot(etv[q * h : (q + 1) * h, :], rhs, preferred_element_type=F32)
            for j in TWO:
                tst[at_dht + i * 2 + j, 0:h, :] = v[:, j * chunk : (j + 1) * chunk]
            for cp in outs(i):
                cp.start()

        for i in TWO:
            stores.extend(outs(i))

    def part(q, p, lo, n):
        r = pl.ds(q * h, h)
        if q == 0:
            return dhp.at[pl.ds(lo, n), p, r]
        return dhp.at[p, pl.ds(lo, n), r]

    def one(q, p, i):
        r = pl.ds(q * h, h)
        return dhp.at[i, p, r] if q == 0 else dhp.at[p, i, r]

    ring1, ring2 = ((yp, ym), (zp, zm)), ((zp, zm), (yp, ym))
    pos1, pos2 = (y, z), (z, y)
    first, second = ({}, {}), ({}, {})

    def send_far(q):
        flush()
        p, (rt, lt) = pos1[q], ring1[q]
        first[q]["far_r"] = remote(part(q, _mod4(p + 2), 0, 2), ya.at[q], rt)
        first[q]["far_l"] = remote(part(q, _mod4(p + 2), 2, 2), yb.at[q], lt)

    def send_near(q):
        flush()
        p, (rt, lt) = pos1[q], ring1[q]
        first[q]["near_r"] = remote(part(q, _mod4(p + 1), 2, 2), yl.at[q, pl.ds(2, 2)], rt)
        first[q]["near_l"] = remote(part(q, _mod4(p - 1), 0, 2), yr.at[q, _top(2)], lt)

    def fetch(i, src):
        return local(src, tst.at[i, _top(h)], tsem.at[i])

    def pass_on(q):
        flush()
        p, (rt, lt) = pos1[q], ring1[q]
        lds = [fetch(i, one(q, _mod4(p + 1), i)) for i in TWO]
        lds += [fetch(2 + i, one(q, _mod4(p - 1), 2 + i)) for i in TWO]
        first[q]["far_r"].wait_recv()
        for i in TWO:
            lds[i].wait()
            _add_rows(ya.at[q, i], [tst.at[i, _top(h)]], min(FEW, h))
        first[q]["sum_r"] = remote(ya.at[q], yl.at[q, _top(2)], rt)
        first[q]["far_l"].wait_recv()
        for i in TWO:
            lds[2 + i].wait()
            _add_rows(yb.at[q, i], [tst.at[2 + i, _top(h)]], min(FEW, h))
        first[q]["sum_l"] = remote(yb.at[q], yr.at[q, pl.ds(2, 2)], lt)

    lo, hi = _top(hc), pl.ds(hc, hc)

    def second_phase(q):
        flush()
        r, (rt, lt) = pos2[q], ring2[q]
        r2, r1, rm1 = _mod4(r + 2), _mod4(r + 1), _mod4(r - 1)
        order = (r2, r1, rm1, r)
        lds = [fetch(i, one(q, pos1[q], k)) for i, k in enumerate(order)]
        for k in NEAR_KEYS:
            first[q][k].wait_recv()
        lds2 = [fetch(4 + i, yr.at[q, k]) for i, k in enumerate(order)]
        for i, k in enumerate(order):
            lds[i].wait()
            lds2[i].wait()
            _add_rows(yl.at[q, k], [tst.at[i, _top(h)], tst.at[4 + i, _top(h)]], min(FEW, h))
            if i == 0:
                second[q]["far_r"] = remote(yl.at[q, r2, lo], za.at[q], rt)
                second[q]["far_l"] = remote(yl.at[q, r2, hi], zb.at[q], lt)
            if i == 1:
                second[q]["near_r"] = remote(yl.at[q, r1, hi], zl.at[q, hi], rt)
            if i == 2:
                second[q]["near_l"] = remote(yl.at[q, rm1, lo], zr.at[q, lo], lt)

    def second_pass(q):
        r, (rt, lt) = pos2[q], ring2[q]
        r1, rm1 = _mod4(r + 1), _mod4(r - 1)
        second[q]["far_r"].wait_recv()
        _add_rows(yl.at[q, r1, lo], [za.at[q]], min(FEW, hc))
        second[q]["sum_r"] = remote(yl.at[q, r1, lo], zl.at[q, lo], rt)
        second[q]["far_l"].wait_recv()
        _add_rows(yl.at[q, rm1, hi], [zb.at[q]], min(FEW, hc))
        second[q]["sum_l"] = remote(yl.at[q, rm1, hi], zr.at[q, hi], lt)

    def last(q):
        r = pos2[q]
        for k in NEAR_KEYS:
            second[q][k].wait_recv()
        n = min(LANES, h)

        @pl.loop(0, h // n)
        def _(i):
            at = pl.ds(pl.multiple_of(i * n, n), n)
            v = yl[q, r, at, :] + zl[q, at, :] + zr[q, at, :]
            od[0, 0, 0:chunk, pl.ds(pl.multiple_of(q * h + i * n, n), n)] = (v * (1.0 / LOGIT_SCALE)).T

    def tiles_far(q, between=None):
        tiles(q, lambda i: (_mod4(pos1[q] + 2), i), between)

    def tiles_near(q):
        tiles(q, lambda i: (_mod4(pos1[q] + 1 + 2 * i), 1 - i))

    def tiles_pass(q):
        tiles(q, lambda i: (_mod4(pos1[q] + 1 + 2 * i), i))

    def tiles_own(q):
        tiles(q, lambda i: (pos1[q], i))

    all_later = 48 - SLOTS

    def dz_first(start, stop):
        dz_rows(in_order, start, stop, SLOTS, SLOTS, wide)

    def dz_later(start, stop):
        dz_rows(later, start, stop, all_later, at_dht, wide)

    with scope("de_far"):
        b0 = de_block(x_far, 0, 0)
        dz_far(16, 32)
        zahead(in_order, SLOTS, wide)
        for l in range(0, tok, nt):
            lanes = pl.ds(l, nt)
            dz_part(few[:, lanes], jnp.int32(dm.main), few_rows, lanes)
        dz[dm.main + FEW : dm.wide, :] = jnp.zeros((FEW, tok), BF16)
        b1 = de_block(x_far, 1, 1, True)
    with scope("dz_1"):
        c0 = sum_add(b0, q_h.at[x_far])
        dz_first(0, 8)
        c0.wait()
        e0 = remote(q_h.at[x_far, half_a], xa, xp)
        dz_first(8, SLOTS)
        zahead(later, at_dht, wide)
    with scope("dh_far1"):
        def between():
            sum_add(b1, q_h.at[x_far])

        tiles_far(1, between)
        c1 = stored(b1, q_h.at[x_far])
        c1.wait()
        e1 = remote(q_h.at[x_far, half_b], xb, xm)
    with scope("dz_2"):
        dz_later(0, 9)
        send_far(1)
    with scope("dh_far0"):
        tiles_far(0)
    with scope("dz_3"):
        dz_later(9, 13)
        send_far(0)
        dz_later(13, all_later)
    with scope("de_2"):
        b2 = de_block(x_p, 1, 0)
        b3 = de_block(x_m, 0, 1)
        c2 = sum_add(b2, q_h.at[x_p])
    with scope("dh_near"):
        tiles_near(1)
        c2.wait()
        e2 = remote(q_h.at[x_p, half_b], xe.at[half_b], xp)
        c3 = sum_add(b3, q_h.at[x_m])
        send_near(1)
        tiles_near(0)
        c3.wait()
        e3 = remote(q_h.at[x_m, half_a], xe.at[half_a], xm)
        send_near(0)
    with scope("dh_pass"):
        tiles_pass(1)
        tiles_pass(0)
        pass_on(1)
    with scope("de_4"):
        b4 = de_block(x_p, 0, 0)
        pass_on(0)
        b5 = de_block(x_m, 1, 1)
        c4 = sum_add(b4, q_h.at[x_p])
    with scope("dh_own"):
        tiles_own(1)
        c5 = sum_add(b5, q_h.at[x_m])
        tiles_own(0)
        c4.wait()
        c5.wait()
    old = list(sent)
    sent.clear()
    with scope("ring"):
        e0.wait_recv()
        e4 = ring_sum(x_p, half_a, ha, xa, 0, xs.at[half_a], xp)
        e1.wait_recv()
        e5 = ring_sum(x_m, half_b, ha + 8, xb, 1, xs.at[half_b], xm)
    with scope("de_6"):
        b6 = de_block(x, 0, 0)
    with scope("de_7"):
        b7 = de_block(x, 1, 1)
        xo_load = local(x4.at[zy, xc], dz.at[_top(chunk)], osem.at[0])
    with scope("second_1"):
        second_phase(1)
    with scope("second_0"):
        second_phase(0)
    with scope("spass_1"):
        second_pass(1)
    with scope("sum_6"):
        e3.wait_recv()
        c6 = early(b6, xe)
        e2.wait_recv()
        c7 = early(b7, xe)
        c6 = sum_add(b6, q_o, c6)
        c7 = sum_add(b7, q_o, c7)
    with scope("spass_0"):
        second_pass(0)
        c6.wait()
        c7.wait()
    def drain(cps):
        while cps:
            cps.pop().wait_send()

    def own_x(r):
        v = dz[r, :].astype(F32)
        inv = lax.rsqrt(jnp.mean(v * v, axis=-1, keepdims=True) + NORM_EPS)
        od[1, 0, r, :] = v * inv
        od[1, 1, r, 0:LANES] = jnp.broadcast_to(inv, (r.size, LANES))

    def own_dg(q):
        lanes = pl.ds(q * h, h)

        def add(i, acc):
            r = pl.ds(pl.multiple_of(i * 8, 8), 8)
            return acc + od[0, 0, r, lanes] * od[1, 0, r, lanes]

        acc = lax.fori_loop(0, chunk // 8, add, jnp.zeros((8, h), F32))
        sm[:, lanes] = jnp.sum(acc, axis=0, keepdims=True)

    def own_dx(r):
        x_hat, u = od[1, 0, r, :], od[0, 0, r, :] * gain
        od[0, 1, r, :] = od[1, 1, r, 0:1] * (u - x_hat * jnp.mean(u * x_hat, axis=-1, keepdims=True))

    with scope("own_x"):
        xo_load.wait()
        _loop_rows(chunk, 16, own_x)
        lse = jnp.where(zy == 0, lse_row[:, :], 0.0)
        loss = jnp.sum(w_row[:, :] * (lse - tgt_row[:, :]))
        sm[:, dim : dim + LANES] = jnp.full((1, LANES), loss / LOG2E)
        drain(old)
    with scope("last_1"):
        last(1)
        own_dg(1)
    with scope("last_0"):
        last(0)
        own_dg(0)

    with scope("small_1"):
        old = [cp for cp in sent if cp is not e4 and cp is not e5]
        near_sums = exchange(sm, got1, near)
        _loop_rows(chunk, 16, own_dx)
        dx_copy = local(od.at[0, 1, _top(chunk)], dx_out, osem.at[0])
        drain(old)
        for cp in near_sums:
            cp.wait()
    with scope("small_2"):
        tot = sm[...]
        for k in range(len(near)):
            tot = tot + got1[k]
        total_v[...] = tot
        all_sums = exchange(total_v, got2, line)
        mine = local(total_v, got2.at[len(line)], osem.at[1])
    with scope("ring_end"):
        for cp in (e4, e5):
            cp.wait()
        dx_copy.wait()
        mine.wait()
    with scope("small_3"):
        for cp in all_sums:
            cp.wait()


def _run(dm, x4, table, gain, labels, mask):
    hbm, vm = pl.BlockSpec(memory_space=HBM), pl.BlockSpec(memory_space=VMEM)
    sd = jax.ShapeDtypeStruct
    d, tok, h, ck, pad, ha = dm.dim, dm.tok, dm.h, dm.chunk, dm.pad, dm.ha
    line, quad, pair = VMEM((1, tok), F32), VMEM((2, 2, h, ck), F32), VMEM((2, h, ck), F32)
    part, shard = VMEM((2, h // 2, ck), F32), sd((pad, d), F32)
    out = pl.pallas_call(
        functools.partial(_kernel, dm),
        name="head",
        out_shape=(
            sd((ck, d), F32), sd((8, 1, d + LANES), F32),
            shard, shard, shard,
            sd((8, pad, d), F32), sd((16, dm.main, ck), F32),
            sd((4, pad, d), F32), sd((ha, d), F32), sd((ha + 8, d), F32),
            sd((4, 4, d, ck), F32), sd((2, 4, h, ck), F32),
        ),
        in_specs=[hbm, vm, vm, vm, vm],
        out_specs=[hbm] * 12,
        scratch_shapes=[
            VMEM((tok, d), BF16), VMEM((d, dm.wide), BF16), VMEM((dm.wide, tok), BF16),
            VMEM((2, 2, ha + 8, d), F32), VMEM((2, ha + 8, d), F32), VMEM((FEW, d), F32), VMEM((8, d), F32),
            quad, quad, VMEM((2, 4, h, ck), F32),
            part, part, pair, pair,
            VMEM((SLOTS, max(h, 2 * dm.rm), ck), F32),
            line, line, line, line, line, line, VMEM((15, 1, tok), F32),
            VMEM((1, d + LANES), F32), VMEM((15, 1, d + LANES), F32), VMEM((1, d + LANES), F32),
            DMA((53,)), DMA((53,)), pltpu.SemaphoreType.REGULAR((2,)),
            DMA((SLOTS,)), DMA((4,)), DMA((2,)), DMA((2,)), DMA((8,)),
        ],
        compiler_params=pltpu.CompilerParams(
            collective_id=0, has_side_effects=True, vmem_limit_bytes=67043328
        ),
    )(x4, table, gain, labels, mask)
    return _write_out(dm, out[2:4], *out[:2])


def _write_kernel(own, ring, dx, small, de_o, dx_o, dg_o, loss_o):
    de_o[:, :] = (own[:, :] + ring[:, :]) * (1.0 / LOGIT_SCALE)
    dx_o[:, :] = dx[:, :]
    total = jnp.sum(small[:, :, :], axis=0)
    d = dg_o.shape[1]
    dg_o[:, :] = total[:, :d]
    loss_o[:, :] = total[:, d : d + 1]


def _write_out(dm, parts, dx, small):
    d, step, blocks = dm.dim, dm.ha + 8, 2
    sd = jax.ShapeDtypeStruct
    some = pl.BlockSpec((step, d), lambda i: (i, 0))
    half = pl.BlockSpec((dm.chunk // blocks, d), lambda i: (i, 0))
    row, one = pl.BlockSpec((1, d), lambda i: (0, 0)), pl.BlockSpec((1, 1), lambda i: (0, 0))
    rows = pl.BlockSpec(small.shape, lambda i: (0, 0, 0))
    return pl.pallas_call(
        _write_kernel,
        name="write_out",
        grid=(blocks,),
        out_shape=(sd((dm.rows, d), F32), sd((dm.chunk, d), F32), sd((1, d), F32), sd((1, 1), F32)),
        in_specs=[some, some, half, rows],
        out_specs=(some, half, row, one),
    )(*parts, dx, small)


def solution(mesh):
    group = mesh.shape[AXIS]

    def local_step(residual, labels, loss_mask, norm_gain, table_shard):
        tokens, dim = residual.shape
        rows = table_shard.shape[0]
        dm = Dims(tokens, dim, rows, group)
        x4 = residual.reshape(16, 8, dm.chunk, dim)
        lab = labels.reshape(16, 8, 1, dm.chunk)
        msk = loss_mask.reshape(16, 8, 1, dm.chunk)
        d_embed, d_res, d_gain, loss = _run(dm, x4, table_shard, norm_gain[None, :], lab, msk)
        return loss.reshape(()), d_res, d_embed, d_gain.reshape(dim)

    return jax.shard_map(
        local_step,
        mesh=mesh,
        in_specs=(P(), P(), P(), P(), P(AXIS, None)),
        out_specs=(P(), P(AXIS, None), P(AXIS, None), P()),
        check_vma=False,
    )
```

```python
import functools
import itertools
import math

import jax
import jax.numpy as jnp
from jax import lax
from jax.experimental import pallas as pl
from jax.experimental.pallas import tpu as pltpu
from jax.sharding import PartitionSpec as P

VOCAB_REAL = 49155
LOGIT_SCALE = 6.0
NORM_EPS = 1e-6

AXIS = "vp"
MESH = pl.DeviceIdType.MESH
F32 = jnp.float32
BF16 = jnp.bfloat16
HBM = pltpu.HBM
VMEM = pltpu.VMEM
DMA = pltpu.SemaphoreType.DMA


def _coords():
    me = lax.axis_index(AXIS)
    return me // 32, (me // 8) % 4, (me // 2) % 4, me % 2


def _dev(z, y, x, c):
    return ((z * 4 + y) * 4 + x) * 2 + c


def _mod4(v):
    return lax.rem(v + 8, 4)


def _barrier(peers):
    sem = pltpu.get_barrier_semaphore()
    for p in peers:
        pl.semaphore_signal(sem, inc=1, device_id=(p,), device_id_type=MESH)
    pl.semaphore_wait(sem, len(peers))


def _remote(src, dst, send, recv, k, dev):
    return pltpu.make_async_remote_copy(
        src_ref=src,
        dst_ref=dst,
        send_sem=send.at[k],
        recv_sem=recv.at[k],
        device_id=(dev,),
        device_id_type=MESH,
    )


LANES = 128


class Dims:
    def __init__(self, tokens, dim, rows, group):
        self.dim, self.rows = dim, rows
        unit = LANES if rows >= LANES else 64
        self.rm = rows // unit * unit
        self.ha = self.rm // 2
        low = max(16, self.ha // 48 * 16)
        self.cuts = ((low, self.ha - low), (0, low))
        self.pad = self.rm + 8
        self.chunk = tokens // group
        self.tok = 16 * self.chunk
        self.nt = 4 * self.chunk
        self.main = 8 * self.rm
        self.wide = self.main + LANES
        self.h = dim // 2


def _top(n):
    return pl.ds(0, n)


def _rem(a, b):
    return a % b if isinstance(a, int) else lax.rem(a, b)


def _pick(test, a, b):
    return (a if test else b) if isinstance(test, bool) else jnp.where(test, a, b)


def _loop_rows(rows, step, fn):
    @pl.loop(0, rows // step)
    def _(i):
        fn(pl.ds(pl.multiple_of(i * step, step), step))


def _add_rows(dst, srcs, step):
    def add(r):
        acc = dst[r, :]
        for s in srcs:
            acc = acc + s[r, :]
        dst[r, :] = acc

    _loop_rows(dst.shape[0], step, add)


SLOTS = 12
FEW = 64
TWO = range(2)
LOG2E = math.log2(math.e)
NEAR_KEYS = ("near_r", "near_l", "sum_r", "sum_l")
scope = jax.named_scope


def _kernel(
    dm, x4, e_ref, g_ref, lab, msk,
    dx_out, got2, q_o, xs, xe, eg, zh, q_h, xa, xb, dhp, yr,
    hv, etv, dz, od, sst, few, oext, ya, yb, yl, za, zb, zl, zr, tst,
    m_row, s_row, w_row, pos_row, lse_row, tgt_row, got, sm, got1, total_v,
    send, recv,
    free, tsem, hsem, dsem, osem, lsem,
):
    z, y, x, c = _coords()
    xc, zy = x * 2 + c, z * 4 + y
    rows, rm, ha, dim, h = dm.rows, dm.rm, dm.ha, dm.dim, dm.h
    chunk, tok, nt, hc = dm.chunk, dm.tok, dm.nt, dm.h // 2
    x_far, x_p, x_m = _mod4(x + 2), _mod4(x + 1), _mod4(x - 1)
    xp, xm = _dev(z, y, x_p, c), _dev(z, y, x_m, c)
    yp, ym = _dev(z, _mod4(y + 1), x, c), _dev(z, _mod4(y - 1), x, c)
    zp, zm = _dev(_mod4(z + 1), y, x, c), _dev(_mod4(z - 1), y, x, c)
    sib = _dev(z, y, x, 1 - c)
    near = [_dev(_mod4(z + a), _mod4(y + b), x, c) for a in range(4) for b in range(4) if a or b]
    line = [_dev(z, y, _mod4(x + a), lax.rem(c + b, 2)) for a in range(4) for b in TWO if a or b]
    bar = pltpu.get_barrier_semaphore()
    for p in (*near, *line):
        pl.semaphore_signal(bar, inc=1, device_id=(p,), device_id_type=MESH)
    sent = []
    ids = itertools.count()

    def remote(src, dst, dev):
        cp = _remote(src, dst, send, recv, next(ids), dev)
        cp.start()
        sent.append(cp)
        return cp

    def exchange(src, dst, devs):
        k = next(ids)
        for i, dev in enumerate(devs):
            _remote(src, dst.at[i], send, recv, k, dev).start()
        whole = dst.at[_top(len(devs))]
        return pltpu.make_async_copy(whole, whole, recv.at[k]), pltpu.make_async_copy(whole, whole, send.at[k])

    def local(src, dst, sem):
        cp = pltpu.make_async_copy(src, dst, sem)
        cp.start()
        return cp

    x_at, ext_at = 2 * rm, 4 * rm

    def xload(k):
        s = lax.rem(k, 4)
        to = dz.at[pl.ds(pl.multiple_of(x_at + s * chunk, chunk), chunk)]
        return pltpu.make_async_copy(x4.at[k, xc], to, tsem.at[s])

    with scope("prep"):
        for k in range(3):
            xload(k).start()
        own = xc
        for j in TWO:
            def widen(r, j=j):
                od[0, j, r, :] = e_ref[pl.ds(j * ha + r.start, r.size), :].astype(F32)

            _loop_rows(ha, 16, widen)
        oext[...] = jnp.zeros_like(oext)
        oext[0 : rows - rm, :] = e_ref[rm:rows, :].astype(F32)
        cps = [local(od.at[0, j, _top(ha)], eg.at[own, pl.ds(j * ha, ha)], hsem.at[j]) for j in TWO]
        cps.append(local(oext, eg.at[own, pl.ds(rm, 8)], hsem.at[2]))
        for cp in cps:
            cp.wait()
        pl.semaphore_wait(bar, 22)

    half_a, half_b = _top(ha), pl.ds(ha, ha + 8)

    def piece(s, r, dev):
        return remote(eg.at[s, r], eg.at[s, r], dev)

    def slot(xx):
        return xx * 2 + c

    r_a, l_b = piece(own, half_a, xp), piece(own, half_b, xm)
    s_o = piece(own, _top(dm.pad), sib)
    r_b, l_a = piece(own, half_b, xp), piece(own, half_a, xm)

    gain = g_ref[...]

    with scope("norm"):
        @pl.loop(0, 16)
        def _(k):
            @pl.when(k < 13)
            def _():
                xload(k + 3).start()

            xload(k).wait()

            def norm(r):
                v = dz[pl.ds(pl.multiple_of(x_at + lax.rem(k, 4) * chunk + r.start, r.size), r.size), :].astype(F32)
                inv = lax.rsqrt(jnp.mean(v * v, axis=-1, keepdims=True) + NORM_EPS)
                hv[pl.ds(pl.multiple_of(k * chunk + r.start, r.size), r.size), :] = (v * inv * gain).astype(BF16)

            _loop_rows(chunk, 16, norm)

    with scope("labels"):
        total = jnp.sum(msk[...])
        for k in range(16):
            at = pl.ds(k * chunk, chunk)
            w_row[:, at] = msk[k, xc] / total
            q = lab[k, xc] - zy * (8 * rows)
            s = jnp.zeros_like(q)
            for i in range(1, 8):
                s = s + jnp.where(q >= i * rows, 1, 0)
            r = q - s * rows
            up = jnp.where(r >= ha, 1, 0)
            at_main = ((s // 2 * 2 + up) * 2 + s % 2) * ha + r - up * ha
            at_ext = dm.main + s * 8 + r - rm
            place = jnp.where(r < rm, at_main, at_ext)
            pos_row[:, at] = jnp.where((q >= 0) & (q < 8 * rows), place, -1).astype(F32)

    def product(lhs, lanes):
        v = lax.dot_general(lhs, hv[lanes, :], (((1,), (1,)), ((), ())), preferred_element_type=F32)
        return v * (LOG2E / LOGIT_SCALE)

    def add_stats(v, lanes):
        m_old, s_old = m_row[:, lanes], s_row[:, lanes]
        m = jnp.maximum(m_old, jnp.max(v, axis=0, keepdims=True))
        s = jnp.sum(jnp.exp2(v - m), axis=0, keepdims=True)
        m_row[:, lanes] = m
        s_row[:, lanes] = s_old * jnp.exp2(m_old - m) + s

    def add_target(v, place, lanes):
        r = lax.broadcasted_iota(jnp.int32, v.shape, 0)
        hit = r.astype(F32) == pos_row[:, lanes] - place.astype(F32)
        tgt_row[:, lanes] += jnp.sum(jnp.where(hit, v, 0.0), axis=0, keepdims=True)

    m_row[:, :] = jnp.full((1, tok), -jnp.inf, F32)
    s_row[:, :] = jnp.zeros((1, tok), F32)
    tgt_row[:, :] = jnp.zeros((1, tok), F32)
    segs = [(half, j) for half in TWO for j in TWO]

    def load(r0, n, xx, cores=TWO):
        return [
            local(
                eg.at[xx[half] * 2 + j, pl.ds(half * ha + r0, n)],
                od.at[j, half, pl.ds(r0, n)],
                hsem.at[half * len(cores) + k],
            )
            for half in TWO
            for k, j in enumerate(cores)
        ]

    def narrow_all(r0, n, src, cores=TWO):
        for half in TWO:
            for j in cores:
                def narrow(r, half=half, j=j):
                    at = pl.multiple_of((half * 2 + j) * ha + r0 + r.start, r.size)
                    dz[pl.ds(at, r.size), :] = src(half, j)[r, :].astype(BF16)

                _loop_rows(n, 16, narrow)

    def load_narrow(r0, n, xx, core):
        for cp in load(r0, n, xx, (core,)):
            cp.wait()
        narrow_all(r0, n, lambda half, j: od.at[j, half, pl.ds(r0, n)], (core,))

    def block(r0, n, xx, loads=(), with_few=False):
        if loads:
            for cp in loads:
                cp.wait()
            narrow_all(r0, n, lambda half, j: od.at[j, half, pl.ds(r0, n)])
        left = [VOCAB_REAL - ((zy * 8 + xx[half] * 2 + j) * rows + half * ha + r0) for half, j in segs]
        w = nt // chunk
        deep = SLOTS // w

        def out(t):
            u = lax.rem(t, deep) * w
            return [
                pltpu.make_async_copy(
                    tst.at[u + i, pl.ds(m * n, n)],
                    zh.at[t * w + i, pl.ds(pl.multiple_of((xx[half] * 2 + half) * rm + j * ha + r0, 8), n)],
                    tsem.at[u + i],
                )
                for i in range(w)
                for m, (half, j) in enumerate(segs)
            ]

        def out_wait(t):
            u = lax.rem(t, deep) * w
            for i in range(w):
                whole = tst.at[u + i, _top(4 * n)]
                pltpu.make_async_copy(whole, zh.at[t * w + i, _top(4 * n)], tsem.at[u + i]).wait()

        @pl.loop(0, tok // nt)
        def _(t):
            @pl.when(t >= deep)
            def _():
                out_wait(t - deep)

            lanes = pl.ds(pl.multiple_of(t * nt, nt), nt)
            lhs = [dz[(half * 2 + j) * ha + r0 : (half * 2 + j) * ha + r0 + n, :] for half, j in segs]
            if with_few:
                lhs.append(dz[ext_at : ext_at + FEW, :])
            v = product(jnp.concatenate(lhs, axis=0), lanes)
            v, v_few = v[: 4 * n], v[4 * n :]
            r = lax.broadcasted_iota(jnp.int32, (n, nt), 0)
            v = [jnp.where(r < left[m], v[m * n : (m + 1) * n], -jnp.inf) for m in range(len(segs))]
            for part_v, (half, j) in zip(v, segs):
                add_target(part_v, (xx[half] * 2 + half) * rm + j * ha + r0, lanes)
            u = lax.rem(t, deep) * w
            for i in range(w):
                for m in range(len(segs)):
                    tst[u + i, m * n : (m + 1) * n, :] = v[m][:, i * chunk : (i + 1) * chunk]
            if with_few:
                r = lax.broadcasted_iota(jnp.int32, v_few.shape, 0)
                ok = ((r & 7) < rows - rm) & ((zy * 8 + (r >> 3)) * rows + rm + (r & 7) < VOCAB_REAL)
                v_few = jnp.where(ok, v_few, -jnp.inf)
                few[:, lanes] = v_few
                add_target(v_few, jnp.int32(dm.main), lanes)
                v.append(v_few)
            v = jnp.concatenate(v, axis=0)
            for cp in out(t):
                cp.start()
            add_stats(v, lanes)

        for t in range(deep):
            out_wait(t + tok // nt - deep)

    def both(xx):
        block(0, ha, xx, load(0, ha, xx))

    def turn(xx):
        for half in TWO:
            base = pl.multiple_of((xx[half] * 2 + half) * rm, rm)

            @pl.loop(0, dim // LANES)
            def _(d, half=half, base=base):
                at = pl.ds(pl.multiple_of(d * LANES, LANES), LANES)
                etv[at, pl.ds(base, rm)] = dz[half * rm : (half + 1) * rm, at].T

    with scope("own"):
        s_o.wait_recv()
        both((x, x))
        turn((x, x))

    with scope("wait_1"):
        r_a.wait_recv()
        last_n = dm.cuts[-1][1]
        spans = [(pl.ds(r0, n), pl.ds(ha + r0, n + 8 * (r0 + n == ha))) for r0, n in dm.cuts]

        def far_pieces(xx, half, to):
            cps = [piece(slot(xx), pair[half], to) for pair in spans[:-1]]
            cps.append(remote(eg.at[slot(xx), spans[-1][half]], sst.at[c, pl.ds(half * last_n, last_n)], to))
            return cps

        r_f = far_pieces(x_m, 0, xp)
        d = [piece(slot(x_m), half_a, sib)]
        l_b.wait_recv()
        l_f = far_pieces(x_p, 1, xm)
        d.append(piece(slot(x_p), half_b, sib))
        for cp in d:
            cp.wait_recv()

    with scope("near_1"):
        both((x_m, x_p))
        turn((x_m, x_p))

    with scope("wait_2"):
        r_b.wait_recv()
        d = [piece(slot(x_m), half_b, sib)]
        l_a.wait_recv()
        d.append(piece(slot(x_p), half_a, sib))
        for cp in d:
            cp.wait_recv()

    with scope("near_2"):
        both((x_p, x_m))
        turn((x_p, x_m))

    far = (x_far, x_far)

    with scope("wait_3"):
        d = []
        for cp, r in zip((r_f[0], l_f[0]), spans[0]):
            cp.wait_recv()
            d.append(piece(slot(x_far), r, sib))
        load_narrow(*dm.cuts[0], far, c)
        for cp in d:
            cp.wait_recv()
    with scope("far_a"):
        ext_loads = [local(eg.at[s, pl.ds(rm, 8)], few.at[pl.ds(s * 8, 8)], lsem.at[s]) for s in range(8)]
        load_narrow(*dm.cuts[0], far, 1 - c)
        for cp in ext_loads:
            cp.wait()
        dz[ext_at : ext_at + FEW, :] = few[...].astype(BF16)
        dz[ext_at + FEW : ext_at + LANES, :] = jnp.zeros((FEW, dim), BF16)
        block(*dm.cuts[0], far, with_few=True)
    with scope("wait_5"):
        r_f[-1].wait_recv()
        l_f[-1].wait_recv()
        both_last = sst.at[c, _top(2 * last_n)]
        over = _remote(both_last, both_last, send, recv, next(ids), sib)
        over.start()

        @pl.loop(0, dim // LANES)
        def _(i):
            at = pl.ds(pl.multiple_of(i * LANES, LANES), LANES)
            etv[at, dm.main : dm.wide] = dz[ext_at : ext_at + LANES, at].T

        def last_rows(half, j):
            return sst.at[j, pl.ds(half * last_n, last_n)]

        narrow_all(0, last_n, last_rows, (c,))
        over.wait_recv()

    with scope("far_c"):
        narrow_all(0, last_n, last_rows, (1 - c,))
        block(0, last_n, far)
        over.wait_send()
        for s in TWO:
            pl.semaphore_signal(free.at[s], inc=1, device_id=(sib,), device_id_type=MESH)

    with scope("turn_far"):
        lse_row[:, :] = m_row[:, :] + jnp.log(s_row[:, :]) * LOG2E
        stats = exchange(lse_row, got, near)
        turn(far)

    wide = 2 * rm

    at_dht = SLOTS - 4

    def chunk_of(zz, yy):
        return _mod4(zz) * 4 + _rem(yy + 8, 4)

    def all_far(i):
        return x_far * wide + i // 16 * rm, _rem(i, 16)

    def in_order(i):
        n = i // 3
        m = n - 7
        k = _pick(n < 7, chunk_of(z + n - 1, y + 2), chunk_of(z + 3 + m // 3, y + 3 + _rem(m + 9, 3)))
        return _mod4(x + 3 + _rem(i, 3)) * wide, _pick(n < 4, chunk_of(z + 2, n), k)

    def later(i):
        return in_order(i + SLOTS)

    def zload(where, i, ring, n):
        at, k = where(i)
        s = _rem(i, ring)
        src = zh.at[k, pl.ds(pl.multiple_of(at, rm), n)]
        return pltpu.make_async_copy(src, tst.at[s, _top(n)], tsem.at[s])

    def zahead(where, ring, n):
        for i in range(ring):
            zload(where, i, ring, n).start()

    with scope("stats"):
        zahead(all_far, SLOTS, rm)
        for cp in stats:
            cp.wait()
        top = lse_row[:, :]
        for k in range(len(near)):
            top = jnp.maximum(top, got[k])
        s = jnp.exp2(lse_row[:, :] - top)
        for k in range(len(near)):
            s = s + jnp.exp2(got[k] - top)
        lse_row[:, :] = top + jnp.log(s) * LOG2E

    def dz_part(v, place, at, lanes):
        r = lax.broadcasted_iota(jnp.int32, v.shape, 0).astype(F32)
        hit = r == pos_row[:, lanes] - place.astype(F32)
        p = jnp.exp2(v - lse_row[:, lanes])
        dz[at, lanes] = (jnp.where(hit, p - 1.0, p) * w_row[:, lanes]).astype(BF16)

    step = min(LANES, rm)

    def dz_rows(where, start, stop, last_tile, ring, n):
        @pl.loop(start, stop)
        def _(i):
            @pl.when((i > 0) & (i + ring - 1 < last_tile))
            def _():
                zload(where, i + ring - 1, ring, n).start()

            zload(where, i, ring, n).wait()
            row, k = where(i)
            lanes = pl.ds(pl.multiple_of(k * chunk, chunk), chunk)

            @pl.loop(0, n // step)
            def _(j):
                at = pl.multiple_of(row + j * step, step)
                r = pl.ds(pl.multiple_of(j * step, step), step)
                dz_part(tst[lax.rem(i, ring), r, :], at, pl.ds(at, step), lanes)

    def dz_far(start, stop):
        dz_rows(all_far, start, stop, 32, SLOTS, rm)

    with scope("dz_far"):
        dz_far(0, 16)

    nd = dim // 2
    few_rows = pl.ds(dm.main, FEW)
    pair_ids = [(next(ids), next(ids)) for _ in TWO]

    def over_d2d(s, n, i):
        lanes = pl.ds(pl.multiple_of(i * nd, nd), nd)
        there = sst.at[s, _top(n), lanes]
        return _remote(od.at[s, 1 - c, _top(n), lanes], there, send, recv, pair_ids[s][0] + i, sib)

    def de_block(xx, half, s, with_few=False):
        at = pl.ds(pl.multiple_of((xx * 2 + half) * rm, rm), rm)
        n = ha + 8 * half
        pl.semaphore_wait(free.at[s], 1)

        @pl.loop(0, 2)
        def _(i):
            lanes = pl.ds(pl.multiple_of(i * nd, nd), nd)
            lhs = jnp.concatenate([dz[at, :], dz[few_rows, :]], axis=0) if with_few else dz[at, :]
            v = jnp.dot(lhs, hv[:, lanes], preferred_element_type=F32)
            if with_few:
                few[:, lanes] = v[rm:]
            for j in TWO:
                od[s, j, 0:ha, lanes] = v[j * ha : (j + 1) * ha]
                if half:
                    od[s, j, ha:n, lanes] = few[pl.ds(pl.multiple_of((xx * 2 + j) * 8, 8), 8), lanes]
            over_d2d(s, n, i).start()

        return half, s, n

    def stored(blk, to):
        half, s, n = blk
        return pltpu.make_async_copy(od.at[s, c, _top(n)], to.at[pl.ds(half * ha, n)], dsem.at[s])

    def early(blk, src):
        half, s, n = blk
        for i in TWO:
            over_d2d(s, n, i).wait_send()
        return local(src.at[pl.ds(half * ha, n)], od.at[s, 1 - c, _top(n)], lsem.at[s])

    def sum_add(blk, to, more=None):
        half, s, n = blk
        for i in TWO:
            over_d2d(s, n, i).wait_recv()
        if more is not None:
            more.wait()

        def add(r):
            v = od[s, c, r, :] + sst[s, r, :]
            od[s, c, r, :] = v if more is None else v + od[s, 1 - c, r, :]

        _loop_rows(n, 8, add)
        if more is None:
            pl.semaphore_signal(free.at[s], inc=1, device_id=(sib,), device_id_type=MESH)
            for i in TWO:
                over_d2d(s, n, i).wait_send()
        cp = stored(blk, to)
        cp.start()
        return cp

    def ring_sum(xx, rows_, n, src, s, dst, dev):
        lds = [
            local(q_h.at[xx, rows_], od.at[s, 0, _top(n)], lsem.at[0]),
            local(src, od.at[s, 1, _top(n)], lsem.at[1]),
        ]
        for cp in lds:
            cp.wait()
        _add_rows(od.at[s, 0, _top(n)], [od.at[s, 1, _top(n)]], 8)
        local(od.at[s, 0, _top(n)], q_h.at[xx, rows_], lsem.at[0]).wait()
        return remote(q_h.at[xx, rows_], dst, dev)

    stores = []

    def flush():
        while stores:
            stores.pop().wait()

    def tiles(q, where, between=None):
        flush()

        def outs(i):
            p, ab = where(i)
            r = pl.ds(q * h, h)
            dsts = [dhp.at[ab * 2 + j, p, r] if q == 0 else dhp.at[p, ab * 2 + j, r] for j in TWO]
            return [
                pltpu.make_async_copy(tst.at[at_dht + i * 2 + j, _top(h)], dst, hsem.at[i * 2 + j])
                for j, dst in enumerate(dsts)
            ]

        @pl.loop(0, 2)
        def _(i):
            if between is not None:
                pl.when(i > 0)(between)
            p, ab = where(i)
            ks = [(ab * 2 + j) * 4 + p if q == 0 else p * 4 + ab * 2 + j for j in TWO]
            rhs = jnp.concatenate([dz[:, pl.ds(pl.multiple_of(k * chunk, chunk), chunk)] for k in ks], axis=1)
            v = jnp.dot(etv[q * h : (q + 1) * h, :], rhs, preferred_element_type=F32)
            for j in TWO:
                tst[at_dht + i * 2 + j, 0:h, :] = v[:, j * chunk : (j + 1) * chunk]
            for cp in outs(i):
                cp.start()

        for i in TWO:
            stores.extend(outs(i))

    def part(q, p, lo, n):
        r = pl.ds(q * h, h)
        if q == 0:
            return dhp.at[pl.ds(lo, n), p, r]
        return dhp.at[p, pl.ds(lo, n), r]

    def one(q, p, i):
        r = pl.ds(q * h, h)
        return dhp.at[i, p, r] if q == 0 else dhp.at[p, i, r]

    ring1, ring2 = ((yp, ym), (zp, zm)), ((zp, zm), (yp, ym))
    pos1, pos2 = (y, z), (z, y)
    first, second = ({}, {}), ({}, {})

    def send_far(q):
        flush()
        p, (rt, lt) = pos1[q], ring1[q]
        first[q]["far_r"] = remote(part(q, _mod4(p + 2), 0, 2), ya.at[q], rt)
        first[q]["far_l"] = remote(part(q, _mod4(p + 2), 2, 2), yb.at[q], lt)

    def send_near(q):
        flush()
        p, (rt, lt) = pos1[q], ring1[q]
        first[q]["near_r"] = remote(part(q, _mod4(p + 1), 2, 2), yl.at[q, pl.ds(2, 2)], rt)
        first[q]["near_l"] = remote(part(q, _mod4(p - 1), 0, 2), yr.at[q, _top(2)], lt)

    def fetch(i, src):
        return local(src, tst.at[i, _top(h)], tsem.at[i])

    def pass_on(q):
        flush()
        p, (rt, lt) = pos1[q], ring1[q]
        lds = [fetch(i, one(q, _mod4(p + 1), i)) for i in TWO]
        lds += [fetch(2 + i, one(q, _mod4(p - 1), 2 + i)) for i in TWO]
        first[q]["far_r"].wait_recv()
        for i in TWO:
            lds[i].wait()
            _add_rows(ya.at[q, i], [tst.at[i, _top(h)]], min(FEW, h))
        first[q]["sum_r"] = remote(ya.at[q], yl.at[q, _top(2)], rt)
        first[q]["far_l"].wait_recv()
        for i in TWO:
            lds[2 + i].wait()
            _add_rows(yb.at[q, i], [tst.at[2 + i, _top(h)]], min(FEW, h))
        first[q]["sum_l"] = remote(yb.at[q], yr.at[q, pl.ds(2, 2)], lt)

    lo, hi = _top(hc), pl.ds(hc, hc)

    def second_phase(q):
        flush()
        r, (rt, lt) = pos2[q], ring2[q]
        r2, r1, rm1 = _mod4(r + 2), _mod4(r + 1), _mod4(r - 1)
        order = (r2, r1, rm1, r)
        lds = [fetch(i, one(q, pos1[q], k)) for i, k in enumerate(order)]
        for k in NEAR_KEYS:
            first[q][k].wait_recv()
        lds2 = [fetch(4 + i, yr.at[q, k]) for i, k in enumerate(order)]
        for i, k in enumerate(order):
            lds[i].wait()
            lds2[i].wait()
            _add_rows(yl.at[q, k], [tst.at[i, _top(h)], tst.at[4 + i, _top(h)]], min(FEW, h))
            if i == 0:
                second[q]["far_r"] = remote(yl.at[q, r2, lo], za.at[q], rt)
                second[q]["far_l"] = remote(yl.at[q, r2, hi], zb.at[q], lt)
            if i == 1:
                second[q]["near_r"] = remote(yl.at[q, r1, hi], zl.at[q, hi], rt)
            if i == 2:
                second[q]["near_l"] = remote(yl.at[q, rm1, lo], zr.at[q, lo], lt)

    def second_pass(q):
        r, (rt, lt) = pos2[q], ring2[q]
        r1, rm1 = _mod4(r + 1), _mod4(r - 1)
        second[q]["far_r"].wait_recv()
        _add_rows(yl.at[q, r1, lo], [za.at[q]], min(FEW, hc))
        second[q]["sum_r"] = remote(yl.at[q, r1, lo], zl.at[q, lo], rt)
        second[q]["far_l"].wait_recv()
        _add_rows(yl.at[q, rm1, hi], [zb.at[q]], min(FEW, hc))
        second[q]["sum_l"] = remote(yl.at[q, rm1, hi], zr.at[q, hi], lt)

    def last(q):
        r = pos2[q]
        for k in NEAR_KEYS:
            second[q][k].wait_recv()
        n = min(LANES, h)

        @pl.loop(0, h // n)
        def _(i):
            at = pl.ds(pl.multiple_of(i * n, n), n)
            v = yl[q, r, at, :] + zl[q, at, :] + zr[q, at, :]
            od[0, 0, 0:chunk, pl.ds(pl.multiple_of(q * h + i * n, n), n)] = (v * (1.0 / LOGIT_SCALE)).T

    def tiles_far(q, between=None):
        tiles(q, lambda i: (_mod4(pos1[q] + 2), i), between)

    def tiles_near(q):
        tiles(q, lambda i: (_mod4(pos1[q] + 1 + 2 * i), 1 - i))

    def tiles_pass(q):
        tiles(q, lambda i: (_mod4(pos1[q] + 1 + 2 * i), i))

    def tiles_own(q):
        tiles(q, lambda i: (pos1[q], i))

    all_later = 48 - SLOTS

    def dz_first(start, stop):
        dz_rows(in_order, start, stop, SLOTS, SLOTS, wide)

    def dz_later(start, stop):
        dz_rows(later, start, stop, all_later, at_dht, wide)

    with scope("de_far"):
        b0 = de_block(x_far, 0, 0)
        dz_far(16, 32)
        zahead(in_order, SLOTS, wide)
        for l in range(0, tok, nt):
            lanes = pl.ds(l, nt)
            dz_part(few[:, lanes], jnp.int32(dm.main), few_rows, lanes)
        dz[dm.main + FEW : dm.wide, :] = jnp.zeros((FEW, tok), BF16)
        b1 = de_block(x_far, 1, 1, True)
    with scope("dz_1"):
        c0 = sum_add(b0, q_h.at[x_far])
        dz_first(0, 8)
        c0.wait()
        e0 = remote(q_h.at[x_far, half_a], xa, xp)
        dz_first(8, SLOTS)
        zahead(later, at_dht, wide)
        c1 = sum_add(b1, q_h.at[x_far])
        e1 = _remote(q_h.at[x_far, half_b], xb, send, recv, next(ids), xm)
        sent.append(e1)
    with scope("dh_far1"):
        def send_e1():
            c1.wait()
            e1.start()

        tiles_far(1, send_e1)
    with scope("dz_2"):
        dz_later(0, 9)
        send_far(1)
    with scope("dh_far0"):
        tiles_far(0)
    with scope("dz_3"):
        dz_later(9, 13)
        send_far(0)
        dz_later(13, all_later)
    with scope("de_2"):
        b2 = de_block(x_p, 1, 0)
        b3 = de_block(x_m, 0, 1)
        c2 = sum_add(b2, q_h.at[x_p])
    with scope("dh_near"):
        tiles_near(1)
        c2.wait()
        e2 = remote(q_h.at[x_p, half_b], xe.at[half_b], xp)
        c3 = sum_add(b3, q_h.at[x_m])
        send_near(1)
        tiles_near(0)
        c3.wait()
        e3 = remote(q_h.at[x_m, half_a], xe.at[half_a], xm)
        send_near(0)
    with scope("dh_pass"):
        tiles_pass(1)
        tiles_pass(0)
        pass_on(1)
    with scope("de_4"):
        b4 = de_block(x_p, 0, 0)
        pass_on(0)
        b5 = de_block(x_m, 1, 1)
        c4 = sum_add(b4, q_h.at[x_p])
    with scope("dh_own"):
        tiles_own(1)
        c5 = sum_add(b5, q_h.at[x_m])
        tiles_own(0)
        c4.wait()
        c5.wait()
    old = list(sent)
    sent.clear()
    with scope("ring"):
        e0.wait_recv()
        e4 = ring_sum(x_p, half_a, ha, xa, 0, xs.at[half_a], xp)
        e1.wait_recv()
        e5 = ring_sum(x_m, half_b, ha + 8, xb, 1, xs.at[half_b], xm)
    with scope("de_6"):
        b6 = de_block(x, 0, 0)
    with scope("de_7"):
        b7 = de_block(x, 1, 1)
        xo_load = local(x4.at[zy, xc], dz.at[_top(chunk)], osem.at[0])
    with scope("second_1"):
        second_phase(1)
    with scope("second_0"):
        second_phase(0)
    with scope("spass_1"):
        second_pass(1)
    with scope("sum_6"):
        e3.wait_recv()
        c6 = early(b6, xe)
        e2.wait_recv()
        c7 = early(b7, xe)
        c6 = sum_add(b6, q_o, c6)
        c7 = sum_add(b7, q_o, c7)
    with scope("spass_0"):
        second_pass(0)
        c6.wait()
        c7.wait()
    def drain(cps):
        while cps:
            cps.pop().wait_send()

    def own_x(r):
        v = dz[r, :].astype(F32)
        inv = lax.rsqrt(jnp.mean(v * v, axis=-1, keepdims=True) + NORM_EPS)
        od[1, 0, r, :] = v * inv
        od[1, 1, r, 0:LANES] = jnp.broadcast_to(inv, (r.size, LANES))

    def own_dg(q):
        lanes = pl.ds(q * h, h)

        def add(i, acc):
            r = pl.ds(pl.multiple_of(i * 8, 8), 8)
            return acc + od[0, 0, r, lanes] * od[1, 0, r, lanes]

        acc = lax.fori_loop(0, chunk // 8, add, jnp.zeros((8, h), F32))
        sm[:, lanes] = jnp.sum(acc, axis=0, keepdims=True)

    def own_dx(r):
        x_hat, u = od[1, 0, r, :], od[0, 0, r, :] * gain
        od[0, 1, r, :] = od[1, 1, r, 0:1] * (u - x_hat * jnp.mean(u * x_hat, axis=-1, keepdims=True))

    with scope("own_x"):
        xo_load.wait()
        _loop_rows(chunk, 16, own_x)
        lse = jnp.where(zy == 0, lse_row[:, :], 0.0)
        loss = jnp.sum(w_row[:, :] * (lse - tgt_row[:, :]))
        sm[:, dim : dim + LANES] = jnp.full((1, LANES), loss / LOG2E)
        drain(old)
    with scope("last_1"):
        last(1)
        own_dg(1)
    with scope("last_0"):
        last(0)
        own_dg(0)

    with scope("small_1"):
        old = [cp for cp in sent if cp is not e4 and cp is not e5]
        near_sums = exchange(sm, got1, near)
        _loop_rows(chunk, 16, own_dx)
        dx_copy = local(od.at[0, 1, _top(chunk)], dx_out, osem.at[0])
        drain(old)
        for cp in near_sums:
            cp.wait()
    with scope("small_2"):
        tot = sm[...]
        for k in range(len(near)):
            tot = tot + got1[k]
        total_v[...] = tot
        all_sums = exchange(total_v, got2, line)
        mine = local(total_v, got2.at[len(line)], osem.at[1])
    with scope("ring_end"):
        for cp in (e4, e5):
            cp.wait()
        dx_copy.wait()
        mine.wait()
    with scope("small_3"):
        for cp in all_sums:
            cp.wait()


def _run(dm, x4, table, gain, labels, mask):
    hbm, vm = pl.BlockSpec(memory_space=HBM), pl.BlockSpec(memory_space=VMEM)
    sd = jax.ShapeDtypeStruct
    d, tok, h, ck, pad, ha = dm.dim, dm.tok, dm.h, dm.chunk, dm.pad, dm.ha
    line, quad, pair = VMEM((1, tok), F32), VMEM((2, 2, h, ck), F32), VMEM((2, h, ck), F32)
    part, shard = VMEM((2, h // 2, ck), F32), sd((pad, d), F32)
    out = pl.pallas_call(
        functools.partial(_kernel, dm),
        name="head",
        out_shape=(
            sd((ck, d), F32), sd((8, 1, d + LANES), F32),
            shard, shard, shard,
            sd((8, pad, d), F32), sd((16, dm.main, ck), F32),
            sd((4, pad, d), F32), sd((ha, d), F32), sd((ha + 8, d), F32),
            sd((4, 4, d, ck), F32), sd((2, 4, h, ck), F32),
        ),
        in_specs=[hbm, vm, vm, vm, vm],
        out_specs=[hbm] * 12,
        scratch_shapes=[
            VMEM((tok, d), BF16), VMEM((d, dm.wide), BF16), VMEM((dm.wide, tok), BF16),
            VMEM((2, 2, ha + 8, d), F32), VMEM((2, ha + 8, d), F32), VMEM((FEW, d), F32), VMEM((8, d), F32),
            quad, quad, VMEM((2, 4, h, ck), F32),
            part, part, pair, pair,
            VMEM((SLOTS, max(h, 2 * dm.rm), ck), F32),
            line, line, line, line, line, line, VMEM((15, 1, tok), F32),
            VMEM((1, d + LANES), F32), VMEM((15, 1, d + LANES), F32), VMEM((1, d + LANES), F32),
            DMA((53,)), DMA((53,)), pltpu.SemaphoreType.REGULAR((2,)),
            DMA((SLOTS,)), DMA((4,)), DMA((2,)), DMA((2,)), DMA((8,)),
        ],
        compiler_params=pltpu.CompilerParams(
            collective_id=0, has_side_effects=True, vmem_limit_bytes=67043328
        ),
    )(x4, table, gain, labels, mask)
    return _write_out(dm, out[2:4], *out[:2])


def _write_kernel(own, ring, dx, small, de_o, dx_o, dg_o, loss_o):
    de_o[:, :] = (own[:, :] + ring[:, :]) * (1.0 / LOGIT_SCALE)
    dx_o[:, :] = dx[:, :]
    total = jnp.sum(small[:, :, :], axis=0)
    d = dg_o.shape[1]
    dg_o[:, :] = total[:, :d]
    loss_o[:, :] = total[:, d : d + 1]


def _write_out(dm, parts, dx, small):
    d, step, blocks = dm.dim, dm.ha + 8, 2
    sd = jax.ShapeDtypeStruct
    some = pl.BlockSpec((step, d), lambda i: (i, 0))
    half = pl.BlockSpec((dm.chunk // blocks, d), lambda i: (i, 0))
    row, one = pl.BlockSpec((1, d), lambda i: (0, 0)), pl.BlockSpec((1, 1), lambda i: (0, 0))
    rows = pl.BlockSpec(small.shape, lambda i: (0, 0, 0))
    return pl.pallas_call(
        _write_kernel,
        name="write_out",
        grid=(blocks,),
        out_shape=(sd((dm.rows, d), F32), sd((dm.chunk, d), F32), sd((1, d), F32), sd((1, 1), F32)),
        in_specs=[some, some, half, rows],
        out_specs=(some, half, row, one),
    )(*parts, dx, small)


def solution(mesh):
    group = mesh.shape[AXIS]

    def local_step(residual, labels, loss_mask, norm_gain, table_shard):
        tokens, dim = residual.shape
        rows = table_shard.shape[0]
        dm = Dims(tokens, dim, rows, group)
        x4 = residual.reshape(16, 8, dm.chunk, dim)
        lab = labels.reshape(16, 8, 1, dm.chunk)
        msk = loss_mask.reshape(16, 8, 1, dm.chunk)
        d_embed, d_res, d_gain, loss = _run(dm, x4, table_shard, norm_gain[None, :], lab, msk)
        return loss.reshape(()), d_res, d_embed, d_gain.reshape(dim)

    return jax.shard_map(
        local_step,
        mesh=mesh,
        in_specs=(P(), P(), P(), P(), P(AXIS, None)),
        out_specs=(P(), P(AXIS, None), P(AXIS, None), P()),
        check_vma=False,
    )
```

```python
import functools
import itertools
import math

import jax
import jax.numpy as jnp
from jax import lax
from jax.experimental import pallas as pl
from jax.experimental.pallas import tpu as pltpu
from jax.sharding import PartitionSpec as P

VOCAB_REAL = 49155
LOGIT_SCALE = 6.0
NORM_EPS = 1e-6

AXIS = "vp"
MESH = pl.DeviceIdType.MESH
F32 = jnp.float32
BF16 = jnp.bfloat16
HBM = pltpu.HBM
VMEM = pltpu.VMEM
DMA = pltpu.SemaphoreType.DMA


def _coords():
    me = lax.axis_index(AXIS)
    return me // 32, (me // 8) % 4, (me // 2) % 4, me % 2


def _dev(z, y, x, c):
    return ((z * 4 + y) * 4 + x) * 2 + c


def _mod4(v):
    return lax.rem(v + 8, 4)


def _barrier(peers):
    sem = pltpu.get_barrier_semaphore()
    for p in peers:
        pl.semaphore_signal(sem, inc=1, device_id=(p,), device_id_type=MESH)
    pl.semaphore_wait(sem, len(peers))


def _remote(src, dst, send, recv, k, dev):
    return pltpu.make_async_remote_copy(
        src_ref=src,
        dst_ref=dst,
        send_sem=send.at[k],
        recv_sem=recv.at[k],
        device_id=(dev,),
        device_id_type=MESH,
    )


LANES = 128


class Dims:
    def __init__(self, tokens, dim, rows, group):
        self.dim, self.rows = dim, rows
        unit = LANES if rows >= LANES else 64
        self.rm = rows // unit * unit
        self.ha = self.rm // 2
        low = max(16, self.ha // 48 * 16)
        self.cuts = ((low, self.ha - low), (0, low))
        self.pad = self.rm + 8
        self.chunk = tokens // group
        self.tok = 16 * self.chunk
        self.nt = 4 * self.chunk
        self.main = 8 * self.rm
        self.wide = self.main + LANES
        self.h = dim // 2


def _top(n):
    return pl.ds(0, n)


def _rem(a, b):
    return a % b if isinstance(a, int) else lax.rem(a, b)


def _pick(test, a, b):
    return (a if test else b) if isinstance(test, bool) else jnp.where(test, a, b)


def _loop_rows(rows, step, fn):
    @pl.loop(0, rows // step)
    def _(i):
        fn(pl.ds(pl.multiple_of(i * step, step), step))


def _add_rows(dst, srcs, step):
    def add(r):
        acc = dst[r, :]
        for s in srcs:
            acc = acc + s[r, :]
        dst[r, :] = acc

    _loop_rows(dst.shape[0], step, add)


SLOTS = 12
FEW = 64
TWO = range(2)
LOG2E = math.log2(math.e)
NEAR_KEYS = ("near_r", "near_l", "sum_r", "sum_l")
scope = jax.named_scope


def _kernel(
    dm, x4, e_ref, g_ref, lab, msk,
    dx_out, got2, q_o, xs, xe, eg, zh, q_h, xa, xb, dhp, yr,
    hv, etv, dz, od, sst, few, oext, ya, yb, yl, za, zb, zl, zr, tst,
    m_row, s_row, w_row, pos_row, lse_row, tgt_row, got, sm, got1, total_v,
    send, recv,
    free, tsem, hsem, dsem, osem, lsem,
):
    z, y, x, c = _coords()
    xc, zy = x * 2 + c, z * 4 + y
    rows, rm, ha, dim, h = dm.rows, dm.rm, dm.ha, dm.dim, dm.h
    chunk, tok, nt, hc = dm.chunk, dm.tok, dm.nt, dm.h // 2
    x_far, x_p, x_m = _mod4(x + 2), _mod4(x + 1), _mod4(x - 1)
    xp, xm = _dev(z, y, x_p, c), _dev(z, y, x_m, c)
    yp, ym = _dev(z, _mod4(y + 1), x, c), _dev(z, _mod4(y - 1), x, c)
    zp, zm = _dev(_mod4(z + 1), y, x, c), _dev(_mod4(z - 1), y, x, c)
    sib = _dev(z, y, x, 1 - c)
    near = [_dev(_mod4(z + a), _mod4(y + b), x, c) for a in range(4) for b in range(4) if a or b]
    line = [_dev(z, y, _mod4(x + a), lax.rem(c + b, 2)) for a in range(4) for b in TWO if a or b]
    bar = pltpu.get_barrier_semaphore()
    for p in (*near, *line):
        pl.semaphore_signal(bar, inc=1, device_id=(p,), device_id_type=MESH)
    sent = []
    ids = itertools.count()

    def remote(src, dst, dev):
        cp = _remote(src, dst, send, recv, next(ids), dev)
        cp.start()
        sent.append(cp)
        return cp

    def exchange(src, dst, devs):
        k = next(ids)
        for i, dev in enumerate(devs):
            _remote(src, dst.at[i], send, recv, k, dev).start()
        whole = dst.at[_top(len(devs))]
        return pltpu.make_async_copy(whole, whole, recv.at[k]), pltpu.make_async_copy(whole, whole, send.at[k])

    def local(src, dst, sem):
        cp = pltpu.make_async_copy(src, dst, sem)
        cp.start()
        return cp

    x_at, ext_at = 2 * rm, 4 * rm

    def xload(k):
        s = lax.rem(k, 4)
        to = dz.at[pl.ds(pl.multiple_of(x_at + s * chunk, chunk), chunk)]
        return pltpu.make_async_copy(x4.at[k, xc], to, tsem.at[s])

    with scope("prep"):
        for k in range(3):
            xload(k).start()
        own = xc
        for j in TWO:
            def widen(r, j=j):
                od[0, j, r, :] = e_ref[pl.ds(j * ha + r.start, r.size), :].astype(F32)

            _loop_rows(ha, 16, widen)
        oext[...] = jnp.zeros_like(oext)
        oext[0 : rows - rm, :] = e_ref[rm:rows, :].astype(F32)
        cps = [local(od.at[0, j, _top(ha)], eg.at[own, pl.ds(j * ha, ha)], hsem.at[j]) for j in TWO]
        cps.append(local(oext, eg.at[own, pl.ds(rm, 8)], hsem.at[2]))
        for cp in cps:
            cp.wait()
        pl.semaphore_wait(bar, 22)

    half_a, half_b = _top(ha), pl.ds(ha, ha + 8)

    def piece(s, r, dev):
        return remote(eg.at[s, r], eg.at[s, r], dev)

    def slot(xx):
        return xx * 2 + c

    r_a, l_b = piece(own, half_a, xp), piece(own, half_b, xm)
    s_o = piece(own, _top(dm.pad), sib)
    r_b, l_a = piece(own, half_b, xp), piece(own, half_a, xm)

    gain = g_ref[...]

    with scope("norm"):
        @pl.loop(0, 16)
        def _(k):
            @pl.when(k < 13)
            def _():
                xload(k + 3).start()

            xload(k).wait()

            def norm(r):
                v = dz[pl.ds(pl.multiple_of(x_at + lax.rem(k, 4) * chunk + r.start, r.size), r.size), :].astype(F32)
                inv = lax.rsqrt(jnp.mean(v * v, axis=-1, keepdims=True) + NORM_EPS)
                hv[pl.ds(pl.multiple_of(k * chunk + r.start, r.size), r.size), :] = (v * inv * gain).astype(BF16)

            _loop_rows(chunk, 16, norm)

    with scope("labels"):
        total = jnp.sum(msk[...])
        for k in range(16):
            at = pl.ds(k * chunk, chunk)
            w_row[:, at] = msk[k, xc] / total
            q = lab[k, xc] - zy * (8 * rows)
            s = jnp.zeros_like(q)
            for i in range(1, 8):
                s = s + jnp.where(q >= i * rows, 1, 0)
            r = q - s * rows
            up = jnp.where(r >= ha, 1, 0)
            at_main = ((s // 2 * 2 + up) * 2 + s % 2) * ha + r - up * ha
            at_ext = dm.main + s * 8 + r - rm
            place = jnp.where(r < rm, at_main, at_ext)
            pos_row[:, at] = jnp.where((q >= 0) & (q < 8 * rows), place, -1).astype(F32)

    def product(lhs, lanes):
        v = lax.dot_general(lhs, hv[lanes, :], (((1,), (1,)), ((), ())), preferred_element_type=F32)
        return v * (LOG2E / LOGIT_SCALE)

    def add_stats(v, lanes):
        m_old, s_old = m_row[:, lanes], s_row[:, lanes]
        m = jnp.maximum(m_old, jnp.max(v, axis=0, keepdims=True))
        s = jnp.sum(jnp.exp2(v - m), axis=0, keepdims=True)
        m_row[:, lanes] = m
        s_row[:, lanes] = s_old * jnp.exp2(m_old - m) + s

    def add_target(v, place, lanes):
        r = lax.broadcasted_iota(jnp.int32, v.shape, 0)
        hit = r.astype(F32) == pos_row[:, lanes] - place.astype(F32)
        tgt_row[:, lanes] += jnp.sum(jnp.where(hit, v, 0.0), axis=0, keepdims=True)

    m_row[:, :] = jnp.full((1, tok), -jnp.inf, F32)
    s_row[:, :] = jnp.zeros((1, tok), F32)
    tgt_row[:, :] = jnp.zeros((1, tok), F32)
    segs = [(half, j) for half in TWO for j in TWO]

    def load(r0, n, xx, cores=TWO):
        return [
            local(
                eg.at[xx[half] * 2 + j, pl.ds(half * ha + r0, n)],
                od.at[j, half, pl.ds(r0, n)],
                hsem.at[half * len(cores) + k],
            )
            for half in TWO
            for k, j in enumerate(cores)
        ]

    def narrow_all(r0, n, src, cores=TWO):
        for half in TWO:
            for j in cores:
                def narrow(r, half=half, j=j):
                    at = pl.multiple_of((half * 2 + j) * ha + r0 + r.start, r.size)
                    dz[pl.ds(at, r.size), :] = src(half, j)[r, :].astype(BF16)

                _loop_rows(n, 16, narrow)

    def load_narrow(r0, n, xx, core):
        for cp in load(r0, n, xx, (core,)):
            cp.wait()
        narrow_all(r0, n, lambda half, j: od.at[j, half, pl.ds(r0, n)], (core,))

    def block(r0, n, xx, loads=(), with_few=False):
        if loads:
            for cp in loads:
                cp.wait()
            narrow_all(r0, n, lambda half, j: od.at[j, half, pl.ds(r0, n)])
        left = [VOCAB_REAL - ((zy * 8 + xx[half] * 2 + j) * rows + half * ha + r0) for half, j in segs]
        w = nt // chunk
        deep = SLOTS // w

        def out(t):
            u = lax.rem(t, deep) * w
            return [
                pltpu.make_async_copy(
                    tst.at[u + i, pl.ds(m * n, n)],
                    zh.at[t * w + i, pl.ds(pl.multiple_of((xx[half] * 2 + half) * rm + j * ha + r0, 8), n)],
                    tsem.at[u + i],
                )
                for i in range(w)
                for m, (half, j) in enumerate(segs)
            ]

        def out_wait(t):
            u = lax.rem(t, deep) * w
            for i in range(w):
                whole = tst.at[u + i, _top(4 * n)]
                pltpu.make_async_copy(whole, zh.at[t * w + i, _top(4 * n)], tsem.at[u + i]).wait()

        @pl.loop(0, tok // nt)
        def _(t):
            @pl.when(t >= deep)
            def _():
                out_wait(t - deep)

            lanes = pl.ds(pl.multiple_of(t * nt, nt), nt)
            lhs = [dz[(half * 2 + j) * ha + r0 : (half * 2 + j) * ha + r0 + n, :] for half, j in segs]
            if with_few:
                lhs.append(dz[ext_at : ext_at + FEW, :])
            v = product(jnp.concatenate(lhs, axis=0), lanes)
            v, v_few = v[: 4 * n], v[4 * n :]
            r = lax.broadcasted_iota(jnp.int32, (n, nt), 0)
            v = [jnp.where(r < left[m], v[m * n : (m + 1) * n], -jnp.inf) for m in range(len(segs))]
            for part_v, (half, j) in zip(v, segs):
                add_target(part_v, (xx[half] * 2 + half) * rm + j * ha + r0, lanes)
            u = lax.rem(t, deep) * w
            for i in range(w):
                for m in range(len(segs)):
                    tst[u + i, m * n : (m + 1) * n, :] = v[m][:, i * chunk : (i + 1) * chunk]
            if with_few:
                r = lax.broadcasted_iota(jnp.int32, v_few.shape, 0)
                ok = ((r & 7) < rows - rm) & ((zy * 8 + (r >> 3)) * rows + rm + (r & 7) < VOCAB_REAL)
                v_few = jnp.where(ok, v_few, -jnp.inf)
                few[:, lanes] = v_few
                add_target(v_few, jnp.int32(dm.main), lanes)
                v.append(v_few)
            v = jnp.concatenate(v, axis=0)
            for cp in out(t):
                cp.start()
            add_stats(v, lanes)

        for t in range(deep):
            out_wait(t + tok // nt - deep)

    def both(xx):
        block(0, ha, xx, load(0, ha, xx))

    def turn(xx):
        for half in TWO:
            base = pl.multiple_of((xx[half] * 2 + half) * rm, rm)

            @pl.loop(0, dim // LANES)
            def _(d, half=half, base=base):
                at = pl.ds(pl.multiple_of(d * LANES, LANES), LANES)
                etv[at, pl.ds(base, rm)] = dz[half * rm : (half + 1) * rm, at].T

    with scope("own"):
        s_o.wait_recv()
        both((x, x))
        turn((x, x))

    with scope("wait_1"):
        r_a.wait_recv()
        last_n = dm.cuts[-1][1]
        spans = [(pl.ds(r0, n), pl.ds(ha + r0, n + 8 * (r0 + n == ha))) for r0, n in dm.cuts]

        def far_pieces(xx, half, to):
            cps = [piece(slot(xx), pair[half], to) for pair in spans[:-1]]
            cps.append(remote(eg.at[slot(xx), spans[-1][half]], sst.at[c, pl.ds(half * last_n, last_n)], to))
            return cps

        r_f = far_pieces(x_m, 0, xp)
        d = [piece(slot(x_m), half_a, sib)]
        l_b.wait_recv()
        l_f = far_pieces(x_p, 1, xm)
        d.append(piece(slot(x_p), half_b, sib))
        for cp in d:
            cp.wait_recv()

    with scope("near_1"):
        both((x_m, x_p))
        turn((x_m, x_p))

    with scope("wait_2"):
        r_b.wait_recv()
        d = [piece(slot(x_m), half_b, sib)]
        l_a.wait_recv()
        d.append(piece(slot(x_p), half_a, sib))
        for cp in d:
            cp.wait_recv()

    with scope("near_2"):
        both((x_p, x_m))
        turn((x_p, x_m))

    far = (x_far, x_far)

    with scope("wait_3"):
        d = []
        for cp, r in zip((r_f[0], l_f[0]), spans[0]):
            cp.wait_recv()
            d.append(piece(slot(x_far), r, sib))
        load_narrow(*dm.cuts[0], far, c)
        for cp in d:
            cp.wait_recv()
    with scope("far_a"):
        ext_loads = [local(eg.at[s, pl.ds(rm, 8)], few.at[pl.ds(s * 8, 8)], lsem.at[s]) for s in range(8)]
        load_narrow(*dm.cuts[0], far, 1 - c)
        for cp in ext_loads:
            cp.wait()
        dz[ext_at : ext_at + FEW, :] = few[...].astype(BF16)
        dz[ext_at + FEW : ext_at + LANES, :] = jnp.zeros((FEW, dim), BF16)
        block(*dm.cuts[0], far, with_few=True)
    with scope("wait_5"):
        r_f[-1].wait_recv()
        l_f[-1].wait_recv()
        both_last = sst.at[c, _top(2 * last_n)]
        over = _remote(both_last, both_last, send, recv, next(ids), sib)
        over.start()

        @pl.loop(0, dim // LANES)
        def _(i):
            at = pl.ds(pl.multiple_of(i * LANES, LANES), LANES)
            etv[at, dm.main : dm.wide] = dz[ext_at : ext_at + LANES, at].T

        def last_rows(half, j):
            return sst.at[j, pl.ds(half * last_n, last_n)]

        narrow_all(0, last_n, last_rows, (c,))
        over.wait_recv()

    with scope("far_c"):
        narrow_all(0, last_n, last_rows, (1 - c,))
        block(0, last_n, far)
        over.wait_send()
        for s in TWO:
            pl.semaphore_signal(free.at[s], inc=1, device_id=(sib,), device_id_type=MESH)

    with scope("turn_far"):
        lse_row[:, :] = m_row[:, :] + jnp.log(s_row[:, :]) * LOG2E
        stats = exchange(lse_row, got, near)
        turn(far)

    wide = 2 * rm

    at_dht = SLOTS - 4

    def chunk_of(zz, yy):
        return _mod4(zz) * 4 + _rem(yy + 8, 4)

    def all_far(i):
        return x_far * wide + i // 16 * rm, _rem(i, 16)

    def in_order(i):
        n = i // 3
        m = n - 7
        k = _pick(n < 7, chunk_of(z + n - 1, y + 2), chunk_of(z + 3 + m // 3, y + 3 + _rem(m + 9, 3)))
        return _mod4(x + 3 + _rem(i, 3)) * wide, _pick(n < 4, chunk_of(z + 2, n), k)

    def later(i):
        return in_order(i + SLOTS)

    def zload(where, i, ring, n):
        at, k = where(i)
        s = _rem(i, ring)
        src = zh.at[k, pl.ds(pl.multiple_of(at, rm), n)]
        return pltpu.make_async_copy(src, tst.at[s, _top(n)], tsem.at[s])

    def zahead(where, ring, n):
        for i in range(ring):
            zload(where, i, ring, n).start()

    with scope("stats"):
        zahead(all_far, SLOTS, rm)
        for cp in stats:
            cp.wait()
        top = lse_row[:, :]
        for k in range(len(near)):
            top = jnp.maximum(top, got[k])
        s = jnp.exp2(lse_row[:, :] - top)
        for k in range(len(near)):
            s = s + jnp.exp2(got[k] - top)
        lse_row[:, :] = top + jnp.log(s) * LOG2E

    def dz_part(v, place, at, lanes):
        r = lax.broadcasted_iota(jnp.int32, v.shape, 0).astype(F32)
        hit = r == pos_row[:, lanes] - place.astype(F32)
        p = jnp.exp2(v - lse_row[:, lanes])
        dz[at, lanes] = (jnp.where(hit, p - 1.0, p) * w_row[:, lanes]).astype(BF16)

    step = min(LANES, rm)

    def dz_rows(where, start, stop, last_tile, ring, n):
        @pl.loop(start, stop)
        def _(i):
            @pl.when((i > 0) & (i + ring - 1 < last_tile))
            def _():
                zload(where, i + ring - 1, ring, n).start()

            zload(where, i, ring, n).wait()
            row, k = where(i)
            lanes = pl.ds(pl.multiple_of(k * chunk, chunk), chunk)

            @pl.loop(0, n // step)
            def _(j):
                at = pl.multiple_of(row + j * step, step)
                r = pl.ds(pl.multiple_of(j * step, step), step)
                dz_part(tst[lax.rem(i, ring), r, :], at, pl.ds(at, step), lanes)

    def dz_far(start, stop):
        dz_rows(all_far, start, stop, 32, SLOTS, rm)

    with scope("dz_far"):
        dz_far(0, 16)

    nd = dim // 2
    few_rows = pl.ds(dm.main, FEW)
    pair_ids = [(next(ids), next(ids)) for _ in TWO]

    def over_d2d(s, n, i):
        lanes = pl.ds(pl.multiple_of(i * nd, nd), nd)
        there = sst.at[s, _top(n), lanes]
        return _remote(od.at[s, 1 - c, _top(n), lanes], there, send, recv, pair_ids[s][0] + i, sib)

    def de_block(xx, half, s, with_few=False):
        at = pl.ds(pl.multiple_of((xx * 2 + half) * rm, rm), rm)
        n = ha + 8 * half
        pl.semaphore_wait(free.at[s], 1)

        @pl.loop(0, 2)
        def _(i):
            lanes = pl.ds(pl.multiple_of(i * nd, nd), nd)
            lhs = jnp.concatenate([dz[at, :], dz[few_rows, :]], axis=0) if with_few else dz[at, :]
            v = jnp.dot(lhs, hv[:, lanes], preferred_element_type=F32)
            if with_few:
                few[:, lanes] = v[rm:]
            for j in TWO:
                od[s, j, 0:ha, lanes] = v[j * ha : (j + 1) * ha]
                if half:
                    od[s, j, ha:n, lanes] = few[pl.ds(pl.multiple_of((xx * 2 + j) * 8, 8), 8), lanes]
            over_d2d(s, n, i).start()

        return half, s, n

    def stored(blk, to):
        half, s, n = blk
        return pltpu.make_async_copy(od.at[s, c, _top(n)], to.at[pl.ds(half * ha, n)], dsem.at[s])

    def early(blk, src):
        half, s, n = blk
        for i in TWO:
            over_d2d(s, n, i).wait_send()
        return local(src.at[pl.ds(half * ha, n)], od.at[s, 1 - c, _top(n)], lsem.at[s])

    def sum_add(blk, to, more=None):
        half, s, n = blk
        for i in TWO:
            over_d2d(s, n, i).wait_recv()
        if more is not None:
            more.wait()

        def add(r):
            v = od[s, c, r, :] + sst[s, r, :]
            od[s, c, r, :] = v if more is None else v + od[s, 1 - c, r, :]

        _loop_rows(n, 8, add)
        if more is None:
            pl.semaphore_signal(free.at[s], inc=1, device_id=(sib,), device_id_type=MESH)
            for i in TWO:
                over_d2d(s, n, i).wait_send()
        cp = stored(blk, to)
        cp.start()
        return cp

    def ring_sum(xx, rows_, n, src, s, dst, dev):
        lds = [
            local(q_h.at[xx, rows_], od.at[s, 0, _top(n)], lsem.at[0]),
            local(src, od.at[s, 1, _top(n)], lsem.at[1]),
        ]
        for cp in lds:
            cp.wait()
        _add_rows(od.at[s, 0, _top(n)], [od.at[s, 1, _top(n)]], 8)
        local(od.at[s, 0, _top(n)], q_h.at[xx, rows_], lsem.at[0]).wait()
        return remote(q_h.at[xx, rows_], dst, dev)

    stores = []

    def flush():
        while stores:
            stores.pop().wait()

    def tiles(q, where, between=None):
        flush()

        def outs(i):
            p, ab = where(i)
            r = pl.ds(q * h, h)
            dsts = [dhp.at[ab * 2 + j, p, r] if q == 0 else dhp.at[p, ab * 2 + j, r] for j in TWO]
            return [
                pltpu.make_async_copy(tst.at[at_dht + i * 2 + j, _top(h)], dst, hsem.at[i * 2 + j])
                for j, dst in enumerate(dsts)
            ]

        @pl.loop(0, 2)
        def _(i):
            if between is not None:
                pl.when(i > 0)(between)
            p, ab = where(i)
            ks = [(ab * 2 + j) * 4 + p if q == 0 else p * 4 + ab * 2 + j for j in TWO]
            rhs = jnp.concatenate([dz[:, pl.ds(pl.multiple_of(k * chunk, chunk), chunk)] for k in ks], axis=1)
            v = jnp.dot(etv[q * h : (q + 1) * h, :], rhs, preferred_element_type=F32)
            for j in TWO:
                tst[at_dht + i * 2 + j, 0:h, :] = v[:, j * chunk : (j + 1) * chunk]
            for cp in outs(i):
                cp.start()

        for i in TWO:
            stores.extend(outs(i))

    def part(q, p, lo, n):
        r = pl.ds(q * h, h)
        if q == 0:
            return dhp.at[pl.ds(lo, n), p, r]
        return dhp.at[p, pl.ds(lo, n), r]

    def one(q, p, i):
        r = pl.ds(q * h, h)
        return dhp.at[i, p, r] if q == 0 else dhp.at[p, i, r]

    ring1, ring2 = ((yp, ym), (zp, zm)), ((zp, zm), (yp, ym))
    pos1, pos2 = (y, z), (z, y)
    first, second = ({}, {}), ({}, {})

    def send_far(q):
        flush()
        p, (rt, lt) = pos1[q], ring1[q]
        first[q]["far_r"] = remote(part(q, _mod4(p + 2), 0, 2), ya.at[q], rt)
        first[q]["far_l"] = remote(part(q, _mod4(p + 2), 2, 2), yb.at[q], lt)

    def send_near(q):
        flush()
        p, (rt, lt) = pos1[q], ring1[q]
        first[q]["near_r"] = remote(part(q, _mod4(p + 1), 2, 2), yl.at[q, pl.ds(2, 2)], rt)
        first[q]["near_l"] = remote(part(q, _mod4(p - 1), 0, 2), yr.at[q, _top(2)], lt)

    def fetch(i, src):
        return local(src, tst.at[i, _top(h)], tsem.at[i])

    def pass_on(q):
        flush()
        p, (rt, lt) = pos1[q], ring1[q]
        lds = [fetch(i, one(q, _mod4(p + 1), i)) for i in TWO]
        lds += [fetch(2 + i, one(q, _mod4(p - 1), 2 + i)) for i in TWO]
        first[q]["far_r"].wait_recv()
        for i in TWO:
            lds[i].wait()
            _add_rows(ya.at[q, i], [tst.at[i, _top(h)]], min(FEW, h))
        first[q]["sum_r"] = remote(ya.at[q], yl.at[q, _top(2)], rt)
        first[q]["far_l"].wait_recv()
        for i in TWO:
            lds[2 + i].wait()
            _add_rows(yb.at[q, i], [tst.at[2 + i, _top(h)]], min(FEW, h))
        first[q]["sum_l"] = remote(yb.at[q], yr.at[q, pl.ds(2, 2)], lt)

    lo, hi = _top(hc), pl.ds(hc, hc)

    def second_phase(q):
        flush()
        r, (rt, lt) = pos2[q], ring2[q]
        r2, r1, rm1 = _mod4(r + 2), _mod4(r + 1), _mod4(r - 1)
        order = (r2, r1, rm1, r)
        lds = [fetch(i, one(q, pos1[q], k)) for i, k in enumerate(order)]
        for k in NEAR_KEYS:
            first[q][k].wait_recv()
        lds2 = [fetch(4 + i, yr.at[q, k]) for i, k in enumerate(order)]
        for i, k in enumerate(order):
            lds[i].wait()
            lds2[i].wait()
            _add_rows(yl.at[q, k], [tst.at[i, _top(h)], tst.at[4 + i, _top(h)]], min(FEW, h))
            if i == 0:
                second[q]["far_r"] = remote(yl.at[q, r2, lo], za.at[q], rt)
                second[q]["far_l"] = remote(yl.at[q, r2, hi], zb.at[q], lt)
            if i == 1:
                second[q]["near_r"] = remote(yl.at[q, r1, hi], zl.at[q, hi], rt)
            if i == 2:
                second[q]["near_l"] = remote(yl.at[q, rm1, lo], zr.at[q, lo], lt)

    def second_pass(q):
        r, (rt, lt) = pos2[q], ring2[q]
        r1, rm1 = _mod4(r + 1), _mod4(r - 1)
        second[q]["far_r"].wait_recv()
        _add_rows(yl.at[q, r1, lo], [za.at[q]], min(FEW, hc))
        second[q]["sum_r"] = remote(yl.at[q, r1, lo], zl.at[q, lo], rt)
        second[q]["far_l"].wait_recv()
        _add_rows(yl.at[q, rm1, hi], [zb.at[q]], min(FEW, hc))
        second[q]["sum_l"] = remote(yl.at[q, rm1, hi], zr.at[q, hi], lt)

    def last(q):
        r = pos2[q]
        for k in NEAR_KEYS:
            second[q][k].wait_recv()
        n = min(LANES, h)

        @pl.loop(0, h // n)
        def _(i):
            at = pl.ds(pl.multiple_of(i * n, n), n)
            v = yl[q, r, at, :] + zl[q, at, :] + zr[q, at, :]
            od[0, 0, 0:chunk, pl.ds(pl.multiple_of(q * h + i * n, n), n)] = (v * (1.0 / LOGIT_SCALE)).T

    def tiles_far(q, between=None):
        tiles(q, lambda i: (_mod4(pos1[q] + 2), i), between)

    def tiles_near(q):
        tiles(q, lambda i: (_mod4(pos1[q] + 1 + 2 * i), 1 - i))

    def tiles_pass(q):
        tiles(q, lambda i: (_mod4(pos1[q] + 1 + 2 * i), i))

    def tiles_own(q):
        tiles(q, lambda i: (pos1[q], i))

    all_later = 48 - SLOTS

    def dz_first(start, stop):
        dz_rows(in_order, start, stop, SLOTS, SLOTS, wide)

    def dz_later(start, stop):
        dz_rows(later, start, stop, all_later, at_dht, wide)

    with scope("de_far"):
        b0 = de_block(x_far, 0, 0)
        dz_far(16, 32)
        zahead(in_order, SLOTS, wide)
        for l in range(0, tok, nt):
            lanes = pl.ds(l, nt)
            dz_part(few[:, lanes], jnp.int32(dm.main), few_rows, lanes)
        dz[dm.main + FEW : dm.wide, :] = jnp.zeros((FEW, tok), BF16)
        b1 = de_block(x_far, 1, 1, True)
    with scope("dz_1"):
        c0 = sum_add(b0, q_h.at[x_far])
        dz_first(0, 8)
        c0.wait()
        e0 = remote(q_h.at[x_far, half_a], xa, xp)
        dz_first(8, SLOTS)
        zahead(later, at_dht, wide)
    with scope("dh_far1"):
        def between():
            sum_add(b1, q_h.at[x_far])

        tiles_far(1, between)
        c1 = stored(b1, q_h.at[x_far])
        c1.wait()
        e1 = remote(q_h.at[x_far, half_b], xb, xm)
    with scope("dz_2"):
        dz_later(0, 9)
        send_far(1)
    with scope("dh_far0"):
        tiles_far(0)
    with scope("dz_3"):
        dz_later(9, 13)
        send_far(0)
        dz_later(13, all_later)
    with scope("de_2"):
        b2 = de_block(x_p, 1, 0)
        b3 = de_block(x_m, 0, 1)
        c2 = sum_add(b2, q_h.at[x_p])
    with scope("dh_near"):
        tiles_near(1)
        c2.wait()
        e2 = remote(q_h.at[x_p, half_b], xe.at[half_b], xp)
        c3 = sum_add(b3, q_h.at[x_m])
        send_near(1)
        tiles_near(0)
        c3.wait()
        e3 = remote(q_h.at[x_m, half_a], xe.at[half_a], xm)
        send_near(0)
    with scope("dh_pass"):
        tiles_pass(1)
        tiles_pass(0)
        pass_on(1)
    with scope("de_4"):
        b4 = de_block(x_p, 0, 0)
        pass_on(0)
        b5 = de_block(x_m, 1, 1)
        c4 = sum_add(b4, q_h.at[x_p])
    with scope("dh_own"):
        tiles_own(1)
        c5 = sum_add(b5, q_h.at[x_m])
        tiles_own(0)
        c4.wait()
        c5.wait()
    old = list(sent)
    sent.clear()
    with scope("ring"):
        e0.wait_recv()
        e4 = ring_sum(x_p, half_a, ha, xa, 0, xs.at[half_a], xp)
        e1.wait_recv()
        e5 = ring_sum(x_m, half_b, ha + 8, xb, 1, xs.at[half_b], xm)
    with scope("de_6"):
        b6 = de_block(x, 0, 0)
    with scope("de_7"):
        b7 = de_block(x, 1, 1)
        xo_load = local(x4.at[zy, xc], dz.at[_top(chunk)], osem.at[0])
    with scope("second_1"):
        second_phase(1)
    with scope("second_0"):
        second_phase(0)
    with scope("spass_1"):
        second_pass(1)
    with scope("sum_6"):
        e3.wait_recv()
        c6 = early(b6, xe)
        e2.wait_recv()
        c7 = early(b7, xe)
        c6 = sum_add(b6, q_o, c6)
        c7 = sum_add(b7, q_o, c7)
    with scope("spass_0"):
        second_pass(0)
        c6.wait()
        c7.wait()
    def drain(cps):
        while cps:
            cps.pop().wait_send()

    def own_x(r):
        v = dz[r, :].astype(F32)
        inv = lax.rsqrt(jnp.mean(v * v, axis=-1, keepdims=True) + NORM_EPS)
        od[1, 0, r, :] = v * inv
        od[1, 1, r, 0:LANES] = jnp.broadcast_to(inv, (r.size, LANES))

    def own_dg(q):
        lanes = pl.ds(q * h, h)

        def add(i, acc):
            r = pl.ds(pl.multiple_of(i * 8, 8), 8)
            return acc + od[0, 0, r, lanes] * od[1, 0, r, lanes]

        acc = lax.fori_loop(0, chunk // 8, add, jnp.zeros((8, h), F32))
        sm[:, lanes] = jnp.sum(acc, axis=0, keepdims=True)

    def own_dx(r):
        x_hat, u = od[1, 0, r, :], od[0, 0, r, :] * gain
        od[0, 1, r, :] = od[1, 1, r, 0:1] * (u - x_hat * jnp.mean(u * x_hat, axis=-1, keepdims=True))

    with scope("own_x"):
        xo_load.wait()
        _loop_rows(chunk, 16, own_x)
        lse = jnp.where(zy == 0, lse_row[:, :], 0.0)
        loss = jnp.sum(w_row[:, :] * (lse - tgt_row[:, :]))
        sm[:, dim : dim + LANES] = jnp.full((1, LANES), loss / LOG2E)
        drain(old)
    with scope("last_1"):
        last(1)
        own_dg(1)
    with scope("last_0"):
        last(0)
        own_dg(0)

    with scope("small_1"):
        old = [cp for cp in sent if cp is not e4 and cp is not e5]
        near_sums = exchange(sm, got1, near)
        _loop_rows(chunk, 16, own_dx)
        dx_copy = local(od.at[0, 1, _top(chunk)], dx_out, osem.at[0])
        drain(old)
        for cp in near_sums:
            cp.wait()
    with scope("small_2"):
        tot = sm[...]
        for k in range(len(near)):
            tot = tot + got1[k]
        total_v[...] = tot
        all_sums = exchange(total_v, got2, line)
        mine = local(total_v, got2.at[len(line)], osem.at[1])
    with scope("ring_end"):
        for cp in (e4, e5):
            cp.wait()
        dx_copy.wait()
        mine.wait()
    with scope("small_3"):
        for cp in all_sums:
            cp.wait()


def _run(dm, x4, table, gain, labels, mask):
    hbm, vm = pl.BlockSpec(memory_space=HBM), pl.BlockSpec(memory_space=VMEM)
    sd = jax.ShapeDtypeStruct
    d, tok, h, ck, pad, ha = dm.dim, dm.tok, dm.h, dm.chunk, dm.pad, dm.ha
    line, quad, pair = VMEM((1, tok), F32), VMEM((2, 2, h, ck), F32), VMEM((2, h, ck), F32)
    part, shard = VMEM((2, h // 2, ck), F32), sd((pad, d), F32)
    out = pl.pallas_call(
        functools.partial(_kernel, dm),
        name="head",
        out_shape=(
            sd((ck, d), F32), sd((8, 1, d + LANES), F32),
            shard, shard, shard,
            sd((8, pad, d), F32), sd((16, dm.main, ck), F32),
            sd((4, pad, d), F32), sd((ha, d), F32), sd((ha + 8, d), F32),
            sd((4, 4, d, ck), F32), sd((2, 4, h, ck), F32),
        ),
        in_specs=[hbm, vm, vm, vm, vm],
        out_specs=[hbm] * 12,
        scratch_shapes=[
            VMEM((tok, d), BF16), VMEM((d, dm.wide), BF16), VMEM((dm.wide, tok), BF16),
            VMEM((2, 2, ha + 8, d), F32), VMEM((2, ha + 8, d), F32), VMEM((FEW, d), F32), VMEM((8, d), F32),
            quad, quad, VMEM((2, 4, h, ck), F32),
            part, part, pair, pair,
            VMEM((SLOTS, max(h, 2 * dm.rm), ck), F32),
            line, line, line, line, line, line, VMEM((15, 1, tok), F32),
            VMEM((1, d + LANES), F32), VMEM((15, 1, d + LANES), F32), VMEM((1, d + LANES), F32),
            DMA((53,)), DMA((53,)), pltpu.SemaphoreType.REGULAR((2,)),
            DMA((SLOTS,)), DMA((4,)), DMA((2,)), DMA((2,)), DMA((8,)),
        ],
        compiler_params=pltpu.CompilerParams(
            collective_id=0, has_side_effects=True, vmem_limit_bytes=67043328
        ),
    )(x4, table, gain, labels, mask)
    return _write_out(dm, out[2:4], *out[:2])


def _write_kernel(own, ring, dx, small, de_o, dx_o, dg_o, loss_o):
    de_o[:, :] = (own[:, :] + ring[:, :]) * (1.0 / LOGIT_SCALE)
    dx_o[:, :] = dx[:, :]
    total = jnp.sum(small[:, :, :], axis=0)
    d = dg_o.shape[1]
    dg_o[:, :] = total[:, :d]
    loss_o[:, :] = total[:, d : d + 1]


def _write_out(dm, parts, dx, small):
    d, step, blocks = dm.dim, dm.ha + 8, 2
    sd = jax.ShapeDtypeStruct
    some = pl.BlockSpec((step, d), lambda i: (i, 0))
    half = pl.BlockSpec((dm.chunk // blocks, d), lambda i: (i, 0))
    row, one = pl.BlockSpec((1, d), lambda i: (0, 0)), pl.BlockSpec((1, 1), lambda i: (0, 0))
    rows = pl.BlockSpec(small.shape, lambda i: (0, 0, 0))
    return pl.pallas_call(
        _write_kernel,
        name="write_out",
        grid=(blocks,),
        out_shape=(sd((dm.rows, d), F32), sd((dm.chunk, d), F32), sd((1, d), F32), sd((1, 1), F32)),
        in_specs=[some, some, half, rows],
        out_specs=(some, half, row, one),
    )(*parts, dx, small)


def solution(mesh):
    group = mesh.shape[AXIS]

    def local_step(residual, labels, loss_mask, norm_gain, table_shard):
        tokens, dim = residual.shape
        rows = table_shard.shape[0]
        dm = Dims(tokens, dim, rows, group)
        x4 = residual.reshape(16, 8, dm.chunk, dim)
        lab = labels.reshape(16, 8, 1, dm.chunk)
        msk = loss_mask.reshape(16, 8, 1, dm.chunk)
        d_embed, d_res, d_gain, loss = _run(dm, x4, table_shard, norm_gain[None, :], lab, msk)
        return loss.reshape(()), d_res, d_embed, d_gain.reshape(dim)

    return jax.shard_map(
        local_step,
        mesh=mesh,
        in_specs=(P(), P(), P(), P(), P(AXIS, None)),
        out_specs=(P(), P(AXIS, None), P(AXIS, None), P()),
        check_vma=False,
    )
```

```python
import functools
import itertools
import math

import jax
import jax.numpy as jnp
from jax import lax
from jax.experimental import pallas as pl
from jax.experimental.pallas import tpu as pltpu
from jax.sharding import PartitionSpec as P

VOCAB_REAL = 49155
LOGIT_SCALE = 6.0
NORM_EPS = 1e-6

AXIS = "vp"
MESH = pl.DeviceIdType.MESH
F32 = jnp.float32
BF16 = jnp.bfloat16
HBM = pltpu.HBM
VMEM = pltpu.VMEM
DMA = pltpu.SemaphoreType.DMA


def _coords():
    me = lax.axis_index(AXIS)
    return me // 32, (me // 8) % 4, (me // 2) % 4, me % 2


def _dev(z, y, x, c):
    return ((z * 4 + y) * 4 + x) * 2 + c


def _mod4(v):
    return lax.rem(v + 8, 4)


def _barrier(peers):
    sem = pltpu.get_barrier_semaphore()
    for p in peers:
        pl.semaphore_signal(sem, inc=1, device_id=(p,), device_id_type=MESH)
    pl.semaphore_wait(sem, len(peers))


def _remote(src, dst, send, recv, k, dev):
    return pltpu.make_async_remote_copy(
        src_ref=src,
        dst_ref=dst,
        send_sem=send.at[k],
        recv_sem=recv.at[k],
        device_id=(dev,),
        device_id_type=MESH,
    )


LANES = 128


class Dims:
    def __init__(self, tokens, dim, rows, group):
        self.dim, self.rows = dim, rows
        unit = LANES if rows >= LANES else 64
        self.rm = rows // unit * unit
        self.ha = self.rm // 2
        low = max(16, self.ha // 48 * 16)
        self.cuts = ((low, self.ha - low), (0, low))
        self.pad = self.rm + 8
        self.chunk = tokens // group
        self.tok = 16 * self.chunk
        self.nt = 4 * self.chunk
        self.main = 8 * self.rm
        self.wide = self.main + LANES
        self.h = dim // 2


def _top(n):
    return pl.ds(0, n)


def _rem(a, b):
    return a % b if isinstance(a, int) else lax.rem(a, b)


def _pick(test, a, b):
    return (a if test else b) if isinstance(test, bool) else jnp.where(test, a, b)


def _loop_rows(rows, step, fn):
    @pl.loop(0, rows // step)
    def _(i):
        fn(pl.ds(pl.multiple_of(i * step, step), step))


def _add_rows(dst, srcs, step):
    def add(r):
        acc = dst[r, :]
        for s in srcs:
            acc = acc + s[r, :]
        dst[r, :] = acc

    _loop_rows(dst.shape[0], step, add)


SLOTS = 12
FEW = 64
TWO = range(2)
LOG2E = math.log2(math.e)
NEAR_KEYS = ("near_r", "near_l", "sum_r", "sum_l")
scope = jax.named_scope


def _kernel(
    dm, x4, e_ref, g_ref, lab, msk,
    dx_out, got2, q_o, xs, xe, eg, zh, q_h, xa, xb, dhp, yr,
    hv, etv, dz, od, sst, few, oext, ya, yb, yl, za, zb, zl, zr, tst,
    m_row, s_row, w_row, pos_row, lse_row, tgt_row, got, sm, got1, total_v,
    send, recv,
    free, tsem, hsem, dsem, osem, lsem,
):
    z, y, x, c = _coords()
    xc, zy = x * 2 + c, z * 4 + y
    rows, rm, ha, dim, h = dm.rows, dm.rm, dm.ha, dm.dim, dm.h
    chunk, tok, nt, hc = dm.chunk, dm.tok, dm.nt, dm.h // 2
    x_far, x_p, x_m = _mod4(x + 2), _mod4(x + 1), _mod4(x - 1)
    xp, xm = _dev(z, y, x_p, c), _dev(z, y, x_m, c)
    yp, ym = _dev(z, _mod4(y + 1), x, c), _dev(z, _mod4(y - 1), x, c)
    zp, zm = _dev(_mod4(z + 1), y, x, c), _dev(_mod4(z - 1), y, x, c)
    sib = _dev(z, y, x, 1 - c)
    near = [_dev(_mod4(z + a), _mod4(y + b), x, c) for a in range(4) for b in range(4) if a or b]
    line = [_dev(z, y, _mod4(x + a), lax.rem(c + b, 2)) for a in range(4) for b in TWO if a or b]
    bar = pltpu.get_barrier_semaphore()
    for p in (*near, *line):
        pl.semaphore_signal(bar, inc=1, device_id=(p,), device_id_type=MESH)
    sent = []
    ids = itertools.count()

    def remote(src, dst, dev):
        cp = _remote(src, dst, send, recv, next(ids), dev)
        cp.start()
        sent.append(cp)
        return cp

    def exchange(src, dst, devs):
        k = next(ids)
        for i, dev in enumerate(devs):
            _remote(src, dst.at[i], send, recv, k, dev).start()
        whole = dst.at[_top(len(devs))]
        return pltpu.make_async_copy(whole, whole, recv.at[k]), pltpu.make_async_copy(whole, whole, send.at[k])

    def local(src, dst, sem):
        cp = pltpu.make_async_copy(src, dst, sem)
        cp.start()
        return cp

    x_at, ext_at = 2 * rm, 4 * rm

    def xload(k):
        s = lax.rem(k, 4)
        to = dz.at[pl.ds(pl.multiple_of(x_at + s * chunk, chunk), chunk)]
        return pltpu.make_async_copy(x4.at[k, xc], to, tsem.at[s])

    with scope("prep"):
        for k in range(3):
            xload(k).start()
        own = xc
        cps = []
        for j in TWO:
            def widen(r, j=j):
                od[0, j, r, :] = e_ref[pl.ds(j * ha + r.start, r.size), :].astype(F32)

            _loop_rows(ha, 16, widen)
            cps.append(local(od.at[0, j, _top(ha)], eg.at[own, pl.ds(j * ha, ha)], hsem.at[j]))
        oext[...] = jnp.zeros_like(oext)
        oext[0 : rows - rm, :] = e_ref[rm:rows, :].astype(F32)
        cps.append(local(oext, eg.at[own, pl.ds(rm, 8)], hsem.at[2]))
        pl.semaphore_wait(bar, 22)

    half_a, half_b = _top(ha), pl.ds(ha, ha + 8)

    def piece(s, r, dev):
        return remote(eg.at[s, r], eg.at[s, r], dev)

    def slot(xx):
        return xx * 2 + c

    cps[0].wait()
    r_a = piece(own, half_a, xp)
    for cp in cps[1:]:
        cp.wait()
    l_b = piece(own, half_b, xm)
    s_o = piece(own, _top(dm.pad), sib)
    r_b, l_a = piece(own, half_b, xp), piece(own, half_a, xm)

    gain = g_ref[...]

    with scope("norm"):
        @pl.loop(0, 16)
        def _(k):
            @pl.when(k < 13)
            def _():
                xload(k + 3).start()

            xload(k).wait()

            def norm(r):
                v = dz[pl.ds(pl.multiple_of(x_at + lax.rem(k, 4) * chunk + r.start, r.size), r.size), :].astype(F32)
                inv = lax.rsqrt(jnp.mean(v * v, axis=-1, keepdims=True) + NORM_EPS)
                hv[pl.ds(pl.multiple_of(k * chunk + r.start, r.size), r.size), :] = (v * inv * gain).astype(BF16)

            _loop_rows(chunk, 16, norm)

    with scope("labels"):
        total = jnp.sum(msk[...])
        for k in range(16):
            at = pl.ds(k * chunk, chunk)
            w_row[:, at] = msk[k, xc] / total
            q = lab[k, xc] - zy * (8 * rows)
            s = jnp.zeros_like(q)
            for i in range(1, 8):
                s = s + jnp.where(q >= i * rows, 1, 0)
            r = q - s * rows
            up = jnp.where(r >= ha, 1, 0)
            at_main = ((s // 2 * 2 + up) * 2 + s % 2) * ha + r - up * ha
            at_ext = dm.main + s * 8 + r - rm
            place = jnp.where(r < rm, at_main, at_ext)
            pos_row[:, at] = jnp.where((q >= 0) & (q < 8 * rows), place, -1).astype(F32)

    def product(lhs, lanes):
        v = lax.dot_general(lhs, hv[lanes, :], (((1,), (1,)), ((), ())), preferred_element_type=F32)
        return v * (LOG2E / LOGIT_SCALE)

    def add_stats(v, lanes):
        m_old, s_old = m_row[:, lanes], s_row[:, lanes]
        m = jnp.maximum(m_old, jnp.max(v, axis=0, keepdims=True))
        s = jnp.sum(jnp.exp2(v - m), axis=0, keepdims=True)
        m_row[:, lanes] = m
        s_row[:, lanes] = s_old * jnp.exp2(m_old - m) + s

    def add_target(v, place, lanes):
        r = lax.broadcasted_iota(jnp.int32, v.shape, 0)
        hit = r.astype(F32) == pos_row[:, lanes] - place.astype(F32)
        tgt_row[:, lanes] += jnp.sum(jnp.where(hit, v, 0.0), axis=0, keepdims=True)

    m_row[:, :] = jnp.full((1, tok), -jnp.inf, F32)
    s_row[:, :] = jnp.zeros((1, tok), F32)
    tgt_row[:, :] = jnp.zeros((1, tok), F32)
    segs = [(half, j) for half in TWO for j in TWO]

    def load(r0, n, xx, cores=TWO):
        return [
            local(
                eg.at[xx[half] * 2 + j, pl.ds(half * ha + r0, n)],
                od.at[j, half, pl.ds(r0, n)],
                hsem.at[half * len(cores) + k],
            )
            for half in TWO
            for k, j in enumerate(cores)
        ]

    def narrow_all(r0, n, src, cores=TWO):
        for half in TWO:
            for j in cores:
                def narrow(r, half=half, j=j):
                    at = pl.multiple_of((half * 2 + j) * ha + r0 + r.start, r.size)
                    dz[pl.ds(at, r.size), :] = src(half, j)[r, :].astype(BF16)

                _loop_rows(n, 16, narrow)

    def load_narrow(r0, n, xx, core):
        for cp in load(r0, n, xx, (core,)):
            cp.wait()
        narrow_all(r0, n, lambda half, j: od.at[j, half, pl.ds(r0, n)], (core,))

    def block(r0, n, xx, loads=(), with_few=False, nt=nt):
        if loads:
            for cp in loads:
                cp.wait()
            narrow_all(r0, n, lambda half, j: od.at[j, half, pl.ds(r0, n)])
        left = [VOCAB_REAL - ((zy * 8 + xx[half] * 2 + j) * rows + half * ha + r0) for half, j in segs]
        w, tall = nt // chunk, len(segs) * n
        pack = tst.shape[1] // tall
        deep = SLOTS // w
        packed = SLOTS * pack >= tok // chunk

        def place(t, i):
            if packed:
                return t * (w // pack) + i // pack, i % pack * tall
            return lax.rem(t, deep) * w + i, 0

        def out(t):
            cps = []
            for i in range(w):
                u, row = place(t, i)
                for m, (half, j) in enumerate(segs):
                    to = pl.ds(pl.multiple_of((xx[half] * 2 + half) * rm + j * ha + r0, 8), n)
                    cps.append(pltpu.make_async_copy(tst.at[u, pl.ds(row + m * n, n)], zh.at[t * w + i, to], tsem.at[u]))
            return cps

        def out_wait(u, rows_):
            whole = tst.at[u, _top(rows_)]
            pltpu.make_async_copy(whole, whole, tsem.at[u]).wait()

        @pl.loop(0, tok // nt)
        def _(t):
            if not packed:
                @pl.when(t >= deep)
                def _():
                    for i in range(w):
                        out_wait(place(t, i)[0], tall)

            lanes = pl.ds(pl.multiple_of(t * nt, nt), nt)
            lhs = [dz[(half * 2 + j) * ha + r0 : (half * 2 + j) * ha + r0 + n, :] for half, j in segs]
            if with_few:
                lhs.append(dz[ext_at : ext_at + FEW, :])
            v = product(jnp.concatenate(lhs, axis=0), lanes)
            v, v_few = v[:tall], v[tall:]
            r = lax.broadcasted_iota(jnp.int32, (n, nt), 0)
            v = [jnp.where(r < left[m], v[m * n : (m + 1) * n], -jnp.inf) for m in range(len(segs))]
            for part_v, (half, j) in zip(v, segs):
                add_target(part_v, (xx[half] * 2 + half) * rm + j * ha + r0, lanes)
            for i in range(w):
                u, row = place(t, i)
                for m in range(len(segs)):
                    tst[u, row + m * n : row + (m + 1) * n, :] = v[m][:, i * chunk : (i + 1) * chunk]
            if with_few:
                r = lax.broadcasted_iota(jnp.int32, v_few.shape, 0)
                ok = ((r & 7) < rows - rm) & ((zy * 8 + (r >> 3)) * rows + rm + (r & 7) < VOCAB_REAL)
                v_few = jnp.where(ok, v_few, -jnp.inf)
                few[:, lanes] = v_few
                add_target(v_few, jnp.int32(dm.main), lanes)
                v.append(v_few)
            v = jnp.concatenate(v, axis=0)
            for cp in out(t):
                cp.start()
            add_stats(v, lanes)

        if packed:
            for u in range(tok // chunk // pack):
                out_wait(u, pack * tall)
        else:
            for u in range(deep * w):
                out_wait(u, tall)

    def both(xx):
        block(0, ha, xx, load(0, ha, xx))

    def turn(xx):
        for half in TWO:
            base = pl.multiple_of((xx[half] * 2 + half) * rm, rm)

            @pl.loop(0, dim // LANES)
            def _(d, half=half, base=base):
                at = pl.ds(pl.multiple_of(d * LANES, LANES), LANES)
                etv[at, pl.ds(base, rm)] = dz[half * rm : (half + 1) * rm, at].T

    with scope("own"):
        s_o.wait_recv()
        both((x, x))
        turn((x, x))

    with scope("wait_1"):
        r_a.wait_recv()
        last_n = dm.cuts[-1][1]
        spans = [(pl.ds(r0, n), pl.ds(ha + r0, n + 8 * (r0 + n == ha))) for r0, n in dm.cuts]

        def far_pieces(xx, half, to):
            cps = [piece(slot(xx), pair[half], to) for pair in spans[:-1]]
            cps.append(remote(eg.at[slot(xx), spans[-1][half]], sst.at[c, pl.ds(half * last_n, last_n)], to))
            return cps

        r_f = far_pieces(x_m, 0, xp)
        d = [piece(slot(x_m), half_a, sib)]
        l_b.wait_recv()
        l_f = far_pieces(x_p, 1, xm)
        d.append(piece(slot(x_p), half_b, sib))
        for cp in d:
            cp.wait_recv()

    with scope("near_1"):
        both((x_m, x_p))
        turn((x_m, x_p))

    with scope("wait_2"):
        r_b.wait_recv()
        d = [piece(slot(x_m), half_b, sib)]
        l_a.wait_recv()
        d.append(piece(slot(x_p), half_a, sib))
        for cp in d:
            cp.wait_recv()

    with scope("near_2"):
        both((x_p, x_m))
        turn((x_p, x_m))

    far = (x_far, x_far)

    with scope("wait_3"):
        d = []
        for cp, r in zip((r_f[0], l_f[0]), spans[0]):
            cp.wait_recv()
            d.append(piece(slot(x_far), r, sib))
        load_narrow(*dm.cuts[0], far, c)
        for cp in d:
            cp.wait_recv()
    with scope("far_a"):
        ext_loads = [local(eg.at[s, pl.ds(rm, 8)], few.at[pl.ds(s * 8, 8)], lsem.at[s]) for s in range(8)]
        load_narrow(*dm.cuts[0], far, 1 - c)
        for cp in ext_loads:
            cp.wait()
        dz[ext_at : ext_at + FEW, :] = few[...].astype(BF16)
        dz[ext_at + FEW : ext_at + LANES, :] = jnp.zeros((FEW, dim), BF16)
        block(*dm.cuts[0], far, with_few=True)
    with scope("wait_5"):
        r_f[-1].wait_recv()
        l_f[-1].wait_recv()
        both_last = sst.at[c, _top(2 * last_n)]
        over = _remote(both_last, both_last, send, recv, next(ids), sib)
        over.start()

        @pl.loop(0, dim // LANES)
        def _(i):
            at = pl.ds(pl.multiple_of(i * LANES, LANES), LANES)
            etv[at, dm.main : dm.wide] = dz[ext_at : ext_at + LANES, at].T

        def last_rows(half, j):
            return sst.at[j, pl.ds(half * last_n, last_n)]

        narrow_all(0, last_n, last_rows, (c,))
        over.wait_recv()

    with scope("far_c"):
        narrow_all(0, last_n, last_rows, (1 - c,))
        block(0, last_n, far, nt=8 * chunk)
        over.wait_send()
        for s in TWO:
            pl.semaphore_signal(free.at[s], inc=1, device_id=(sib,), device_id_type=MESH)

    with scope("turn_far"):
        lse_row[:, :] = m_row[:, :] + jnp.log(s_row[:, :]) * LOG2E
        stats = exchange(lse_row, got, near)
        turn(far)

    wide = 2 * rm

    at_dht = SLOTS - 4

    def chunk_of(zz, yy):
        return _mod4(zz) * 4 + _rem(yy + 8, 4)

    def all_far(i):
        return x_far * wide + i // 16 * rm, _rem(i, 16)

    def in_order(i):
        n = i // 3
        m = n - 7
        k = _pick(n < 7, chunk_of(z + n - 1, y + 2), chunk_of(z + 3 + m // 3, y + 3 + _rem(m + 9, 3)))
        return _mod4(x + 3 + _rem(i, 3)) * wide, _pick(n < 4, chunk_of(z + 2, n), k)

    def later(i):
        return in_order(i + SLOTS)

    def zload(where, i, ring, n):
        at, k = where(i)
        s = _rem(i, ring)
        src = zh.at[k, pl.ds(pl.multiple_of(at, rm), n)]
        return pltpu.make_async_copy(src, tst.at[s, _top(n)], tsem.at[s])

    def zahead(where, ring, n):
        for i in range(ring):
            zload(where, i, ring, n).start()

    with scope("stats"):
        zahead(all_far, SLOTS, rm)
        for cp in stats:
            cp.wait()
        top = lse_row[:, :]
        for k in range(len(near)):
            top = jnp.maximum(top, got[k])
        s = jnp.exp2(lse_row[:, :] - top)
        for k in range(len(near)):
            s = s + jnp.exp2(got[k] - top)
        lse_row[:, :] = top + jnp.log(s) * LOG2E

    def dz_part(v, place, at, lanes):
        r = lax.broadcasted_iota(jnp.int32, v.shape, 0).astype(F32)
        hit = r == pos_row[:, lanes] - place.astype(F32)
        p = jnp.exp2(v - lse_row[:, lanes])
        dz[at, lanes] = (jnp.where(hit, p - 1.0, p) * w_row[:, lanes]).astype(BF16)

    step = min(LANES, rm)

    def dz_rows(where, start, stop, last_tile, ring, n):
        @pl.loop(start, stop)
        def _(i):
            @pl.when((i > 0) & (i + ring - 1 < last_tile))
            def _():
                zload(where, i + ring - 1, ring, n).start()

            zload(where, i, ring, n).wait()
            row, k = where(i)
            lanes = pl.ds(pl.multiple_of(k * chunk, chunk), chunk)

            @pl.loop(0, n // step)
            def _(j):
                at = pl.multiple_of(row + j * step, step)
                r = pl.ds(pl.multiple_of(j * step, step), step)
                dz_part(tst[lax.rem(i, ring), r, :], at, pl.ds(at, step), lanes)

    def dz_far(start, stop):
        dz_rows(all_far, start, stop, 32, SLOTS, rm)

    with scope("dz_far"):
        dz_far(0, 16)

    nd = dim // 2
    few_rows = pl.ds(dm.main, FEW)
    pair_ids = [(next(ids), next(ids)) for _ in TWO]

    def over_d2d(s, n, i):
        lanes = pl.ds(pl.multiple_of(i * nd, nd), nd)
        there = sst.at[s, _top(n), lanes]
        return _remote(od.at[s, 1 - c, _top(n), lanes], there, send, recv, pair_ids[s][0] + i, sib)

    def de_block(xx, half, s, with_few=False):
        at = pl.ds(pl.multiple_of((xx * 2 + half) * rm, rm), rm)
        n = ha + 8 * half
        pl.semaphore_wait(free.at[s], 1)

        @pl.loop(0, 2)
        def _(i):
            lanes = pl.ds(pl.multiple_of(i * nd, nd), nd)
            lhs = jnp.concatenate([dz[at, :], dz[few_rows, :]], axis=0) if with_few else dz[at, :]
            v = jnp.dot(lhs, hv[:, lanes], preferred_element_type=F32)
            if with_few:
                few[:, lanes] = v[rm:]
            for j in TWO:
                od[s, j, 0:ha, lanes] = v[j * ha : (j + 1) * ha]
                if half:
                    od[s, j, ha:n, lanes] = few[pl.ds(pl.multiple_of((xx * 2 + j) * 8, 8), 8), lanes]
            over_d2d(s, n, i).start()

        return half, s, n

    def stored(blk, to):
        half, s, n = blk
        return pltpu.make_async_copy(od.at[s, c, _top(n)], to.at[pl.ds(half * ha, n)], dsem.at[s])

    def early(blk, src):
        half, s, n = blk
        for i in TWO:
            over_d2d(s, n, i).wait_send()
        return local(src.at[pl.ds(half * ha, n)], od.at[s, 1 - c, _top(n)], lsem.at[s])

    def sum_add(blk, to, more=None):
        half, s, n = blk
        for i in TWO:
            over_d2d(s, n, i).wait_recv()
        if more is not None:
            more.wait()

        def add(r):
            v = od[s, c, r, :] + sst[s, r, :]
            od[s, c, r, :] = v if more is None else v + od[s, 1 - c, r, :]

        _loop_rows(n, 8, add)
        if more is None:
            pl.semaphore_signal(free.at[s], inc=1, device_id=(sib,), device_id_type=MESH)
            for i in TWO:
                over_d2d(s, n, i).wait_send()
        cp = stored(blk, to)
        cp.start()
        return cp

    def ring_sum(xx, rows_, n, src, s, dst, dev):
        lds = [
            local(q_h.at[xx, rows_], od.at[s, 0, _top(n)], lsem.at[0]),
            local(src, od.at[s, 1, _top(n)], lsem.at[1]),
        ]
        for cp in lds:
            cp.wait()
        _add_rows(od.at[s, 0, _top(n)], [od.at[s, 1, _top(n)]], 8)
        local(od.at[s, 0, _top(n)], q_h.at[xx, rows_], lsem.at[0]).wait()
        return remote(q_h.at[xx, rows_], dst, dev)

    stores = []

    def flush():
        while stores:
            stores.pop().wait()

    def tiles(q, where, between=None):
        flush()

        def outs(i):
            p, ab = where(i)
            r = pl.ds(q * h, h)
            dsts = [dhp.at[ab * 2 + j, p, r] if q == 0 else dhp.at[p, ab * 2 + j, r] for j in TWO]
            return [
                pltpu.make_async_copy(tst.at[at_dht + i * 2 + j, _top(h)], dst, hsem.at[i * 2 + j])
                for j, dst in enumerate(dsts)
            ]

        @pl.loop(0, 2)
        def _(i):
            if between is not None:
                pl.when(i > 0)(between)
            p, ab = where(i)
            ks = [(ab * 2 + j) * 4 + p if q == 0 else p * 4 + ab * 2 + j for j in TWO]
            rhs = jnp.concatenate([dz[:, pl.ds(pl.multiple_of(k * chunk, chunk), chunk)] for k in ks], axis=1)
            v = jnp.dot(etv[q * h : (q + 1) * h, :], rhs, preferred_element_type=F32)
            for j in TWO:
                tst[at_dht + i * 2 + j, 0:h, :] = v[:, j * chunk : (j + 1) * chunk]
            for cp in outs(i):
                cp.start()

        for i in TWO:
            stores.extend(outs(i))

    def part(q, p, lo, n):
        r = pl.ds(q * h, h)
        if q == 0:
            return dhp.at[pl.ds(lo, n), p, r]
        return dhp.at[p, pl.ds(lo, n), r]

    def one(q, p, i):
        r = pl.ds(q * h, h)
        return dhp.at[i, p, r] if q == 0 else dhp.at[p, i, r]

    ring1, ring2 = ((yp, ym), (zp, zm)), ((zp, zm), (yp, ym))
    pos1, pos2 = (y, z), (z, y)
    first, second = ({}, {}), ({}, {})

    def send_far(q):
        flush()
        p, (rt, lt) = pos1[q], ring1[q]
        first[q]["far_r"] = remote(part(q, _mod4(p + 2), 0, 2), ya.at[q], rt)
        first[q]["far_l"] = remote(part(q, _mod4(p + 2), 2, 2), yb.at[q], lt)

    def send_near(q):
        flush()
        p, (rt, lt) = pos1[q], ring1[q]
        first[q]["near_r"] = remote(part(q, _mod4(p + 1), 2, 2), yl.at[q, pl.ds(2, 2)], rt)
        first[q]["near_l"] = remote(part(q, _mod4(p - 1), 0, 2), yr.at[q, _top(2)], lt)

    def fetch(i, src):
        return local(src, tst.at[i, _top(h)], tsem.at[i])

    def pass_on(q):
        flush()
        p, (rt, lt) = pos1[q], ring1[q]
        lds = [fetch(i, one(q, _mod4(p + 1), i)) for i in TWO]
        lds += [fetch(2 + i, one(q, _mod4(p - 1), 2 + i)) for i in TWO]
        first[q]["far_r"].wait_recv()
        for i in TWO:
            lds[i].wait()
            _add_rows(ya.at[q, i], [tst.at[i, _top(h)]], min(FEW, h))
        first[q]["sum_r"] = remote(ya.at[q], yl.at[q, _top(2)], rt)
        first[q]["far_l"].wait_recv()
        for i in TWO:
            lds[2 + i].wait()
            _add_rows(yb.at[q, i], [tst.at[2 + i, _top(h)]], min(FEW, h))
        first[q]["sum_l"] = remote(yb.at[q], yr.at[q, pl.ds(2, 2)], lt)

    lo, hi = _top(hc), pl.ds(hc, hc)

    def second_phase(q):
        flush()
        r, (rt, lt) = pos2[q], ring2[q]
        r2, r1, rm1 = _mod4(r + 2), _mod4(r + 1), _mod4(r - 1)
        order = (r2, r1, rm1, r)
        lds = [fetch(i, one(q, pos1[q], k)) for i, k in enumerate(order)]
        for k in NEAR_KEYS:
            first[q][k].wait_recv()
        lds2 = [fetch(4 + i, yr.at[q, k]) for i, k in enumerate(order)]
        for i, k in enumerate(order):
            lds[i].wait()
            lds2[i].wait()
            _add_rows(yl.at[q, k], [tst.at[i, _top(h)], tst.at[4 + i, _top(h)]], min(FEW, h))
            if i == 0:
                second[q]["far_r"] = remote(yl.at[q, r2, lo], za.at[q], rt)
                second[q]["far_l"] = remote(yl.at[q, r2, hi], zb.at[q], lt)
            if i == 1:
                second[q]["near_r"] = remote(yl.at[q, r1, hi], zl.at[q, hi], rt)
            if i == 2:
                second[q]["near_l"] = remote(yl.at[q, rm1, lo], zr.at[q, lo], lt)

    def second_pass(q):
        r, (rt, lt) = pos2[q], ring2[q]
        r1, rm1 = _mod4(r + 1), _mod4(r - 1)
        second[q]["far_r"].wait_recv()
        _add_rows(yl.at[q, r1, lo], [za.at[q]], min(FEW, hc))
        second[q]["sum_r"] = remote(yl.at[q, r1, lo], zl.at[q, lo], rt)
        second[q]["far_l"].wait_recv()
        _add_rows(yl.at[q, rm1, hi], [zb.at[q]], min(FEW, hc))
        second[q]["sum_l"] = remote(yl.at[q, rm1, hi], zr.at[q, hi], lt)

    def last(q):
        r = pos2[q]
        for k in NEAR_KEYS:
            second[q][k].wait_recv()
        n = min(LANES, h)

        @pl.loop(0, h // n)
        def _(i):
            at = pl.ds(pl.multiple_of(i * n, n), n)
            v = yl[q, r, at, :] + zl[q, at, :] + zr[q, at, :]
            od[0, 0, 0:chunk, pl.ds(pl.multiple_of(q * h + i * n, n), n)] = (v * (1.0 / LOGIT_SCALE)).T

    def tiles_far(q, between=None):
        tiles(q, lambda i: (_mod4(pos1[q] + 2), i), between)

    def tiles_near(q):
        tiles(q, lambda i: (_mod4(pos1[q] + 1 + 2 * i), 1 - i))

    def tiles_pass(q):
        tiles(q, lambda i: (_mod4(pos1[q] + 1 + 2 * i), i))

    def tiles_own(q):
        tiles(q, lambda i: (pos1[q], i))

    all_later = 48 - SLOTS

    def dz_first(start, stop):
        dz_rows(in_order, start, stop, SLOTS, SLOTS, wide)

    def dz_later(start, stop):
        dz_rows(later, start, stop, all_later, at_dht, wide)

    with scope("de_far"):
        b0 = de_block(x_far, 0, 0)
        dz_far(16, 32)
        zahead(in_order, SLOTS, wide)
        for l in range(0, tok, nt):
            lanes = pl.ds(l, nt)
            dz_part(few[:, lanes], jnp.int32(dm.main), few_rows, lanes)
        dz[dm.main + FEW : dm.wide, :] = jnp.zeros((FEW, tok), BF16)
        b1 = de_block(x_far, 1, 1, True)
    with scope("dz_1"):
        c0 = sum_add(b0, q_h.at[x_far])
        dz_first(0, 8)
        c0.wait()
        e0 = remote(q_h.at[x_far, half_a], xa, xp)
        dz_first(8, SLOTS)
        zahead(later, at_dht, wide)
    with scope("dh_far1"):
        def between():
            sum_add(b1, q_h.at[x_far])

        tiles_far(1, between)
        c1 = stored(b1, q_h.at[x_far])
        c1.wait()
        e1 = remote(q_h.at[x_far, half_b], xb, xm)
    with scope("dz_2"):
        dz_later(0, 9)
        send_far(1)
    with scope("dh_far0"):
        tiles_far(0)
    with scope("dz_3"):
        dz_later(9, 13)
        send_far(0)
        dz_later(13, all_later)
    with scope("de_2"):
        b2 = de_block(x_p, 1, 0)
        b3 = de_block(x_m, 0, 1)
        c2 = sum_add(b2, q_h.at[x_p])
    with scope("dh_near"):
        tiles_near(1)
        c2.wait()
        e2 = remote(q_h.at[x_p, half_b], xe.at[half_b], xp)
        c3 = sum_add(b3, q_h.at[x_m])
        send_near(1)
        tiles_near(0)
        c3.wait()
        e3 = remote(q_h.at[x_m, half_a], xe.at[half_a], xm)
        send_near(0)
    with scope("dh_pass"):
        tiles_pass(1)
        tiles_pass(0)
        pass_on(1)
    with scope("de_4"):
        b4 = de_block(x_p, 0, 0)
        pass_on(0)
        b5 = de_block(x_m, 1, 1)
        c4 = sum_add(b4, q_h.at[x_p])
    with scope("dh_own"):
        tiles_own(1)
        c5 = sum_add(b5, q_h.at[x_m])
        tiles_own(0)
        c4.wait()
        c5.wait()
    old = list(sent)
    sent.clear()
    with scope("ring"):
        e0.wait_recv()
        e4 = ring_sum(x_p, half_a, ha, xa, 0, xs.at[half_a], xp)
        e1.wait_recv()
        e5 = ring_sum(x_m, half_b, ha + 8, xb, 1, xs.at[half_b], xm)
    with scope("de_6"):
        b6 = de_block(x, 0, 0)
    with scope("de_7"):
        b7 = de_block(x, 1, 1)
        xo_load = local(x4.at[zy, xc], dz.at[_top(chunk)], osem.at[0])
    with scope("second_1"):
        second_phase(1)
    with scope("second_0"):
        second_phase(0)
    with scope("spass_1"):
        second_pass(1)
    with scope("sum_6"):
        e3.wait_recv()
        c6 = early(b6, xe)
        e2.wait_recv()
        c7 = early(b7, xe)
        c6 = sum_add(b6, q_o, c6)
        c7 = sum_add(b7, q_o, c7)
    with scope("spass_0"):
        second_pass(0)
        c6.wait()
        c7.wait()
    def drain(cps):
        while cps:
            cps.pop().wait_send()

    def own_x(r):
        v = dz[r, :].astype(F32)
        inv = lax.rsqrt(jnp.mean(v * v, axis=-1, keepdims=True) + NORM_EPS)
        od[1, 0, r, :] = v * inv
        od[1, 1, r, 0:LANES] = jnp.broadcast_to(inv, (r.size, LANES))

    def own_dg(q):
        lanes = pl.ds(q * h, h)

        def add(i, acc):
            r = pl.ds(pl.multiple_of(i * 8, 8), 8)
            return acc + od[0, 0, r, lanes] * od[1, 0, r, lanes]

        acc = lax.fori_loop(0, chunk // 8, add, jnp.zeros((8, h), F32))
        sm[:, lanes] = jnp.sum(acc, axis=0, keepdims=True)

    def own_dx(r):
        x_hat, u = od[1, 0, r, :], od[0, 0, r, :] * gain
        od[0, 1, r, :] = od[1, 1, r, 0:1] * (u - x_hat * jnp.mean(u * x_hat, axis=-1, keepdims=True))

    with scope("own_x"):
        xo_load.wait()
        _loop_rows(chunk, 16, own_x)
        lse = jnp.where(zy == 0, lse_row[:, :], 0.0)
        loss = jnp.sum(w_row[:, :] * (lse - tgt_row[:, :]))
        sm[:, dim : dim + LANES] = jnp.full((1, LANES), loss / LOG2E)
        drain(old)
    with scope("last_1"):
        last(1)
        own_dg(1)
    with scope("last_0"):
        last(0)
        own_dg(0)

    with scope("small_1"):
        old = [cp for cp in sent if cp is not e4 and cp is not e5]
        near_sums = exchange(sm, got1, near)
        _loop_rows(chunk, 16, own_dx)
        dx_copy = local(od.at[0, 1, _top(chunk)], dx_out, osem.at[0])
        drain(old)
        for cp in near_sums:
            cp.wait()
    with scope("small_2"):
        tot = sm[...]
        for k in range(len(near)):
            tot = tot + got1[k]
        total_v[...] = tot
        all_sums = exchange(total_v, got2, line)
        mine = local(total_v, got2.at[len(line)], osem.at[1])
    with scope("ring_end"):
        for cp in (e4, e5):
            cp.wait()
        dx_copy.wait()
        mine.wait()
    with scope("small_3"):
        for cp in all_sums:
            cp.wait()


def _run(dm, x4, table, gain, labels, mask):
    hbm, vm = pl.BlockSpec(memory_space=HBM), pl.BlockSpec(memory_space=VMEM)
    sd = jax.ShapeDtypeStruct
    d, tok, h, ck, pad, ha = dm.dim, dm.tok, dm.h, dm.chunk, dm.pad, dm.ha
    line, quad, pair = VMEM((1, tok), F32), VMEM((2, 2, h, ck), F32), VMEM((2, h, ck), F32)
    part, shard = VMEM((2, h // 2, ck), F32), sd((pad, d), F32)
    out = pl.pallas_call(
        functools.partial(_kernel, dm),
        name="head",
        out_shape=(
            sd((ck, d), F32), sd((8, 1, d + LANES), F32),
            shard, shard, shard,
            sd((8, pad, d), F32), sd((16, dm.main, ck), F32),
            sd((4, pad, d), F32), sd((ha, d), F32), sd((ha + 8, d), F32),
            sd((4, 4, d, ck), F32), sd((2, 4, h, ck), F32),
        ),
        in_specs=[hbm, vm, vm, vm, vm],
        out_specs=[hbm] * 12,
        scratch_shapes=[
            VMEM((tok, d), BF16), VMEM((d, dm.wide), BF16), VMEM((dm.wide, tok), BF16),
            VMEM((2, 2, ha + 8, d), F32), VMEM((2, ha + 8, d), F32), VMEM((FEW, d), F32), VMEM((8, d), F32),
            quad, quad, VMEM((2, 4, h, ck), F32),
            part, part, pair, pair,
            VMEM((SLOTS, max(h, 2 * dm.rm), ck), F32),
            line, line, line, line, line, line, VMEM((15, 1, tok), F32),
            VMEM((1, d + LANES), F32), VMEM((15, 1, d + LANES), F32), VMEM((1, d + LANES), F32),
            DMA((53,)), DMA((53,)), pltpu.SemaphoreType.REGULAR((2,)),
            DMA((SLOTS,)), DMA((4,)), DMA((2,)), DMA((2,)), DMA((8,)),
        ],
        compiler_params=pltpu.CompilerParams(
            collective_id=0, has_side_effects=True, vmem_limit_bytes=67043328
        ),
    )(x4, table, gain, labels, mask)
    return _write_out(dm, out[2:4], *out[:2])


def _write_kernel(own, ring, dx, small, de_o, dx_o, dg_o, loss_o):
    de_o[:, :] = (own[:, :] + ring[:, :]) * (1.0 / LOGIT_SCALE)
    dx_o[:, :] = dx[:, :]
    total = jnp.sum(small[:, :, :], axis=0)
    d = dg_o.shape[1]
    dg_o[:, :] = total[:, :d]
    loss_o[:, :] = total[:, d : d + 1]


def _write_out(dm, parts, dx, small):
    d, step, blocks = dm.dim, dm.ha + 8, 2
    sd = jax.ShapeDtypeStruct
    some = pl.BlockSpec((step, d), lambda i: (i, 0))
    half = pl.BlockSpec((dm.chunk // blocks, d), lambda i: (i, 0))
    row, one = pl.BlockSpec((1, d), lambda i: (0, 0)), pl.BlockSpec((1, 1), lambda i: (0, 0))
    rows = pl.BlockSpec(small.shape, lambda i: (0, 0, 0))
    return pl.pallas_call(
        _write_kernel,
        name="write_out",
        grid=(blocks,),
        out_shape=(sd((dm.rows, d), F32), sd((dm.chunk, d), F32), sd((1, d), F32), sd((1, 1), F32)),
        in_specs=[some, some, half, rows],
        out_specs=(some, half, row, one),
    )(*parts, dx, small)


def solution(mesh):
    group = mesh.shape[AXIS]

    def local_step(residual, labels, loss_mask, norm_gain, table_shard):
        tokens, dim = residual.shape
        rows = table_shard.shape[0]
        dm = Dims(tokens, dim, rows, group)
        x4 = residual.reshape(16, 8, dm.chunk, dim)
        lab = labels.reshape(16, 8, 1, dm.chunk)
        msk = loss_mask.reshape(16, 8, 1, dm.chunk)
        d_embed, d_res, d_gain, loss = _run(dm, x4, table_shard, norm_gain[None, :], lab, msk)
        return loss.reshape(()), d_res, d_embed, d_gain.reshape(dim)

    return jax.shard_map(
        local_step,
        mesh=mesh,
        in_specs=(P(), P(), P(), P(), P(AXIS, None)),
        out_specs=(P(), P(AXIS, None), P(AXIS, None), P()),
        check_vma=False,
    )
```

```python
import functools
import itertools
import math

import jax
import jax.numpy as jnp
from jax import lax
from jax.experimental import pallas as pl
from jax.experimental.pallas import tpu as pltpu
from jax.sharding import PartitionSpec as P

VOCAB_REAL = 49155
LOGIT_SCALE = 6.0
NORM_EPS = 1e-6

AXIS = "vp"
MESH = pl.DeviceIdType.MESH
F32 = jnp.float32
BF16 = jnp.bfloat16
HBM = pltpu.HBM
VMEM = pltpu.VMEM
DMA = pltpu.SemaphoreType.DMA


def _coords():
    me = lax.axis_index(AXIS)
    return me // 32, (me // 8) % 4, (me // 2) % 4, me % 2


def _dev(z, y, x, c):
    return ((z * 4 + y) * 4 + x) * 2 + c


def _mod4(v):
    return lax.rem(v + 8, 4)


def _barrier(peers):
    sem = pltpu.get_barrier_semaphore()
    for p in peers:
        pl.semaphore_signal(sem, inc=1, device_id=(p,), device_id_type=MESH)
    pl.semaphore_wait(sem, len(peers))


def _remote(src, dst, send, recv, k, dev):
    return pltpu.make_async_remote_copy(
        src_ref=src,
        dst_ref=dst,
        send_sem=send.at[k],
        recv_sem=recv.at[k],
        device_id=(dev,),
        device_id_type=MESH,
    )


LANES = 128


class Dims:
    def __init__(self, tokens, dim, rows, group):
        self.dim, self.rows = dim, rows
        unit = LANES if rows >= LANES else 64
        self.rm = rows // unit * unit
        self.ha = self.rm // 2
        low = max(16, self.ha // 48 * 16)
        self.cuts = ((low, self.ha - low), (0, low))
        self.pad = self.rm + 8
        self.chunk = tokens // group
        self.tok = 16 * self.chunk
        self.nt = 4 * self.chunk
        self.main = 8 * self.rm
        self.wide = self.main + LANES
        self.h = dim // 2


def _top(n):
    return pl.ds(0, n)


def _rem(a, b):
    return a % b if isinstance(a, int) else lax.rem(a, b)


def _pick(test, a, b):
    return (a if test else b) if isinstance(test, bool) else jnp.where(test, a, b)


def _loop_rows(rows, step, fn):
    @pl.loop(0, rows // step)
    def _(i):
        fn(pl.ds(pl.multiple_of(i * step, step), step))


def _add_rows(dst, srcs, step):
    def add(r):
        acc = dst[r, :]
        for s in srcs:
            acc = acc + s[r, :]
        dst[r, :] = acc

    _loop_rows(dst.shape[0], step, add)


SLOTS = 12
FEW = 64
TWO = range(2)
LOG2E = math.log2(math.e)
NEAR_KEYS = ("near_r", "near_l", "sum_r", "sum_l")
scope = jax.named_scope


def _kernel(
    dm, x4, e_ref, g_ref, lab, msk,
    dx_out, got2, q_o, xs, xe, eg, zh, q_h, xa, xb, dhp, yr,
    hv, etv, dz, od, sst, few, oext, ya, yb, yl, za, zb, zl, zr, tst,
    m_row, s_row, w_row, pos_row, lse_row, tgt_row, got, sm, got1, total_v,
    send, recv,
    free, tsem, hsem, dsem, osem, lsem,
):
    z, y, x, c = _coords()
    xc, zy = x * 2 + c, z * 4 + y
    rows, rm, ha, dim, h = dm.rows, dm.rm, dm.ha, dm.dim, dm.h
    chunk, tok, nt, hc = dm.chunk, dm.tok, dm.nt, dm.h // 2
    x_far, x_p, x_m = _mod4(x + 2), _mod4(x + 1), _mod4(x - 1)
    xp, xm = _dev(z, y, x_p, c), _dev(z, y, x_m, c)
    yp, ym = _dev(z, _mod4(y + 1), x, c), _dev(z, _mod4(y - 1), x, c)
    zp, zm = _dev(_mod4(z + 1), y, x, c), _dev(_mod4(z - 1), y, x, c)
    sib = _dev(z, y, x, 1 - c)
    near = [_dev(_mod4(z + a), _mod4(y + b), x, c) for a in range(4) for b in range(4) if a or b]
    steps = [(a, b) for a in range(4) for b in TWO if a or b]
    line = [_dev(z, _mod4(y + 1), _mod4(x + a), lax.rem(c + b, 2)) for a, b in steps]
    back = [_dev(z, _mod4(y - 1), _mod4(x - a), lax.rem(c + b, 2)) for a, b in steps]
    bar = pltpu.get_barrier_semaphore()
    for p in (*near, *back, xp, xm, sib):
        pl.semaphore_signal(bar, inc=1, device_id=(p,), device_id_type=MESH)
    sent = []
    ids = itertools.count()

    def remote(src, dst, dev):
        cp = _remote(src, dst, send, recv, next(ids), dev)
        cp.start()
        sent.append(cp)
        return cp

    def exchange(src, dst, devs):
        k = next(ids)
        for i, dev in enumerate(devs):
            _remote(src, dst.at[i], send, recv, k, dev).start()
        whole = dst.at[_top(len(devs))]
        return pltpu.make_async_copy(whole, whole, recv.at[k]), pltpu.make_async_copy(whole, whole, send.at[k])

    def local(src, dst, sem):
        cp = pltpu.make_async_copy(src, dst, sem)
        cp.start()
        return cp

    x_at, ext_at = 2 * rm, 4 * rm

    def xload(k):
        s = lax.rem(k, 4)
        to = dz.at[pl.ds(pl.multiple_of(x_at + s * chunk, chunk), chunk)]
        return pltpu.make_async_copy(x4.at[k, xc], to, tsem.at[s])

    with scope("prep"):
        for k in range(3):
            xload(k).start()
        own = xc
        cps = []
        for j in TWO:
            def widen(r, j=j):
                od[0, j, r, :] = e_ref[pl.ds(j * ha + r.start, r.size), :].astype(F32)

            _loop_rows(ha, 16, widen)
            cps.append(local(od.at[0, j, _top(ha)], eg.at[own, pl.ds(j * ha, ha)], hsem.at[j]))
        oext[...] = jnp.zeros_like(oext)
        oext[0 : rows - rm, :] = e_ref[rm:rows, :].astype(F32)
        cps.append(local(oext, eg.at[own, pl.ds(rm, 8)], hsem.at[2]))
        pl.semaphore_wait(bar, len(near) + len(back) + 3)

    half_a, half_b = _top(ha), pl.ds(ha, ha + 8)

    def piece(s, r, dev):
        return remote(eg.at[s, r], eg.at[s, r], dev)

    def slot(xx):
        return xx * 2 + c

    cps[0].wait()
    r_a = piece(own, half_a, xp)
    for cp in cps[1:]:
        cp.wait()
    l_b = piece(own, half_b, xm)
    s_o = piece(own, _top(dm.pad), sib)
    r_b, l_a = piece(own, half_b, xp), piece(own, half_a, xm)

    gain = g_ref[...]

    with scope("norm"):
        @pl.loop(0, 16)
        def _(k):
            @pl.when(k < 13)
            def _():
                xload(k + 3).start()

            xload(k).wait()

            def norm(r):
                v = dz[pl.ds(pl.multiple_of(x_at + lax.rem(k, 4) * chunk + r.start, r.size), r.size), :].astype(F32)
                inv = lax.rsqrt(jnp.mean(v * v, axis=-1, keepdims=True) + NORM_EPS)
                hv[pl.ds(pl.multiple_of(k * chunk + r.start, r.size), r.size), :] = (v * inv * gain).astype(BF16)

            _loop_rows(chunk, 16, norm)

    with scope("labels"):
        total = jnp.sum(msk[...])
        for k in range(16):
            at = pl.ds(k * chunk, chunk)
            w_row[:, at] = msk[k, xc] / total
            q = lab[k, xc] - zy * (8 * rows)
            s = jnp.zeros_like(q)
            for i in range(1, 8):
                s = s + jnp.where(q >= i * rows, 1, 0)
            r = q - s * rows
            up = jnp.where(r >= ha, 1, 0)
            at_main = ((s // 2 * 2 + up) * 2 + s % 2) * ha + r - up * ha
            at_ext = dm.main + s * 8 + r - rm
            place = jnp.where(r < rm, at_main, at_ext)
            pos_row[:, at] = jnp.where((q >= 0) & (q < 8 * rows), place, -1).astype(F32)

    def product(lhs, lanes):
        v = lax.dot_general(lhs, hv[lanes, :], (((1,), (1,)), ((), ())), preferred_element_type=F32)
        return v * (LOG2E / LOGIT_SCALE)

    def add_stats(v, lanes):
        m_old, s_old = m_row[:, lanes], s_row[:, lanes]
        m = jnp.maximum(m_old, jnp.max(v, axis=0, keepdims=True))
        s = jnp.sum(jnp.exp2(v - m), axis=0, keepdims=True)
        m_row[:, lanes] = m
        s_row[:, lanes] = s_old * jnp.exp2(m_old - m) + s

    def add_target(v, place, lanes):
        r = lax.broadcasted_iota(jnp.int32, v.shape, 0)
        hit = r.astype(F32) == pos_row[:, lanes] - place.astype(F32)
        tgt_row[:, lanes] += jnp.sum(jnp.where(hit, v, 0.0), axis=0, keepdims=True)

    m_row[:, :] = jnp.full((1, tok), -jnp.inf, F32)
    s_row[:, :] = jnp.zeros((1, tok), F32)
    tgt_row[:, :] = jnp.zeros((1, tok), F32)
    segs = [(half, j) for half in TWO for j in TWO]

    def load(r0, n, xx, cores=TWO):
        return [
            local(
                eg.at[xx[half] * 2 + j, pl.ds(half * ha + r0, n)],
                od.at[j, half, pl.ds(r0, n)],
                hsem.at[half * len(cores) + k],
            )
            for half in TWO
            for k, j in enumerate(cores)
        ]

    def narrow_all(r0, n, src, cores=TWO):
        for half in TWO:
            for j in cores:
                def narrow(r, half=half, j=j):
                    at = pl.multiple_of((half * 2 + j) * ha + r0 + r.start, r.size)
                    dz[pl.ds(at, r.size), :] = src(half, j)[r, :].astype(BF16)

                _loop_rows(n, 16, narrow)

    def load_narrow(r0, n, xx, core):
        for cp in load(r0, n, xx, (core,)):
            cp.wait()
        narrow_all(r0, n, lambda half, j: od.at[j, half, pl.ds(r0, n)], (core,))

    def block(r0, n, xx, loads=(), with_few=False, nt=nt):
        if loads:
            for cp in loads:
                cp.wait()
            narrow_all(r0, n, lambda half, j: od.at[j, half, pl.ds(r0, n)])
        left = [VOCAB_REAL - ((zy * 8 + xx[half] * 2 + j) * rows + half * ha + r0) for half, j in segs]
        w, tall = nt // chunk, len(segs) * n
        pack = tst.shape[1] // tall
        deep = SLOTS // w
        packed = SLOTS * pack >= tok // chunk

        def place(t, i):
            if packed:
                return t * (w // pack) + i // pack, i % pack * tall
            return lax.rem(t, deep) * w + i, 0

        def out(t):
            cps = []
            for i in range(w):
                u, row = place(t, i)
                for m, (half, j) in enumerate(segs):
                    to = pl.ds(pl.multiple_of((xx[half] * 2 + half) * rm + j * ha + r0, 8), n)
                    cps.append(pltpu.make_async_copy(tst.at[u, pl.ds(row + m * n, n)], zh.at[t * w + i, to], tsem.at[u]))
            return cps

        def out_wait(u, rows_):
            whole = tst.at[u, _top(rows_)]
            pltpu.make_async_copy(whole, whole, tsem.at[u]).wait()

        @pl.loop(0, tok // nt)
        def _(t):
            if not packed:
                @pl.when(t >= deep)
                def _():
                    for i in range(w):
                        out_wait(place(t, i)[0], tall)

            lanes = pl.ds(pl.multiple_of(t * nt, nt), nt)
            lhs = [dz[(half * 2 + j) * ha + r0 : (half * 2 + j) * ha + r0 + n, :] for half, j in segs]
            if with_few:
                lhs.append(dz[ext_at : ext_at + FEW, :])
            v = product(jnp.concatenate(lhs, axis=0), lanes)
            v, v_few = v[:tall], v[tall:]
            r = lax.broadcasted_iota(jnp.int32, (n, nt), 0)
            v = [jnp.where(r < left[m], v[m * n : (m + 1) * n], -jnp.inf) for m in range(len(segs))]
            for part_v, (half, j) in zip(v, segs):
                add_target(part_v, (xx[half] * 2 + half) * rm + j * ha + r0, lanes)
            for i in range(w):
                u, row = place(t, i)
                for m in range(len(segs)):
                    tst[u, row + m * n : row + (m + 1) * n, :] = v[m][:, i * chunk : (i + 1) * chunk]
            if with_few:
                r = lax.broadcasted_iota(jnp.int32, v_few.shape, 0)
                ok = ((r & 7) < rows - rm) & ((zy * 8 + (r >> 3)) * rows + rm + (r & 7) < VOCAB_REAL)
                v_few = jnp.where(ok, v_few, -jnp.inf)
                few[:, lanes] = v_few
                add_target(v_few, jnp.int32(dm.main), lanes)
                v.append(v_few)
            v = jnp.concatenate(v, axis=0)
            for cp in out(t):
                cp.start()
            add_stats(v, lanes)

        if packed:
            for u in range(tok // chunk // pack):
                out_wait(u, pack * tall)
        else:
            for u in range(deep * w):
                out_wait(u, tall)

    def both(xx):
        block(0, ha, xx, load(0, ha, xx))

    def turn(xx):
        for half in TWO:
            base = pl.multiple_of((xx[half] * 2 + half) * rm, rm)

            @pl.loop(0, dim // LANES)
            def _(d, half=half, base=base):
                at = pl.ds(pl.multiple_of(d * LANES, LANES), LANES)
                etv[at, pl.ds(base, rm)] = dz[half * rm : (half + 1) * rm, at].T

    with scope("own"):
        s_o.wait_recv()
        both((x, x))
        turn((x, x))

    with scope("wait_1"):
        r_a.wait_recv()
        last_n = dm.cuts[-1][1]
        spans = [(pl.ds(r0, n), pl.ds(ha + r0, n + 8 * (r0 + n == ha))) for r0, n in dm.cuts]

        def far_pieces(xx, half, to):
            cps = [piece(slot(xx), pair[half], to) for pair in spans[:-1]]
            cps.append(remote(eg.at[slot(xx), spans[-1][half]], sst.at[c, pl.ds(half * last_n, last_n)], to))
            return cps

        r_f = far_pieces(x_m, 0, xp)
        d = [piece(slot(x_m), half_a, sib)]
        l_b.wait_recv()
        l_f = far_pieces(x_p, 1, xm)
        d.append(piece(slot(x_p), half_b, sib))
        for cp in d:
            cp.wait_recv()

    with scope("near_1"):
        both((x_m, x_p))
        turn((x_m, x_p))

    with scope("wait_2"):
        r_b.wait_recv()
        d = [piece(slot(x_m), half_b, sib)]
        l_a.wait_recv()
        d.append(piece(slot(x_p), half_a, sib))
        for cp in d:
            cp.wait_recv()

    with scope("near_2"):
        both((x_p, x_m))
        turn((x_p, x_m))

    far = (x_far, x_far)

    with scope("wait_3"):
        d = []
        for cp, r in zip((r_f[0], l_f[0]), spans[0]):
            cp.wait_recv()
            d.append(piece(slot(x_far), r, sib))
        load_narrow(*dm.cuts[0], far, c)
        for cp in d:
            cp.wait_recv()
    with scope("far_a"):
        ext_loads = [local(eg.at[s, pl.ds(rm, 8)], few.at[pl.ds(s * 8, 8)], lsem.at[s]) for s in range(8)]
        load_narrow(*dm.cuts[0], far, 1 - c)
        for cp in ext_loads:
            cp.wait()
        dz[ext_at : ext_at + FEW, :] = few[...].astype(BF16)
        dz[ext_at + FEW : ext_at + LANES, :] = jnp.zeros((FEW, dim), BF16)
        block(*dm.cuts[0], far, with_few=True)
    with scope("wait_5"):
        r_f[-1].wait_recv()
        l_f[-1].wait_recv()
        both_last = sst.at[c, _top(2 * last_n)]
        over = _remote(both_last, both_last, send, recv, next(ids), sib)
        over.start()

        @pl.loop(0, dim // LANES)
        def _(i):
            at = pl.ds(pl.multiple_of(i * LANES, LANES), LANES)
            etv[at, dm.main : dm.wide] = dz[ext_at : ext_at + LANES, at].T

        def last_rows(half, j):
            return sst.at[j, pl.ds(half * last_n, last_n)]

        narrow_all(0, last_n, last_rows, (c,))
        over.wait_recv()

    with scope("far_c"):
        narrow_all(0, last_n, last_rows, (1 - c,))
        block(0, last_n, far, nt=8 * chunk)
        over.wait_send()
        for s in TWO:
            pl.semaphore_signal(free.at[s], inc=1, device_id=(sib,), device_id_type=MESH)

    with scope("turn_far"):
        lse_row[:, :] = m_row[:, :] + jnp.log(s_row[:, :]) * LOG2E
        stats = exchange(lse_row, got, near)
        turn(far)

    wide = 2 * rm

    at_dht = SLOTS - 4

    def chunk_of(zz, yy):
        return _mod4(zz) * 4 + _rem(yy + 8, 4)

    def all_far(i):
        return x_far * wide + i // 16 * rm, _rem(i, 16)

    def in_order(i):
        n = i // 3
        m = n - 7
        k = _pick(n < 7, chunk_of(z + n - 1, y + 2), chunk_of(z + 3 + m // 3, y + 3 + _rem(m + 9, 3)))
        return _mod4(x + 3 + _rem(i, 3)) * wide, _pick(n < 4, chunk_of(z + 2, n), k)

    def later(i):
        return in_order(i + SLOTS)

    def zload(where, i, ring, n):
        at, k = where(i)
        s = _rem(i, ring)
        src = zh.at[k, pl.ds(pl.multiple_of(at, rm), n)]
        return pltpu.make_async_copy(src, tst.at[s, _top(n)], tsem.at[s])

    def zahead(where, ring, n):
        for i in range(ring):
            zload(where, i, ring, n).start()

    with scope("stats"):
        zahead(all_far, SLOTS, rm)
        for cp in stats:
            cp.wait()
        top = lse_row[:, :]
        for k in range(len(near)):
            top = jnp.maximum(top, got[k])
        s = jnp.exp2(lse_row[:, :] - top)
        for k in range(len(near)):
            s = s + jnp.exp2(got[k] - top)
        lse_row[:, :] = top + jnp.log(s) * LOG2E

    def dz_part(v, place, at, lanes):
        r = lax.broadcasted_iota(jnp.int32, v.shape, 0).astype(F32)
        hit = r == pos_row[:, lanes] - place.astype(F32)
        p = jnp.exp2(v - lse_row[:, lanes])
        dz[at, lanes] = (jnp.where(hit, p - 1.0, p) * w_row[:, lanes]).astype(BF16)

    step = min(LANES, rm)

    def dz_rows(where, start, stop, last_tile, ring, n):
        @pl.loop(start, stop)
        def _(i):
            @pl.when((i > 0) & (i + ring - 1 < last_tile))
            def _():
                zload(where, i + ring - 1, ring, n).start()

            zload(where, i, ring, n).wait()
            row, k = where(i)
            lanes = pl.ds(pl.multiple_of(k * chunk, chunk), chunk)

            @pl.loop(0, n // step)
            def _(j):
                at = pl.multiple_of(row + j * step, step)
                r = pl.ds(pl.multiple_of(j * step, step), step)
                dz_part(tst[lax.rem(i, ring), r, :], at, pl.ds(at, step), lanes)

    def dz_far(start, stop):
        dz_rows(all_far, start, stop, 32, SLOTS, rm)

    with scope("dz_far"):
        dz_far(0, 16)

    nd = dim // 2
    few_rows = pl.ds(dm.main, FEW)
    pair_ids = [(next(ids), next(ids)) for _ in TWO]

    def over_d2d(s, n, i):
        lanes = pl.ds(pl.multiple_of(i * nd, nd), nd)
        there = sst.at[s, _top(n), lanes]
        return _remote(od.at[s, 1 - c, _top(n), lanes], there, send, recv, pair_ids[s][0] + i, sib)

    def de_block(xx, half, s, with_few=False):
        at = pl.ds(pl.multiple_of((xx * 2 + half) * rm, rm), rm)
        n = ha + 8 * half
        pl.semaphore_wait(free.at[s], 1)

        @pl.loop(0, 2)
        def _(i):
            lanes = pl.ds(pl.multiple_of(i * nd, nd), nd)
            lhs = jnp.concatenate([dz[at, :], dz[few_rows, :]], axis=0) if with_few else dz[at, :]
            v = jnp.dot(lhs, hv[:, lanes], preferred_element_type=F32)
            if with_few:
                few[:, lanes] = v[rm:]
            for j in TWO:
                od[s, j, 0:ha, lanes] = v[j * ha : (j + 1) * ha]
                if half:
                    od[s, j, ha:n, lanes] = few[pl.ds(pl.multiple_of((xx * 2 + j) * 8, 8), 8), lanes]
            over_d2d(s, n, i).start()

        return half, s, n

    def stored(blk, to):
        half, s, n = blk
        return pltpu.make_async_copy(od.at[s, c, _top(n)], to.at[pl.ds(half * ha, n)], dsem.at[s])

    def early(blk, src):
        half, s, n = blk
        for i in TWO:
            over_d2d(s, n, i).wait_send()
        return local(src.at[pl.ds(half * ha, n)], od.at[s, 1 - c, _top(n)], lsem.at[s])

    def sum_add(blk, to, more=None):
        half, s, n = blk
        for i in TWO:
            over_d2d(s, n, i).wait_recv()
        if more is not None:
            more.wait()

        def add(r):
            v = od[s, c, r, :] + sst[s, r, :]
            od[s, c, r, :] = v if more is None else v + od[s, 1 - c, r, :]

        _loop_rows(n, 8, add)
        if more is None:
            pl.semaphore_signal(free.at[s], inc=1, device_id=(sib,), device_id_type=MESH)
            for i in TWO:
                over_d2d(s, n, i).wait_send()
        cp = stored(blk, to)
        cp.start()
        return cp

    def ring_sum(xx, rows_, n, src, s, dst, dev):
        lds = [
            local(q_h.at[xx, rows_], od.at[s, 0, _top(n)], lsem.at[0]),
            local(src, od.at[s, 1, _top(n)], lsem.at[1]),
        ]
        for cp in lds:
            cp.wait()
        _add_rows(od.at[s, 0, _top(n)], [od.at[s, 1, _top(n)]], 8)
        local(od.at[s, 0, _top(n)], q_h.at[xx, rows_], lsem.at[0]).wait()
        return remote(q_h.at[xx, rows_], dst, dev)

    stores = []

    def flush():
        while stores:
            stores.pop().wait()

    def tiles(q, where, between=None):
        flush()

        def outs(i):
            p, ab = where(i)
            r = pl.ds(q * h, h)
            dsts = [dhp.at[ab * 2 + j, p, r] if q == 0 else dhp.at[p, ab * 2 + j, r] for j in TWO]
            return [
                pltpu.make_async_copy(tst.at[at_dht + i * 2 + j, _top(h)], dst, hsem.at[i * 2 + j])
                for j, dst in enumerate(dsts)
            ]

        @pl.loop(0, 2)
        def _(i):
            if between is not None:
                pl.when(i > 0)(between)
            p, ab = where(i)
            ks = [(ab * 2 + j) * 4 + p if q == 0 else p * 4 + ab * 2 + j for j in TWO]
            rhs = jnp.concatenate([dz[:, pl.ds(pl.multiple_of(k * chunk, chunk), chunk)] for k in ks], axis=1)
            v = jnp.dot(etv[q * h : (q + 1) * h, :], rhs, preferred_element_type=F32)
            for j in TWO:
                tst[at_dht + i * 2 + j, 0:h, :] = v[:, j * chunk : (j + 1) * chunk]
            for cp in outs(i):
                cp.start()

        for i in TWO:
            stores.extend(outs(i))

    def part(q, p, lo, n):
        r = pl.ds(q * h, h)
        if q == 0:
            return dhp.at[pl.ds(lo, n), p, r]
        return dhp.at[p, pl.ds(lo, n), r]

    def one(q, p, i):
        r = pl.ds(q * h, h)
        return dhp.at[i, p, r] if q == 0 else dhp.at[p, i, r]

    ring1, ring2 = ((yp, ym), (zp, zm)), ((zp, zm), (yp, ym))
    pos1, pos2 = (y, z), (z, y)
    first, second = ({}, {}), ({}, {})

    def send_far(q):
        flush()
        p, (rt, lt) = pos1[q], ring1[q]
        first[q]["far_r"] = remote(part(q, _mod4(p + 2), 0, 2), ya.at[q], rt)
        first[q]["far_l"] = remote(part(q, _mod4(p + 2), 2, 2), yb.at[q], lt)

    def send_near(q):
        flush()
        p, (rt, lt) = pos1[q], ring1[q]
        first[q]["near_r"] = remote(part(q, _mod4(p + 1), 2, 2), yl.at[q, pl.ds(2, 2)], rt)
        first[q]["near_l"] = remote(part(q, _mod4(p - 1), 0, 2), yr.at[q, _top(2)], lt)

    def fetch(i, src):
        return local(src, tst.at[i, _top(h)], tsem.at[i])

    def pass_on(q):
        flush()
        p, (rt, lt) = pos1[q], ring1[q]
        lds = [fetch(i, one(q, _mod4(p + 1), i)) for i in TWO]
        lds += [fetch(2 + i, one(q, _mod4(p - 1), 2 + i)) for i in TWO]
        first[q]["far_r"].wait_recv()
        for i in TWO:
            lds[i].wait()
            _add_rows(ya.at[q, i], [tst.at[i, _top(h)]], min(FEW, h))
        first[q]["sum_r"] = remote(ya.at[q], yl.at[q, _top(2)], rt)
        first[q]["far_l"].wait_recv()
        for i in TWO:
            lds[2 + i].wait()
            _add_rows(yb.at[q, i], [tst.at[2 + i, _top(h)]], min(FEW, h))
        first[q]["sum_l"] = remote(yb.at[q], yr.at[q, pl.ds(2, 2)], lt)

    lo, hi = _top(hc), pl.ds(hc, hc)

    def second_phase(q):
        flush()
        r, (rt, lt) = pos2[q], ring2[q]
        r2, r1, rm1 = _mod4(r + 2), _mod4(r + 1), _mod4(r - 1)
        order = (r2, r1, rm1, r)
        lds = [fetch(i, one(q, pos1[q], k)) for i, k in enumerate(order)]
        for k in NEAR_KEYS:
            first[q][k].wait_recv()
        lds2 = [fetch(4 + i, yr.at[q, k]) for i, k in enumerate(order)]
        for i, k in enumerate(order):
            lds[i].wait()
            lds2[i].wait()
            _add_rows(yl.at[q, k], [tst.at[i, _top(h)], tst.at[4 + i, _top(h)]], min(FEW, h))
            if i == 0:
                second[q]["far_r"] = remote(yl.at[q, r2, lo], za.at[q], rt)
                second[q]["far_l"] = remote(yl.at[q, r2, hi], zb.at[q], lt)
            if i == 1:
                second[q]["near_r"] = remote(yl.at[q, r1, hi], zl.at[q, hi], rt)
            if i == 2:
                second[q]["near_l"] = remote(yl.at[q, rm1, lo], zr.at[q, lo], lt)

    def second_pass(q):
        r, (rt, lt) = pos2[q], ring2[q]
        r1, rm1 = _mod4(r + 1), _mod4(r - 1)
        second[q]["far_r"].wait_recv()
        _add_rows(yl.at[q, r1, lo], [za.at[q]], min(FEW, hc))
        second[q]["sum_r"] = remote(yl.at[q, r1, lo], zl.at[q, lo], rt)
        second[q]["far_l"].wait_recv()
        _add_rows(yl.at[q, rm1, hi], [zb.at[q]], min(FEW, hc))
        second[q]["sum_l"] = remote(yl.at[q, rm1, hi], zr.at[q, hi], lt)

    def last(q):
        r = pos2[q]
        for k in NEAR_KEYS:
            second[q][k].wait_recv()
        n = min(LANES, h)

        @pl.loop(0, h // n)
        def _(i):
            at = pl.ds(pl.multiple_of(i * n, n), n)
            v = yl[q, r, at, :] + zl[q, at, :] + zr[q, at, :]
            od[0, 0, 0:chunk, pl.ds(pl.multiple_of(q * h + i * n, n), n)] = (v * (1.0 / LOGIT_SCALE)).T

    def tiles_far(q, between=None):
        tiles(q, lambda i: (_mod4(pos1[q] + 2), i), between)

    def tiles_near(q):
        tiles(q, lambda i: (_mod4(pos1[q] + 1 + 2 * i), 1 - i))

    def tiles_pass(q):
        tiles(q, lambda i: (_mod4(pos1[q] + 1 + 2 * i), i))

    def tiles_own(q):
        tiles(q, lambda i: (pos1[q], i))

    all_later = 48 - SLOTS

    def dz_first(start, stop):
        dz_rows(in_order, start, stop, SLOTS, SLOTS, wide)

    def dz_later(start, stop):
        dz_rows(later, start, stop, all_later, at_dht, wide)

    with scope("de_far"):
        b0 = de_block(x_far, 0, 0)
        dz_far(16, 32)
        zahead(in_order, SLOTS, wide)
        for l in range(0, tok, nt):
            lanes = pl.ds(l, nt)
            dz_part(few[:, lanes], jnp.int32(dm.main), few_rows, lanes)
        dz[dm.main + FEW : dm.wide, :] = jnp.zeros((FEW, tok), BF16)
        b1 = de_block(x_far, 1, 1, True)
    with scope("dz_1"):
        c0 = sum_add(b0, q_h.at[x_far])
        dz_first(0, 8)
        c0.wait()
        e0 = remote(q_h.at[x_far, half_a], xa, xp)
        dz_first(8, SLOTS)
        zahead(later, at_dht, wide)
    with scope("dh_far1"):
        def between():
            sum_add(b1, q_h.at[x_far])

        tiles_far(1, between)
        c1 = stored(b1, q_h.at[x_far])
        c1.wait()
        e1 = remote(q_h.at[x_far, half_b], xb, xm)
    with scope("dz_2"):
        dz_later(0, 9)
        send_far(1)
    with scope("dh_far0"):
        tiles_far(0)
    with scope("dz_3"):
        dz_later(9, 13)
        send_far(0)
        dz_later(13, all_later)
    with scope("de_2"):
        b2 = de_block(x_p, 1, 0)
        b3 = de_block(x_m, 0, 1)
        c2 = sum_add(b2, q_h.at[x_p])
    with scope("dh_near"):
        tiles_near(1)
        c2.wait()
        e2 = remote(q_h.at[x_p, half_b], xe.at[half_b], xp)
        c3 = sum_add(b3, q_h.at[x_m])
        send_near(1)
        tiles_near(0)
        c3.wait()
        e3 = remote(q_h.at[x_m, half_a], xe.at[half_a], xm)
        send_near(0)
    with scope("dh_pass"):
        tiles_pass(1)
        tiles_pass(0)
        pass_on(1)
    with scope("de_4"):
        b4 = de_block(x_p, 0, 0)
        pass_on(0)
        b5 = de_block(x_m, 1, 1)
        c4 = sum_add(b4, q_h.at[x_p])
    with scope("dh_own"):
        tiles_own(1)
        c5 = sum_add(b5, q_h.at[x_m])
        tiles_own(0)
        c4.wait()
        c5.wait()
    old = list(sent)
    sent.clear()
    with scope("ring"):
        e0.wait_recv()
        e4 = ring_sum(x_p, half_a, ha, xa, 0, xs.at[half_a], xp)
        e1.wait_recv()
        e5 = ring_sum(x_m, half_b, ha + 8, xb, 1, xs.at[half_b], xm)
    with scope("de_6"):
        b6 = de_block(x, 0, 0)
    with scope("de_7"):
        b7 = de_block(x, 1, 1)
        xo_load = local(x4.at[zy, xc], dz.at[_top(chunk)], osem.at[0])
    with scope("second_1"):
        second_phase(1)
    with scope("second_0"):
        second_phase(0)
    with scope("spass_1"):
        second_pass(1)
    with scope("sum_6"):
        e3.wait_recv()
        c6 = early(b6, xe)
        e2.wait_recv()
        c7 = early(b7, xe)
        c6 = sum_add(b6, q_o, c6)
        c7 = sum_add(b7, q_o, c7)
    with scope("spass_0"):
        second_pass(0)
        c6.wait()
        c7.wait()
    def drain(cps):
        while cps:
            cps.pop().wait_send()

    def own_x(r):
        v = dz[r, :].astype(F32)
        inv = lax.rsqrt(jnp.mean(v * v, axis=-1, keepdims=True) + NORM_EPS)
        od[1, 0, r, :] = v * inv
        od[1, 1, r, 0:LANES] = jnp.broadcast_to(inv, (r.size, LANES))

    def own_dg(q):
        lanes = pl.ds(q * h, h)

        def add(i, acc):
            r = pl.ds(pl.multiple_of(i * 8, 8), 8)
            return acc + od[0, 0, r, lanes] * od[1, 0, r, lanes]

        acc = lax.fori_loop(0, chunk // 8, add, jnp.zeros((8, h), F32))
        sm[:, lanes] = jnp.sum(acc, axis=0, keepdims=True)

    def own_dx(r):
        x_hat, u = od[1, 0, r, :], od[0, 0, r, :] * gain
        od[0, 1, r, :] = od[1, 1, r, 0:1] * (u - x_hat * jnp.mean(u * x_hat, axis=-1, keepdims=True))

    with scope("own_x"):
        xo_load.wait()
        _loop_rows(chunk, 16, own_x)
        lse = jnp.where(zy == 0, lse_row[:, :], 0.0)
        loss = jnp.sum(w_row[:, :] * (lse - tgt_row[:, :]))
        sm[:, dim : dim + LANES] = jnp.full((1, LANES), loss / LOG2E)
        drain(old)
    with scope("last_1"):
        last(1)
        own_dg(1)
    with scope("last_0"):
        last(0)
        own_dg(0)

    with scope("small_1"):
        old = [cp for cp in sent if cp is not e4 and cp is not e5]
        near_sums = exchange(sm, got1, near)
        _loop_rows(chunk, 16, own_dx)
        dx_copy = local(od.at[0, 1, _top(chunk)], dx_out, osem.at[0])
        drain(old)
        for cp in near_sums:
            cp.wait()
    with scope("small_2"):
        tot = sm[...]
        for k in range(len(near)):
            tot = tot + got1[k]
        total_v[...] = tot
        all_sums = exchange(total_v, got2, line)
        mine = local(total_v, got2.at[len(line)], osem.at[1])
    with scope("ring_end"):
        for cp in (e4, e5):
            cp.wait()
        dx_copy.wait()
        mine.wait()
    with scope("small_3"):
        for cp in all_sums:
            cp.wait()


def _run(dm, x4, table, gain, labels, mask):
    hbm, vm = pl.BlockSpec(memory_space=HBM), pl.BlockSpec(memory_space=VMEM)
    sd = jax.ShapeDtypeStruct
    d, tok, h, ck, pad, ha = dm.dim, dm.tok, dm.h, dm.chunk, dm.pad, dm.ha
    line, quad, pair = VMEM((1, tok), F32), VMEM((2, 2, h, ck), F32), VMEM((2, h, ck), F32)
    part, shard = VMEM((2, h // 2, ck), F32), sd((pad, d), F32)
    out = pl.pallas_call(
        functools.partial(_kernel, dm),
        name="head",
        out_shape=(
            sd((ck, d), F32), sd((8, 1, d + LANES), F32),
            shard, shard, shard,
            sd((8, pad, d), F32), sd((16, dm.main, ck), F32),
            sd((4, pad, d), F32), sd((ha, d), F32), sd((ha + 8, d), F32),
            sd((4, 4, d, ck), F32), sd((2, 4, h, ck), F32),
        ),
        in_specs=[hbm, vm, vm, vm, vm],
        out_specs=[hbm] * 12,
        scratch_shapes=[
            VMEM((tok, d), BF16), VMEM((d, dm.wide), BF16), VMEM((dm.wide, tok), BF16),
            VMEM((2, 2, ha + 8, d), F32), VMEM((2, ha + 8, d), F32), VMEM((FEW, d), F32), VMEM((8, d), F32),
            quad, quad, VMEM((2, 4, h, ck), F32),
            part, part, pair, pair,
            VMEM((SLOTS, max(h, 2 * dm.rm), ck), F32),
            line, line, line, line, line, line, VMEM((15, 1, tok), F32),
            VMEM((1, d + LANES), F32), VMEM((15, 1, d + LANES), F32), VMEM((1, d + LANES), F32),
            DMA((53,)), DMA((53,)), pltpu.SemaphoreType.REGULAR((2,)),
            DMA((SLOTS,)), DMA((4,)), DMA((2,)), DMA((2,)), DMA((8,)),
        ],
        compiler_params=pltpu.CompilerParams(
            collective_id=0, has_side_effects=True, vmem_limit_bytes=67043328
        ),
    )(x4, table, gain, labels, mask)
    return _write_out(dm, out[2:4], *out[:2])


def _write_kernel(own, ring, dx, small, de_o, dx_o, dg_o, loss_o):
    de_o[:, :] = (own[:, :] + ring[:, :]) * (1.0 / LOGIT_SCALE)
    dx_o[:, :] = dx[:, :]
    total = jnp.sum(small[:, :, :], axis=0)
    d = dg_o.shape[1]
    dg_o[:, :] = total[:, :d]
    loss_o[:, :] = total[:, d : d + 1]


def _write_out(dm, parts, dx, small):
    d, step, blocks = dm.dim, dm.ha + 8, 2
    sd = jax.ShapeDtypeStruct
    some = pl.BlockSpec((step, d), lambda i: (i, 0))
    half = pl.BlockSpec((dm.chunk // blocks, d), lambda i: (i, 0))
    row, one = pl.BlockSpec((1, d), lambda i: (0, 0)), pl.BlockSpec((1, 1), lambda i: (0, 0))
    rows = pl.BlockSpec(small.shape, lambda i: (0, 0, 0))
    return pl.pallas_call(
        _write_kernel,
        name="write_out",
        grid=(blocks,),
        out_shape=(sd((dm.rows, d), F32), sd((dm.chunk, d), F32), sd((1, d), F32), sd((1, 1), F32)),
        in_specs=[some, some, half, rows],
        out_specs=(some, half, row, one),
    )(*parts, dx, small)


def solution(mesh):
    group = mesh.shape[AXIS]

    def local_step(residual, labels, loss_mask, norm_gain, table_shard):
        tokens, dim = residual.shape
        rows = table_shard.shape[0]
        dm = Dims(tokens, dim, rows, group)
        x4 = residual.reshape(16, 8, dm.chunk, dim)
        lab = labels.reshape(16, 8, 1, dm.chunk)
        msk = loss_mask.reshape(16, 8, 1, dm.chunk)
        d_embed, d_res, d_gain, loss = _run(dm, x4, table_shard, norm_gain[None, :], lab, msk)
        return loss.reshape(()), d_res, d_embed, d_gain.reshape(dim)

    return jax.shard_map(
        local_step,
        mesh=mesh,
        in_specs=(P(), P(), P(), P(), P(AXIS, None)),
        out_specs=(P(), P(AXIS, None), P(AXIS, None), P()),
        check_vma=False,
    )
```

```python
import functools
import itertools
import math

import jax
import jax.numpy as jnp
from jax import lax
from jax.experimental import pallas as pl
from jax.experimental.pallas import tpu as pltpu
from jax.sharding import PartitionSpec as P

VOCAB_REAL = 49155
LOGIT_SCALE = 6.0
NORM_EPS = 1e-6

AXIS = "vp"
MESH = pl.DeviceIdType.MESH
F32 = jnp.float32
BF16 = jnp.bfloat16
HBM = pltpu.HBM
VMEM = pltpu.VMEM
DMA = pltpu.SemaphoreType.DMA


def _coords():
    me = lax.axis_index(AXIS)
    return me // 32, (me // 8) % 4, (me // 2) % 4, me % 2


def _dev(z, y, x, c):
    return ((z * 4 + y) * 4 + x) * 2 + c


def _mod4(v):
    return lax.rem(v + 8, 4)


def _barrier(peers):
    sem = pltpu.get_barrier_semaphore()
    for p in peers:
        pl.semaphore_signal(sem, inc=1, device_id=(p,), device_id_type=MESH)
    pl.semaphore_wait(sem, len(peers))


def _remote(src, dst, send, recv, k, dev):
    return pltpu.make_async_remote_copy(
        src_ref=src,
        dst_ref=dst,
        send_sem=send.at[k],
        recv_sem=recv.at[k],
        device_id=(dev,),
        device_id_type=MESH,
    )


LANES = 128


class Dims:
    def __init__(self, tokens, dim, rows, group):
        self.dim, self.rows = dim, rows
        unit = LANES if rows >= LANES else 64
        self.rm = rows // unit * unit
        self.ha = self.rm // 2
        low = max(16, self.ha // 48 * 16)
        self.cuts = ((low, self.ha - low), (0, low))
        self.pad = self.rm + 8
        self.chunk = tokens // group
        self.tok = 16 * self.chunk
        self.nt = 4 * self.chunk
        self.main = 8 * self.rm
        self.wide = self.main + LANES
        self.h = dim // 2


def _top(n):
    return pl.ds(0, n)


def _rem(a, b):
    return a % b if isinstance(a, int) else lax.rem(a, b)


def _pick(test, a, b):
    return (a if test else b) if isinstance(test, bool) else jnp.where(test, a, b)


def _loop_rows(rows, step, fn):
    @pl.loop(0, rows // step)
    def _(i):
        fn(pl.ds(pl.multiple_of(i * step, step), step))


def _add_rows(dst, srcs, step):
    def add(r):
        acc = dst[r, :]
        for s in srcs:
            acc = acc + s[r, :]
        dst[r, :] = acc

    _loop_rows(dst.shape[0], step, add)


SLOTS = 12
FEW = 64
TWO = range(2)
LOG2E = math.log2(math.e)
NEAR_KEYS = ("near_r", "near_l", "sum_r", "sum_l")
scope = jax.named_scope


def _kernel(
    dm, x4, e_ref, g_ref, lab, msk,
    dx_out, got2, q_o, xs, xe, eg, zh, q_h, xa, xb, dhp, yr,
    hv, etv, dz, od, sst, few, oext, ya, yb, yl, za, zb, zl, zr, tst,
    m_row, s_row, w_row, pos_row, lse_row, tgt_row, got, sm, got1, total_v,
    send, recv,
    free, tsem, hsem, dsem, osem, lsem,
):
    z, y, x, c = _coords()
    xc, zy = x * 2 + c, z * 4 + y
    rows, rm, ha, dim, h = dm.rows, dm.rm, dm.ha, dm.dim, dm.h
    chunk, tok, nt, hc = dm.chunk, dm.tok, dm.nt, dm.h // 2
    x_far, x_p, x_m = _mod4(x + 2), _mod4(x + 1), _mod4(x - 1)
    xp, xm = _dev(z, y, x_p, c), _dev(z, y, x_m, c)
    yp, ym = _dev(z, _mod4(y + 1), x, c), _dev(z, _mod4(y - 1), x, c)
    zp, zm = _dev(_mod4(z + 1), y, x, c), _dev(_mod4(z - 1), y, x, c)
    sib = _dev(z, y, x, 1 - c)
    near = [_dev(_mod4(z + a), _mod4(y + b), x, c) for a in range(4) for b in range(4) if a or b]
    line = [_dev(z, y, _mod4(x + a), lax.rem(c + b, 2)) for a in range(4) for b in TWO if a or b]
    bar = pltpu.get_barrier_semaphore()
    for p in (*near, *line):
        pl.semaphore_signal(bar, inc=1, device_id=(p,), device_id_type=MESH)
    sent = []
    ids = itertools.count()

    def remote(src, dst, dev):
        cp = _remote(src, dst, send, recv, next(ids), dev)
        cp.start()
        sent.append(cp)
        return cp

    def exchange(src, dst, devs):
        k = next(ids)
        for i, dev in enumerate(devs):
            _remote(src, dst.at[i], send, recv, k, dev).start()
        whole = dst.at[_top(len(devs))]
        return pltpu.make_async_copy(whole, whole, recv.at[k]), pltpu.make_async_copy(whole, whole, send.at[k])

    def local(src, dst, sem):
        cp = pltpu.make_async_copy(src, dst, sem)
        cp.start()
        return cp

    x_at, ext_at = 2 * rm, 4 * rm

    def xload(k):
        s = lax.rem(k, 4)
        to = dz.at[pl.ds(pl.multiple_of(x_at + s * chunk, chunk), chunk)]
        return pltpu.make_async_copy(x4.at[k, xc], to, tsem.at[s])

    with scope("prep"):
        for k in range(3):
            xload(k).start()
        own = xc
        cps = []
        for j in TWO:
            def widen(r, j=j):
                od[0, j, r, :] = e_ref[pl.ds(j * ha + r.start, r.size), :].astype(F32)

            _loop_rows(ha, 16, widen)
            cps.append(local(od.at[0, j, _top(ha)], eg.at[own, pl.ds(j * ha, ha)], hsem.at[j]))
        oext[...] = jnp.zeros_like(oext)
        oext[0 : rows - rm, :] = e_ref[rm:rows, :].astype(F32)
        cps.append(local(oext, eg.at[own, pl.ds(rm, 8)], hsem.at[2]))
        pl.semaphore_wait(bar, 22)

    half_a, half_b = _top(ha), pl.ds(ha, ha + 8)
    cut = ha + 8
    part_r, part_l, strip = _top(cut), pl.ds(cut, dm.pad - cut), pl.ds(ha, cut - ha)

    def piece(s, r, dev):
        return remote(eg.at[s, r], eg.at[s, r], dev)

    def slot(xx):
        return xx * 2 + c

    cps[0].wait()
    r_a = piece(own, half_a, xp)
    for cp in cps[1:]:
        cp.wait()
    l_b = piece(own, half_b, xm)
    s_o = piece(own, _top(dm.pad), sib)
    r_b, l_a = piece(own, half_b, xp), piece(own, half_a, xm)

    gain = g_ref[...]

    with scope("norm"):
        @pl.loop(0, 16)
        def _(k):
            @pl.when(k < 13)
            def _():
                xload(k + 3).start()

            xload(k).wait()

            def norm(r):
                v = dz[pl.ds(pl.multiple_of(x_at + lax.rem(k, 4) * chunk + r.start, r.size), r.size), :].astype(F32)
                inv = lax.rsqrt(jnp.mean(v * v, axis=-1, keepdims=True) + NORM_EPS)
                hv[pl.ds(pl.multiple_of(k * chunk + r.start, r.size), r.size), :] = (v * inv * gain).astype(BF16)

            _loop_rows(chunk, 16, norm)

    with scope("labels"):
        total = jnp.sum(msk[...])
        for k in range(16):
            at = pl.ds(k * chunk, chunk)
            w_row[:, at] = msk[k, xc] / total
            q = lab[k, xc] - zy * (8 * rows)
            s = jnp.zeros_like(q)
            for i in range(1, 8):
                s = s + jnp.where(q >= i * rows, 1, 0)
            r = q - s * rows
            up = jnp.where(r >= ha, 1, 0)
            at_main = ((s // 2 * 2 + up) * 2 + s % 2) * ha + r - up * ha
            at_ext = dm.main + s * 8 + r - rm
            place = jnp.where(r < rm, at_main, at_ext)
            pos_row[:, at] = jnp.where((q >= 0) & (q < 8 * rows), place, -1).astype(F32)

    def product(lhs, lanes):
        v = lax.dot_general(lhs, hv[lanes, :], (((1,), (1,)), ((), ())), preferred_element_type=F32)
        return v * (LOG2E / LOGIT_SCALE)

    def add_stats(v, lanes):
        m_old, s_old = m_row[:, lanes], s_row[:, lanes]
        m = jnp.maximum(m_old, jnp.max(v, axis=0, keepdims=True))
        s = jnp.sum(jnp.exp2(v - m), axis=0, keepdims=True)
        m_row[:, lanes] = m
        s_row[:, lanes] = s_old * jnp.exp2(m_old - m) + s

    def add_target(v, place, lanes):
        r = lax.broadcasted_iota(jnp.int32, v.shape, 0)
        hit = r.astype(F32) == pos_row[:, lanes] - place.astype(F32)
        tgt_row[:, lanes] += jnp.sum(jnp.where(hit, v, 0.0), axis=0, keepdims=True)

    m_row[:, :] = jnp.full((1, tok), -jnp.inf, F32)
    s_row[:, :] = jnp.zeros((1, tok), F32)
    tgt_row[:, :] = jnp.zeros((1, tok), F32)
    segs = [(half, j) for half in TWO for j in TWO]

    def load(r0, n, xx, cores=TWO):
        return [
            local(
                eg.at[xx[half] * 2 + j, pl.ds(half * ha + r0, n)],
                od.at[j, half, pl.ds(r0, n)],
                hsem.at[half * len(cores) + k],
            )
            for half in TWO
            for k, j in enumerate(cores)
        ]

    def narrow_all(r0, n, src, cores=TWO):
        for half in TWO:
            for j in cores:
                def narrow(r, half=half, j=j):
                    at = pl.multiple_of((half * 2 + j) * ha + r0 + r.start, r.size)
                    dz[pl.ds(at, r.size), :] = src(half, j)[r, :].astype(BF16)

                _loop_rows(n, 16, narrow)

    def load_narrow(r0, n, xx, core):
        for cp in load(r0, n, xx, (core,)):
            cp.wait()
        narrow_all(r0, n, lambda half, j: od.at[j, half, pl.ds(r0, n)], (core,))

    def block(r0, n, xx, loads=(), with_few=False, nt=nt):
        if loads:
            for cp in loads:
                cp.wait()
            narrow_all(r0, n, lambda half, j: od.at[j, half, pl.ds(r0, n)])
        left = [VOCAB_REAL - ((zy * 8 + xx[half] * 2 + j) * rows + half * ha + r0) for half, j in segs]
        w, tall = nt // chunk, len(segs) * n
        pack = tst.shape[1] // tall
        deep = SLOTS // w
        packed = SLOTS * pack >= tok // chunk

        def place(t, i):
            if packed:
                return t * (w // pack) + i // pack, i % pack * tall
            return lax.rem(t, deep) * w + i, 0

        def out(t):
            cps = []
            for i in range(w):
                u, row = place(t, i)
                for m, (half, j) in enumerate(segs):
                    to = pl.ds(pl.multiple_of((xx[half] * 2 + half) * rm + j * ha + r0, 8), n)
                    cps.append(pltpu.make_async_copy(tst.at[u, pl.ds(row + m * n, n)], zh.at[t * w + i, to], tsem.at[u]))
            return cps

        def out_wait(u, rows_):
            whole = tst.at[u, _top(rows_)]
            pltpu.make_async_copy(whole, whole, tsem.at[u]).wait()

        @pl.loop(0, tok // nt)
        def _(t):
            if not packed:
                @pl.when(t >= deep)
                def _():
                    for i in range(w):
                        out_wait(place(t, i)[0], tall)

            lanes = pl.ds(pl.multiple_of(t * nt, nt), nt)
            lhs = [dz[(half * 2 + j) * ha + r0 : (half * 2 + j) * ha + r0 + n, :] for half, j in segs]
            if with_few:
                lhs.append(dz[ext_at : ext_at + FEW, :])
            v = product(jnp.concatenate(lhs, axis=0), lanes)
            v, v_few = v[:tall], v[tall:]
            r = lax.broadcasted_iota(jnp.int32, (n, nt), 0)
            v = [jnp.where(r < left[m], v[m * n : (m + 1) * n], -jnp.inf) for m in range(len(segs))]
            for part_v, (half, j) in zip(v, segs):
                add_target(part_v, (xx[half] * 2 + half) * rm + j * ha + r0, lanes)
            for i in range(w):
                u, row = place(t, i)
                for m in range(len(segs)):
                    tst[u, row + m * n : row + (m + 1) * n, :] = v[m][:, i * chunk : (i + 1) * chunk]
            if with_few:
                r = lax.broadcasted_iota(jnp.int32, v_few.shape, 0)
                ok = ((r & 7) < rows - rm) & ((zy * 8 + (r >> 3)) * rows + rm + (r & 7) < VOCAB_REAL)
                v_few = jnp.where(ok, v_few, -jnp.inf)
                few[:, lanes] = v_few
                add_target(v_few, jnp.int32(dm.main), lanes)
                v.append(v_few)
            v = jnp.concatenate(v, axis=0)
            for cp in out(t):
                cp.start()
            add_stats(v, lanes)

        if packed:
            for u in range(tok // chunk // pack):
                out_wait(u, pack * tall)
        else:
            for u in range(deep * w):
                out_wait(u, tall)

    def both(xx):
        block(0, ha, xx, load(0, ha, xx))

    def turn(xx):
        for half in TWO:
            base = pl.multiple_of((xx[half] * 2 + half) * rm, rm)

            @pl.loop(0, dim // LANES)
            def _(d, half=half, base=base):
                at = pl.ds(pl.multiple_of(d * LANES, LANES), LANES)
                etv[at, pl.ds(base, rm)] = dz[half * rm : (half + 1) * rm, at].T

    with scope("own"):
        s_o.wait_recv()
        both((x, x))
        turn((x, x))

    with scope("wait_1"):
        r_a.wait_recv()
        last_n = dm.cuts[-1][1]
        spans = [(pl.ds(r0, n), pl.ds(ha + r0, n + 8 * (r0 + n == ha))) for r0, n in dm.cuts]

        def far_pieces(xx, half, to):
            cps = [piece(slot(xx), pair[half], to) for pair in spans[:-1]]
            cps.append(remote(eg.at[slot(xx), spans[-1][half]], sst.at[c, pl.ds(half * last_n, last_n)], to))
            return cps

        r_f = far_pieces(x_m, 0, xp)
        d = [piece(slot(x_m), half_a, sib)]
        l_b.wait_recv()
        l_f = far_pieces(x_p, 1, xm)
        d.append(piece(slot(x_p), half_b, sib))
        for cp in d:
            cp.wait_recv()

    with scope("near_1"):
        both((x_m, x_p))
        turn((x_m, x_p))

    with scope("wait_2"):
        r_b.wait_recv()
        d = [piece(slot(x_m), half_b, sib)]
        l_a.wait_recv()
        d.append(piece(slot(x_p), half_a, sib))
        for cp in d:
            cp.wait_recv()

    with scope("near_2"):
        both((x_p, x_m))
        turn((x_p, x_m))

    far = (x_far, x_far)

    with scope("wait_3"):
        d = []
        for cp, r in zip((r_f[0], l_f[0]), spans[0]):
            cp.wait_recv()
            d.append(piece(slot(x_far), r, sib))
        load_narrow(*dm.cuts[0], far, c)
        for cp in d:
            cp.wait_recv()
    with scope("far_a"):
        ext_loads = [local(eg.at[s, pl.ds(rm, 8)], few.at[pl.ds(s * 8, 8)], lsem.at[s]) for s in range(8)]
        load_narrow(*dm.cuts[0], far, 1 - c)
        for cp in ext_loads:
            cp.wait()
        dz[ext_at : ext_at + FEW, :] = few[...].astype(BF16)
        dz[ext_at + FEW : ext_at + LANES, :] = jnp.zeros((FEW, dim), BF16)
        block(*dm.cuts[0], far, with_few=True)
    with scope("wait_5"):
        r_f[-1].wait_recv()
        l_f[-1].wait_recv()
        both_last = sst.at[c, _top(2 * last_n)]
        over = _remote(both_last, both_last, send, recv, next(ids), sib)
        over.start()

        @pl.loop(0, dim // LANES)
        def _(i):
            at = pl.ds(pl.multiple_of(i * LANES, LANES), LANES)
            etv[at, dm.main : dm.wide] = dz[ext_at : ext_at + LANES, at].T

        def last_rows(half, j):
            return sst.at[j, pl.ds(half * last_n, last_n)]

        narrow_all(0, last_n, last_rows, (c,))
        over.wait_recv()

    with scope("far_c"):
        narrow_all(0, last_n, last_rows, (1 - c,))
        block(0, last_n, far, nt=8 * chunk)
        over.wait_send()
        for s in TWO:
            pl.semaphore_signal(free.at[s], inc=1, device_id=(sib,), device_id_type=MESH)

    with scope("turn_far"):
        lse_row[:, :] = m_row[:, :] + jnp.log(s_row[:, :]) * LOG2E
        stats = exchange(lse_row, got, near)
        turn(far)

    wide = 2 * rm

    at_dht = SLOTS - 4

    def chunk_of(zz, yy):
        return _mod4(zz) * 4 + _rem(yy + 8, 4)

    def all_far(i):
        return x_far * wide + i // 16 * rm, _rem(i, 16)

    def in_order(i):
        n = i // 3
        m = n - 7
        k = _pick(n < 7, chunk_of(z + n - 1, y + 2), chunk_of(z + 3 + m // 3, y + 3 + _rem(m + 9, 3)))
        return _mod4(x + 3 + _rem(i, 3)) * wide, _pick(n < 4, chunk_of(z + 2, n), k)

    def later(i):
        return in_order(i + SLOTS)

    def zload(where, i, ring, n):
        at, k = where(i)
        s = _rem(i, ring)
        src = zh.at[k, pl.ds(pl.multiple_of(at, rm), n)]
        return pltpu.make_async_copy(src, tst.at[s, _top(n)], tsem.at[s])

    def zahead(where, ring, n):
        for i in range(ring):
            zload(where, i, ring, n).start()

    with scope("stats"):
        zahead(all_far, SLOTS, rm)
        for cp in stats:
            cp.wait()
        top = lse_row[:, :]
        for k in range(len(near)):
            top = jnp.maximum(top, got[k])
        s = jnp.exp2(lse_row[:, :] - top)
        for k in range(len(near)):
            s = s + jnp.exp2(got[k] - top)
        lse_row[:, :] = top + jnp.log(s) * LOG2E

    def dz_part(v, place, at, lanes):
        r = lax.broadcasted_iota(jnp.int32, v.shape, 0).astype(F32)
        hit = r == pos_row[:, lanes] - place.astype(F32)
        p = jnp.exp2(v - lse_row[:, lanes])
        dz[at, lanes] = (jnp.where(hit, p - 1.0, p) * w_row[:, lanes]).astype(BF16)

    step = min(LANES, rm)

    def dz_rows(where, start, stop, last_tile, ring, n):
        @pl.loop(start, stop)
        def _(i):
            @pl.when((i > 0) & (i + ring - 1 < last_tile))
            def _():
                zload(where, i + ring - 1, ring, n).start()

            zload(where, i, ring, n).wait()
            row, k = where(i)
            lanes = pl.ds(pl.multiple_of(k * chunk, chunk), chunk)

            @pl.loop(0, n // step)
            def _(j):
                at = pl.multiple_of(row + j * step, step)
                r = pl.ds(pl.multiple_of(j * step, step), step)
                dz_part(tst[lax.rem(i, ring), r, :], at, pl.ds(at, step), lanes)

    def dz_far(start, stop):
        dz_rows(all_far, start, stop, 32, SLOTS, rm)

    with scope("dz_far"):
        dz_far(0, 16)

    nd = dim // 2
    few_rows = pl.ds(dm.main, FEW)
    pair_ids = [(next(ids), next(ids)) for _ in TWO]

    def over_d2d(s, n, i):
        lanes = pl.ds(pl.multiple_of(i * nd, nd), nd)
        there = sst.at[s, _top(n), lanes]
        return _remote(od.at[s, 1 - c, _top(n), lanes], there, send, recv, pair_ids[s][0] + i, sib)

    def de_block(xx, half, s, with_few=False):
        at = pl.ds(pl.multiple_of((xx * 2 + half) * rm, rm), rm)
        n = ha + 8 * half
        pl.semaphore_wait(free.at[s], 1)

        @pl.loop(0, 2)
        def _(i):
            lanes = pl.ds(pl.multiple_of(i * nd, nd), nd)
            lhs = jnp.concatenate([dz[at, :], dz[few_rows, :]], axis=0) if with_few else dz[at, :]
            v = jnp.dot(lhs, hv[:, lanes], preferred_element_type=F32)
            if with_few:
                few[:, lanes] = v[rm:]
            for j in TWO:
                od[s, j, 0:ha, lanes] = v[j * ha : (j + 1) * ha]
                if half:
                    od[s, j, ha:n, lanes] = few[pl.ds(pl.multiple_of((xx * 2 + j) * 8, 8), 8), lanes]
            over_d2d(s, n, i).start()

        return half, s, n

    def stored(blk, to):
        half, s, n = blk
        return pltpu.make_async_copy(od.at[s, c, _top(n)], to.at[pl.ds(half * ha, n)], dsem.at[s])

    def early(blk, src):
        half, s, n = blk
        for i in TWO:
            over_d2d(s, n, i).wait_send()
        return local(src.at[pl.ds(half * ha, n)], od.at[s, 1 - c, _top(n)], lsem.at[s])

    def sum_add(blk, to, more=None):
        half, s, n = blk
        for i in TWO:
            over_d2d(s, n, i).wait_recv()
        if more is not None:
            more.wait()

        def add(r):
            v = od[s, c, r, :] + sst[s, r, :]
            od[s, c, r, :] = v if more is None else v + od[s, 1 - c, r, :]

        _loop_rows(n, 8, add)
        if more is None:
            pl.semaphore_signal(free.at[s], inc=1, device_id=(sib,), device_id_type=MESH)
            for i in TWO:
                over_d2d(s, n, i).wait_send()
        cp = stored(blk, to)
        cp.start()
        return cp

    def ring_sum(xx, rows_, n, src, s, dst, dev):
        lds = [
            local(q_h.at[xx, rows_], od.at[s, 0, _top(n)], lsem.at[0]),
            local(src, od.at[s, 1, _top(n)], lsem.at[1]),
        ]
        for cp in lds:
            cp.wait()
        _add_rows(od.at[s, 0, _top(n)], [od.at[s, 1, _top(n)]], 8)
        local(od.at[s, 0, _top(n)], q_h.at[xx, rows_], lsem.at[0]).wait()
        return remote(q_h.at[xx, rows_], dst, dev)

    stores = []

    def flush():
        while stores:
            stores.pop().wait()

    def tiles(q, where, between=None):
        flush()

        def outs(i):
            p, ab = where(i)
            r = pl.ds(q * h, h)
            dsts = [dhp.at[ab * 2 + j, p, r] if q == 0 else dhp.at[p, ab * 2 + j, r] for j in TWO]
            return [
                pltpu.make_async_copy(tst.at[at_dht + i * 2 + j, _top(h)], dst, hsem.at[i * 2 + j])
                for j, dst in enumerate(dsts)
            ]

        @pl.loop(0, 2)
        def _(i):
            if between is not None:
                pl.when(i > 0)(between)
            p, ab = where(i)
            ks = [(ab * 2 + j) * 4 + p if q == 0 else p * 4 + ab * 2 + j for j in TWO]
            rhs = jnp.concatenate([dz[:, pl.ds(pl.multiple_of(k * chunk, chunk), chunk)] for k in ks], axis=1)
            v = jnp.dot(etv[q * h : (q + 1) * h, :], rhs, preferred_element_type=F32)
            for j in TWO:
                tst[at_dht + i * 2 + j, 0:h, :] = v[:, j * chunk : (j + 1) * chunk]
            for cp in outs(i):
                cp.start()

        for i in TWO:
            stores.extend(outs(i))

    def part(q, p, lo, n):
        r = pl.ds(q * h, h)
        if q == 0:
            return dhp.at[pl.ds(lo, n), p, r]
        return dhp.at[p, pl.ds(lo, n), r]

    def one(q, p, i):
        r = pl.ds(q * h, h)
        return dhp.at[i, p, r] if q == 0 else dhp.at[p, i, r]

    ring1, ring2 = ((yp, ym), (zp, zm)), ((zp, zm), (yp, ym))
    pos1, pos2 = (y, z), (z, y)
    first, second = ({}, {}), ({}, {})

    def send_far(q):
        flush()
        p, (rt, lt) = pos1[q], ring1[q]
        first[q]["far_r"] = remote(part(q, _mod4(p + 2), 0, 2), ya.at[q], rt)
        first[q]["far_l"] = remote(part(q, _mod4(p + 2), 2, 2), yb.at[q], lt)

    def send_near(q):
        flush()
        p, (rt, lt) = pos1[q], ring1[q]
        first[q]["near_r"] = remote(part(q, _mod4(p + 1), 2, 2), yl.at[q, pl.ds(2, 2)], rt)
        first[q]["near_l"] = remote(part(q, _mod4(p - 1), 0, 2), yr.at[q, _top(2)], lt)

    def fetch(i, src):
        return local(src, tst.at[i, _top(h)], tsem.at[i])

    def pass_on(q):
        flush()
        p, (rt, lt) = pos1[q], ring1[q]
        lds = [fetch(i, one(q, _mod4(p + 1), i)) for i in TWO]
        lds += [fetch(2 + i, one(q, _mod4(p - 1), 2 + i)) for i in TWO]
        first[q]["far_r"].wait_recv()
        for i in TWO:
            lds[i].wait()
            _add_rows(ya.at[q, i], [tst.at[i, _top(h)]], min(FEW, h))
        first[q]["sum_r"] = remote(ya.at[q], yl.at[q, _top(2)], rt)
        first[q]["far_l"].wait_recv()
        for i in TWO:
            lds[2 + i].wait()
            _add_rows(yb.at[q, i], [tst.at[2 + i, _top(h)]], min(FEW, h))
        first[q]["sum_l"] = remote(yb.at[q], yr.at[q, pl.ds(2, 2)], lt)

    lo, hi = _top(hc), pl.ds(hc, hc)

    def second_phase(q):
        flush()
        r, (rt, lt) = pos2[q], ring2[q]
        r2, r1, rm1 = _mod4(r + 2), _mod4(r + 1), _mod4(r - 1)
        order = (r2, r1, rm1, r)
        lds = [fetch(i, one(q, pos1[q], k)) for i, k in enumerate(order)]
        for k in NEAR_KEYS:
            first[q][k].wait_recv()
        lds2 = [fetch(4 + i, yr.at[q, k]) for i, k in enumerate(order)]
        for i, k in enumerate(order):
            lds[i].wait()
            lds2[i].wait()
            _add_rows(yl.at[q, k], [tst.at[i, _top(h)], tst.at[4 + i, _top(h)]], min(FEW, h))
            if i == 0:
                second[q]["far_r"] = remote(yl.at[q, r2, lo], za.at[q], rt)
                second[q]["far_l"] = remote(yl.at[q, r2, hi], zb.at[q], lt)
            if i == 1:
                second[q]["near_r"] = remote(yl.at[q, r1, hi], zl.at[q, hi], rt)
            if i == 2:
                second[q]["near_l"] = remote(yl.at[q, rm1, lo], zr.at[q, lo], lt)

    def second_pass(q):
        r, (rt, lt) = pos2[q], ring2[q]
        r1, rm1 = _mod4(r + 1), _mod4(r - 1)
        second[q]["far_r"].wait_recv()
        _add_rows(yl.at[q, r1, lo], [za.at[q]], min(FEW, hc))
        second[q]["sum_r"] = remote(yl.at[q, r1, lo], zl.at[q, lo], rt)
        second[q]["far_l"].wait_recv()
        _add_rows(yl.at[q, rm1, hi], [zb.at[q]], min(FEW, hc))
        second[q]["sum_l"] = remote(yl.at[q, rm1, hi], zr.at[q, hi], lt)

    def last(q):
        r = pos2[q]
        for k in NEAR_KEYS:
            second[q][k].wait_recv()
        n = min(LANES, h)

        @pl.loop(0, h // n)
        def _(i):
            at = pl.ds(pl.multiple_of(i * n, n), n)
            v = yl[q, r, at, :] + zl[q, at, :] + zr[q, at, :]
            od[0, 0, 0:chunk, pl.ds(pl.multiple_of(q * h + i * n, n), n)] = (v * (1.0 / LOGIT_SCALE)).T

    def tiles_far(q, between=None):
        tiles(q, lambda i: (_mod4(pos1[q] + 2), i), between)

    def tiles_near(q):
        tiles(q, lambda i: (_mod4(pos1[q] + 1 + 2 * i), 1 - i))

    def tiles_pass(q):
        tiles(q, lambda i: (_mod4(pos1[q] + 1 + 2 * i), i))

    def tiles_own(q):
        tiles(q, lambda i: (pos1[q], i))

    all_later = 48 - SLOTS

    def dz_first(start, stop):
        dz_rows(in_order, start, stop, SLOTS, SLOTS, wide)

    def dz_later(start, stop):
        dz_rows(later, start, stop, all_later, at_dht, wide)

    with scope("de_far"):
        b0 = de_block(x_far, 0, 0)
        dz_far(16, 32)
        zahead(in_order, SLOTS, wide)
        for l in range(0, tok, nt):
            lanes = pl.ds(l, nt)
            dz_part(few[:, lanes], jnp.int32(dm.main), few_rows, lanes)
        dz[dm.main + FEW : dm.wide, :] = jnp.zeros((FEW, tok), BF16)
        b1 = de_block(x_far, 1, 1, True)
    with scope("dz_1"):
        c0 = sum_add(b0, q_h.at[x_far])
        dz_first(0, 8)
        c0.wait()
        e0 = [remote(q_h.at[x_far, half_a], xa.at[half_a], xp)]
        dz_first(8, SLOTS)
        zahead(later, at_dht, wide)
    with scope("dh_far1"):
        def between():
            sum_add(b1, q_h.at[x_far])

        tiles_far(1, between)
        c1 = stored(b1, q_h.at[x_far])
        c1.wait()
        e1 = remote(q_h.at[x_far, part_l], xb, xm)
        e0.append(remote(q_h.at[x_far, strip], xa.at[strip], xp))
    with scope("dz_2"):
        dz_later(0, 9)
        send_far(1)
    with scope("dh_far0"):
        tiles_far(0)
    with scope("dz_3"):
        dz_later(9, 13)
        send_far(0)
        dz_later(13, all_later)
    with scope("de_2"):
        b2 = de_block(x_p, 1, 0)
        b3 = de_block(x_m, 0, 1)
        c2 = sum_add(b2, q_h.at[x_p])
    with scope("dh_near"):
        tiles_near(1)
        c2.wait()
        e2 = remote(q_h.at[x_p, part_l], xe.at[part_l], xp)
        c3 = sum_add(b3, q_h.at[x_m])
        send_near(1)
        tiles_near(0)
        c3.wait()
        e3 = [remote(q_h.at[x_m, half_a], xe.at[half_a], xm)]
        send_near(0)
    with scope("dh_pass"):
        tiles_pass(1)
        tiles_pass(0)
        pass_on(1)
    with scope("de_4"):
        b4 = de_block(x_p, 0, 0)
        pass_on(0)
        b5 = de_block(x_m, 1, 1)
        c4 = sum_add(b4, q_h.at[x_p])
    with scope("dh_own"):
        tiles_own(1)
        c5 = sum_add(b5, q_h.at[x_m])
        tiles_own(0)
        c4.wait()
        c5.wait()
        e3.append(remote(q_h.at[x_m, strip], xe.at[strip], xm))
    old = list(sent)
    sent.clear()
    with scope("ring"):
        for cp in e0:
            cp.wait_recv()
        e4 = ring_sum(x_p, part_r, cut, xa, 0, xs.at[part_r], xp)
        e1.wait_recv()
        e5 = ring_sum(x_m, part_l, dm.pad - cut, xb, 1, xs.at[part_l], xm)
    with scope("de_6"):
        b6 = de_block(x, 0, 0)
    with scope("de_7"):
        b7 = de_block(x, 1, 1)
        xo_load = local(x4.at[zy, xc], dz.at[_top(chunk)], osem.at[0])
    with scope("second_1"):
        second_phase(1)
    with scope("second_0"):
        second_phase(0)
    with scope("spass_1"):
        second_pass(1)
    with scope("sum_6"):
        for cp in e3:
            cp.wait_recv()
        c6 = early(b6, xe)
        e2.wait_recv()
        c7 = early(b7, xe)
        c6 = sum_add(b6, q_o, c6)
        c7 = sum_add(b7, q_o, c7)
    with scope("spass_0"):
        second_pass(0)
        c6.wait()
        c7.wait()
    def drain(cps):
        while cps:
            cps.pop().wait_send()

    def own_x(r):
        v = dz[r, :].astype(F32)
        inv = lax.rsqrt(jnp.mean(v * v, axis=-1, keepdims=True) + NORM_EPS)
        od[1, 0, r, :] = v * inv
        od[1, 1, r, 0:LANES] = jnp.broadcast_to(inv, (r.size, LANES))

    def own_dg(q):
        lanes = pl.ds(q * h, h)

        def add(i, acc):
            r = pl.ds(pl.multiple_of(i * 8, 8), 8)
            return acc + od[0, 0, r, lanes] * od[1, 0, r, lanes]

        acc = lax.fori_loop(0, chunk // 8, add, jnp.zeros((8, h), F32))
        sm[:, lanes] = jnp.sum(acc, axis=0, keepdims=True)

    def own_dx(r):
        x_hat, u = od[1, 0, r, :], od[0, 0, r, :] * gain
        od[0, 1, r, :] = od[1, 1, r, 0:1] * (u - x_hat * jnp.mean(u * x_hat, axis=-1, keepdims=True))

    with scope("own_x"):
        xo_load.wait()
        _loop_rows(chunk, 16, own_x)
        lse = jnp.where(zy == 0, lse_row[:, :], 0.0)
        loss = jnp.sum(w_row[:, :] * (lse - tgt_row[:, :]))
        sm[:, dim : dim + LANES] = jnp.full((1, LANES), loss / LOG2E)
        drain(old)
    with scope("last_1"):
        last(1)
        own_dg(1)
    with scope("last_0"):
        last(0)
        own_dg(0)

    with scope("small_1"):
        old = [cp for cp in sent if cp is not e4 and cp is not e5]
        near_sums = exchange(sm, got1, near)
        _loop_rows(chunk, 16, own_dx)
        dx_copy = local(od.at[0, 1, _top(chunk)], dx_out, osem.at[0])
        drain(old)
        for cp in near_sums:
            cp.wait()
    with scope("small_2"):
        tot = sm[...]
        for k in range(len(near)):
            tot = tot + got1[k]
        total_v[...] = tot
        all_sums = exchange(total_v, got2, line)
        mine = local(total_v, got2.at[len(line)], osem.at[1])
    with scope("ring_end"):
        for cp in (e4, e5):
            cp.wait()
        dx_copy.wait()
        mine.wait()
    with scope("small_3"):
        for cp in all_sums:
            cp.wait()


def _run(dm, x4, table, gain, labels, mask):
    hbm, vm = pl.BlockSpec(memory_space=HBM), pl.BlockSpec(memory_space=VMEM)
    sd = jax.ShapeDtypeStruct
    d, tok, h, ck, pad, ha = dm.dim, dm.tok, dm.h, dm.chunk, dm.pad, dm.ha
    line, quad, pair = VMEM((1, tok), F32), VMEM((2, 2, h, ck), F32), VMEM((2, h, ck), F32)
    part, shard = VMEM((2, h // 2, ck), F32), sd((pad, d), F32)
    out = pl.pallas_call(
        functools.partial(_kernel, dm),
        name="head",
        out_shape=(
            sd((ck, d), F32), sd((8, 1, d + LANES), F32),
            shard, shard, shard,
            sd((8, pad, d), F32), sd((16, dm.main, ck), F32),
            sd((4, pad, d), F32), sd((ha + 8, d), F32), sd((ha, d), F32),
            sd((4, 4, d, ck), F32), sd((2, 4, h, ck), F32),
        ),
        in_specs=[hbm, vm, vm, vm, vm],
        out_specs=[hbm] * 12,
        scratch_shapes=[
            VMEM((tok, d), BF16), VMEM((d, dm.wide), BF16), VMEM((dm.wide, tok), BF16),
            VMEM((2, 2, ha + 8, d), F32), VMEM((2, ha + 8, d), F32), VMEM((FEW, d), F32), VMEM((8, d), F32),
            quad, quad, VMEM((2, 4, h, ck), F32),
            part, part, pair, pair,
            VMEM((SLOTS, max(h, 2 * dm.rm), ck), F32),
            line, line, line, line, line, line, VMEM((15, 1, tok), F32),
            VMEM((1, d + LANES), F32), VMEM((15, 1, d + LANES), F32), VMEM((1, d + LANES), F32),
            DMA((55,)), DMA((55,)), pltpu.SemaphoreType.REGULAR((2,)),
            DMA((SLOTS,)), DMA((4,)), DMA((2,)), DMA((2,)), DMA((8,)),
        ],
        compiler_params=pltpu.CompilerParams(
            collective_id=0, has_side_effects=True, vmem_limit_bytes=67043328
        ),
    )(x4, table, gain, labels, mask)
    return _write_out(dm, out[2:4], *out[:2])


def _write_kernel(own, ring, dx, small, de_o, dx_o, dg_o, loss_o):
    de_o[:, :] = (own[:, :] + ring[:, :]) * (1.0 / LOGIT_SCALE)
    dx_o[:, :] = dx[:, :]
    total = jnp.sum(small[:, :, :], axis=0)
    d = dg_o.shape[1]
    dg_o[:, :] = total[:, :d]
    loss_o[:, :] = total[:, d : d + 1]


def _write_out(dm, parts, dx, small):
    d, step, blocks = dm.dim, dm.ha + 8, 2
    sd = jax.ShapeDtypeStruct
    some = pl.BlockSpec((step, d), lambda i: (i, 0))
    half = pl.BlockSpec((dm.chunk // blocks, d), lambda i: (i, 0))
    row, one = pl.BlockSpec((1, d), lambda i: (0, 0)), pl.BlockSpec((1, 1), lambda i: (0, 0))
    rows = pl.BlockSpec(small.shape, lambda i: (0, 0, 0))
    return pl.pallas_call(
        _write_kernel,
        name="write_out",
        grid=(blocks,),
        out_shape=(sd((dm.rows, d), F32), sd((dm.chunk, d), F32), sd((1, d), F32), sd((1, 1), F32)),
        in_specs=[some, some, half, rows],
        out_specs=(some, half, row, one),
    )(*parts, dx, small)


def solution(mesh):
    group = mesh.shape[AXIS]

    def local_step(residual, labels, loss_mask, norm_gain, table_shard):
        tokens, dim = residual.shape
        rows = table_shard.shape[0]
        dm = Dims(tokens, dim, rows, group)
        x4 = residual.reshape(16, 8, dm.chunk, dim)
        lab = labels.reshape(16, 8, 1, dm.chunk)
        msk = loss_mask.reshape(16, 8, 1, dm.chunk)
        d_embed, d_res, d_gain, loss = _run(dm, x4, table_shard, norm_gain[None, :], lab, msk)
        return loss.reshape(()), d_res, d_embed, d_gain.reshape(dim)

    return jax.shard_map(
        local_step,
        mesh=mesh,
        in_specs=(P(), P(), P(), P(), P(AXIS, None)),
        out_specs=(P(), P(AXIS, None), P(AXIS, None), P()),
        check_vma=False,
    )
```

```python
import functools
import itertools
import math

import jax
import jax.numpy as jnp
from jax import lax
from jax.experimental import pallas as pl
from jax.experimental.pallas import tpu as pltpu
from jax.sharding import PartitionSpec as P

VOCAB_REAL = 49155
LOGIT_SCALE = 6.0
NORM_EPS = 1e-6

AXIS = "vp"
MESH = pl.DeviceIdType.MESH
F32 = jnp.float32
BF16 = jnp.bfloat16
HBM = pltpu.HBM
VMEM = pltpu.VMEM
DMA = pltpu.SemaphoreType.DMA


def _coords():
    me = lax.axis_index(AXIS)
    return me // 32, (me // 8) % 4, (me // 2) % 4, me % 2


def _dev(z, y, x, c):
    return ((z * 4 + y) * 4 + x) * 2 + c


def _mod4(v):
    return lax.rem(v + 8, 4)


def _barrier(peers):
    sem = pltpu.get_barrier_semaphore()
    for p in peers:
        pl.semaphore_signal(sem, inc=1, device_id=(p,), device_id_type=MESH)
    pl.semaphore_wait(sem, len(peers))


def _remote(src, dst, send, recv, k, dev):
    return pltpu.make_async_remote_copy(
        src_ref=src,
        dst_ref=dst,
        send_sem=send.at[k],
        recv_sem=recv.at[k],
        device_id=(dev,),
        device_id_type=MESH,
    )


LANES = 128


class Dims:
    def __init__(self, tokens, dim, rows, group):
        self.dim, self.rows = dim, rows
        unit = LANES if rows >= LANES else 64
        self.rm = rows // unit * unit
        self.ha = self.rm // 2
        low = max(16, self.ha // 48 * 16)
        self.cuts = ((low, self.ha - low), (0, low))
        self.pad = self.rm + 8
        self.chunk = tokens // group
        self.tok = 16 * self.chunk
        self.nt = 4 * self.chunk
        self.main = 8 * self.rm
        self.wide = self.main + LANES
        self.h = dim // 2


def _top(n):
    return pl.ds(0, n)


def _rem(a, b):
    return a % b if isinstance(a, int) else lax.rem(a, b)


def _pick(test, a, b):
    return (a if test else b) if isinstance(test, bool) else jnp.where(test, a, b)


def _loop_rows(rows, step, fn):
    @pl.loop(0, rows // step)
    def _(i):
        fn(pl.ds(pl.multiple_of(i * step, step), step))


def _add_rows(dst, srcs, step):
    def add(r):
        acc = dst[r, :]
        for s in srcs:
            acc = acc + s[r, :]
        dst[r, :] = acc

    _loop_rows(dst.shape[0], step, add)


SLOTS = 12
FEW = 64
TWO = range(2)
LOG2E = math.log2(math.e)
NEAR_KEYS = ("near_r", "near_l", "sum_r", "sum_l")
scope = jax.named_scope


def _kernel(
    dm, x4, e_ref, g_ref, lab, msk,
    dx_out, got2, q_o, xs, xe, eg, zh, q_h, xa, xb, dhp, yr,
    hv, etv, dz, od, sst, few, oext, ya, yb, yl, za, zb, zl, zr, tst,
    m_row, s_row, w_row, pos_row, lse_row, tgt_row, got, sm, got1, total_v,
    send, recv,
    free, tsem, hsem, dsem, osem, lsem,
):
    z, y, x, c = _coords()
    xc, zy = x * 2 + c, z * 4 + y
    rows, rm, ha, dim, h = dm.rows, dm.rm, dm.ha, dm.dim, dm.h
    chunk, tok, nt, hc = dm.chunk, dm.tok, dm.nt, dm.h // 2
    x_far, x_p, x_m = _mod4(x + 2), _mod4(x + 1), _mod4(x - 1)
    xp, xm = _dev(z, y, x_p, c), _dev(z, y, x_m, c)
    yp, ym = _dev(z, _mod4(y + 1), x, c), _dev(z, _mod4(y - 1), x, c)
    zp, zm = _dev(_mod4(z + 1), y, x, c), _dev(_mod4(z - 1), y, x, c)
    sib = _dev(z, y, x, 1 - c)
    near = [_dev(_mod4(z + a), _mod4(y + b), x, c) for a in range(4) for b in range(4) if a or b]
    line = [_dev(z, y, _mod4(x + a), lax.rem(c + b, 2)) for a in range(4) for b in TWO if a or b]
    bar = pltpu.get_barrier_semaphore()
    for p in (*near, *line):
        pl.semaphore_signal(bar, inc=1, device_id=(p,), device_id_type=MESH)
    sent = []
    ids = itertools.count()

    def remote(src, dst, dev):
        cp = _remote(src, dst, send, recv, next(ids), dev)
        cp.start()
        sent.append(cp)
        return cp

    def exchange(src, dst, devs):
        k = next(ids)
        for i, dev in enumerate(devs):
            _remote(src, dst.at[i], send, recv, k, dev).start()
        whole = dst.at[_top(len(devs))]
        return pltpu.make_async_copy(whole, whole, recv.at[k]), pltpu.make_async_copy(whole, whole, send.at[k])

    def local(src, dst, sem):
        cp = pltpu.make_async_copy(src, dst, sem)
        cp.start()
        return cp

    x_at, ext_at = 2 * rm, 4 * rm

    def xload(k):
        s = lax.rem(k, 4)
        to = dz.at[pl.ds(pl.multiple_of(x_at + s * chunk, chunk), chunk)]
        return pltpu.make_async_copy(x4.at[k, xc], to, tsem.at[s])

    with scope("prep"):
        for k in range(3):
            xload(k).start()
        own = xc
        cps = []
        for j in TWO:
            def widen(r, j=j):
                od[0, j, r, :] = e_ref[pl.ds(j * ha + r.start, r.size), :].astype(F32)

            _loop_rows(ha, 16, widen)
            cps.append(local(od.at[0, j, _top(ha)], eg.at[own, pl.ds(j * ha, ha)], hsem.at[j]))
        oext[...] = jnp.zeros_like(oext)
        oext[0 : rows - rm, :] = e_ref[rm:rows, :].astype(F32)
        cps.append(local(oext, eg.at[own, pl.ds(rm, 8)], hsem.at[2]))
        pl.semaphore_wait(bar, 22)

    half_a, half_b = _top(ha), pl.ds(ha, ha + 8)
    cut = ha + 8
    part_r, part_l, strip = _top(cut), pl.ds(cut, dm.pad - cut), pl.ds(ha, cut - ha)

    def piece(s, r, dev):
        return remote(eg.at[s, r], eg.at[s, r], dev)

    def slot(xx):
        return xx * 2 + c

    cps[0].wait()
    r_a = piece(own, half_a, xp)
    for cp in cps[1:]:
        cp.wait()
    l_b = piece(own, half_b, xm)
    s_o = piece(own, _top(dm.pad), sib)
    r_b, l_a = piece(own, half_b, xp), piece(own, half_a, xm)

    gain = g_ref[...]

    with scope("norm"):
        @pl.loop(0, 16)
        def _(k):
            @pl.when(k < 13)
            def _():
                xload(k + 3).start()

            xload(k).wait()

            def norm(r):
                v = dz[pl.ds(pl.multiple_of(x_at + lax.rem(k, 4) * chunk + r.start, r.size), r.size), :].astype(F32)
                inv = lax.rsqrt(jnp.mean(v * v, axis=-1, keepdims=True) + NORM_EPS)
                hv[pl.ds(pl.multiple_of(k * chunk + r.start, r.size), r.size), :] = (v * inv * gain).astype(BF16)

            _loop_rows(chunk, 16, norm)

    with scope("labels"):
        total = jnp.sum(msk[...])
        for k in range(16):
            at = pl.ds(k * chunk, chunk)
            w_row[:, at] = msk[k, xc] / total
            q = lab[k, xc] - zy * (8 * rows)
            s = jnp.zeros_like(q)
            for i in range(1, 8):
                s = s + jnp.where(q >= i * rows, 1, 0)
            r = q - s * rows
            up = jnp.where(r >= ha, 1, 0)
            at_main = ((s // 2 * 2 + up) * 2 + s % 2) * ha + r - up * ha
            at_ext = dm.main + s * 8 + r - rm
            place = jnp.where(r < rm, at_main, at_ext)
            pos_row[:, at] = jnp.where((q >= 0) & (q < 8 * rows), place, -1).astype(F32)

    def product(lhs, lanes):
        v = lax.dot_general(lhs, hv[lanes, :], (((1,), (1,)), ((), ())), preferred_element_type=F32)
        return v * (LOG2E / LOGIT_SCALE)

    def add_stats(v, lanes):
        m_old, s_old = m_row[:, lanes], s_row[:, lanes]
        m = jnp.maximum(m_old, jnp.max(v, axis=0, keepdims=True))
        s = jnp.sum(jnp.exp2(v - m), axis=0, keepdims=True)
        m_row[:, lanes] = m
        s_row[:, lanes] = s_old * jnp.exp2(m_old - m) + s

    def add_target(v, place, lanes):
        r = lax.broadcasted_iota(jnp.int32, v.shape, 0)
        hit = r.astype(F32) == pos_row[:, lanes] - place.astype(F32)
        tgt_row[:, lanes] += jnp.sum(jnp.where(hit, v, 0.0), axis=0, keepdims=True)

    m_row[:, :] = jnp.full((1, tok), -jnp.inf, F32)
    s_row[:, :] = jnp.zeros((1, tok), F32)
    tgt_row[:, :] = jnp.zeros((1, tok), F32)
    segs = [(half, j) for half in TWO for j in TWO]

    def load(r0, n, xx, cores=TWO):
        return [
            local(
                eg.at[xx[half] * 2 + j, pl.ds(half * ha + r0, n)],
                od.at[j, half, pl.ds(r0, n)],
                hsem.at[half * len(cores) + k],
            )
            for half in TWO
            for k, j in enumerate(cores)
        ]

    def narrow_all(r0, n, src, cores=TWO):
        for half in TWO:
            for j in cores:
                def narrow(r, half=half, j=j):
                    at = pl.multiple_of((half * 2 + j) * ha + r0 + r.start, r.size)
                    dz[pl.ds(at, r.size), :] = src(half, j)[r, :].astype(BF16)

                _loop_rows(n, 16, narrow)

    def load_narrow(r0, n, xx, core):
        for cp in load(r0, n, xx, (core,)):
            cp.wait()
        narrow_all(r0, n, lambda half, j: od.at[j, half, pl.ds(r0, n)], (core,))

    def block(r0, n, xx, loads=(), with_few=False, nt=nt):
        if loads:
            for cp in loads:
                cp.wait()
            narrow_all(r0, n, lambda half, j: od.at[j, half, pl.ds(r0, n)])
        left = [VOCAB_REAL - ((zy * 8 + xx[half] * 2 + j) * rows + half * ha + r0) for half, j in segs]
        w, tall = nt // chunk, len(segs) * n
        pack = tst.shape[1] // tall
        deep = SLOTS // w
        packed = SLOTS * pack >= tok // chunk

        def place(t, i):
            if packed:
                return t * (w // pack) + i // pack, i % pack * tall
            return lax.rem(t, deep) * w + i, 0

        def out(t):
            cps = []
            for i in range(w):
                u, row = place(t, i)
                for m, (half, j) in enumerate(segs):
                    to = pl.ds(pl.multiple_of((xx[half] * 2 + half) * rm + j * ha + r0, 8), n)
                    cps.append(pltpu.make_async_copy(tst.at[u, pl.ds(row + m * n, n)], zh.at[t * w + i, to], tsem.at[u]))
            return cps

        def out_wait(u, rows_):
            whole = tst.at[u, _top(rows_)]
            pltpu.make_async_copy(whole, whole, tsem.at[u]).wait()

        @pl.loop(0, tok // nt)
        def _(t):
            if not packed:
                @pl.when(t >= deep)
                def _():
                    for i in range(w):
                        out_wait(place(t, i)[0], tall)

            lanes = pl.ds(pl.multiple_of(t * nt, nt), nt)
            lhs = [dz[(half * 2 + j) * ha + r0 : (half * 2 + j) * ha + r0 + n, :] for half, j in segs]
            if with_few:
                lhs.append(dz[ext_at : ext_at + FEW, :])
            v = product(jnp.concatenate(lhs, axis=0), lanes)
            v, v_few = v[:tall], v[tall:]
            r = lax.broadcasted_iota(jnp.int32, (n, nt), 0)
            v = [jnp.where(r < left[m], v[m * n : (m + 1) * n], -jnp.inf) for m in range(len(segs))]
            for part_v, (half, j) in zip(v, segs):
                add_target(part_v, (xx[half] * 2 + half) * rm + j * ha + r0, lanes)
            for i in range(w):
                u, row = place(t, i)
                for m in range(len(segs)):
                    tst[u, row + m * n : row + (m + 1) * n, :] = v[m][:, i * chunk : (i + 1) * chunk]
            if with_few:
                r = lax.broadcasted_iota(jnp.int32, v_few.shape, 0)
                ok = ((r & 7) < rows - rm) & ((zy * 8 + (r >> 3)) * rows + rm + (r & 7) < VOCAB_REAL)
                v_few = jnp.where(ok, v_few, -jnp.inf)
                few[:, lanes] = v_few
                add_target(v_few, jnp.int32(dm.main), lanes)
                v.append(v_few)
            v = jnp.concatenate(v, axis=0)
            for cp in out(t):
                cp.start()
            add_stats(v, lanes)

        if packed:
            for u in range(tok // chunk // pack):
                out_wait(u, pack * tall)
        else:
            for u in range(deep * w):
                out_wait(u, tall)

    def both(xx):
        block(0, ha, xx, load(0, ha, xx))

    def turn(xx):
        for half in TWO:
            base = pl.multiple_of((xx[half] * 2 + half) * rm, rm)

            @pl.loop(0, dim // LANES)
            def _(d, half=half, base=base):
                at = pl.ds(pl.multiple_of(d * LANES, LANES), LANES)
                etv[at, pl.ds(base, rm)] = dz[half * rm : (half + 1) * rm, at].T

    with scope("own"):
        s_o.wait_recv()
        both((x, x))
        turn((x, x))

    with scope("wait_1"):
        r_a.wait_recv()
        last_n = dm.cuts[-1][1]
        spans = [(pl.ds(r0, n), pl.ds(ha + r0, n + 8 * (r0 + n == ha))) for r0, n in dm.cuts]

        def far_pieces(xx, half, to):
            cps = [piece(slot(xx), pair[half], to) for pair in spans[:-1]]
            cps.append(remote(eg.at[slot(xx), spans[-1][half]], sst.at[c, pl.ds(half * last_n, last_n)], to))
            return cps

        r_f = far_pieces(x_m, 0, xp)
        d = [piece(slot(x_m), half_a, sib)]
        l_b.wait_recv()
        l_f = far_pieces(x_p, 1, xm)
        d.append(piece(slot(x_p), half_b, sib))
        for cp in d:
            cp.wait_recv()

    with scope("near_1"):
        both((x_m, x_p))
        turn((x_m, x_p))

    with scope("wait_2"):
        r_b.wait_recv()
        d = [piece(slot(x_m), half_b, sib)]
        l_a.wait_recv()
        d.append(piece(slot(x_p), half_a, sib))
        for cp in d:
            cp.wait_recv()

    with scope("near_2"):
        both((x_p, x_m))
        turn((x_p, x_m))

    far = (x_far, x_far)

    with scope("wait_3"):
        d = []
        for cp, r in zip((r_f[0], l_f[0]), spans[0]):
            cp.wait_recv()
            d.append(piece(slot(x_far), r, sib))
        load_narrow(*dm.cuts[0], far, c)
        for cp in d:
            cp.wait_recv()
    with scope("far_a"):
        ext_loads = [local(eg.at[s, pl.ds(rm, 8)], few.at[pl.ds(s * 8, 8)], lsem.at[s]) for s in range(8)]
        load_narrow(*dm.cuts[0], far, 1 - c)
        for cp in ext_loads:
            cp.wait()
        dz[ext_at : ext_at + FEW, :] = few[...].astype(BF16)
        dz[ext_at + FEW : ext_at + LANES, :] = jnp.zeros((FEW, dim), BF16)
        block(*dm.cuts[0], far, with_few=True)
    with scope("wait_5"):
        over = []
        for half, cp in enumerate((r_f[-1], l_f[-1])):
            cp.wait_recv()
            ref = sst.at[c, pl.ds(half * last_n, last_n)]
            over.append(_remote(ref, ref, send, recv, next(ids), sib))
            over[-1].start()

        @pl.loop(0, dim // LANES)
        def _(i):
            at = pl.ds(pl.multiple_of(i * LANES, LANES), LANES)
            etv[at, dm.main : dm.wide] = dz[ext_at : ext_at + LANES, at].T

        def last_rows(half, j):
            return sst.at[j, pl.ds(half * last_n, last_n)]

        narrow_all(0, last_n, last_rows, (c,))
        for cp in over:
            cp.wait_recv()

    with scope("far_c"):
        narrow_all(0, last_n, last_rows, (1 - c,))
        block(0, last_n, far, nt=8 * chunk)
        for cp in over:
            cp.wait_send()
        for s in TWO:
            pl.semaphore_signal(free.at[s], inc=1, device_id=(sib,), device_id_type=MESH)

    with scope("turn_far"):
        lse_row[:, :] = m_row[:, :] + jnp.log(s_row[:, :]) * LOG2E
        stats = exchange(lse_row, got, near)
        turn(far)

    wide = 2 * rm

    at_dht = SLOTS - 4

    def chunk_of(zz, yy):
        return _mod4(zz) * 4 + _rem(yy + 8, 4)

    def all_far(i):
        return x_far * wide + i // 16 * rm, _rem(i, 16)

    def in_order(i):
        n = i // 3
        m = n - 7
        k = _pick(n < 7, chunk_of(z + n - 1, y + 2), chunk_of(z + 3 + m // 3, y + 3 + _rem(m + 9, 3)))
        return _mod4(x + 3 + _rem(i, 3)) * wide, _pick(n < 4, chunk_of(z + 2, n), k)

    def later(i):
        return in_order(i + SLOTS)

    def zload(where, i, ring, n):
        at, k = where(i)
        s = _rem(i, ring)
        src = zh.at[k, pl.ds(pl.multiple_of(at, rm), n)]
        return pltpu.make_async_copy(src, tst.at[s, _top(n)], tsem.at[s])

    def zahead(where, ring, n):
        for i in range(ring):
            zload(where, i, ring, n).start()

    with scope("stats"):
        zahead(all_far, SLOTS, rm)
        for cp in stats:
            cp.wait()
        top = lse_row[:, :]
        for k in range(len(near)):
            top = jnp.maximum(top, got[k])
        s = jnp.exp2(lse_row[:, :] - top)
        for k in range(len(near)):
            s = s + jnp.exp2(got[k] - top)
        lse_row[:, :] = top + jnp.log(s) * LOG2E

    def dz_part(v, place, at, lanes):
        r = lax.broadcasted_iota(jnp.int32, v.shape, 0).astype(F32)
        hit = r == pos_row[:, lanes] - place.astype(F32)
        p = jnp.exp2(v - lse_row[:, lanes])
        dz[at, lanes] = (jnp.where(hit, p - 1.0, p) * w_row[:, lanes]).astype(BF16)

    step = min(LANES, rm)

    def dz_rows(where, start, stop, last_tile, ring, n):
        @pl.loop(start, stop)
        def _(i):
            @pl.when((i > 0) & (i + ring - 1 < last_tile))
            def _():
                zload(where, i + ring - 1, ring, n).start()

            zload(where, i, ring, n).wait()
            row, k = where(i)
            lanes = pl.ds(pl.multiple_of(k * chunk, chunk), chunk)

            @pl.loop(0, n // step)
            def _(j):
                at = pl.multiple_of(row + j * step, step)
                r = pl.ds(pl.multiple_of(j * step, step), step)
                dz_part(tst[lax.rem(i, ring), r, :], at, pl.ds(at, step), lanes)

    def dz_far(start, stop):
        dz_rows(all_far, start, stop, 32, SLOTS, rm)

    with scope("dz_far"):
        dz_far(0, 16)

    nd = dim // 2
    few_rows = pl.ds(dm.main, FEW)
    pair_ids = [(next(ids), next(ids)) for _ in TWO]

    def over_d2d(s, n, i):
        lanes = pl.ds(pl.multiple_of(i * nd, nd), nd)
        there = sst.at[s, _top(n), lanes]
        return _remote(od.at[s, 1 - c, _top(n), lanes], there, send, recv, pair_ids[s][0] + i, sib)

    def de_block(xx, half, s, with_few=False):
        at = pl.ds(pl.multiple_of((xx * 2 + half) * rm, rm), rm)
        n = ha + 8 * half
        pl.semaphore_wait(free.at[s], 1)

        @pl.loop(0, 2)
        def _(i):
            lanes = pl.ds(pl.multiple_of(i * nd, nd), nd)
            lhs = jnp.concatenate([dz[at, :], dz[few_rows, :]], axis=0) if with_few else dz[at, :]
            v = jnp.dot(lhs, hv[:, lanes], preferred_element_type=F32)
            if with_few:
                few[:, lanes] = v[rm:]
            for j in TWO:
                od[s, j, 0:ha, lanes] = v[j * ha : (j + 1) * ha]
                if half:
                    od[s, j, ha:n, lanes] = few[pl.ds(pl.multiple_of((xx * 2 + j) * 8, 8), 8), lanes]
            over_d2d(s, n, i).start()

        return half, s, n

    def stored(blk, to):
        half, s, n = blk
        return pltpu.make_async_copy(od.at[s, c, _top(n)], to.at[pl.ds(half * ha, n)], dsem.at[s])

    def early(blk, src):
        half, s, n = blk
        for i in TWO:
            over_d2d(s, n, i).wait_send()
        return local(src.at[pl.ds(half * ha, n)], od.at[s, 1 - c, _top(n)], lsem.at[s])

    def sum_add(blk, to, more=None):
        half, s, n = blk
        for i in TWO:
            over_d2d(s, n, i).wait_recv()
        if more is not None:
            more.wait()

        def add(r):
            v = od[s, c, r, :] + sst[s, r, :]
            od[s, c, r, :] = v if more is None else v + od[s, 1 - c, r, :]

        _loop_rows(n, 8, add)
        if more is None:
            pl.semaphore_signal(free.at[s], inc=1, device_id=(sib,), device_id_type=MESH)
            for i in TWO:
                over_d2d(s, n, i).wait_send()
        cp = stored(blk, to)
        cp.start()
        return cp

    def ring_sum(xx, rows_, n, src, s, dst, dev):
        lds = [
            local(q_h.at[xx, rows_], od.at[s, 0, _top(n)], lsem.at[0]),
            local(src, od.at[s, 1, _top(n)], lsem.at[1]),
        ]
        for cp in lds:
            cp.wait()
        _add_rows(od.at[s, 0, _top(n)], [od.at[s, 1, _top(n)]], 8)
        local(od.at[s, 0, _top(n)], q_h.at[xx, rows_], lsem.at[0]).wait()
        return remote(q_h.at[xx, rows_], dst, dev)

    stores = []

    def flush():
        while stores:
            stores.pop().wait()

    def tiles(q, where, between=None):
        flush()

        def outs(i):
            p, ab = where(i)
            r = pl.ds(q * h, h)
            dsts = [dhp.at[ab * 2 + j, p, r] if q == 0 else dhp.at[p, ab * 2 + j, r] for j in TWO]
            return [
                pltpu.make_async_copy(tst.at[at_dht + i * 2 + j, _top(h)], dst, hsem.at[i * 2 + j])
                for j, dst in enumerate(dsts)
            ]

        @pl.loop(0, 2)
        def _(i):
            if between is not None:
                pl.when(i > 0)(between)
            p, ab = where(i)
            ks = [(ab * 2 + j) * 4 + p if q == 0 else p * 4 + ab * 2 + j for j in TWO]
            rhs = jnp.concatenate([dz[:, pl.ds(pl.multiple_of(k * chunk, chunk), chunk)] for k in ks], axis=1)
            v = jnp.dot(etv[q * h : (q + 1) * h, :], rhs, preferred_element_type=F32)
            for j in TWO:
                tst[at_dht + i * 2 + j, 0:h, :] = v[:, j * chunk : (j + 1) * chunk]
            for cp in outs(i):
                cp.start()

        for i in TWO:
            stores.extend(outs(i))

    def part(q, p, lo, n):
        r = pl.ds(q * h, h)
        if q == 0:
            return dhp.at[pl.ds(lo, n), p, r]
        return dhp.at[p, pl.ds(lo, n), r]

    def one(q, p, i):
        r = pl.ds(q * h, h)
        return dhp.at[i, p, r] if q == 0 else dhp.at[p, i, r]

    ring1, ring2 = ((yp, ym), (zp, zm)), ((zp, zm), (yp, ym))
    pos1, pos2 = (y, z), (z, y)
    first, second = ({}, {}), ({}, {})

    def send_far(q):
        flush()
        p, (rt, lt) = pos1[q], ring1[q]
        first[q]["far_r"] = remote(part(q, _mod4(p + 2), 0, 2), ya.at[q], rt)
        first[q]["far_l"] = remote(part(q, _mod4(p + 2), 2, 2), yb.at[q], lt)

    def send_near(q):
        flush()
        p, (rt, lt) = pos1[q], ring1[q]
        first[q]["near_r"] = remote(part(q, _mod4(p + 1), 2, 2), yl.at[q, pl.ds(2, 2)], rt)
        first[q]["near_l"] = remote(part(q, _mod4(p - 1), 0, 2), yr.at[q, _top(2)], lt)

    def fetch(i, src):
        return local(src, tst.at[i, _top(h)], tsem.at[i])

    def pass_on(q):
        flush()
        p, (rt, lt) = pos1[q], ring1[q]
        lds = [fetch(i, one(q, _mod4(p + 1), i)) for i in TWO]
        lds += [fetch(2 + i, one(q, _mod4(p - 1), 2 + i)) for i in TWO]
        first[q]["far_r"].wait_recv()
        for i in TWO:
            lds[i].wait()
            _add_rows(ya.at[q, i], [tst.at[i, _top(h)]], min(FEW, h))
        first[q]["sum_r"] = remote(ya.at[q], yl.at[q, _top(2)], rt)
        first[q]["far_l"].wait_recv()
        for i in TWO:
            lds[2 + i].wait()
            _add_rows(yb.at[q, i], [tst.at[2 + i, _top(h)]], min(FEW, h))
        first[q]["sum_l"] = remote(yb.at[q], yr.at[q, pl.ds(2, 2)], lt)

    lo, hi = _top(hc), pl.ds(hc, hc)

    def second_phase(q):
        flush()
        r, (rt, lt) = pos2[q], ring2[q]
        r2, r1, rm1 = _mod4(r + 2), _mod4(r + 1), _mod4(r - 1)
        order = (r2, r1, rm1, r)
        lds = [fetch(i, one(q, pos1[q], k)) for i, k in enumerate(order)]
        for k in NEAR_KEYS:
            first[q][k].wait_recv()
        lds2 = [fetch(4 + i, yr.at[q, k]) for i, k in enumerate(order)]
        for i, k in enumerate(order):
            lds[i].wait()
            lds2[i].wait()
            _add_rows(yl.at[q, k], [tst.at[i, _top(h)], tst.at[4 + i, _top(h)]], min(FEW, h))
            if i == 0:
                second[q]["far_r"] = remote(yl.at[q, r2, lo], za.at[q], rt)
                second[q]["far_l"] = remote(yl.at[q, r2, hi], zb.at[q], lt)
            if i == 1:
                second[q]["near_r"] = remote(yl.at[q, r1, hi], zl.at[q, hi], rt)
            if i == 2:
                second[q]["near_l"] = remote(yl.at[q, rm1, lo], zr.at[q, lo], lt)

    def second_pass(q):
        r, (rt, lt) = pos2[q], ring2[q]
        r1, rm1 = _mod4(r + 1), _mod4(r - 1)
        second[q]["far_r"].wait_recv()
        _add_rows(yl.at[q, r1, lo], [za.at[q]], min(FEW, hc))
        second[q]["sum_r"] = remote(yl.at[q, r1, lo], zl.at[q, lo], rt)
        second[q]["far_l"].wait_recv()
        _add_rows(yl.at[q, rm1, hi], [zb.at[q]], min(FEW, hc))
        second[q]["sum_l"] = remote(yl.at[q, rm1, hi], zr.at[q, hi], lt)

    def last(q):
        r = pos2[q]
        for k in NEAR_KEYS:
            second[q][k].wait_recv()
        n = min(LANES, h)

        @pl.loop(0, h // n)
        def _(i):
            at = pl.ds(pl.multiple_of(i * n, n), n)
            v = yl[q, r, at, :] + zl[q, at, :] + zr[q, at, :]
            od[0, 0, 0:chunk, pl.ds(pl.multiple_of(q * h + i * n, n), n)] = (v * (1.0 / LOGIT_SCALE)).T

    def tiles_far(q, between=None):
        tiles(q, lambda i: (_mod4(pos1[q] + 2), i), between)

    def tiles_near(q):
        tiles(q, lambda i: (_mod4(pos1[q] + 1 + 2 * i), 1 - i))

    def tiles_pass(q):
        tiles(q, lambda i: (_mod4(pos1[q] + 1 + 2 * i), i))

    def tiles_own(q):
        tiles(q, lambda i: (pos1[q], i))

    all_later = 48 - SLOTS

    def dz_first(start, stop):
        dz_rows(in_order, start, stop, SLOTS, SLOTS, wide)

    def dz_later(start, stop):
        dz_rows(later, start, stop, all_later, at_dht, wide)

    with scope("de_far"):
        b0 = de_block(x_far, 0, 0)
        dz_far(16, 32)
        zahead(in_order, SLOTS, wide)
        for l in range(0, tok, nt):
            lanes = pl.ds(l, nt)
            dz_part(few[:, lanes], jnp.int32(dm.main), few_rows, lanes)
        dz[dm.main + FEW : dm.wide, :] = jnp.zeros((FEW, tok), BF16)
        b1 = de_block(x_far, 1, 1, True)
    with scope("dz_1"):
        c0 = sum_add(b0, q_h.at[x_far])
        dz_first(0, 8)
        c0.wait()
        e0 = [remote(q_h.at[x_far, half_a], xa.at[half_a], xp)]
        dz_first(8, SLOTS)
        zahead(later, at_dht, wide)
    with scope("dh_far1"):
        def between():
            sum_add(b1, q_h.at[x_far])

        tiles_far(1, between)
        c1 = stored(b1, q_h.at[x_far])
        c1.wait()
        e1 = remote(q_h.at[x_far, part_l], xb, xm)
        e0.append(remote(q_h.at[x_far, strip], xa.at[strip], xp))
    with scope("dz_2"):
        dz_later(0, 9)
        send_far(1)
    with scope("dh_far0"):
        tiles_far(0)
    with scope("dz_3"):
        dz_later(9, 13)
        send_far(0)
        dz_later(13, all_later)
    with scope("de_2"):
        b2 = de_block(x_p, 1, 0)
        b3 = de_block(x_m, 0, 1)
        c2 = sum_add(b2, q_h.at[x_p])
    with scope("dh_near"):
        tiles_near(1)
        c2.wait()
        e2 = remote(q_h.at[x_p, part_l], xe.at[part_l], xp)
        c3 = sum_add(b3, q_h.at[x_m])
        send_near(1)
        tiles_near(0)
        c3.wait()
        e3 = [remote(q_h.at[x_m, half_a], xe.at[half_a], xm)]
        send_near(0)
    with scope("dh_pass"):
        tiles_pass(1)
        tiles_pass(0)
        pass_on(1)
    with scope("de_4"):
        b4 = de_block(x_p, 0, 0)
        pass_on(0)
        b5 = de_block(x_m, 1, 1)
        c4 = sum_add(b4, q_h.at[x_p])
    with scope("dh_own"):
        tiles_own(1)
        c5 = sum_add(b5, q_h.at[x_m])
        tiles_own(0)
        c4.wait()
        c5.wait()
        e3.append(remote(q_h.at[x_m, strip], xe.at[strip], xm))
    old = list(sent)
    sent.clear()
    with scope("ring"):
        for cp in e0:
            cp.wait_recv()
        e4 = ring_sum(x_p, part_r, cut, xa, 0, xs.at[part_r], xp)
        e1.wait_recv()
        e5 = ring_sum(x_m, part_l, dm.pad - cut, xb, 1, xs.at[part_l], xm)
    with scope("de_6"):
        b6 = de_block(x, 0, 0)
    with scope("de_7"):
        b7 = de_block(x, 1, 1)
        xo_load = local(x4.at[zy, xc], dz.at[_top(chunk)], osem.at[0])
    with scope("second_1"):
        second_phase(1)
    with scope("second_0"):
        second_phase(0)
    with scope("spass_1"):
        second_pass(1)
    with scope("sum_6"):
        for cp in e3:
            cp.wait_recv()
        c6 = early(b6, xe)
        e2.wait_recv()
        c7 = early(b7, xe)
        c6 = sum_add(b6, q_o, c6)
        c7 = sum_add(b7, q_o, c7)
    with scope("spass_0"):
        second_pass(0)
        c6.wait()
        c7.wait()
    def drain(cps):
        while cps:
            cps.pop().wait_send()

    def own_x(r):
        v = dz[r, :].astype(F32)
        inv = lax.rsqrt(jnp.mean(v * v, axis=-1, keepdims=True) + NORM_EPS)
        od[1, 0, r, :] = v * inv
        od[1, 1, r, 0:LANES] = jnp.broadcast_to(inv, (r.size, LANES))

    def own_dg(q):
        lanes = pl.ds(q * h, h)

        def add(i, acc):
            r = pl.ds(pl.multiple_of(i * 8, 8), 8)
            return acc + od[0, 0, r, lanes] * od[1, 0, r, lanes]

        acc = lax.fori_loop(0, chunk // 8, add, jnp.zeros((8, h), F32))
        sm[:, lanes] = jnp.sum(acc, axis=0, keepdims=True)

    def own_dx(r):
        x_hat, u = od[1, 0, r, :], od[0, 0, r, :] * gain
        od[0, 1, r, :] = od[1, 1, r, 0:1] * (u - x_hat * jnp.mean(u * x_hat, axis=-1, keepdims=True))

    with scope("own_x"):
        xo_load.wait()
        _loop_rows(chunk, 16, own_x)
        lse = jnp.where(zy == 0, lse_row[:, :], 0.0)
        loss = jnp.sum(w_row[:, :] * (lse - tgt_row[:, :]))
        sm[:, dim : dim + LANES] = jnp.full((1, LANES), loss / LOG2E)
        drain(old)
    with scope("last_1"):
        last(1)
        own_dg(1)
    with scope("last_0"):
        last(0)
        own_dg(0)

    with scope("small_1"):
        old = [cp for cp in sent if cp is not e4 and cp is not e5]
        near_sums = exchange(sm, got1, near)
        _loop_rows(chunk, 16, own_dx)
        dx_copy = local(od.at[0, 1, _top(chunk)], dx_out, osem.at[0])
        drain(old)
        for cp in near_sums:
            cp.wait()
    with scope("small_2"):
        tot = sm[...]
        for k in range(len(near)):
            tot = tot + got1[k]
        total_v[...] = tot
        all_sums = exchange(total_v, got2, line)
        mine = local(total_v, got2.at[len(line)], osem.at[1])
    with scope("ring_end"):
        for cp in (e4, e5):
            cp.wait()
        dx_copy.wait()
        mine.wait()
    with scope("small_3"):
        for cp in all_sums:
            cp.wait()


def _run(dm, x4, table, gain, labels, mask):
    hbm, vm = pl.BlockSpec(memory_space=HBM), pl.BlockSpec(memory_space=VMEM)
    sd = jax.ShapeDtypeStruct
    d, tok, h, ck, pad, ha = dm.dim, dm.tok, dm.h, dm.chunk, dm.pad, dm.ha
    line, quad, pair = VMEM((1, tok), F32), VMEM((2, 2, h, ck), F32), VMEM((2, h, ck), F32)
    part, shard = VMEM((2, h // 2, ck), F32), sd((pad, d), F32)
    out = pl.pallas_call(
        functools.partial(_kernel, dm),
        name="head",
        out_shape=(
            sd((ck, d), F32), sd((8, 1, d + LANES), F32),
            shard, shard, shard,
            sd((8, pad, d), F32), sd((16, dm.main, ck), F32),
            sd((4, pad, d), F32), sd((ha + 8, d), F32), sd((ha, d), F32),
            sd((4, 4, d, ck), F32), sd((2, 4, h, ck), F32),
        ),
        in_specs=[hbm, vm, vm, vm, vm],
        out_specs=[hbm] * 12,
        scratch_shapes=[
            VMEM((tok, d), BF16), VMEM((d, dm.wide), BF16), VMEM((dm.wide, tok), BF16),
            VMEM((2, 2, ha + 8, d), F32), VMEM((2, ha + 8, d), F32), VMEM((FEW, d), F32), VMEM((8, d), F32),
            quad, quad, VMEM((2, 4, h, ck), F32),
            part, part, pair, pair,
            VMEM((SLOTS, max(h, 2 * dm.rm), ck), F32),
            line, line, line, line, line, line, VMEM((15, 1, tok), F32),
            VMEM((1, d + LANES), F32), VMEM((15, 1, d + LANES), F32), VMEM((1, d + LANES), F32),
            DMA((56,)), DMA((56,)), pltpu.SemaphoreType.REGULAR((2,)),
            DMA((SLOTS,)), DMA((4,)), DMA((2,)), DMA((2,)), DMA((8,)),
        ],
        compiler_params=pltpu.CompilerParams(
            collective_id=0, has_side_effects=True, vmem_limit_bytes=67043328
        ),
    )(x4, table, gain, labels, mask)
    return _write_out(dm, out[2:4], *out[:2])


def _write_kernel(own, ring, dx, small, de_o, dx_o, dg_o, loss_o):
    de_o[:, :] = (own[:, :] + ring[:, :]) * (1.0 / LOGIT_SCALE)
    dx_o[:, :] = dx[:, :]
    total = jnp.sum(small[:, :, :], axis=0)
    d = dg_o.shape[1]
    dg_o[:, :] = total[:, :d]
    loss_o[:, :] = total[:, d : d + 1]


def _write_out(dm, parts, dx, small):
    d, step, blocks = dm.dim, dm.ha + 8, 2
    sd = jax.ShapeDtypeStruct
    some = pl.BlockSpec((step, d), lambda i: (i, 0))
    half = pl.BlockSpec((dm.chunk // blocks, d), lambda i: (i, 0))
    row, one = pl.BlockSpec((1, d), lambda i: (0, 0)), pl.BlockSpec((1, 1), lambda i: (0, 0))
    rows = pl.BlockSpec(small.shape, lambda i: (0, 0, 0))
    return pl.pallas_call(
        _write_kernel,
        name="write_out",
        grid=(blocks,),
        out_shape=(sd((dm.rows, d), F32), sd((dm.chunk, d), F32), sd((1, d), F32), sd((1, 1), F32)),
        in_specs=[some, some, half, rows],
        out_specs=(some, half, row, one),
    )(*parts, dx, small)


def solution(mesh):
    group = mesh.shape[AXIS]

    def local_step(residual, labels, loss_mask, norm_gain, table_shard):
        tokens, dim = residual.shape
        rows = table_shard.shape[0]
        dm = Dims(tokens, dim, rows, group)
        x4 = residual.reshape(16, 8, dm.chunk, dim)
        lab = labels.reshape(16, 8, 1, dm.chunk)
        msk = loss_mask.reshape(16, 8, 1, dm.chunk)
        d_embed, d_res, d_gain, loss = _run(dm, x4, table_shard, norm_gain[None, :], lab, msk)
        return loss.reshape(()), d_res, d_embed, d_gain.reshape(dim)

    return jax.shard_map(
        local_step,
        mesh=mesh,
        in_specs=(P(), P(), P(), P(), P(AXIS, None)),
        out_specs=(P(), P(AXIS, None), P(AXIS, None), P()),
        check_vma=False,
    )
```

```python
import functools
import itertools
import math

import jax
import jax.numpy as jnp
from jax import lax
from jax.experimental import pallas as pl
from jax.experimental.pallas import tpu as pltpu
from jax.sharding import PartitionSpec as P

VOCAB_REAL = 49155
LOGIT_SCALE = 6.0
NORM_EPS = 1e-6

AXIS = "vp"
MESH = pl.DeviceIdType.MESH
F32 = jnp.float32
BF16 = jnp.bfloat16
HBM = pltpu.HBM
VMEM = pltpu.VMEM
DMA = pltpu.SemaphoreType.DMA


def _coords():
    me = lax.axis_index(AXIS)
    return me // 32, (me // 8) % 4, (me // 2) % 4, me % 2


def _dev(z, y, x, c):
    return ((z * 4 + y) * 4 + x) * 2 + c


def _mod4(v):
    return lax.rem(v + 8, 4)


def _barrier(peers):
    sem = pltpu.get_barrier_semaphore()
    for p in peers:
        pl.semaphore_signal(sem, inc=1, device_id=(p,), device_id_type=MESH)
    pl.semaphore_wait(sem, len(peers))


def _remote(src, dst, send, recv, k, dev):
    return pltpu.make_async_remote_copy(
        src_ref=src,
        dst_ref=dst,
        send_sem=send.at[k],
        recv_sem=recv.at[k],
        device_id=(dev,),
        device_id_type=MESH,
    )


LANES = 128


class Dims:
    def __init__(self, tokens, dim, rows, group):
        self.dim, self.rows = dim, rows
        unit = LANES if rows >= LANES else 64
        self.rm = rows // unit * unit
        self.ha = self.rm // 2
        low = max(16, self.ha // 48 * 16)
        self.cuts = ((low, self.ha - low), (0, low))
        self.pad = self.rm + 8
        self.chunk = tokens // group
        self.tok = 16 * self.chunk
        self.nt = 4 * self.chunk
        self.main = 8 * self.rm
        self.wide = self.main + LANES
        self.h = dim // 2


def _top(n):
    return pl.ds(0, n)


def _rem(a, b):
    return a % b if isinstance(a, int) else lax.rem(a, b)


def _pick(test, a, b):
    return (a if test else b) if isinstance(test, bool) else jnp.where(test, a, b)


def _loop_rows(rows, step, fn):
    @pl.loop(0, rows // step)
    def _(i):
        fn(pl.ds(pl.multiple_of(i * step, step), step))


def _add_rows(dst, srcs, step):
    def add(r):
        acc = dst[r, :]
        for s in srcs:
            acc = acc + s[r, :]
        dst[r, :] = acc

    _loop_rows(dst.shape[0], step, add)


SLOTS = 12
FEW = 64
TWO = range(2)
LOG2E = math.log2(math.e)
NEAR_KEYS = ("near_r", "near_l", "sum_r", "sum_l")
scope = jax.named_scope


def _kernel(
    dm, x4, e_ref, g_ref, lab, msk,
    dx_out, got2, q_o, xs, xe, eg, zh, q_h, xa, xb, dhp, yr,
    hv, etv, dz, od, sst, few, oext, ya, yb, yl, za, zb, zl, zr, tst,
    m_row, s_row, w_row, pos_row, lse_row, tgt_row, got, sm, got1, total_v,
    send, recv,
    free, tsem, hsem, dsem, osem, lsem,
):
    z, y, x, c = _coords()
    xc, zy = x * 2 + c, z * 4 + y
    rows, rm, ha, dim, h = dm.rows, dm.rm, dm.ha, dm.dim, dm.h
    chunk, tok, nt, hc = dm.chunk, dm.tok, dm.nt, dm.h // 2
    x_far, x_p, x_m = _mod4(x + 2), _mod4(x + 1), _mod4(x - 1)
    xp, xm = _dev(z, y, x_p, c), _dev(z, y, x_m, c)
    yp, ym = _dev(z, _mod4(y + 1), x, c), _dev(z, _mod4(y - 1), x, c)
    zp, zm = _dev(_mod4(z + 1), y, x, c), _dev(_mod4(z - 1), y, x, c)
    sib = _dev(z, y, x, 1 - c)
    near = [_dev(_mod4(z + a), _mod4(y + b), x, c) for a in range(4) for b in range(4) if a or b]
    line = [_dev(z, y, _mod4(x + a), lax.rem(c + b, 2)) for a in range(4) for b in TWO if a or b]
    bar = pltpu.get_barrier_semaphore()
    for p in (*near, *line):
        pl.semaphore_signal(bar, inc=1, device_id=(p,), device_id_type=MESH)
    sent = []
    ids = itertools.count()

    def remote(src, dst, dev):
        cp = _remote(src, dst, send, recv, next(ids), dev)
        cp.start()
        sent.append(cp)
        return cp

    def exchange(src, dst, devs):
        k = next(ids)
        for i, dev in enumerate(devs):
            _remote(src, dst.at[i], send, recv, k, dev).start()
        whole = dst.at[_top(len(devs))]
        return pltpu.make_async_copy(whole, whole, recv.at[k]), pltpu.make_async_copy(whole, whole, send.at[k])

    def local(src, dst, sem):
        cp = pltpu.make_async_copy(src, dst, sem)
        cp.start()
        return cp

    x_at, ext_at = 2 * rm, 4 * rm

    def xload(k):
        s = lax.rem(k, 4)
        to = dz.at[pl.ds(pl.multiple_of(x_at + s * chunk, chunk), chunk)]
        return pltpu.make_async_copy(x4.at[k, xc], to, tsem.at[s])

    with scope("prep"):
        for k in range(3):
            xload(k).start()
        own = xc
        cps = []
        for j in TWO:
            def widen(r, j=j):
                od[0, j, r, :] = e_ref[pl.ds(j * ha + r.start, r.size), :].astype(F32)

            _loop_rows(ha, 16, widen)
            cps.append(local(od.at[0, j, _top(ha)], eg.at[own, pl.ds(j * ha, ha)], hsem.at[j]))
        oext[...] = jnp.zeros_like(oext)
        oext[0 : rows - rm, :] = e_ref[rm:rows, :].astype(F32)
        cps.append(local(oext, eg.at[own, pl.ds(rm, 8)], hsem.at[2]))
        pl.semaphore_wait(bar, 22)

    half_a, half_b = _top(ha), pl.ds(ha, ha + 8)
    cut = ha + 8
    part_r, part_l, strip = _top(cut), pl.ds(cut, dm.pad - cut), pl.ds(ha, cut - ha)

    def piece(s, r, dev):
        return remote(eg.at[s, r], eg.at[s, r], dev)

    def slot(xx):
        return xx * 2 + c

    cps[0].wait()
    r_a = piece(own, half_a, xp)
    for cp in cps[1:]:
        cp.wait()
    l_b = piece(own, half_b, xm)
    s_o = piece(own, _top(dm.pad), sib)
    r_b, l_a = piece(own, half_b, xp), piece(own, half_a, xm)

    gain = g_ref[...]

    with scope("norm"):
        @pl.loop(0, 16)
        def _(k):
            @pl.when(k < 13)
            def _():
                xload(k + 3).start()

            xload(k).wait()

            def norm(r):
                v = dz[pl.ds(pl.multiple_of(x_at + lax.rem(k, 4) * chunk + r.start, r.size), r.size), :].astype(F32)
                inv = lax.rsqrt(jnp.mean(v * v, axis=-1, keepdims=True) + NORM_EPS)
                hv[pl.ds(pl.multiple_of(k * chunk + r.start, r.size), r.size), :] = (v * inv * gain).astype(BF16)

            _loop_rows(chunk, 16, norm)

    with scope("labels"):
        total = jnp.sum(msk[...])
        for k in range(16):
            at = pl.ds(k * chunk, chunk)
            w_row[:, at] = msk[k, xc] / total
            q = lab[k, xc] - zy * (8 * rows)
            s = jnp.zeros_like(q)
            for i in range(1, 8):
                s = s + jnp.where(q >= i * rows, 1, 0)
            r = q - s * rows
            up = jnp.where(r >= ha, 1, 0)
            at_main = ((s // 2 * 2 + up) * 2 + s % 2) * ha + r - up * ha
            at_ext = dm.main + s * 8 + r - rm
            place = jnp.where(r < rm, at_main, at_ext)
            pos_row[:, at] = jnp.where((q >= 0) & (q < 8 * rows), place, -1).astype(F32)

    def product(lhs, lanes):
        v = lax.dot_general(lhs, hv[lanes, :], (((1,), (1,)), ((), ())), preferred_element_type=F32)
        return v * (LOG2E / LOGIT_SCALE)

    def add_stats(v, lanes):
        m_old, s_old = m_row[:, lanes], s_row[:, lanes]
        m = jnp.maximum(m_old, jnp.max(v, axis=0, keepdims=True))
        s = jnp.sum(jnp.exp2(v - m), axis=0, keepdims=True)
        m_row[:, lanes] = m
        s_row[:, lanes] = s_old * jnp.exp2(m_old - m) + s

    def add_target(v, place, lanes):
        r = lax.broadcasted_iota(jnp.int32, v.shape, 0)
        hit = r.astype(F32) == pos_row[:, lanes] - place.astype(F32)
        tgt_row[:, lanes] += jnp.sum(jnp.where(hit, v, 0.0), axis=0, keepdims=True)

    m_row[:, :] = jnp.full((1, tok), -jnp.inf, F32)
    s_row[:, :] = jnp.zeros((1, tok), F32)
    tgt_row[:, :] = jnp.zeros((1, tok), F32)
    segs = [(half, j) for half in TWO for j in TWO]

    def load(r0, n, xx, cores=TWO):
        return [
            local(
                eg.at[xx[half] * 2 + j, pl.ds(half * ha + r0, n)],
                od.at[j, half, pl.ds(r0, n)],
                hsem.at[half * len(cores) + k],
            )
            for half in TWO
            for k, j in enumerate(cores)
        ]

    def narrow_all(r0, n, src, cores=TWO):
        for half in TWO:
            for j in cores:
                def narrow(r, half=half, j=j):
                    at = pl.multiple_of((half * 2 + j) * ha + r0 + r.start, r.size)
                    dz[pl.ds(at, r.size), :] = src(half, j)[r, :].astype(BF16)

                _loop_rows(n, 16, narrow)

    def load_narrow(r0, n, xx, core):
        for cp in load(r0, n, xx, (core,)):
            cp.wait()
        narrow_all(r0, n, lambda half, j: od.at[j, half, pl.ds(r0, n)], (core,))

    def block(r0, n, xx, loads=(), with_few=False, nt=nt):
        if loads:
            for cp in loads:
                cp.wait()
            narrow_all(r0, n, lambda half, j: od.at[j, half, pl.ds(r0, n)])
        left = [VOCAB_REAL - ((zy * 8 + xx[half] * 2 + j) * rows + half * ha + r0) for half, j in segs]
        w, tall = nt // chunk, len(segs) * n
        pack = tst.shape[1] // tall
        deep = SLOTS // w
        packed = SLOTS * pack >= tok // chunk

        def place(t, i):
            if packed:
                return t * (w // pack) + i // pack, i % pack * tall
            return lax.rem(t, deep) * w + i, 0

        def out(t):
            cps = []
            for i in range(w):
                u, row = place(t, i)
                for m, (half, j) in enumerate(segs):
                    to = pl.ds(pl.multiple_of((xx[half] * 2 + half) * rm + j * ha + r0, 8), n)
                    cps.append(pltpu.make_async_copy(tst.at[u, pl.ds(row + m * n, n)], zh.at[t * w + i, to], tsem.at[u]))
            return cps

        def out_wait(u, rows_):
            whole = tst.at[u, _top(rows_)]
            pltpu.make_async_copy(whole, whole, tsem.at[u]).wait()

        @pl.loop(0, tok // nt)
        def _(t):
            if not packed:
                @pl.when(t >= deep)
                def _():
                    for i in range(w):
                        out_wait(place(t, i)[0], tall)

            lanes = pl.ds(pl.multiple_of(t * nt, nt), nt)
            lhs = [dz[(half * 2 + j) * ha + r0 : (half * 2 + j) * ha + r0 + n, :] for half, j in segs]
            if with_few:
                lhs.append(dz[ext_at : ext_at + FEW, :])
            v = product(jnp.concatenate(lhs, axis=0), lanes)
            v, v_few = v[:tall], v[tall:]
            r = lax.broadcasted_iota(jnp.int32, (n, nt), 0)
            v = [jnp.where(r < left[m], v[m * n : (m + 1) * n], -jnp.inf) for m in range(len(segs))]
            for part_v, (half, j) in zip(v, segs):
                add_target(part_v, (xx[half] * 2 + half) * rm + j * ha + r0, lanes)
            for i in range(w):
                u, row = place(t, i)
                for m in range(len(segs)):
                    tst[u, row + m * n : row + (m + 1) * n, :] = v[m][:, i * chunk : (i + 1) * chunk]
            if with_few:
                r = lax.broadcasted_iota(jnp.int32, v_few.shape, 0)
                ok = ((r & 7) < rows - rm) & ((zy * 8 + (r >> 3)) * rows + rm + (r & 7) < VOCAB_REAL)
                v_few = jnp.where(ok, v_few, -jnp.inf)
                few[:, lanes] = v_few
                add_target(v_few, jnp.int32(dm.main), lanes)
                v.append(v_few)
            v = jnp.concatenate(v, axis=0)
            for cp in out(t):
                cp.start()
            add_stats(v, lanes)

        if packed:
            for u in range(tok // chunk // pack):
                out_wait(u, pack * tall)
        else:
            for u in range(deep * w):
                out_wait(u, tall)

    def both(xx):
        block(0, ha, xx, load(0, ha, xx))

    def turn(xx):
        for half in TWO:
            base = pl.multiple_of((xx[half] * 2 + half) * rm, rm)

            @pl.loop(0, dim // LANES)
            def _(d, half=half, base=base):
                at = pl.ds(pl.multiple_of(d * LANES, LANES), LANES)
                etv[at, pl.ds(base, rm)] = dz[half * rm : (half + 1) * rm, at].T

    with scope("own"):
        s_o.wait_recv()
        both((x, x))
        turn((x, x))

    with scope("wait_1"):
        r_a.wait_recv()
        last_n = dm.cuts[-1][1]
        spans = [(pl.ds(r0, n), pl.ds(ha + r0, n + 8 * (r0 + n == ha))) for r0, n in dm.cuts]

        def far_pieces(xx, half, to):
            cps = [piece(slot(xx), pair[half], to) for pair in spans[:-1]]
            cps.append(remote(eg.at[slot(xx), spans[-1][half]], sst.at[c, pl.ds(half * last_n, last_n)], to))
            return cps

        r_f = far_pieces(x_m, 0, xp)
        d = [piece(slot(x_m), half_a, sib)]
        l_b.wait_recv()
        l_f = far_pieces(x_p, 1, xm)
        d.append(piece(slot(x_p), half_b, sib))
        for cp in d:
            cp.wait_recv()

    with scope("near_1"):
        both((x_m, x_p))
        turn((x_m, x_p))

    with scope("wait_2"):
        r_b.wait_recv()
        d = [piece(slot(x_m), half_b, sib)]
        l_a.wait_recv()
        d.append(piece(slot(x_p), half_a, sib))
        for cp in d:
            cp.wait_recv()

    with scope("near_2"):
        both((x_p, x_m))
        turn((x_p, x_m))

    far = (x_far, x_far)

    with scope("wait_3"):
        d = []
        for cp, r in zip((r_f[0], l_f[0]), spans[0]):
            cp.wait_recv()
            d.append(piece(slot(x_far), r, sib))
        load_narrow(*dm.cuts[0], far, c)
        for cp in d:
            cp.wait_recv()
    with scope("far_a"):
        ext_loads = [local(eg.at[s, pl.ds(rm, 8)], few.at[pl.ds(s * 8, 8)], lsem.at[s]) for s in range(8)]
        load_narrow(*dm.cuts[0], far, 1 - c)
        for cp in ext_loads:
            cp.wait()
        dz[ext_at : ext_at + FEW, :] = few[...].astype(BF16)
        dz[ext_at + FEW : ext_at + LANES, :] = jnp.zeros((FEW, dim), BF16)
        block(*dm.cuts[0], far, with_few=True)
    with scope("wait_5"):
        over = []
        for half, cp in enumerate((r_f[-1], l_f[-1])):
            cp.wait_recv()
            ref = sst.at[c, pl.ds(half * last_n, last_n)]
            over.append(_remote(ref, ref, send, recv, next(ids), sib))
            over[-1].start()

        @pl.loop(0, dim // LANES)
        def _(i):
            at = pl.ds(pl.multiple_of(i * LANES, LANES), LANES)
            etv[at, dm.main : dm.wide] = dz[ext_at : ext_at + LANES, at].T

        def last_rows(half, j):
            return sst.at[j, pl.ds(half * last_n, last_n)]

        narrow_all(0, last_n, last_rows, (c,))
        for cp in over:
            cp.wait_recv()

    with scope("far_c"):
        narrow_all(0, last_n, last_rows, (1 - c,))
        block(0, last_n, far, nt=8 * chunk)
        for cp in over:
            cp.wait_send()
        for s in TWO:
            pl.semaphore_signal(free.at[s], inc=1, device_id=(sib,), device_id_type=MESH)

    with scope("turn_far"):
        lse_row[:, :] = m_row[:, :] + jnp.log(s_row[:, :]) * LOG2E
        stats = exchange(lse_row, got, near)
        turn(far)

    wide = 2 * rm

    at_dht = SLOTS - 4

    def chunk_of(zz, yy):
        return _mod4(zz) * 4 + _rem(yy + 8, 4)

    def all_far(i):
        return x_far * wide + i // 16 * rm, _rem(i, 16)

    def in_order(i):
        n = i // 3
        m = n - 7
        k = _pick(n < 7, chunk_of(z + n - 1, y + 2), chunk_of(z + 3 + m // 3, y + 3 + _rem(m + 9, 3)))
        return _mod4(x + 3 + _rem(i, 3)) * wide, _pick(n < 4, chunk_of(z + 2, n), k)

    def later(i):
        return in_order(i + SLOTS)

    def zload(where, i, ring, n):
        at, k = where(i)
        s = _rem(i, ring)
        src = zh.at[k, pl.ds(pl.multiple_of(at, rm), n)]
        return pltpu.make_async_copy(src, tst.at[s, _top(n)], tsem.at[s])

    def zahead(where, ring, n):
        for i in range(ring):
            zload(where, i, ring, n).start()

    with scope("stats"):
        zahead(all_far, SLOTS, rm)
        for cp in stats:
            cp.wait()
        top = lse_row[:, :]
        for k in range(len(near)):
            top = jnp.maximum(top, got[k])
        s = jnp.exp2(lse_row[:, :] - top)
        for k in range(len(near)):
            s = s + jnp.exp2(got[k] - top)
        lse_row[:, :] = top + jnp.log(s) * LOG2E

    def dz_part(v, place, at, lanes):
        r = lax.broadcasted_iota(jnp.int32, v.shape, 0).astype(F32)
        hit = r == pos_row[:, lanes] - place.astype(F32)
        p = jnp.exp2(v - lse_row[:, lanes])
        dz[at, lanes] = (jnp.where(hit, p - 1.0, p) * w_row[:, lanes]).astype(BF16)

    step = min(LANES, rm)

    def dz_rows(where, start, stop, last_tile, ring, n):
        @pl.loop(start, stop)
        def _(i):
            @pl.when((i > 0) & (i + ring - 1 < last_tile))
            def _():
                zload(where, i + ring - 1, ring, n).start()

            zload(where, i, ring, n).wait()
            row, k = where(i)
            lanes = pl.ds(pl.multiple_of(k * chunk, chunk), chunk)

            @pl.loop(0, n // step)
            def _(j):
                at = pl.multiple_of(row + j * step, step)
                r = pl.ds(pl.multiple_of(j * step, step), step)
                dz_part(tst[lax.rem(i, ring), r, :], at, pl.ds(at, step), lanes)

    def dz_far(start, stop):
        dz_rows(all_far, start, stop, 32, SLOTS, rm)

    with scope("dz_far"):
        dz_far(0, 16)

    nd = dim // 2
    few_rows = pl.ds(dm.main, FEW)
    pair_ids = [(next(ids), next(ids)) for _ in TWO]

    def over_d2d(s, n, i):
        lanes = pl.ds(pl.multiple_of(i * nd, nd), nd)
        there = sst.at[s, _top(n), lanes]
        return _remote(od.at[s, 1 - c, _top(n), lanes], there, send, recv, pair_ids[s][0] + i, sib)

    def de_block(xx, half, s, with_few=False):
        at = pl.ds(pl.multiple_of((xx * 2 + half) * rm, rm), rm)
        n = ha + 8 * half
        pl.semaphore_wait(free.at[s], 1)

        @pl.loop(0, 2)
        def _(i):
            lanes = pl.ds(pl.multiple_of(i * nd, nd), nd)
            lhs = jnp.concatenate([dz[at, :], dz[few_rows, :]], axis=0) if with_few else dz[at, :]
            v = jnp.dot(lhs, hv[:, lanes], preferred_element_type=F32)
            if with_few:
                few[:, lanes] = v[rm:]
            for j in TWO:
                od[s, j, 0:ha, lanes] = v[j * ha : (j + 1) * ha]
                if half:
                    od[s, j, ha:n, lanes] = few[pl.ds(pl.multiple_of((xx * 2 + j) * 8, 8), 8), lanes]
            over_d2d(s, n, i).start()

        return half, s, n

    def stored(blk, to):
        half, s, n = blk
        return pltpu.make_async_copy(od.at[s, c, _top(n)], to.at[pl.ds(half * ha, n)], dsem.at[s])

    def early(blk, src):
        half, s, n = blk
        for i in TWO:
            over_d2d(s, n, i).wait_send()
        return local(src.at[pl.ds(half * ha, n)], od.at[s, 1 - c, _top(n)], lsem.at[s])

    def sum_add(blk, to, more=None):
        half, s, n = blk
        for i in TWO:
            over_d2d(s, n, i).wait_recv()
        if more is not None:
            more.wait()

        def add(r):
            v = od[s, c, r, :] + sst[s, r, :]
            od[s, c, r, :] = v if more is None else v + od[s, 1 - c, r, :]

        _loop_rows(n, 8, add)
        if more is None:
            pl.semaphore_signal(free.at[s], inc=1, device_id=(sib,), device_id_type=MESH)
            for i in TWO:
                over_d2d(s, n, i).wait_send()
        cp = stored(blk, to)
        cp.start()
        return cp

    def ring_sum(xx, rows_, n, src, s, dst, dev):
        lds = [
            local(q_h.at[xx, rows_], od.at[s, 0, _top(n)], lsem.at[0]),
            local(src, od.at[s, 1, _top(n)], lsem.at[1]),
        ]
        for cp in lds:
            cp.wait()
        _add_rows(od.at[s, 0, _top(n)], [od.at[s, 1, _top(n)]], 8)
        local(od.at[s, 0, _top(n)], q_h.at[xx, rows_], lsem.at[0]).wait()
        return remote(q_h.at[xx, rows_], dst, dev)

    stores = []

    def flush():
        while stores:
            stores.pop().wait()

    def tiles(q, where, between=None):
        flush()

        def outs(i):
            p, ab = where(i)
            r = pl.ds(q * h, h)
            dsts = [dhp.at[ab * 2 + j, p, r] if q == 0 else dhp.at[p, ab * 2 + j, r] for j in TWO]
            return [
                pltpu.make_async_copy(tst.at[at_dht + i * 2 + j, _top(h)], dst, hsem.at[i * 2 + j])
                for j, dst in enumerate(dsts)
            ]

        @pl.loop(0, 2)
        def _(i):
            if between is not None:
                pl.when(i > 0)(between)
            p, ab = where(i)
            ks = [(ab * 2 + j) * 4 + p if q == 0 else p * 4 + ab * 2 + j for j in TWO]
            rhs = jnp.concatenate([dz[:, pl.ds(pl.multiple_of(k * chunk, chunk), chunk)] for k in ks], axis=1)
            v = jnp.dot(etv[q * h : (q + 1) * h, :], rhs, preferred_element_type=F32)
            for j in TWO:
                tst[at_dht + i * 2 + j, 0:h, :] = v[:, j * chunk : (j + 1) * chunk]
            for cp in outs(i):
                cp.start()

        for i in TWO:
            stores.extend(outs(i))

    def part(q, p, lo, n):
        r = pl.ds(q * h, h)
        if q == 0:
            return dhp.at[pl.ds(lo, n), p, r]
        return dhp.at[p, pl.ds(lo, n), r]

    def one(q, p, i):
        r = pl.ds(q * h, h)
        return dhp.at[i, p, r] if q == 0 else dhp.at[p, i, r]

    ring1, ring2 = ((yp, ym), (zp, zm)), ((zp, zm), (yp, ym))
    pos1, pos2 = (y, z), (z, y)
    first, second = ({}, {}), ({}, {})

    def send_far(q):
        flush()
        p, (rt, lt) = pos1[q], ring1[q]
        first[q]["far_r"] = remote(part(q, _mod4(p + 2), 0, 2), ya.at[q], rt)
        first[q]["far_l"] = remote(part(q, _mod4(p + 2), 2, 2), yb.at[q], lt)

    def send_near(q):
        flush()
        p, (rt, lt) = pos1[q], ring1[q]
        first[q]["near_r"] = remote(part(q, _mod4(p + 1), 2, 2), yl.at[q, pl.ds(2, 2)], rt)
        first[q]["near_l"] = remote(part(q, _mod4(p - 1), 0, 2), yr.at[q, _top(2)], lt)

    def fetch(i, src):
        return local(src, tst.at[i, _top(h)], tsem.at[i])

    def pass_on(q):
        flush()
        p, (rt, lt) = pos1[q], ring1[q]
        lds = [fetch(i, one(q, _mod4(p + 1), i)) for i in TWO]
        lds += [fetch(2 + i, one(q, _mod4(p - 1), 2 + i)) for i in TWO]
        first[q]["far_r"].wait_recv()
        for i in TWO:
            lds[i].wait()
            _add_rows(ya.at[q, i], [tst.at[i, _top(h)]], min(FEW, h))
        first[q]["sum_r"] = remote(ya.at[q], yl.at[q, _top(2)], rt)
        first[q]["far_l"].wait_recv()
        for i in TWO:
            lds[2 + i].wait()
            _add_rows(yb.at[q, i], [tst.at[2 + i, _top(h)]], min(FEW, h))
        first[q]["sum_l"] = remote(yb.at[q], yr.at[q, pl.ds(2, 2)], lt)

    lo, hi = _top(hc), pl.ds(hc, hc)

    def second_phase(q):
        flush()
        r, (rt, lt) = pos2[q], ring2[q]
        r2, r1, rm1 = _mod4(r + 2), _mod4(r + 1), _mod4(r - 1)
        order = (r2, r1, rm1, r)
        lds = [fetch(i, one(q, pos1[q], k)) for i, k in enumerate(order)]
        for k in NEAR_KEYS:
            first[q][k].wait_recv()
        lds2 = [fetch(4 + i, yr.at[q, k]) for i, k in enumerate(order)]
        for i, k in enumerate(order):
            lds[i].wait()
            lds2[i].wait()
            _add_rows(yl.at[q, k], [tst.at[i, _top(h)], tst.at[4 + i, _top(h)]], min(FEW, h))
            if i == 0:
                second[q]["far_r"] = remote(yl.at[q, r2, lo], za.at[q], rt)
                second[q]["far_l"] = remote(yl.at[q, r2, hi], zb.at[q], lt)
            if i == 1:
                second[q]["near_r"] = remote(yl.at[q, r1, hi], zl.at[q, hi], rt)
            if i == 2:
                second[q]["near_l"] = remote(yl.at[q, rm1, lo], zr.at[q, lo], lt)

    def second_pass(q):
        r, (rt, lt) = pos2[q], ring2[q]
        r1, rm1 = _mod4(r + 1), _mod4(r - 1)
        second[q]["far_r"].wait_recv()
        _add_rows(yl.at[q, r1, lo], [za.at[q]], min(FEW, hc))
        second[q]["sum_r"] = remote(yl.at[q, r1, lo], zl.at[q, lo], rt)
        second[q]["far_l"].wait_recv()
        _add_rows(yl.at[q, rm1, hi], [zb.at[q]], min(FEW, hc))
        second[q]["sum_l"] = remote(yl.at[q, rm1, hi], zr.at[q, hi], lt)

    def last(q):
        r = pos2[q]
        for k in NEAR_KEYS:
            second[q][k].wait_recv()
        n = min(LANES, h)

        @pl.loop(0, h // n)
        def _(i):
            at = pl.ds(pl.multiple_of(i * n, n), n)
            v = yl[q, r, at, :] + zl[q, at, :] + zr[q, at, :]
            od[0, 0, 0:chunk, pl.ds(pl.multiple_of(q * h + i * n, n), n)] = (v * (1.0 / LOGIT_SCALE)).T

    def tiles_far(q, between=None):
        tiles(q, lambda i: (_mod4(pos1[q] + 2), i), between)

    def tiles_near(q):
        tiles(q, lambda i: (_mod4(pos1[q] + 1 + 2 * i), 1 - i))

    def tiles_pass(q):
        tiles(q, lambda i: (_mod4(pos1[q] + 1 + 2 * i), i))

    def tiles_own(q):
        tiles(q, lambda i: (pos1[q], i))

    all_later = 48 - SLOTS

    def dz_first(start, stop):
        dz_rows(in_order, start, stop, SLOTS, SLOTS, wide)

    def dz_later(start, stop):
        dz_rows(later, start, stop, all_later, at_dht, wide)

    with scope("de_far"):
        b0 = de_block(x_far, 0, 0)
        dz_far(16, 32)
        zahead(in_order, SLOTS, wide)
        for l in range(0, tok, nt):
            lanes = pl.ds(l, nt)
            dz_part(few[:, lanes], jnp.int32(dm.main), few_rows, lanes)
        dz[dm.main + FEW : dm.wide, :] = jnp.zeros((FEW, tok), BF16)
        b1 = de_block(x_far, 1, 1, True)
    with scope("dz_1"):
        c0 = sum_add(b0, q_h.at[x_far])
        dz_first(0, 8)
        c0.wait()
        e0 = [remote(q_h.at[x_far, half_a], xa.at[half_a], xp)]
        dz_first(8, SLOTS)
        zahead(later, at_dht, wide)
    with scope("dh_far1"):
        def between():
            sum_add(b1, q_h.at[x_far])

        tiles_far(1, between)
        c1 = stored(b1, q_h.at[x_far])
        c1.wait()
        e1 = remote(q_h.at[x_far, part_l], xb, xm)
        e0.append(remote(q_h.at[x_far, strip], xa.at[strip], xp))
    with scope("dz_2"):
        dz_later(0, 9)
        send_far(1)
    with scope("dh_far0"):
        tiles_far(0)
    with scope("dz_3"):
        dz_later(9, 13)
        send_far(0)
        dz_later(13, all_later)
    with scope("de_2"):
        b2 = de_block(x_p, 1, 0)
        b3 = de_block(x_m, 0, 1)
        c2 = sum_add(b2, q_h.at[x_p])
    with scope("dh_near"):
        tiles_near(1)
        c2.wait()
        e2 = remote(q_h.at[x_p, part_l], xe.at[part_l], xp)
        c3 = sum_add(b3, q_h.at[x_m])
        send_near(1)
        tiles_near(0)
        c3.wait()
        e3 = [remote(q_h.at[x_m, half_a], xe.at[half_a], xm)]
        send_near(0)
    with scope("dh_pass"):
        tiles_pass(1)
        tiles_pass(0)
        pass_on(1)
    with scope("de_4"):
        b4 = de_block(x_p, 0, 0)
        pass_on(0)
        b5 = de_block(x_m, 1, 1)
        c4 = sum_add(b4, q_h.at[x_p])
    with scope("dh_own"):
        tiles_own(1)
        c5 = sum_add(b5, q_h.at[x_m])
        tiles_own(0)
        c4.wait()
        c5.wait()
        e3.append(remote(q_h.at[x_m, strip], xe.at[strip], xm))
    old = list(sent)
    sent.clear()
    with scope("ring"):
        for cp in e0:
            cp.wait_recv()
        e4 = ring_sum(x_p, part_r, cut, xa, 0, xs.at[part_r], xp)
        e1.wait_recv()
        e5 = ring_sum(x_m, part_l, dm.pad - cut, xb, 1, xs.at[part_l], xm)
    with scope("de_6"):
        b6 = de_block(x, 0, 0)
    with scope("de_7"):
        b7 = de_block(x, 1, 1)
        xo_load = local(x4.at[zy, xc], dz.at[_top(chunk)], osem.at[0])
    with scope("second_1"):
        second_phase(1)
    with scope("second_0"):
        second_phase(0)
    with scope("spass_1"):
        second_pass(1)
    with scope("sum_6"):
        for cp in e3:
            cp.wait_recv()
        c6 = early(b6, xe)
        e2.wait_recv()
        c7 = early(b7, xe)
        c6 = sum_add(b6, q_o, c6)
        c7 = sum_add(b7, q_o, c7)
    with scope("spass_0"):
        second_pass(0)
        c6.wait()
        c7.wait()
    def drain(cps):
        while cps:
            cps.pop().wait_send()

    def own_x(r):
        v = dz[r, :].astype(F32)
        inv = lax.rsqrt(jnp.mean(v * v, axis=-1, keepdims=True) + NORM_EPS)
        od[1, 0, r, :] = v * inv
        od[1, 1, r, 0:LANES] = jnp.broadcast_to(inv, (r.size, LANES))

    def own_dg(q):
        lanes = pl.ds(q * h, h)

        def add(i, acc):
            r = pl.ds(pl.multiple_of(i * 8, 8), 8)
            return acc + od[0, 0, r, lanes] * od[1, 0, r, lanes]

        acc = lax.fori_loop(0, chunk // 8, add, jnp.zeros((8, h), F32))
        sm[:, lanes] = jnp.sum(acc, axis=0, keepdims=True)

    def own_dx(r):
        x_hat, u = od[1, 0, r, :], od[0, 0, r, :] * gain
        od[0, 1, r, :] = od[1, 1, r, 0:1] * (u - x_hat * jnp.mean(u * x_hat, axis=-1, keepdims=True))

    with scope("own_x"):
        xo_load.wait()
        _loop_rows(chunk, 16, own_x)
        lse = jnp.where(zy == 0, lse_row[:, :], 0.0)
        loss = jnp.sum(w_row[:, :] * (lse - tgt_row[:, :]))
        sm[:, dim : dim + LANES] = jnp.full((1, LANES), loss / LOG2E)
        drain(old)
    with scope("last_1"):
        last(1)
        own_dg(1)
    with scope("last_0"):
        last(0)
        own_dg(0)

    with scope("small_1"):
        old = [cp for cp in sent if cp is not e4 and cp is not e5]
        near_sums = exchange(sm, got1, near)
        _loop_rows(chunk, 16, own_dx)
        dx_copy = local(od.at[0, 1, _top(chunk)], dx_out, osem.at[0])
        drain(old)
        for cp in near_sums:
            cp.wait()
    with scope("small_2"):
        tot = sm[...]
        for k in range(len(near)):
            tot = tot + got1[k]
        total_v[...] = tot
        all_sums = exchange(total_v, got2, line)
        mine = local(total_v, got2.at[len(line)], osem.at[1])
    with scope("ring_end"):
        for cp in (e4, e5):
            cp.wait()
        dx_copy.wait()
        mine.wait()
    with scope("small_3"):
        for cp in all_sums:
            cp.wait()


def _run(dm, x4, table, gain, labels, mask):
    hbm, vm = pl.BlockSpec(memory_space=HBM), pl.BlockSpec(memory_space=VMEM)
    sd = jax.ShapeDtypeStruct
    d, tok, h, ck, pad, ha = dm.dim, dm.tok, dm.h, dm.chunk, dm.pad, dm.ha
    line, quad, pair = VMEM((1, tok), F32), VMEM((2, 2, h, ck), F32), VMEM((2, h, ck), F32)
    part, shard = VMEM((2, h // 2, ck), F32), sd((pad, d), F32)
    out = pl.pallas_call(
        functools.partial(_kernel, dm),
        name="head",
        out_shape=(
            sd((ck, d), F32), sd((8, 1, d + LANES), F32),
            shard, shard, shard,
            sd((8, pad, d), F32), sd((16, dm.main, ck), F32),
            sd((4, pad, d), F32), sd((ha + 8, d), F32), sd((ha, d), F32),
            sd((4, 4, d, ck), F32), sd((2, 4, h, ck), F32),
        ),
        in_specs=[hbm, vm, vm, vm, vm],
        out_specs=[hbm] * 12,
        scratch_shapes=[
            VMEM((tok, d), BF16), VMEM((d, dm.wide), BF16), VMEM((dm.wide, tok), BF16),
            VMEM((2, 2, ha + 8, d), F32), VMEM((2, ha + 8, d), F32), VMEM((FEW, d), F32), VMEM((8, d), F32),
            quad, quad, VMEM((2, 4, h, ck), F32),
            part, part, pair, pair,
            VMEM((SLOTS, max(h, 2 * dm.rm), ck), F32),
            line, line, line, line, line, line, VMEM((15, 1, tok), F32),
            VMEM((1, d + LANES), F32), VMEM((15, 1, d + LANES), F32), VMEM((1, d + LANES), F32),
            DMA((56,)), DMA((56,)), pltpu.SemaphoreType.REGULAR((2,)),
            DMA((SLOTS,)), DMA((4,)), DMA((2,)), DMA((2,)), DMA((8,)),
        ],
        compiler_params=pltpu.CompilerParams(
            collective_id=0, has_side_effects=True, vmem_limit_bytes=67043328
        ),
    )(x4, table, gain, labels, mask)
    return _write_out(dm, out[2:4], *out[:2])


def _write_kernel(own, ring, dx, small, de_o, dx_o, dg_o, loss_o):
    de_o[:, :] = (own[:, :] + ring[:, :]) * (1.0 / LOGIT_SCALE)
    dx_o[:, :] = dx[:, :]
    total = jnp.sum(small[:, :, :], axis=0)
    d = dg_o.shape[1]
    dg_o[:, :] = total[:, :d]
    loss_o[:, :] = total[:, d : d + 1]


def _write_out(dm, parts, dx, small):
    d, blocks = dm.dim, 4
    step = -(-dm.pad // (8 * blocks)) * 8
    sd = jax.ShapeDtypeStruct
    some = pl.BlockSpec((step, d), lambda i: (i, 0))
    half = pl.BlockSpec((dm.chunk // blocks, d), lambda i: (i, 0))
    row, one = pl.BlockSpec((1, d), lambda i: (0, 0)), pl.BlockSpec((1, 1), lambda i: (0, 0))
    rows = pl.BlockSpec(small.shape, lambda i: (0, 0, 0))
    return pl.pallas_call(
        _write_kernel,
        name="write_out",
        grid=(blocks,),
        out_shape=(sd((dm.rows, d), F32), sd((dm.chunk, d), F32), sd((1, d), F32), sd((1, 1), F32)),
        in_specs=[some, some, half, rows],
        out_specs=(some, half, row, one),
    )(*parts, dx, small)


def solution(mesh):
    group = mesh.shape[AXIS]

    def local_step(residual, labels, loss_mask, norm_gain, table_shard):
        tokens, dim = residual.shape
        rows = table_shard.shape[0]
        dm = Dims(tokens, dim, rows, group)
        x4 = residual.reshape(16, 8, dm.chunk, dim)
        lab = labels.reshape(16, 8, 1, dm.chunk)
        msk = loss_mask.reshape(16, 8, 1, dm.chunk)
        d_embed, d_res, d_gain, loss = _run(dm, x4, table_shard, norm_gain[None, :], lab, msk)
        return loss.reshape(()), d_res, d_embed, d_gain.reshape(dim)

    return jax.shard_map(
        local_step,
        mesh=mesh,
        in_specs=(P(), P(), P(), P(), P(AXIS, None)),
        out_specs=(P(), P(AXIS, None), P(AXIS, None), P()),
        check_vma=False,
    )
```
